32 devices in a mesh: dp: 8 (over z, y), tp: 4 (over x, core).
Axes of the slice: x: 2, y: 2, z: 4, core: 2. Of those that a mesh axis runs over, the one named last changes fastest.
Arguments:
- block_input: bfloat16 [4096, 2048], P(('dp', 'tp')), may hold values from -6 to 6
- segment_ids: int32 [8, 512], P('dp'), may hold values from 0 to 1, never falling along the last dimension, each value on 1 to 320 neighbouring positions
- w_qkv: bfloat16 [2048, 6144], P('dp', 'tp'), may hold values from -2 to 2
- b_qkv: float32 [8, 512], P('tp', 'dp'), may hold values from -3 to 3
- w_out: bfloat16 [2048, 2048], P('tp', 'dp'), may hold values from -0.5 to 0.5
- b_out: float32 [2048], P(('dp', 'tp')), may hold values from -3 to 3
- w_fc1: bfloat16 [2048, 8192], P('dp', 'tp'), may hold values from -0.125 to 0.125
- b_fc1: float32 [128, 64], P('tp', 'dp'), may hold values from -3 to 3
- w_fc2: bfloat16 [8192, 2048], P('tp', 'dp'), may hold values from -0.0625 to 0.0625
- b_fc2: float32 [2048], P(('dp', 'tp')), may hold values from -3 to 3
- ln1_gain: float32 [2048], P(('dp', 'tp')), may hold values from 0.1 to 1.9
- ln1_bias: float32 [2048], P(('dp', 'tp')), may hold values from -3 to 3
- ln2_gain: float32 [2048], P(('dp', 'tp')), may hold values from 0.1 to 1.9
- ln2_bias: float32 [2048], P(('dp', 'tp')), may hold values from -3 to 3
- cotangent: bfloat16 [4096, 2048], P(('dp', 'tp')), may hold values from -6 to 6
Outputs:
- block_output: bfloat16 [4096, 2048], P(('dp', 'tp'))
- input_grad: float32 [4096, 2048], P(('dp', 'tp'))
- w_qkv_grad: float32 [2048, 6144], P('dp', 'tp')
- b_qkv_grad: float32 [8, 512], P('tp', 'dp')
- w_out_grad: float32 [2048, 2048], P('tp', 'dp')
- b_out_grad: float32 [2048], P(('dp', 'tp'))
- w_fc1_grad: float32 [2048, 8192], P('dp', 'tp')
- b_fc1_grad: float32 [128, 64], P('tp', 'dp')
- w_fc2_grad: float32 [8192, 2048], P('tp', 'dp')
- b_fc2_grad: float32 [2048], P(('dp', 'tp'))
- ln1_gain_grad: float32 [2048], P(('dp', 'tp'))
- ln1_bias_grad: float32 [2048], P(('dp', 'tp'))
- ln2_gain_grad: float32 [2048], P(('dp', 'tp'))
- ln2_bias_grad: float32 [2048], P(('dp', 'tp'))
The draws below stay inside these ranges and needn't reach their ends.
Inputs may be any that keep to these rules, and one draw needn't show every extreme that they name: `segment_ids`: ids never fall along a sequence; each sequence holds two documents.
All inputs are finite; a program needn't handle non-finite values.
Results may differ from the reference program's by a relative error of at most 0.034.
Values may be sent and summed in bfloat16 or wider, within the bound.
A program may use at most 192 MiB of HBM per device.

```python
import math
import jax
import jax.numpy as jnp
import numpy as np
from jax import lax

D = 2048
H = 8
HD = 256
ROT = 64
FF = 8192
SEQ = 512
SEQS_ALL = 8
TOKENS = 4096


def draw_block_input(key, part):
    base = jnp.clip(jax.random.normal(key, (TOKENS, D), jnp.float32), -6.0, 6.0)
    return base.astype(jnp.bfloat16)


def draw_w_qkv(key, part):
    base = jnp.clip(jax.random.normal(key, (D, H, 3, HD), jnp.float32), -6.0, 6.0) * D ** (-0.5)
    return jnp.clip(base, -2.0, 2.0).reshape(D, 3 * D).astype(jnp.bfloat16)


def with_spikes(result, rng, source, target, shards_of, factor):
    owner, partner = [(jnp.arange(result.shape[dim]) // (result.shape[dim] // shards_of)).reshape([-1 if axis == dim else 1 for axis in range(result.ndim)]) for dim in (source, target)]
    chosen = jax.random.permutation(rng, shards_of)[partner]
    strong = (owner == chosen) | (owner == (partner + shards_of // 2) % shards_of)
    return jnp.where(strong, factor * result, result)


def level_of(stream_key, dims, split, least, top_value):
    loudness = 1.0
    for dim, blocks in split:
        draws = jax.random.uniform(jax.random.fold_in(jax.random.fold_in(stream_key, 6), dim), (blocks,), jnp.float32, least / len(split), top_value / len(split))
        loudness = loudness * jnp.repeat(jnp.exp(draws), dims[dim] // blocks).reshape((-1,) + (1,) * (len(dims) - 1 - dim))
    return loudness


def length_profile(number_of, total, limit, slope):
    portions = [(1 << 20) // math.isqrt(grade ** slope) + 1 for grade in range(2, number_of + 1)]
    spare, given = total - limit - (number_of - 1), [1] * (number_of - 1)
    while spare > 0:
        movable = [i for i in range(number_of - 1) if given[i] < limit]
        pool, remaining = sum([portions[i] for i in movable]), spare
        for i in movable:
            addition = min(limit - given[i], max(1, remaining * portions[i] // pool), spare)
            given[i] = given[i] + addition
            spare = spare - addition
    return np.array([limit] + given)


def uneven_parts(rng, number_of, total, reach, lean):
    if number_of == 2:
        one = jax.random.randint(rng, (), max(1, total - reach), min(reach, total - 1) + 1)
        return jnp.stack([one, total - one])
    tallies = jnp.asarray(length_profile(number_of, total, reach, lean), jnp.int32)
    twos = (number_of - 1) // 2
    giver, receiver = tallies[1:1 + 2 * twos:2], tallies[2:2 + 2 * twos:2]
    slack = jnp.minimum(giver - 1, reach - receiver)
    moved = jax.random.randint(jax.random.fold_in(rng, 1), (twos,), 0, 1 << 20) % (slack + 1)
    tallies = tallies.at[1:1 + 2 * twos:2].set(giver - moved).at[2:2 + 2 * twos:2].set(receiver + moved)
    return tallies[jax.random.permutation(jax.random.fold_in(rng, 2), number_of)]


def gaussian(rng, extent, deviation, most, cuts=(), kind=jnp.bfloat16):
    array = jax.random.normal(rng, extent, jnp.float32) * deviation
    if len(cuts) > 0:
        array = level_of(rng, extent, cuts, -0.22, 0.18) * array
    return jnp.clip(array, min=-most, max=most).astype(kind)


def heavy_noise(rng, dims, width, limit, cuts, heavy, kind=jnp.bfloat16):
    result = width * jax.random.normal(rng, dims, jnp.float32)
    if cuts:
        result = result * level_of(rng, dims, cuts, -0.22, 0.18)
    return jnp.clip(with_spikes(result, jax.random.fold_in(rng, 3), *heavy), -limit, limit).astype(kind)


def setup_inputs(seed: int = 0) -> dict:
    seeds = jax.random.split(jax.random.key(seed), 16)
    block_input = draw_block_input(jax.random.fold_in(seeds[15], 71), 0)
    segment_ids = jax.vmap(lambda own: jnp.searchsorted(jnp.cumsum(uneven_parts(own, 2, SEQ, 5 * SEQ // 8, 0)), jnp.arange(SEQ), side="right"))(jax.random.split(seeds[1], SEQS_ALL)).reshape((SEQS_ALL, SEQ)).astype(jnp.int32)
    w_qkv = draw_w_qkv(jax.random.fold_in(seeds[15], 71), 0)
    b_qkv = gaussian(seeds[3], (H, 2 * HD), 0.5, 3.0, ((0, 4), (1, 8)), jnp.float32)
    w_out = gaussian(seeds[4], (D, D), (D // 16) ** -0.5, 0.5, ((0, 4), (1, 8)))
    b_out = gaussian(seeds[5], (D,), 0.4, 3.0, ((0, 32),), jnp.float32)
    w_fc1 = gaussian(seeds[6], (D, FF), D ** -0.5, 0.125, ((0, 8), (1, 4)))
    b_fc1 = gaussian(seeds[7], (FF // 64, 64), 0.5, 3.0, ((0, 4), (1, 8)), jnp.float32)
    w_fc2 = gaussian(seeds[8], (FF, D), FF ** -0.5, 0.0625, ((0, 4), (1, 8)))
    b_fc2 = gaussian(seeds[9], (D,), 0.4, 3.0, ((0, 32),), jnp.float32)
    ln1_gain = jnp.clip(1.0 + 0.18 * jax.random.normal(seeds[10], (D,), jnp.float32), 0.1, 1.9)
    ln1_bias = gaussian(seeds[11], (D,), 0.5, 3.0, ((0, 32),), jnp.float32)
    ln2_gain = jnp.clip(1.0 + 0.18 * jax.random.normal(seeds[12], (D,), jnp.float32), 0.1, 1.9)
    ln2_bias = gaussian(seeds[13], (D,), 0.5, 3.0, ((0, 32),), jnp.float32)
    cotangent = heavy_noise(seeds[14], (TOKENS, D), 1.0, 6.0, ((0, 32),), (0, 1, 32, 2.75))
    return dict(block_input=block_input, segment_ids=segment_ids, w_qkv=w_qkv, b_qkv=b_qkv, w_out=w_out, b_out=b_out, w_fc1=w_fc1, b_fc1=b_fc1, w_fc2=w_fc2, b_fc2=b_fc2, ln1_gain=ln1_gain, ln1_bias=ln1_bias, ln2_gain=ln2_gain, ln2_bias=ln2_bias, cotangent=cotangent)


EPS = 1e-05
NEG_FILL = -1e+30

def lead_dot(left, right):
    return lax.dot_general(left, right, (((0,), (0,)), ((), ())), preferred_element_type=jnp.float32)

def tail_dot(left, right):
    return lax.dot_general(left, right, (((1,), (1,)), ((), ())), preferred_element_type=jnp.float32)

def normalize(values):
    row_mean = lax.optimization_barrier(jnp.mean(values, axis=-1, keepdims=True))
    centered = values - row_mean
    row_var = lax.optimization_barrier(jnp.mean(centered * centered, axis=-1, keepdims=True))
    inv_std = lax.rsqrt(row_var + EPS)
    return (centered * inv_std, inv_std)

def norm_back(upstream, normed_x, inv_std, gain_vec):
    scaled = upstream * gain_vec
    return inv_std * (scaled - lax.optimization_barrier(jnp.mean(scaled, axis=-1, keepdims=True)) - normed_x * lax.optimization_barrier(jnp.mean(scaled * normed_x, axis=-1, keepdims=True)))

def gelu_value(pre_act):
    return 0.5 * pre_act * (1.0 + jax.scipy.special.erf(pre_act * 2.0 ** (-0.5)))

def gelu_slope(pre_act):
    return 0.5 * (1.0 + jax.scipy.special.erf(pre_act * 2.0 ** (-0.5))) + pre_act * jnp.exp(-0.5 * pre_act * pre_act) * (2.0 * math.pi) ** (-0.5)

def rotary_tables(row_count):
    half_rot = ROT // 2
    position = (jnp.arange(row_count, dtype=jnp.int32) % SEQ).astype(jnp.float32)
    inverse = jnp.exp(jnp.arange(half_rot, dtype=jnp.float32) * (-2.0 * math.log(10000.0) / ROT))
    angle = position[:, None] * inverse[None, :]
    return (jnp.cos(angle)[:, None, :], jnp.sin(angle)[:, None, :])

def rotate(block, cosine_table, sine_table):
    half_rot = ROT // 2
    lower = block[..., :half_rot]
    upper = block[..., half_rot:ROT]
    return jnp.concatenate([lower * cosine_table - upper * sine_table, upper * cosine_table + lower * sine_table, block[..., ROT:]], axis=-1)

def unrotate(block, cosine_table, sine_table):
    half_rot = ROT // 2
    lower = block[..., :half_rot]
    upper = block[..., half_rot:ROT]
    return jnp.concatenate([lower * cosine_table + upper * sine_table, upper * cosine_table - lower * sine_table, block[..., ROT:]], axis=-1)

def widen_bias(bias_rows):
    zeros = jnp.zeros((bias_rows.shape[0], HD), jnp.float32)
    return jnp.concatenate([bias_rows[:, :HD], zeros, bias_rows[:, HD:]], axis=1).reshape(-1)

def narrow_grad(column_sums, head_count):
    grouped = column_sums.reshape(head_count, 3, HD)
    return jnp.concatenate([grouped[:, 0], grouped[:, 2]], axis=-1)

def allowed_pairs(segment):
    position = jnp.arange(segment.shape[0], dtype=jnp.int32)
    return ((position[None, :] <= position[:, None]) & (segment[:, None] == segment[None, :]))[None]

def attend(query_rows, key_rows, value_rows, segment):
    score_scale = HD ** (-0.5)
    allowed = allowed_pairs(segment)
    scores = jnp.einsum('qhd,khd->hqk', query_rows.astype(jnp.float32), key_rows.astype(jnp.float32)) * score_scale
    masked = jnp.where(allowed, scores, NEG_FILL)
    peak_score = lax.optimization_barrier(jnp.max(masked, axis=-1, keepdims=True))
    log_total = peak_score + jnp.log(lax.optimization_barrier(jnp.sum(jnp.where(allowed, jnp.exp(masked - peak_score), 0.0), axis=-1, keepdims=True)))
    prob_low = jnp.where(allowed, jnp.exp(masked - log_total), 0.0).astype(jnp.bfloat16)
    context = jnp.einsum('hqk,khd->qhd', prob_low.astype(jnp.float32), value_rows.astype(jnp.float32)).astype(jnp.bfloat16)
    return (context, log_total)

def attend_back(query_rows, key_rows, value_rows, segment, context, log_total, context_cot):
    score_scale = HD ** (-0.5)
    allowed = allowed_pairs(segment)
    scores = jnp.einsum('qhd,khd->hqk', query_rows.astype(jnp.float32), key_rows.astype(jnp.float32)) * score_scale
    masked = jnp.where(allowed, scores, NEG_FILL)
    prob_full = jnp.where(allowed, jnp.exp(masked - log_total), 0.0)
    prob_low = prob_full.astype(jnp.bfloat16)
    cot_wide = context_cot.astype(jnp.float32)
    prob_cot = jnp.einsum('qhd,khd->hqk', cot_wide, value_rows.astype(jnp.float32))
    row_delta = lax.optimization_barrier(jnp.sum(cot_wide * context.astype(jnp.float32), axis=-1)).T[:, :, None]
    score_cot = (prob_full * (prob_cot - row_delta)).astype(jnp.bfloat16).astype(jnp.float32)
    query_cot = jnp.einsum('hqk,khd->qhd', score_cot, key_rows.astype(jnp.float32)) * score_scale
    key_cot = jnp.einsum('hqk,qhd->khd', score_cot, query_rows.astype(jnp.float32)) * score_scale
    value_cot = jnp.einsum('hqk,qhd->khd', prob_low.astype(jnp.float32), cot_wide)
    return (query_cot, key_cot, value_cot)

def reference(block_input, segment_ids, w_qkv, b_qkv, w_out, b_out, w_fc1, b_fc1, w_fc2, b_fc2, ln1_gain, ln1_bias, ln2_gain, ln2_bias, cotangent):
    seq_count = segment_ids.shape[0]
    cosine_table, sine_table = rotary_tables(SEQ)
    qkv_bias = widen_bias(b_qkv)
    up_bias = b_fc1.reshape(-1)

    def seq_step(running, pieces):
        rows_in, cot_in, segment = pieces
        own_rows = rows_in.astype(jnp.float32)
        normed_x, inv_std = normalize(own_rows)
        norm_one = (normed_x * ln1_gain + ln1_bias).astype(jnp.bfloat16)
        norm_two = (normed_x * ln2_gain + ln2_bias).astype(jnp.bfloat16)
        qkv = (jnp.dot(norm_one, w_qkv, preferred_element_type=jnp.float32) + qkv_bias).reshape(SEQ, H, 3, HD)
        query_rows = rotate(qkv[:, :, 0], cosine_table, sine_table).astype(jnp.bfloat16)
        key_rows = rotate(qkv[:, :, 1], cosine_table, sine_table).astype(jnp.bfloat16)
        value_rows = qkv[:, :, 2].astype(jnp.bfloat16)
        context, log_total = attend(query_rows, key_rows, value_rows, segment)
        context_flat = context.reshape(SEQ, D)
        pre_act = jnp.dot(norm_two, w_fc1, preferred_element_type=jnp.float32) + up_bias
        hidden = gelu_value(pre_act).astype(jnp.bfloat16)
        branches = jnp.dot(context_flat, w_out, preferred_element_type=jnp.float32) + jnp.dot(hidden, w_fc2, preferred_element_type=jnp.float32)
        block_output = (own_rows + branches + b_out + b_fc2).astype(jnp.bfloat16)
        context_cot = tail_dot(cot_in, w_out).astype(jnp.bfloat16)
        act_cot = tail_dot(cot_in, w_fc2) * gelu_slope(pre_act)
        act_low = act_cot.astype(jnp.bfloat16)
        query_cot, key_cot, value_cot = attend_back(query_rows, key_rows, value_rows, segment, context, log_total, context_cot.reshape(SEQ, H, HD))
        qkv_cot = jnp.stack([unrotate(query_cot, cosine_table, sine_table), unrotate(key_cot, cosine_table, sine_table), value_cot], axis=2).reshape(SEQ, 3 * D)
        qkv_low = qkv_cot.astype(jnp.bfloat16)
        norm_one_cot = tail_dot(qkv_low, w_qkv)
        norm_two_cot = tail_dot(act_low, w_fc1)
        cot_own = cot_in.astype(jnp.float32)
        input_grad = cot_own + norm_back(norm_one_cot, normed_x, inv_std, ln1_gain) + norm_back(norm_two_cot, normed_x, inv_std, ln2_gain)
        updates = (lead_dot(norm_one, qkv_low), lax.optimization_barrier(jnp.sum(qkv_cot, axis=0)), lead_dot(context_flat, cot_in), lax.optimization_barrier(jnp.sum(cot_own, axis=0)), lead_dot(norm_two, act_low), lax.optimization_barrier(jnp.sum(act_cot, axis=0)), lead_dot(hidden, cot_in), lax.optimization_barrier(jnp.sum(norm_one_cot * normed_x, axis=0)), lax.optimization_barrier(jnp.sum(norm_one_cot, axis=0)), lax.optimization_barrier(jnp.sum(norm_two_cot * normed_x, axis=0)), lax.optimization_barrier(jnp.sum(norm_two_cot, axis=0)))
        return (jax.tree.map(jnp.add, running, updates), (block_output, input_grad))
    shapes = ((D, 3 * D), (3 * D,), (D, D), (D,), (D, FF), (FF,), (FF, D), (D,), (D,), (D,), (D,))
    initial = tuple((jnp.zeros(shape, jnp.float32) for shape in shapes))
    totals, outputs = lax.scan(seq_step, initial, (block_input.reshape(seq_count, SEQ, D), cotangent.reshape(seq_count, SEQ, D), segment_ids))
    block_output = outputs[0].reshape(seq_count * SEQ, D)
    input_grad = outputs[1].reshape(seq_count * SEQ, D)
    return (block_output, input_grad, totals[0], narrow_grad(totals[1], H), totals[2], totals[3], totals[4], totals[5].reshape(FF // 64, 64), totals[6], totals[3], totals[7], totals[8], totals[9], totals[10])
```

```python
import math

import jax
import jax.numpy as jnp
from jax import lax
from jax.sharding import PartitionSpec as P

HD = 256
ROT = 64
SEQ = 512
INNER = 4
EPS = 1e-05
NEG_FILL = -1e30
F32 = jnp.float32
BF16 = jnp.bfloat16
AXES = ("dp", "tp")


def dot(left, right, contract):
    return lax.dot_general(left, right, (contract, ((), ())), preferred_element_type=F32)


def mm(left, right):
    return dot(left, right, ((1,), (0,)))


def mm_tail(left, right):
    return dot(left, right, ((1,), (1,)))


def mm_lead(left, right):
    return dot(left, right, ((0,), (0,)))


def gelu_half(pre_act):
    return 0.5 * (1.0 + jax.scipy.special.erf(pre_act * 2.0 ** (-0.5)))


def gelu_slope(pre_act):
    return gelu_half(pre_act) + pre_act * jnp.exp(-0.5 * pre_act * pre_act) * (2.0 * math.pi) ** (-0.5)


def rotate(block, cosine, sine):
    half = ROT // 2
    lower, upper = block[..., :half], block[..., half:ROT]
    return jnp.concatenate(
        [lower * cosine - upper * sine, upper * cosine + lower * sine, block[..., ROT:]], axis=-1
    )


def solution(mesh):
    dp_n, tp_n = mesh.shape["dp"], mesh.shape["tp"]
    outer = dp_n // INNER
    devices = dp_n * tp_n

    def send(value, dp_xor, tp_xor, keep=None):
        pairs = []
        for d in range(dp_n):
            for t in range(tp_n):
                if keep is None or keep(d, t):
                    pairs.append((d * tp_n + t, (d ^ dp_xor) * tp_n + (t ^ tp_xor)))
        return lax.ppermute(value, AXES, pairs)

    def gather_small(value, flat):
        held = value[None]
        step = 1
        while step < devices:
            dp_xor, tp_xor = step // tp_n, step % tp_n
            other = send(held, dp_xor, tp_xor)
            high = (flat // step) % 2 == 1
            held = jnp.concatenate(
                [jnp.where(high, other, held), jnp.where(high, held, other)], axis=0
            )
            step *= 2
        return held

    def scatter_small(value, flat):
        held = value
        step = devices // 2
        while step >= 1:
            dp_xor, tp_xor = step // tp_n, step % tp_n
            high = (flat // step) % 2 == 1
            first, second = held[:step], held[step:]
            other = send(jnp.where(high, first, second), dp_xor, tp_xor)
            held = jnp.where(high, second, first) + other
            step //= 2
        return held[0]

    def gather_rows(own):
        z = send(own, 2, 0)
        y = send(own, 1, 0)
        x = send(own, 0, 2)
        yz = send(z, 1, 0)
        xz = send(z, 0, 2)
        xy = send(y, 0, 2)
        xyz = send(yz, 0, 2)
        here = jnp.concatenate([own, z, y, yz, x, xz, xy, xyz], axis=0)
        return jnp.concatenate([here, send(here, 0, 1)], axis=0)

    def scatter_rows(value):
        for dp_xor, tp_xor in ((0, 1), (0, 2), (1, 0), (2, 0)):
            half = value.shape[0] // 2
            other = send(value[half:], dp_xor, tp_xor)
            value = value[:half].astype(F32) + other.astype(F32)
            if half > value.shape[0] or (dp_xor, tp_xor) != (2, 0):
                value = value.astype(BF16)
        return value

    def on_device(
        block_input, segment_ids, w_qkv, b_qkv, w_out, b_out, w_fc1, b_fc1, w_fc2, b_fc2,
        ln1_gain, ln1_bias, ln2_gain, ln2_bias, cotangent,
    ):
        d = lax.axis_index("dp")
        t = lax.axis_index("tp")
        flat = d * tp_n + t
        inner = d % INNER
        core = t % 2
        lead = (inner // 2) == core
        rows, width = block_input.shape
        depth = w_qkv.shape[0]
        hidden_here = w_fc1.shape[1] // INNER
        head_here = w_out.shape[0] // HD
        heads = head_here * tp_n
        quarter = SEQ // tp_n
        qkv_bits = b_qkv.shape[1]

        vec = jnp.stack([ln1_gain, ln1_bias, ln2_gain, ln2_bias, b_out + b_fc2]).reshape(-1)
        seg_part = lax.dynamic_slice(segment_ids.reshape(-1), (t * quarter,), (quarter,))
        sizes = [vec.size, b_qkv.size, b_fc1.size, quarter]
        payload = jnp.concatenate(
            [vec, b_qkv.reshape(-1), b_fc1.reshape(-1), seg_part.astype(F32)]
        )
        small = gather_small(payload, flat)
        cuts = [0]
        for size in sizes:
            cuts.append(cuts[-1] + size)
        vecs = small[:, : cuts[1]].reshape(devices, 5, -1).transpose(1, 0, 2).reshape(5, width)
        gain_one, shift_one, gain_two, shift_two, out_bias = (vecs[k][None] for k in range(5))
        qkv_bias_all = (
            small[:, cuts[1] : cuts[2]]
            .reshape(dp_n, tp_n, head_here, qkv_bits)
            .transpose(1, 2, 0, 3)
            .reshape(heads, 2 * HD)
        )
        head = (t // 2) * INNER + inner
        qkv_bias = lax.dynamic_slice(qkv_bias_all, (head, 0), (1, 2 * HD))
        up_rows, up_cols = b_fc1.shape
        up_bias_all = (
            small[:, cuts[2] : cuts[3]]
            .reshape(dp_n, tp_n, up_rows, up_cols)
            .transpose(1, 2, 0, 3)
            .reshape(tp_n * INNER, hidden_here)
        )
        up_bias = lax.dynamic_slice(up_bias_all, (t * INNER + inner, 0), (1, hidden_here))
        seg_all = small[:, cuts[3] : cuts[4]].reshape(dp_n, tp_n, quarter)

        mlp_all = jnp.concatenate(
            [
                w_fc1.reshape(depth, INNER, hidden_here).transpose(1, 0, 2),
                w_fc2.reshape(INNER, hidden_here, depth).transpose(0, 2, 1),
            ],
            axis=2,
        )
        att_all = jnp.concatenate(
            [
                w_qkv.reshape(depth, head_here, 3 * HD).transpose(1, 0, 2),
                w_out.reshape(head_here, HD, depth).transpose(0, 2, 1),
            ],
            axis=2,
        )

        def pick(stacked, index):
            return lax.dynamic_index_in_dim(stacked, index, 0, keepdims=False)

        mlp_cut = [pick(mlp_all, inner ^ k) for k in range(INNER)]
        att_cut = [pick(att_all, (inner ^ k) % 2) for k in range(2)]

        with jax.named_scope("rows"):
            both = gather_rows(jnp.concatenate([block_input, cotangent], axis=1))

        def place(total, piece, s):
            return lax.dynamic_update_slice(total, piece, ((d ^ s) * depth, 0))

        with jax.named_scope("mlp_in"):
            mlp_got = [mlp_cut[0]] + [send(mlp_cut[s % INNER], s, 0) for s in range(1, dp_n)]
        with jax.named_scope("att_in"):
            att_got = [jnp.where(lead, att_cut[0], jnp.zeros_like(att_cut[0]))] + [
                send(att_cut[s % 2], s, 0, lambda dd, tt, s=s: ((dd ^ s) % INNER) // 2 == tt % 2)
                for s in range(1, dp_n)
            ]
        mlp_w = jnp.zeros((width, mlp_all.shape[2]), BF16)
        for s in range(dp_n):
            mlp_w = place(mlp_w, mlp_got[s], s)
        att_w = jnp.zeros((width, att_all.shape[2]), BF16)
        for s in range(dp_n):
            att_w = place(att_w, att_got[s], s)
        att_pass = send(att_w, 0, 1, lambda dd, tt: (dd % INNER) // 2 == tt % 2)
        att_w = jnp.where(lead, att_w, att_pass)
        up_w, down_w = mlp_w[:, :hidden_here], mlp_w[:, hidden_here:]
        qkv_w, out_w = att_w[:, : 3 * HD], att_w[:, 3 * HD :]

        x_rows, cot_rows = both[:, :width].astype(F32), both[:, width:]
        row_mean = jnp.mean(x_rows, axis=-1, keepdims=True)
        centered = x_rows - row_mean
        row_var = jnp.mean(centered * centered, axis=-1, keepdims=True)
        inv_std = lax.rsqrt(row_var + EPS)
        normed = centered * inv_std
        norm_two = (normed * gain_two + shift_two).astype(BF16)

        def mine(value):
            split = value.reshape((2, 2, 2, 2, rows) + value.shape[1:])
            cut = lax.dynamic_index_in_dim(split, core, 3, keepdims=False)
            return jnp.moveaxis(cut, 2, 0).reshape((2 * SEQ,) + value.shape[1:])

        def unmine(value):
            split = value.reshape((2, 2, 2, rows) + value.shape[1:])
            cut = jnp.moveaxis(split, 0, 2)[:, :, :, None]
            where = (jnp.arange(2) == core).reshape((1, 1, 1, 2) + (1,) * value.ndim)
            full = jnp.where(where, cut, jnp.zeros_like(cut))
            return full.reshape((16 * rows,) + value.shape[1:])

        norm_one = (mine(normed) * gain_one + shift_one).astype(BF16)
        cot_mine = mine(cot_rows)

        pre_act = mm(norm_two, up_w) + up_bias
        half_gelu = gelu_half(pre_act)
        hidden = (pre_act * half_gelu).astype(BF16)
        down_grad = mm_lead(cot_rows, hidden)
        act_cot = mm(cot_rows, down_w) * gelu_slope(pre_act)
        up_bias_part = jnp.sum(act_cot, axis=0)
        act_low = act_cot.astype(BF16)
        up_grad = mm_lead(norm_two, act_low)
        mlp_grad = jnp.concatenate([up_grad.astype(BF16), down_grad.astype(BF16)], axis=1)

        def cut_block(value, s):
            return lax.dynamic_slice(value, ((d ^ s) * depth, 0), (depth, value.shape[1]))

        with jax.named_scope("mlp_out"):
            mlp_back = [cut_block(mlp_grad, 0)] + [
                send(cut_block(mlp_grad, s), s, 0) for s in range(1, dp_n)
            ]

        order = jnp.stack([t ^ ((k % 2) * 2 + k // 2) for k in range(4)])
        position = (order[:, None] * quarter + jnp.arange(quarter)[None]).reshape(-1)
        inverse = jnp.exp(jnp.arange(ROT // 2, dtype=F32) * (-2.0 * math.log(10000.0) / ROT))
        angle = position.astype(F32)[:, None] * inverse[None]
        cosine, sine = jnp.cos(angle)[None], jnp.sin(angle)[None]
        segs = []
        for dy in range(2):
            seq = (d // INNER) * INNER + (inner ^ (core * 2 + dy))
            rows_of = lax.dynamic_index_in_dim(seg_all, seq, 0, keepdims=False)
            segs.append(jnp.take(rows_of, order, axis=0).reshape(-1))
        segs = jnp.stack(segs)
        allowed = (position[None, :] <= position[:, None])[None] & (
            segs[:, :, None] == segs[:, None, :]
        )
        qkv = mm(norm_one, qkv_w)
        query = rotate((qkv[:, :HD] + qkv_bias[:, :HD]).reshape(2, SEQ, HD), cosine, sine).astype(BF16)
        key = rotate(qkv[:, HD : 2 * HD].reshape(2, SEQ, HD), cosine, sine).astype(BF16)
        val = (qkv[:, 2 * HD :] + qkv_bias[:, HD:]).astype(BF16).reshape(2, SEQ, HD)
        scale = HD ** (-0.5)

        def ein(eq, left, right):
            return jnp.einsum(eq, left, right, preferred_element_type=F32)

        masked = jnp.where(allowed, ein("sqd,skd->sqk", query, key) * scale, NEG_FILL)
        peak = jnp.max(masked, axis=-1, keepdims=True)
        log_total = peak + jnp.log(
            jnp.sum(jnp.where(allowed, jnp.exp(masked - peak), 0.0), axis=-1, keepdims=True)
        )
        prob_full = jnp.where(allowed, jnp.exp(masked - log_total), 0.0)
        prob_low = prob_full.astype(BF16)
        context = ein("sqk,skd->sqd", prob_low, val).astype(BF16)
        context_cot = mm(cot_mine, out_w).astype(BF16).reshape(2, SEQ, HD)
        prob_cot = ein("sqd,skd->sqk", context_cot, val)
        row_delta = jnp.sum(context_cot.astype(F32) * context.astype(F32), axis=-1, keepdims=True)
        score_cot = (prob_full * (prob_cot - row_delta)).astype(BF16)
        query_cot = rotate(ein("sqk,skd->sqd", score_cot, key) * scale, cosine, -sine)
        key_cot = rotate(ein("sqk,sqd->skd", score_cot, query) * scale, cosine, -sine)
        val_cot = ein("sqk,sqd->skd", prob_low, context_cot)
        qkv_cot = jnp.concatenate([query_cot, key_cot, val_cot], axis=-1).reshape(2 * SEQ, 3 * HD)
        qkv_bias_part = jnp.concatenate(
            [jnp.sum(query_cot, axis=(0, 1)), jnp.sum(val_cot, axis=(0, 1))]
        )
        qkv_low = qkv_cot.astype(BF16)
        context_flat = context.reshape(2 * SEQ, HD)
        att_grad = jnp.concatenate(
            [mm_lead(norm_one, qkv_low).astype(BF16), mm_lead(cot_mine, context_flat).astype(BF16)],
            axis=1,
        )
        att_pair = send(att_grad, 0, 1, lambda dd, tt: (dd % INNER) // 2 != tt % 2)
        att_grad = (att_grad.astype(F32) + att_pair.astype(F32)).astype(BF16)
        with jax.named_scope("att_out"):
            own_att = cut_block(att_grad, 0)
            att_back = [jnp.where(lead, own_att, jnp.zeros_like(own_att))] + [
                send(cut_block(att_grad, s), s, 0, lambda dd, tt: (dd % INNER) // 2 == tt % 2)
                for s in range(1, dp_n)
            ]

        left = jnp.concatenate([hidden, unmine(context_flat)], axis=1)
        right = jnp.concatenate([down_w, out_w], axis=1)
        with jax.named_scope("branch"):
            branch = scatter_rows(mm_tail(left, right).astype(BF16))
        block_output = (block_input.astype(F32) + branch + out_bias).astype(BF16)

        one_part = mm_tail(qkv_low, qkv_w)
        two_part = mm_tail(act_low, up_w)
        vec_terms = jnp.stack(
            [
                jnp.sum(one_part * mine(normed), axis=0),
                jnp.sum(one_part, axis=0),
                jnp.sum(two_part * normed, axis=0),
                jnp.sum(two_part, axis=0),
                jnp.sum(cotangent.astype(F32), axis=0),
            ]
        )
        scaled_part = (two_part * gain_two + unmine(one_part * gain_one)).astype(BF16)
        with jax.named_scope("normback"):
            scaled = scatter_rows(scaled_part)
        normed_own = normed[:rows]
        input_grad = cotangent.astype(F32) + inv_std[:rows] * (
            scaled
            - jnp.mean(scaled, axis=-1, keepdims=True)
            - normed_own * jnp.mean(scaled * normed_own, axis=-1, keepdims=True)
        )

        head_hot = (jnp.arange(heads) == head).astype(F32)[:, None]
        qkv_small = (
            (head_hot * qkv_bias_part[None])
            .reshape(tp_n, head_here, dp_n, qkv_bits)
            .transpose(2, 0, 1, 3)
            .reshape(devices, -1)
        )
        up_hot = (jnp.arange(tp_n * INNER) == t * INNER + inner).astype(F32)[:, None]
        up_small = (
            (up_hot * up_bias_part[None])
            .reshape(tp_n, up_rows, dp_n, up_cols)
            .transpose(2, 0, 1, 3)
            .reshape(devices, -1)
        )
        vec_small = vec_terms.reshape(5, devices, -1).transpose(1, 0, 2).reshape(devices, -1)
        with jax.named_scope("small_out"):
            own = scatter_small(jnp.concatenate([vec_small, qkv_small, up_small], axis=1), flat)
        vec_own = own[: cuts[1]].reshape(5, -1)
        qkv_bias_grad = own[cuts[1] : cuts[2]].reshape(b_qkv.shape)
        up_bias_grad = own[cuts[2] : cuts[3]].reshape(b_fc1.shape)

        up_total = jnp.zeros(w_fc1.shape, F32)
        down_total = jnp.zeros(w_fc2.shape, F32)
        for k in range(INNER):
            total = sum(mlp_back[s].astype(F32) for s in range(k, dp_n, INNER))
            at = (inner ^ k) * hidden_here
            up_total = lax.dynamic_update_slice(up_total, total[:, :hidden_here], (0, at))
            down_total = lax.dynamic_update_slice(down_total, total[:, hidden_here:].T, (at, 0))
        att_sum = [sum(att_back[s].astype(F32) for s in range(k, dp_n, 2)) for k in range(2)]
        odd = inner % 2 == 1
        att_first = jnp.where(odd, att_sum[1], att_sum[0])
        att_second = jnp.where(odd, att_sum[0], att_sum[1])
        qkv_total = jnp.concatenate([att_first[:, : 3 * HD], att_second[:, : 3 * HD]], axis=1)
        out_total = jnp.concatenate([att_first[:, 3 * HD :].T, att_second[:, 3 * HD :].T], axis=0)
        return (
            block_output, input_grad, qkv_total, qkv_bias_grad, out_total, vec_own[4],
            up_total, up_bias_grad, down_total, vec_own[4],
            vec_own[0], vec_own[1], vec_own[2], vec_own[3],
        )

    row, vec = P(AXES, None), P(AXES)
    col, low = P("dp", "tp"), P("tp", "dp")
    return jax.shard_map(
        on_device,
        mesh=mesh,
        in_specs=(row, P("dp", None), col, low, low, vec, col, low, low, vec, vec, vec, vec, vec, row),
        out_specs=(row, row, col, low, low, vec, col, low, low, vec, vec, vec, vec, vec),
        check_vma=False,
    )
```

```python
import functools
import math

import jax
import jax.numpy as jnp
from jax import lax
from jax.experimental import pallas as pl
from jax.experimental.pallas import tpu as pltpu
from jax.sharding import PartitionSpec as P

HD = 256
ROT = 64
SEQ = 512
INNER = 4
EPS = 1e-05
NEG_FILL = -1e30
F32 = jnp.float32
BF16 = jnp.bfloat16
AXES = ("dp", "tp")
MESH = pl.DeviceIdType.MESH
PAY = 1024


def dot(left, right, contract):
    return lax.dot_general(left, right, (contract, ((), ())), preferred_element_type=F32)


def mm(left, right):
    return dot(left, right, ((1,), (0,)))


def mm_tail(left, right):
    return dot(left, right, ((1,), (1,)))


def mm_lead(left, right):
    return dot(left, right, ((0,), (0,)))


def gelu_half(pre_act):
    return 0.5 * (1.0 + jax.scipy.special.erf(pre_act * 2.0 ** (-0.5)))


def gelu_slope(pre_act):
    return gelu_half(pre_act) + pre_act * jnp.exp(-0.5 * pre_act * pre_act) * (2.0 * math.pi) ** (-0.5)


def rotate(block, cosine, sine):
    half = ROT // 2
    lower, upper = block[..., :half], block[..., half:ROT]
    return jnp.concatenate(
        [lower * cosine - upper * sine, upper * cosine + lower * sine, block[..., ROT:]], axis=-1
    )


def gather_kernel(
    dp_n, tp_n, wide,
    x_ref, cot_ref, fc1_ref, fc2_ref, qkv_ref, out_ref, pay_ref,
    xs_ref, cots_ref, up_ref, down_ref, att_ref, proj_ref, small_ref,
    row_send, row_recv, mlp_send, mlp_recv, att_send, att_recv, pass_send, pass_recv,
    small_send, small_recv, local_sem,
):
    d = lax.axis_index("dp")
    t = lax.axis_index("tp")
    inner = d % INNER
    core = t % 2
    depth = fc1_ref.shape[0]
    hidden = fc1_ref.shape[1] // INNER

    barrier = pltpu.get_barrier_semaphore()
    for s in range(1, dp_n):
        pl.semaphore_signal(barrier, inc=1, device_id=(d ^ s, t), device_id_type=MESH)
    for k in (1, 2):
        pl.semaphore_signal(barrier, inc=1, device_id=(d, t ^ k), device_id_type=MESH)

    def remote(src, dst, send_sem, recv_sem, dp_xor, tp_xor):
        return pltpu.make_async_remote_copy(
            src_ref=src, dst_ref=dst, send_sem=send_sem, recv_sem=recv_sem,
            device_id=(d ^ dp_xor, t ^ tp_xor), device_id_type=MESH,
        )

    hop = {1: (2, 0), 2: (1, 0), 4: (0, 2), 8: (0, 1)}
    pairs = ((x_ref, xs_ref), (cot_ref, cots_ref))

    def row_copy(a, k, bit):
        own, full = pairs[a]
        src = own if k == 0 else full.at[k]
        return remote(src, full.at[k + bit], row_send.at[a, k + bit], row_recv.at[a, k + bit], *hop[bit])

    def columns(ref, index, size):
        return ref.at[:, pl.ds(pl.multiple_of(index * size, 128), size)]

    def lines(ref, index, size):
        return ref.at[pl.ds(pl.multiple_of(index * size, 8), size), :]

    def across(ref, index, size):
        return columns(ref, index, size) if wide else ref.at[index]

    def mlp_copies(s):
        target = inner ^ (s % INNER)
        return (
            (columns(fc1_ref, target, hidden), lines(up_ref, d, depth)),
            (lines(fc2_ref, target, hidden), across(down_ref, d, depth)),
        )

    def att_copies(s):
        target = (inner ^ (s % INNER)) % 2
        return (
            (columns(qkv_ref, target, 3 * HD), lines(att_ref, d, depth)),
            (lines(out_ref, target, HD), across(proj_ref, d, depth)),
        )

    def att_land(s):
        return (lines(att_ref, d ^ s, depth), across(proj_ref, d ^ s, depth))

    def mlp_land(s):
        return (lines(up_ref, d ^ s, depth), across(down_ref, d ^ s, depth))

    local = []
    def stay(src, dst):
        copy = pltpu.make_async_copy(src, dst, local_sem.at[len(local)])
        copy.start()
        local.append(copy)

    lead = (inner // 2) == core
    pltpu.sync_copy(pay_ref, small_ref.at[0])
    pl.semaphore_wait(barrier, dp_n + 1)

    started = []
    def start(copy):
        copy.start()
        started.append(copy)

    def start_rows(k, bit):
        for a in range(2):
            start(row_copy(a, k, bit))

    def wait_rows(k):
        bit = 1
        while bit * 2 <= k:
            bit *= 2
        for a in range(2):
            row_copy(a, k - bit, bit).wait_recv()

    def start_mlp(s):
        for a, (src, dst) in enumerate(mlp_copies(s)):
            start(remote(src, dst, mlp_send.at[a, s], mlp_recv.at[a, s], s, 0))

    def att_active(s):
        return ((inner ^ (s % INNER)) // 2) == core

    def start_att(s):
        @pl.when(att_active(s))
        def _():
            for a, (src, dst) in enumerate(att_copies(s)):
                remote(src, dst, att_send.at[a, s], att_recv.at[a, s], s, 0).start()

    def pass_att(s):
        lands = att_land(s)
        return [
            remote(land, land, pass_send.at[a, s], pass_recv.at[a, s], 0, 1)
            for a, land in enumerate(lands)
        ]

    def small_copy(step, dp_xor, tp_xor, n):
        return remote(
            small_ref.at[pl.ds(0, n)], small_ref.at[pl.ds(n, n)],
            small_send.at[step], small_recv.at[step], dp_xor, tp_xor,
        )

    hops = []
    n = 1
    while n < dp_n * tp_n:
        hops.append((n // tp_n, n % tp_n, n))
        n *= 2
    even = [s for s in range(2, dp_n, 2)]
    even.sort(key=lambda s: -(s >= INNER))
    odd = [s for s in range(1, dp_n, 2)]
    odd.sort(key=lambda s: -(s >= INNER))

    small = [small_copy(k, *h) for k, h in enumerate(hops)]
    small[0].start()
    for bit in (1, 2, 4):
        start_rows(0, bit)
    start_rows(0, 8)
    for s in even:
        start_mlp(s)
    stay(x_ref, xs_ref.at[0])
    stay(cot_ref, cots_ref.at[0])
    for src, dst in mlp_copies(0):
        stay(src, dst)

    @pl.when(lead)
    def _():
        for a, (src, dst) in enumerate(att_copies(0)):
            copy = pltpu.make_async_copy(src, dst, local_sem.at[4 + a])
            copy.start()

    for k in range(len(small)):
        small[k].wait_recv()
        if k + 1 < len(small):
            small[k + 1].start()
    wait_rows(1)
    start_rows(1, 2)
    start_rows(1, 4)
    start_rows(1, 8)
    wait_rows(2)
    start_rows(2, 4)
    start_rows(2, 8)
    for s in odd:
        start_mlp(s)
    for s in even + odd:
        start_att(s)
    wait_rows(3)
    start_rows(3, 4)
    start_rows(3, 8)
    wait_rows(4)
    start_rows(4, 8)

    @pl.when(lead)
    def _():
        for a, (src, dst) in enumerate(att_copies(0)):
            pltpu.make_async_copy(src, dst, local_sem.at[4 + a]).wait()
        for copy in pass_att(0):
            copy.start()

    for k in (5, 6, 7):
        wait_rows(k)
        start_rows(k, 8)
    for k in range(8, 16):
        wait_rows(k)
    for s in even + odd:
        for a, dst in enumerate(mlp_land(s)):
            remote(dst, dst, mlp_send.at[a, s], mlp_recv.at[a, s], s, 0).wait_recv()
    for s in even + odd:
        @pl.when(lead)
        def _():
            for a, dst in enumerate(att_land(s)):
                remote(dst, dst, att_send.at[a, s], att_recv.at[a, s], s, 0).wait_recv()
            for copy in pass_att(s):
                copy.start()

    @pl.when(jnp.logical_not(lead))
    def _():
        for s in range(dp_n):
            for copy in pass_att(s):
                copy.wait_recv()

    @pl.when(lead)
    def _():
        for s in range(dp_n):
            for copy in pass_att(s):
                copy.wait_send()

    for s in range(1, dp_n):
        @pl.when(att_active(s))
        def _():
            for a, (src, dst) in enumerate(att_copies(s)):
                remote(src, dst, att_send.at[a, s], att_recv.at[a, s], s, 0).wait_send()
    for copy in started:
        copy.wait_send()
    for copy in small:
        copy.wait_send()
    for copy in local:
        copy.wait()


def solution(mesh):
    dp_n, tp_n = mesh.shape["dp"], mesh.shape["tp"]
    outer = dp_n // INNER
    devices = dp_n * tp_n

    def send(value, dp_xor, tp_xor, keep=None):
        pairs = []
        for d in range(dp_n):
            for t in range(tp_n):
                if keep is None or keep(d, t):
                    pairs.append((d * tp_n + t, (d ^ dp_xor) * tp_n + (t ^ tp_xor)))
        return lax.ppermute(value, AXES, pairs)

    def scatter_small(value, flat):
        held = value
        step = devices // 2
        while step >= 1:
            dp_xor, tp_xor = step // tp_n, step % tp_n
            high = (flat // step) % 2 == 1
            first, second = held[:step], held[step:]
            other = send(jnp.where(high, first, second), dp_xor, tp_xor)
            held = jnp.where(high, second, first) + other
            step //= 2
        return held[0]

    def scatter_rows(value):
        for dp_xor, tp_xor in ((0, 1), (0, 2), (1, 0), (2, 0)):
            half = value.shape[0] // 2
            other = send(value[half:], dp_xor, tp_xor)
            value = value[:half].astype(F32) + other.astype(F32)
            if half > value.shape[0] or (dp_xor, tp_xor) != (2, 0):
                value = value.astype(BF16)
        return value

    def on_device(
        block_input, segment_ids, w_qkv, b_qkv, w_out, b_out, w_fc1, b_fc1, w_fc2, b_fc2,
        ln1_gain, ln1_bias, ln2_gain, ln2_bias, cotangent,
    ):
        d = lax.axis_index("dp")
        t = lax.axis_index("tp")
        flat = d * tp_n + t
        inner = d % INNER
        core = t % 2
        lead = (inner // 2) == core
        rows, width = block_input.shape
        depth = w_qkv.shape[0]
        hidden_here = w_fc1.shape[1] // INNER
        head_here = w_out.shape[0] // HD
        heads = head_here * tp_n
        quarter = SEQ // tp_n
        qkv_bits = b_qkv.shape[1]

        vec = jnp.stack([ln1_gain, ln1_bias, ln2_gain, ln2_bias, b_out + b_fc2]).reshape(-1)
        seg_part = lax.dynamic_slice(segment_ids.reshape(-1), (t * quarter,), (quarter,))
        sizes = [vec.size, b_qkv.size, b_fc1.size, quarter]
        payload = jnp.concatenate(
            [vec, b_qkv.reshape(-1), b_fc1.reshape(-1), seg_part.astype(F32)]
        )
        depth_wide = depth % 128 == 0
        flat_shape = lambda lead_n: (lead_n, width) if depth_wide else (dp_n, lead_n, depth)
        spread = lambda v: v if depth_wide else v.transpose(1, 0, 2).reshape(v.shape[1], width)
        payload = jnp.pad(payload, (0, PAY - payload.size)).reshape(8, PAY // 8)
        like = lambda *shape: jax.ShapeDtypeStruct(shape, BF16)
        dma = pltpu.SemaphoreType.DMA
        hop_count = (devices - 1).bit_length()
        any_spec = pl.BlockSpec(memory_space=pl.ANY)
        x_all, cot_all, up_w, down_w, qkv_w, out_w, small = pl.pallas_call(
            functools.partial(gather_kernel, dp_n, tp_n, depth_wide),
            out_shape=(
                like(16, rows, width),
                like(16, rows, width),
                like(width, hidden_here),
                like(*flat_shape(hidden_here)),
                like(width, 3 * HD),
                like(*flat_shape(HD)),
                jax.ShapeDtypeStruct((devices, 8, PAY // 8), F32),
            ),
            in_specs=[any_spec] * 7,
            out_specs=(any_spec,) * 7,
            scratch_shapes=[
                dma((2, 16)), dma((2, 16)), dma((2, dp_n)), dma((2, dp_n)),
                dma((2, dp_n)), dma((2, dp_n)), dma((2, dp_n)), dma((2, dp_n)),
                dma((hop_count,)), dma((hop_count,)), dma((6,)),
            ],
            compiler_params=pltpu.CompilerParams(collective_id=0, has_side_effects=True),
            name="gather_phase",
        )(block_input, cotangent, w_fc1, w_fc2, w_qkv, w_out, payload)
        down_w, out_w = spread(down_w), spread(out_w)
        small = jnp.take(small.reshape(devices, PAY), flat ^ jnp.arange(devices), axis=0)
        cuts = [0]
        for size in sizes:
            cuts.append(cuts[-1] + size)
        vecs = small[:, : cuts[1]].reshape(devices, 5, -1).transpose(1, 0, 2).reshape(5, width)
        gain_one, shift_one, gain_two, shift_two, out_bias = (vecs[k][None] for k in range(5))
        qkv_bias_all = (
            small[:, cuts[1] : cuts[2]]
            .reshape(dp_n, tp_n, head_here, qkv_bits)
            .transpose(1, 2, 0, 3)
            .reshape(heads, 2 * HD)
        )
        head = (t // 2) * INNER + inner
        qkv_bias = lax.dynamic_slice(qkv_bias_all, (head, 0), (1, 2 * HD))
        up_rows, up_cols = b_fc1.shape
        up_bias_all = (
            small[:, cuts[2] : cuts[3]]
            .reshape(dp_n, tp_n, up_rows, up_cols)
            .transpose(1, 2, 0, 3)
            .reshape(tp_n * INNER, hidden_here)
        )
        up_bias = lax.dynamic_slice(up_bias_all, (t * INNER + inner, 0), (1, hidden_here))
        seg_all = small[:, cuts[3] : cuts[4]].reshape(dp_n, tp_n, quarter)

        x_rows = x_all.reshape(16 * rows, width).astype(F32)
        cot_rows = cot_all.reshape(16 * rows, width)
        row_mean = jnp.mean(x_rows, axis=-1, keepdims=True)
        centered = x_rows - row_mean
        row_var = jnp.mean(centered * centered, axis=-1, keepdims=True)
        inv_std = lax.rsqrt(row_var + EPS)
        normed = centered * inv_std
        norm_two = (normed * gain_two + shift_two).astype(BF16)

        def mine(value):
            split = value.reshape((2, 2, 2, 2, rows) + value.shape[1:])
            cut = lax.dynamic_index_in_dim(split, core, 3, keepdims=False)
            return jnp.moveaxis(cut, 2, 0).reshape((2 * SEQ,) + value.shape[1:])

        def unmine(value):
            split = value.reshape((2, 2, 2, rows) + value.shape[1:])
            cut = jnp.moveaxis(split, 0, 2)[:, :, :, None]
            where = (jnp.arange(2) == core).reshape((1, 1, 1, 2) + (1,) * value.ndim)
            full = jnp.where(where, cut, jnp.zeros_like(cut))
            return full.reshape((16 * rows,) + value.shape[1:])

        norm_one = (mine(normed) * gain_one + shift_one).astype(BF16)
        cot_mine = mine(cot_rows)

        pre_act = mm(norm_two, up_w) + up_bias
        half_gelu = gelu_half(pre_act)
        hidden = (pre_act * half_gelu).astype(BF16)
        down_grad = mm_lead(hidden, cot_rows)
        act_cot = mm_tail(cot_rows, down_w) * gelu_slope(pre_act)
        up_bias_part = jnp.sum(act_cot, axis=0)
        act_low = act_cot.astype(BF16)
        up_grad = mm_lead(norm_two, act_low)
        up_grad, down_grad = up_grad.astype(BF16), down_grad.astype(BF16)

        def cut_block(value, s):
            return lax.dynamic_slice(value, ((d ^ s) * depth, 0), (depth, value.shape[1]))

        def cut_across(value, s):
            return lax.dynamic_slice(value, (0, (d ^ s) * depth), (value.shape[0], depth))

        with jax.named_scope("mlp_out"):
            up_back = [cut_block(up_grad, 0)] + [
                send(cut_block(up_grad, s), s, 0) for s in range(1, dp_n)
            ]
            down_back = [cut_across(down_grad, 0)] + [
                send(cut_across(down_grad, s), s, 0) for s in range(1, dp_n)
            ]

        order = jnp.stack([t ^ ((k % 2) * 2 + k // 2) for k in range(4)])
        position = (order[:, None] * quarter + jnp.arange(quarter)[None]).reshape(-1)
        inverse = jnp.exp(jnp.arange(ROT // 2, dtype=F32) * (-2.0 * math.log(10000.0) / ROT))
        angle = position.astype(F32)[:, None] * inverse[None]
        cosine, sine = jnp.cos(angle)[None], jnp.sin(angle)[None]
        segs = []
        for dy in range(2):
            seq = (d // INNER) * INNER + (inner ^ (core * 2 + dy))
            rows_of = lax.dynamic_index_in_dim(seg_all, seq, 0, keepdims=False)
            segs.append(jnp.take(rows_of, order, axis=0).reshape(-1))
        segs = jnp.stack(segs)
        allowed = (position[None, :] <= position[:, None])[None] & (
            segs[:, :, None] == segs[:, None, :]
        )
        qkv = mm(norm_one, qkv_w)
        query = rotate((qkv[:, :HD] + qkv_bias[:, :HD]).reshape(2, SEQ, HD), cosine, sine).astype(BF16)
        key = rotate(qkv[:, HD : 2 * HD].reshape(2, SEQ, HD), cosine, sine).astype(BF16)
        val = (qkv[:, 2 * HD :] + qkv_bias[:, HD:]).astype(BF16).reshape(2, SEQ, HD)
        scale = HD ** (-0.5)

        def ein(eq, left, right):
            return jnp.einsum(eq, left, right, preferred_element_type=F32)

        masked = jnp.where(allowed, ein("sqd,skd->sqk", query, key) * scale, NEG_FILL)
        peak = jnp.max(masked, axis=-1, keepdims=True)
        log_total = peak + jnp.log(
            jnp.sum(jnp.where(allowed, jnp.exp(masked - peak), 0.0), axis=-1, keepdims=True)
        )
        prob_full = jnp.where(allowed, jnp.exp(masked - log_total), 0.0)
        prob_low = prob_full.astype(BF16)
        context = ein("sqk,skd->sqd", prob_low, val).astype(BF16)
        context_cot = mm_tail(cot_mine, out_w).astype(BF16).reshape(2, SEQ, HD)
        prob_cot = ein("sqd,skd->sqk", context_cot, val)
        row_delta = jnp.sum(context_cot.astype(F32) * context.astype(F32), axis=-1, keepdims=True)
        score_cot = (prob_full * (prob_cot - row_delta)).astype(BF16)
        query_cot = rotate(ein("sqk,skd->sqd", score_cot, key) * scale, cosine, -sine)
        key_cot = rotate(ein("sqk,sqd->skd", score_cot, query) * scale, cosine, -sine)
        val_cot = ein("sqk,sqd->skd", prob_low, context_cot)
        qkv_cot = jnp.concatenate([query_cot, key_cot, val_cot], axis=-1).reshape(2 * SEQ, 3 * HD)
        qkv_bias_part = jnp.concatenate(
            [jnp.sum(query_cot, axis=(0, 1)), jnp.sum(val_cot, axis=(0, 1))]
        )
        qkv_low = qkv_cot.astype(BF16)
        context_flat = context.reshape(2 * SEQ, HD)
        att_grad = jnp.concatenate(
            [mm_lead(norm_one, qkv_low).astype(BF16), mm_lead(cot_mine, context_flat).astype(BF16)],
            axis=1,
        )
        att_pair = send(att_grad, 0, 1, lambda dd, tt: (dd % INNER) // 2 != tt % 2)
        att_grad = (att_grad.astype(F32) + att_pair.astype(F32)).astype(BF16)
        with jax.named_scope("att_out"):
            own_att = cut_block(att_grad, 0)
            att_back = [jnp.where(lead, own_att, jnp.zeros_like(own_att))] + [
                send(cut_block(att_grad, s), s, 0, lambda dd, tt: (dd % INNER) // 2 == tt % 2)
                for s in range(1, dp_n)
            ]

        left = jnp.concatenate([hidden, unmine(context_flat)], axis=1)
        right = jnp.concatenate([down_w, out_w], axis=0)
        with jax.named_scope("branch"):
            branch = scatter_rows(mm(left, right).astype(BF16))
        block_output = (block_input.astype(F32) + branch + out_bias).astype(BF16)

        one_part = mm_tail(qkv_low, qkv_w)
        two_part = mm_tail(act_low, up_w)
        vec_terms = jnp.stack(
            [
                jnp.sum(one_part * mine(normed), axis=0),
                jnp.sum(one_part, axis=0),
                jnp.sum(two_part * normed, axis=0),
                jnp.sum(two_part, axis=0),
                jnp.sum(cotangent.astype(F32), axis=0),
            ]
        )
        scaled_part = (two_part * gain_two + unmine(one_part * gain_one)).astype(BF16)
        with jax.named_scope("normback"):
            scaled = scatter_rows(scaled_part)
        normed_own = normed[:rows]
        input_grad = cotangent.astype(F32) + inv_std[:rows] * (
            scaled
            - jnp.mean(scaled, axis=-1, keepdims=True)
            - normed_own * jnp.mean(scaled * normed_own, axis=-1, keepdims=True)
        )

        head_hot = (jnp.arange(heads) == head).astype(F32)[:, None]
        qkv_small = (
            (head_hot * qkv_bias_part[None])
            .reshape(tp_n, head_here, dp_n, qkv_bits)
            .transpose(2, 0, 1, 3)
            .reshape(devices, -1)
        )
        up_hot = (jnp.arange(tp_n * INNER) == t * INNER + inner).astype(F32)[:, None]
        up_small = (
            (up_hot * up_bias_part[None])
            .reshape(tp_n, up_rows, dp_n, up_cols)
            .transpose(2, 0, 1, 3)
            .reshape(devices, -1)
        )
        vec_small = vec_terms.reshape(5, devices, -1).transpose(1, 0, 2).reshape(devices, -1)
        with jax.named_scope("small_out"):
            own = scatter_small(jnp.concatenate([vec_small, qkv_small, up_small], axis=1), flat)
        vec_own = own[: cuts[1]].reshape(5, -1)
        qkv_bias_grad = own[cuts[1] : cuts[2]].reshape(b_qkv.shape)
        up_bias_grad = own[cuts[2] : cuts[3]].reshape(b_fc1.shape)

        up_total = jnp.zeros(w_fc1.shape, F32)
        down_total = jnp.zeros(w_fc2.shape, F32)
        for k in range(INNER):
            at = (inner ^ k) * hidden_here
            up_sum = sum(up_back[s].astype(F32) for s in range(k, dp_n, INNER))
            down_sum = sum(down_back[s].astype(F32) for s in range(k, dp_n, INNER))
            up_total = lax.dynamic_update_slice(up_total, up_sum, (0, at))
            down_total = lax.dynamic_update_slice(down_total, down_sum, (at, 0))
        att_sum = [sum(att_back[s].astype(F32) for s in range(k, dp_n, 2)) for k in range(2)]
        odd = inner % 2 == 1
        att_first = jnp.where(odd, att_sum[1], att_sum[0])
        att_second = jnp.where(odd, att_sum[0], att_sum[1])
        qkv_total = jnp.concatenate([att_first[:, : 3 * HD], att_second[:, : 3 * HD]], axis=1)
        out_total = jnp.concatenate([att_first[:, 3 * HD :].T, att_second[:, 3 * HD :].T], axis=0)
        return (
            block_output, input_grad, qkv_total, qkv_bias_grad, out_total, vec_own[4],
            up_total, up_bias_grad, down_total, vec_own[4],
            vec_own[0], vec_own[1], vec_own[2], vec_own[3],
        )

    row, vec = P(AXES, None), P(AXES)
    col, low = P("dp", "tp"), P("tp", "dp")
    return jax.shard_map(
        on_device,
        mesh=mesh,
        in_specs=(row, P("dp", None), col, low, low, vec, col, low, low, vec, vec, vec, vec, vec, row),
        out_specs=(row, row, col, low, low, vec, col, low, low, vec, vec, vec, vec, vec),
        check_vma=False,
    )
```

```python
import functools
import math

import jax
import jax.numpy as jnp
import numpy as np
from jax import lax
from jax.experimental import pallas as pl
from jax.experimental.pallas import tpu as pltpu
from jax.sharding import PartitionSpec as P

HD = 256
ROT = 64
SEQ = 512
INNER = 4
EPS = 1e-05
NEG_FILL = -1e30
F32 = jnp.float32
BF16 = jnp.bfloat16
AXES = ("dp", "tp")
MESH = pl.DeviceIdType.MESH
PAY = 1024


def dot(left, right, contract):
    return lax.dot_general(left, right, (contract, ((), ())), preferred_element_type=F32)


def mm(left, right):
    return dot(left, right, ((1,), (0,)))


def mm_tail(left, right):
    return dot(left, right, ((1,), (1,)))


def mm_lead(left, right):
    return dot(left, right, ((0,), (0,)))


def gelu_half(pre_act):
    return 0.5 * (1.0 + jax.scipy.special.erf(pre_act * 2.0 ** (-0.5)))


def gelu_slope(pre_act):
    return gelu_half(pre_act) + pre_act * jnp.exp(-0.5 * pre_act * pre_act) * (2.0 * math.pi) ** (-0.5)


def rotate(block, cosine, sine):
    half = ROT // 2
    lower, upper = block[..., :half], block[..., half:ROT]
    return jnp.concatenate(
        [lower * cosine - upper * sine, upper * cosine + lower * sine, block[..., ROT:]], axis=-1
    )


def gather_kernel(
    dp_n, tp_n, wide,
    x_ref, cot_ref, fc1_ref, fc2_ref, qkv_ref, out_ref, pay_ref,
    xs_ref, cots_ref, up_ref, down_ref, att_ref, proj_ref, small_ref,
    row_send, row_recv, mlp_send, mlp_recv, att_send, att_recv, pass_send, pass_recv,
    small_send, small_recv, local_sem,
):
    d = lax.axis_index("dp")
    t = lax.axis_index("tp")
    inner = d % INNER
    core = t % 2
    depth = fc1_ref.shape[0]
    hidden = fc1_ref.shape[1] // INNER

    barrier = pltpu.get_barrier_semaphore()
    for s in range(1, dp_n):
        pl.semaphore_signal(barrier, inc=1, device_id=(d ^ s, t), device_id_type=MESH)
    for k in (1, 2):
        pl.semaphore_signal(barrier, inc=1, device_id=(d, t ^ k), device_id_type=MESH)

    def remote(src, dst, send_sem, recv_sem, dp_xor, tp_xor):
        return pltpu.make_async_remote_copy(
            src_ref=src, dst_ref=dst, send_sem=send_sem, recv_sem=recv_sem,
            device_id=(d ^ dp_xor, t ^ tp_xor), device_id_type=MESH,
        )

    hop = {1: (2, 0), 2: (1, 0), 4: (0, 2), 8: (0, 1)}
    pairs = ((x_ref, xs_ref), (cot_ref, cots_ref))

    def row_copy(a, k, bit):
        own, full = pairs[a]
        src = own if k == 0 else full.at[k]
        return remote(src, full.at[k + bit], row_send.at[a, k + bit], row_recv.at[a, k + bit], *hop[bit])

    def columns(ref, index, size):
        return ref.at[:, pl.ds(pl.multiple_of(index * size, 128), size)]

    def lines(ref, index, size):
        return ref.at[pl.ds(pl.multiple_of(index * size, 8), size), :]

    def across(ref, index, size):
        return columns(ref, index, size) if wide else ref.at[index]

    def mlp_copies(s):
        target = inner ^ (s % INNER)
        return (
            (columns(fc1_ref, target, hidden), lines(up_ref, d, depth)),
            (lines(fc2_ref, target, hidden), across(down_ref, d, depth)),
        )

    def att_copies(s):
        target = (inner ^ (s % INNER)) % 2
        return (
            (columns(qkv_ref, target, 3 * HD), lines(att_ref, d, depth)),
            (lines(out_ref, target, HD), across(proj_ref, d, depth)),
        )

    def att_land(s):
        return (lines(att_ref, d ^ s, depth), across(proj_ref, d ^ s, depth))

    def mlp_land(s):
        return (lines(up_ref, d ^ s, depth), across(down_ref, d ^ s, depth))

    local = []
    def stay(src, dst):
        copy = pltpu.make_async_copy(src, dst, local_sem.at[len(local)])
        copy.start()
        local.append(copy)

    lead = (inner // 2) == core
    pltpu.sync_copy(pay_ref, small_ref.at[0])
    pl.semaphore_wait(barrier, dp_n + 1)

    started = []
    def start(copy):
        copy.start()
        started.append(copy)

    def start_rows(k, bit):
        for a in range(2):
            start(row_copy(a, k, bit))

    def wait_rows(k):
        bit = 1
        while bit * 2 <= k:
            bit *= 2
        for a in range(2):
            row_copy(a, k - bit, bit).wait_recv()

    def start_mlp(s):
        for a, (src, dst) in enumerate(mlp_copies(s)):
            start(remote(src, dst, mlp_send.at[a, s], mlp_recv.at[a, s], s, 0))

    def att_active(s):
        return ((inner ^ (s % INNER)) // 2) == core

    def start_att(s):
        @pl.when(att_active(s))
        def _():
            for a, (src, dst) in enumerate(att_copies(s)):
                remote(src, dst, att_send.at[a, s], att_recv.at[a, s], s, 0).start()

    def pass_att(s):
        lands = att_land(s)
        return [
            remote(land, land, pass_send.at[a, s], pass_recv.at[a, s], 0, 1)
            for a, land in enumerate(lands)
        ]

    def small_copy(step, dp_xor, tp_xor, n):
        return remote(
            small_ref.at[pl.ds(0, n)], small_ref.at[pl.ds(n, n)],
            small_send.at[step], small_recv.at[step], dp_xor, tp_xor,
        )

    hops = []
    n = 1
    while n < dp_n * tp_n:
        hops.append((n // tp_n, n % tp_n, n))
        n *= 2
    even = [s for s in range(2, dp_n, 2)]
    even.sort(key=lambda s: -(s >= INNER))
    odd = [s for s in range(1, dp_n, 2)]
    odd.sort(key=lambda s: -(s >= INNER))

    small = [small_copy(k, *h) for k, h in enumerate(hops)]
    small[0].start()
    for bit in (1, 2, 4):
        start_rows(0, bit)
    start_rows(0, 8)
    for s in even:
        start_mlp(s)
    stay(x_ref, xs_ref.at[0])
    stay(cot_ref, cots_ref.at[0])
    for src, dst in mlp_copies(0):
        stay(src, dst)

    @pl.when(lead)
    def _():
        for a, (src, dst) in enumerate(att_copies(0)):
            copy = pltpu.make_async_copy(src, dst, local_sem.at[4 + a])
            copy.start()

    for k in range(len(small)):
        small[k].wait_recv()
        if k + 1 < len(small):
            small[k + 1].start()
    wait_rows(1)
    start_rows(1, 2)
    start_rows(1, 4)
    start_rows(1, 8)
    wait_rows(2)
    start_rows(2, 4)
    start_rows(2, 8)
    for s in odd:
        start_mlp(s)
    for s in even + odd:
        start_att(s)
    wait_rows(3)
    start_rows(3, 4)
    start_rows(3, 8)
    wait_rows(4)
    start_rows(4, 8)

    @pl.when(lead)
    def _():
        for a, (src, dst) in enumerate(att_copies(0)):
            pltpu.make_async_copy(src, dst, local_sem.at[4 + a]).wait()
        for copy in pass_att(0):
            copy.start()

    for k in (5, 6, 7):
        wait_rows(k)
        start_rows(k, 8)
    for k in range(8, 16):
        wait_rows(k)
    for s in even + odd:
        for a, dst in enumerate(mlp_land(s)):
            remote(dst, dst, mlp_send.at[a, s], mlp_recv.at[a, s], s, 0).wait_recv()
    for s in even + odd:
        @pl.when(lead)
        def _():
            for a, dst in enumerate(att_land(s)):
                remote(dst, dst, att_send.at[a, s], att_recv.at[a, s], s, 0).wait_recv()
            for copy in pass_att(s):
                copy.start()

    @pl.when(jnp.logical_not(lead))
    def _():
        for s in range(dp_n):
            for copy in pass_att(s):
                copy.wait_recv()

    @pl.when(lead)
    def _():
        for s in range(dp_n):
            for copy in pass_att(s):
                copy.wait_send()

    for s in range(1, dp_n):
        @pl.when(att_active(s))
        def _():
            for a, (src, dst) in enumerate(att_copies(s)):
                remote(src, dst, att_send.at[a, s], att_recv.at[a, s], s, 0).wait_send()
    for copy in started:
        copy.wait_send()
    for copy in small:
        copy.wait_send()
    for copy in local:
        copy.wait()


def span(start, size, unit):
    return pl.ds(start if isinstance(start, int) else pl.multiple_of(start, unit), size)


def lane_cut(ref, start, size):
    return ref.at[:, span(start, size, 128)]


def row_cut(ref, start, size):
    return ref.at[span(start, size, 16), :]


def columns_of(rows8):
    pad = jnp.zeros((120, 128), F32)
    return jnp.transpose(jnp.concatenate([rows8, pad], axis=0))


def fused_kernel(
    dp_n, tp_n,
    x_ref, cot_ref, fc1_ref, fc2_ref, qkv_ref, out_ref, pay_ref, rope_ref,
    block_out, input_out, up_out, down_out, qkv_out, proj_out, tail_out,
    gu_hbm, gd_hbm, ru_hbm, rd_hbm, ra_hbm,
    xs, cots, n2, up_t, down_w, pre, hid_t, act_t, ring, stats, vecs, sums, up_sum,
    att_w, proj_w, n1, q_s, k_s, v_s, prob, ctx, ctx_t, cctx, low, low_t, gx,
    rope, small, small_in, keys, queries, qkv_bias, qkv_sum,
    row_send, row_recv, mlp_send, mlp_recv, att_send, att_recv, pass_send, pass_recv,
    small_send, small_recv, back_send, back_recv, g_send, g_recv, g_local,
    rs_send, rs_recv, pair_send, pair_recv, ga_send, ga_recv,
    local_sem, out_sem, credit,
):
    d = lax.axis_index("dp")
    t = lax.axis_index("tp")
    flat = d * tp_n + t
    inner = d % INNER
    core = t % 2
    lead = (inner // 2) == core
    follow = jnp.logical_not(lead)
    rows, width = x_ref.shape
    depth = fc1_ref.shape[0]
    hidden = fc1_ref.shape[1] // INNER
    devices = dp_n * tp_n
    slots = 16
    tokens = slots * rows
    scale = HD ** (-0.5)
    chunk = 512

    barrier = pltpu.get_barrier_semaphore()
    for s in range(1, dp_n):
        pl.semaphore_signal(barrier, inc=1, device_id=(d ^ s, t), device_id_type=MESH)
    for k in (1, 2):
        pl.semaphore_signal(barrier, inc=1, device_id=(d, t ^ k), device_id_type=MESH)

    def remote(src, dst, send_sem, recv_sem, dp_xor, tp_xor):
        return pltpu.make_async_remote_copy(
            src_ref=src, dst_ref=dst, send_sem=send_sem, recv_sem=recv_sem,
            device_id=(d ^ dp_xor, t ^ tp_xor), device_id_type=MESH,
        )

    started = []

    def start(copy):
        copy.start()
        started.append(copy)

    hop = {1: (2, 0), 2: (1, 0), 4: (0, 2), 8: (0, 1)}

    def slot(ref, k):
        return row_cut(ref, k * rows, rows)

    def row_copy(a, k, bit):
        own, full = ((x_ref, xs), (cot_ref, cots))[a]
        src = own if k == 0 else slot(full, k)
        return remote(
            src, slot(full, k + bit), row_send.at[a, k + bit], row_recv.at[a, k + bit], *hop[bit]
        )

    row_started = ([], [])

    def start_row(a, k, *bits):
        for bit in bits:
            copy = row_copy(a, k, bit)
            copy.start()
            row_started[a].append(copy)

    def wait_row(a, k):
        bit = 1
        while bit * 2 <= k:
            bit *= 2
        row_copy(a, k - bit, bit).wait_recv()

    def w1_piece(i):
        return gx.at[depth : depth + hidden, pl.ds(pl.multiple_of(i * depth, 128), depth)]

    def mlp_copy(a, s):
        target = inner ^ (s % INNER)
        src = w1_piece(target) if a == 0 else row_cut(fc2_ref, target * hidden, hidden)
        dst = lane_cut((up_t, down_w)[a], d * depth, depth)
        if s == 0:
            return src, dst
        return remote(src, dst, mlp_send.at[a, s], mlp_recv.at[a, s], s, 0)

    mlp_started = ([], [])

    def start_mlp(a, s):
        copy = mlp_copy(a, s)
        copy.start()
        mlp_started[a].append(copy)

    def mlp_wait(a, s):
        dst = lane_cut((up_t, down_w)[a], (d ^ s) * depth, depth)
        remote(dst, dst, mlp_send.at[a, s], mlp_recv.at[a, s], s, 0).wait_recv()

    def att_active(s):
        return ((inner ^ (s % INNER)) // 2) == core

    def att_pairs(s):
        target = (inner ^ (s % INNER)) % 2
        return (
            (lane_cut(qkv_ref, target * 3 * HD, 3 * HD), row_cut(att_w, d * depth, depth)),
            (row_cut(out_ref, target * HD, HD), lane_cut(proj_w, d * depth, depth)),
        )

    def att_land(s):
        return (row_cut(att_w, (d ^ s) * depth, depth), lane_cut(proj_w, (d ^ s) * depth, depth))

    def start_att(s):
        @pl.when(att_active(s))
        def _():
            for a, (src, dst) in enumerate(att_pairs(s)):
                remote(src, dst, att_send.at[a, s], att_recv.at[a, s], s, 0).start()

    def pass_att(s):
        return [
            remote(land, land, pass_send.at[a, s], pass_recv.at[a, s], 0, 1)
            for a, land in enumerate(att_land(s))
        ]

    local = []

    def stay(src, dst):
        copy = pltpu.make_async_copy(src, dst, local_sem.at[len(local)])
        copy.start()
        local.append(copy)
        return copy

    fc1_in = stay(fc1_ref, gx.at[0:depth, :])
    pay_in = stay(pay_ref, small.at[0])
    x_in = stay(x_ref, slot(xs, 0))
    cot_in = stay(cot_ref, slot(cots, 0))
    down_in = stay(*mlp_copy(1, 0))
    rope_in = stay(rope_ref, rope)
    pay_in.wait()
    pl.semaphore_wait(barrier, dp_n + 1)

    hops = []
    n = 1
    while n < devices:
        hops.append((n // tp_n, n % tp_n, n))
        n *= 2
    small_copies = [
        remote(
            small.at[pl.ds(0, n)], small.at[pl.ds(n, n)],
            small_send.at[k], small_recv.at[k], dp_xor, tp_xor,
        )
        for k, (dp_xor, tp_xor, n) in enumerate(hops)
    ]
    even = sorted(range(2, dp_n, 2), key=lambda s: -(s >= INNER))
    odd = sorted(range(1, dp_n, 2), key=lambda s: -(s >= INNER))

    small_copies[0].start()
    start_row(0, 0, 1, 2, 4, 8)
    start_row(1, 0, 1, 2, 8)
    fc1_in.wait()
    for i in range(INNER):
        piece = gx[0:depth, i * hidden : (i + 1) * hidden].astype(F32)
        gx[depth : depth + hidden, i * depth : (i + 1) * depth] = jnp.transpose(piece).astype(BF16)
    for s in even:
        start_mlp(0, s)
    up_in = stay(*mlp_copy(0, 0))

    @pl.when(lead)
    def _():
        for a, (src, dst) in enumerate(att_pairs(0)):
            pltpu.make_async_copy(src, dst, local_sem.at[20 + a]).start()

    for k in range(len(small_copies)):
        small_copies[k].wait_recv()
        if k + 1 < len(small_copies):
            small_copies[k + 1].start()
    half = lax.broadcasted_iota(jnp.int32, (8, 128), 1) < 64
    for j in range(devices // 2):
        left = small[flat ^ (2 * j), 0]
        right = small[flat ^ (2 * j + 1), 0]
        vecs[:, j * 128 : (j + 1) * 128] = jnp.where(half, left, right)
    bias8 = jnp.zeros((8, 128), F32)
    head8 = jnp.zeros((8, 128), F32)
    head_rel = core ^ (inner // 2)
    for s in range(dp_n):
        bias8 = bias8 + small[s * tp_n, 1 + inner // 2]
        head8 = head8 + small[s * tp_n + head_rel, 3]
    second = inner % 2 == 1
    bias_t = columns_of(bias8)
    up_bias = jnp.concatenate(
        [jnp.where(second, bias_t[:, 4 + k : 5 + k], bias_t[:, k : k + 1]) for k in range(4)], axis=0
    )
    head4 = jnp.where(second, head8[4:], head8[:4])
    qkv_bias[0:1, :] = jnp.concatenate([head4[k : k + 1] for k in range(4)], axis=1)
    lane = lax.broadcasted_iota(jnp.int32, (1, 128), 1)
    keys[...] = jnp.zeros_like(keys)
    for q in range(4):
        at = slice(q * 128, (q + 1) * 128)
        keys[0:1, at] = ((t ^ ((q % 2) * 2 + q // 2)) * 128 + lane).astype(F32)
        for dy in range(2):
            peer = (core * 2 + dy) * tp_n + (q % 2) * 2 + q // 2
            keys[1 + dy : 2 + dy, at] = small[peer, 0][5:6, :]
        queries[at, :] = columns_of(keys[:, at])

    wait_row(0, 1)
    start_row(0, 1, 2, 4, 8)
    wait_row(0, 2)
    start_row(0, 2, 4, 8)
    for s in odd:
        start_mlp(0, s)
    wait_row(1, 1)
    start_row(1, 1, 2, 8)
    wait_row(1, 2)
    start_row(1, 2, 8)
    for s in even + odd:
        start_mlp(1, s)

    def norm_slot(k):
        @pl.loop(0, rows // 16)
        def _(j):
            at = pl.ds(pl.multiple_of(k * rows + j * 16, 16), 16)
            value = xs[at, :].astype(F32)
            mean = jnp.mean(value, axis=-1, keepdims=True)
            centered = value - mean
            inv = lax.rsqrt(jnp.mean(centered * centered, axis=-1, keepdims=True) + EPS)
            n2[at, :] = (centered * inv * vecs[2:3, :] + vecs[3:4, :]).astype(BF16)
            stats[at, 0:64] = jnp.broadcast_to(mean, (16, 64))
            stats[at, 64:128] = jnp.broadcast_to(inv, (16, 64))

    x_in.wait()
    norm_slot(0)
    wait_row(0, 3)
    start_row(0, 3, 4, 8)
    start_row(1, 0, 4)
    start_row(1, 1, 4)
    start_row(1, 2, 4)
    for k in (1, 2, 3):
        norm_slot(k)
    wait_row(1, 3)
    start_row(1, 3, 4, 8)
    for s in even + odd:
        start_att(s)
    for k in (4, 5, 6, 7):
        wait_row(0, k)
        start_row(0, k, 8)
        norm_slot(k)
    for k in range(8, 16):
        wait_row(0, k)
        norm_slot(k)
    for k in (4, 5):
        wait_row(1, k)
        start_row(1, k, 8)

    up_in.wait()
    for s in even + odd:
        mlp_wait(0, s)

    @pl.loop(0, tokens // chunk)
    def _(j):
        at = pl.ds(pl.multiple_of(j * chunk, chunk), chunk)
        value = mm_tail(up_t[...], n2[at, :]) + up_bias
        pre[:, at] = value
        hid_t[:, at] = (value * gelu_half(value)).astype(BF16)

    for k in (6, 7):
        wait_row(1, k)
        start_row(1, k, 8)
    cot_in.wait()
    for k in range(8, 16):
        wait_row(1, k)
    sums[...] = jnp.zeros_like(sums)

    @pl.loop(0, rows // 16)
    def _(j):
        at = pl.ds(pl.multiple_of(j * 16, 16), 16)
        sums[4:5, :] += jnp.sum(cots[at, :].astype(F32), axis=0, keepdims=True)

    def g_send_copy(a, s):
        at = pl.ds(pl.multiple_of(s * depth, 128), depth)
        return remote(
            (gu_hbm, gd_hbm)[a].at[:, at], (ru_hbm, rd_hbm)[a].at[:, at],
            g_send.at[a, s], g_recv.at[a, s], s, 0,
        )

    def g_local_copy(a, s, b, dst):
        at = pl.ds(pl.multiple_of(s * depth, 128), depth)
        return pltpu.make_async_copy(ring.at[b], dst.at[:, at], g_local.at[b])

    def grads(a):
        left, right = ((act_t, n2), (hid_t, cots))[a]
        stage, own = ((gu_hbm, ru_hbm), (gd_hbm, rd_hbm))[a]

        def block(s, b):
            at = pl.ds(pl.multiple_of((d ^ s) * depth, 128), depth)
            ring[b] = mm(left[...], right[:, at]).astype(BF16)

        @pl.loop(0, dp_n - 1)
        def _(k):
            s = dp_n - 1 - k
            b = k % 3

            @pl.when(k >= 2)
            def _():
                g_local_copy(a, s + 2, (k + 1) % 3, stage).wait()
                g_send_copy(a, s + 2).start()

            block(s, b)
            g_local_copy(a, s, b, stage).start()

        last = dp_n - 2
        for k in (last - 1, last):
            s = dp_n - 1 - k
            g_local_copy(a, s, k % 3, stage).wait()
            g_send_copy(a, s).start()
        b = (last + 1) % 3
        block(0, b)
        copy = g_local_copy(a, 0, b, own)
        copy.start()
        copy.wait()

    grads(1)
    down_in.wait()
    for s in even + odd:
        mlp_wait(1, s)
    up_sum[...] = jnp.zeros_like(up_sum)

    @pl.loop(0, tokens // chunk)
    def _(j):
        at = pl.ds(pl.multiple_of(j * chunk, chunk), chunk)
        value = mm_tail(down_w[...], cots[at, :]) * gelu_slope(pre[:, at])
        up_sum[:, 0:1] += jnp.sum(value, axis=1, keepdims=True)
        act_t[:, at] = value.astype(BF16)

    grads(0)

    @pl.loop(0, tokens // 256)
    def _(j):
        at = pl.ds(pl.multiple_of(j * 256, 256), 256)
        act = jnp.transpose(act_t[:, at].astype(F32)).astype(BF16)
        mean, inv = stats[at, 0:1], stats[at, 64:65]

        @pl.loop(0, width // chunk)
        def _(c):
            lanes = pl.ds(pl.multiple_of(c * chunk, chunk), chunk)
            part = mm(act, up_t[:, lanes])
            normed = (xs[at, lanes].astype(F32) - mean) * inv
            sums[2:3, lanes] += jnp.sum(part * normed, axis=0, keepdims=True)
            sums[3:4, lanes] += jnp.sum(part, axis=0, keepdims=True)
            n2[at, lanes] = (part * vecs[2:3, lanes]).astype(BF16)

    def mine(dy, q):
        return ((q // 2) * 8 + (q % 2) * 4 + dy * 2 + core) * rows

    for dy in range(2):
        for q in range(4):
            @pl.loop(0, rows // 16)
            def _(j):
                at = pl.ds(pl.multiple_of(mine(dy, q) + j * 16, 16), 16)
                to = pl.ds(pl.multiple_of(dy * SEQ + q * rows + j * 16, 16), 16)
                normed = (xs[at, :].astype(F32) - stats[at, 0:1]) * stats[at, 64:65]
                n1[to, :] = (normed * vecs[0:1, :] + vecs[1:2, :]).astype(BF16)

    for copy in row_started[0] + mlp_started[0]:
        copy.wait_send()
    pl.semaphore_signal(credit.at[0], inc=1, device_id=(d, t ^ 1), device_id_type=MESH)
    pl.semaphore_signal(credit.at[1], inc=1, device_id=(d, t ^ 2), device_id_type=MESH)

    @pl.when(lead)
    def _():
        for a, (src, dst) in enumerate(att_pairs(0)):
            pltpu.make_async_copy(src, dst, local_sem.at[20 + a]).wait()
        for copy in pass_att(0):
            copy.start()
        for s in even + odd:
            for a, dst in enumerate(att_land(s)):
                remote(dst, dst, att_send.at[a, s], att_recv.at[a, s], s, 0).wait_recv()
            for copy in pass_att(s):
                copy.start()

    @pl.when(follow)
    def _():
        for s in range(dp_n):
            for copy in pass_att(s):
                copy.wait_recv()

    rope_in.wait()
    lanes128 = lax.broadcasted_iota(jnp.int32, (SEQ, 128), 1)

    def rope_tables(sign):
        at = [pl.ds(pl.multiple_of((t ^ ((q % 2) * 2 + q // 2)) * 128, 128), 128) for q in range(4)]
        cosine = jnp.concatenate([rope[0, a, :] for a in at], axis=0)
        sine = jnp.concatenate([rope[1, a, :] for a in at], axis=0) * sign
        lower = jnp.where(lanes128 < ROT // 2, -sine, 0.0)
        upper = jnp.where((lanes128 >= ROT // 2) & (lanes128 < ROT), sine, 0.0)
        return cosine, lower, upper

    def turn(value, tables):
        cosine, lower, upper = tables
        head = value[:, :128]
        head = (
            head * cosine
            + pltpu.roll(head, 128 - ROT // 2, 1) * lower
            + pltpu.roll(head, ROT // 2, 1) * upper
        )
        return jnp.concatenate([head, value[:, 128:]], axis=1)

    @pl.loop(0, 2)
    def _(dy):
        at = pl.ds(pl.multiple_of(dy * SEQ, SEQ), SEQ)
        tables = rope_tables(1.0)
        rows_in = n1[at, :]
        value = mm(rows_in, att_w[:, :HD]) + qkv_bias[0:1, :HD]
        query = turn(value, tables).astype(BF16)
        key = turn(mm(rows_in, att_w[:, HD : 2 * HD]), tables).astype(BF16)
        val = (mm(rows_in, att_w[:, 2 * HD :]) + qkv_bias[0:1, HD:]).astype(BF16)
        q_s[at, :] = query
        k_s[at, :] = key
        v_s[at, :] = val
        seg_q = jnp.where(dy == 0, queries[:, 1:2], queries[:, 2:3])
        seg_k = jnp.where(dy == 0, keys[1:2, :], keys[2:3, :])
        allowed = (keys[0:1, :] <= queries[:, 0:1]) & (seg_q == seg_k)
        scores = jnp.where(allowed, mm_tail(query, key) * scale, NEG_FILL)
        peak = jnp.max(scores, axis=-1, keepdims=True)
        total = jnp.where(allowed, jnp.exp(scores - peak), 0.0)
        share = (total / jnp.sum(total, axis=-1, keepdims=True)).astype(BF16)
        prob[at, :] = share
        got = mm(share, val)
        ctx[at, :] = got.astype(BF16)
        ctx_t[:, at] = jnp.transpose(got).astype(BF16)

    def cot_mine(dy, lanes):
        parts = [cots[pl.ds(pl.multiple_of(mine(dy, q), 128), rows), lanes] for q in range(4)]
        return jnp.concatenate(parts, axis=0)

    for dy in range(2):
        cctx[dy * SEQ : (dy + 1) * SEQ, :] = mm_tail(cot_mine(dy, slice(None)), proj_w[...]).astype(BF16)

    @pl.loop(0, width // chunk)
    def _(c):
        lanes = pl.ds(pl.multiple_of(c * chunk, chunk), chunk)
        both = jnp.concatenate([cot_mine(0, lanes), cot_mine(1, lanes)], axis=0)
        gx[3 * HD : 4 * HD, lanes] = mm(ctx_t[...], both).astype(BF16)

    for copy in row_started[1]:
        copy.wait_send()
    for dc in range(2):
        for dx in range(2):
            for dy in range(2):
                pair = dc * 4 + dx * 2 + dy
                spot = dy * SEQ + (dc * 2 + dx) * rows
                at = slice(pair * 256, pair * 256 + 256)
                hid = jnp.transpose(hid_t[:, at].astype(F32)).astype(BF16)

                @pl.loop(0, width // chunk)
                def _(c):
                    lanes = pl.ds(pl.multiple_of(c * chunk, chunk), chunk)
                    base = mm(hid, down_w[:, lanes])
                    extra = mm(ctx[spot : spot + rows, :], proj_w[:, lanes])
                    here = core == 0
                    first = base[:rows] + jnp.where(here, extra, 0.0)
                    other = base[rows:] + jnp.where(here, 0.0, extra)
                    cots[at, lanes] = jnp.concatenate([first, other], axis=0).astype(BF16)
    for bit in (2, 1):
        dp_xor, tp_xor = hop[bit]
        pl.semaphore_signal(
            credit.at[1 + (3 - bit)], inc=1, device_id=(d ^ dp_xor, t ^ tp_xor), device_id_type=MESH
        )
    own_x = row_cut(hid_t, 3 * rows, rows)
    own_cot = row_cut(down_w, 3 * rows, rows)
    x_again = stay(x_ref, own_x)
    cot_again = stay(cot_ref, own_cot)

    bufs = (cots, n2)

    def landing(a, bit, j, there):
        if bit == 8:
            if a == 0:
                side = core if there else 1 - core
                return row_cut(xs, (2 * j + side) * rows, rows)
            return row_cut(n1, j * rows, rows)
        if bit == 4:
            return row_cut((act_t, up_t)[a], j * rows, rows)
        base = (down_w, hid_t)[a]
        return row_cut(base, (j if bit == 2 else 2) * rows, rows)

    def rs_copy(a, bit, j):
        return remote(
            slot(bufs[a], bit + j), landing(a, bit, j, True),
            rs_send.at[a, bit + j], rs_recv.at[a, bit + j], *hop[bit],
        )

    def rs_start(a, bit, j):
        start(rs_copy(a, bit, j))

    def rs_add(a, bit, j):
        land = landing(a, bit, j, False)
        remote(land, land, rs_send.at[a, bit + j], rs_recv.at[a, bit + j], *hop[bit]).wait_recv()
        here = slot(bufs[a], j)

        @pl.loop(0, rows // 16)
        def _(i):
            at = pl.ds(pl.multiple_of(i * 16, 16), 16)
            here[at, :] = (here[at, :].astype(F32) + land[at, :].astype(F32)).astype(BF16)

    pl.semaphore_wait(credit.at[0], 1)
    for j in (7, 5, 6, 4, 3, 1, 2, 0):
        rs_start(0, 8, j)

    qkv_sum[...] = jnp.zeros_like(qkv_sum)

    def backward(dy):
        at = slice(dy * SEQ, (dy + 1) * SEQ)
        tables = rope_tables(-1.0)
        share = prob[at, :].astype(F32)
        got = cctx[at, :]
        delta = jnp.sum(got.astype(F32) * ctx[at, :].astype(F32), axis=-1, keepdims=True)
        score_cot = share * (mm_tail(got, v_s[at, :]) - delta)
        value_cot = mm(jnp.transpose(share).astype(BF16), got)
        query_cot = turn(mm(score_cot.astype(BF16), k_s[at, :]) * scale, tables)
        key_cot = turn(mm(jnp.transpose(score_cot).astype(BF16), q_s[at, :]) * scale, tables)
        qkv_sum[0:1, :HD] += jnp.sum(query_cot, axis=0, keepdims=True)
        qkv_sum[0:1, HD:] += jnp.sum(value_cot, axis=0, keepdims=True)
        for k, part in enumerate((query_cot, key_cot, value_cot)):
            low[at, k * HD : (k + 1) * HD] = part.astype(BF16)
            low_t[k * HD : (k + 1) * HD, at] = jnp.transpose(part).astype(BF16)

    backward(0)
    pl.semaphore_wait(credit.at[1], 1)
    for j in (7, 5, 6, 4):
        rs_add(0, 8, j)
        rs_start(0, 4, j - 4)
    for j in (3, 1, 2, 0):
        rs_add(0, 8, j)

    @pl.when(lead)
    def _():
        pl.semaphore_signal(credit.at[4], inc=1, device_id=(d, t ^ 1), device_id_type=MESH)

    backward(1)

    @pl.loop(0, width // chunk)
    def _(c):
        lanes = pl.ds(pl.multiple_of(c * chunk, chunk), chunk)
        gx[0 : 3 * HD, lanes] = mm(low_t[...], n1[:, lanes]).astype(BF16)

    pl.semaphore_signal(credit.at[5], inc=1, device_id=(d, t ^ 1), device_id_type=MESH)

    def pair_copy(j):
        return remote(
            row_cut(gx, j * rows, rows), row_cut(xs, (2 * j + core) * rows, rows),
            pair_send.at[j], pair_recv.at[j], 0, 1,
        )

    @pl.when(follow)
    def _():
        pl.semaphore_wait(credit.at[4], 1)
        for j in range(8):
            pair_copy(j).start()

    for dy in range(2):
        for q in range(4):
            at = pl.ds(pl.multiple_of(mine(dy, q), 128), rows)
            piece = low[dy * SEQ + q * rows : dy * SEQ + (q + 1) * rows, :]

            @pl.loop(0, width // chunk)
            def _(c):
                lanes = pl.ds(pl.multiple_of(c * chunk, chunk), chunk)
                part = mm_tail(piece, att_w[lanes, :])
                normed = (xs[at, lanes].astype(F32) - stats[at, 0:1]) * stats[at, 64:65]
                sums[0:1, lanes] += jnp.sum(part * normed, axis=0, keepdims=True)
                sums[1:2, lanes] += jnp.sum(part, axis=0, keepdims=True)
                n2[at, lanes] = (n2[at, lanes].astype(F32) + part * vecs[0:1, lanes]).astype(BF16)

    pl.semaphore_wait(credit.at[5], 1)
    for j in (7, 5, 6, 4, 3, 1, 2, 0):
        rs_start(1, 8, j)

    def ga_copy(s):
        return remote(
            lane_cut(gx, (d ^ s) * depth, depth), ra_hbm.at[:, s * depth : (s + 1) * depth],
            ga_send.at[s], ga_recv.at[s], s, 0,
        )

    @pl.when(lead)
    def _():
        for j in range(8):
            land = row_cut(xs, (2 * j + 1 - core) * rows, rows)
            remote(land, land, pair_send.at[j], pair_recv.at[j], 0, 1).wait_recv()

            @pl.loop(0, rows // 16)
            def _(i):
                at = pl.ds(pl.multiple_of(j * rows + i * 16, 16), 16)
                there = pl.ds(pl.multiple_of(i * 16, 16), 16)
                gx[at, :] = (gx[at, :].astype(F32) + land[there, :].astype(F32)).astype(BF16)

        for s in even + odd:
            ga_copy(s).start()
        pltpu.make_async_copy(
            lane_cut(gx, d * depth, depth), ra_hbm.at[:, 0:depth], local_sem.at[22]
        ).start()

    for copy in small_copies:
        copy.wait_send()
    small[...] = jnp.zeros_like(small)
    for a in range(devices):
        owner = flat ^ a
        small[a, 0] = sums[:, pl.ds(pl.multiple_of((owner // 2) * 128, 128), 128)]
    blank = jnp.zeros((4, 128), F32)
    up_rows = [jnp.transpose(up_sum[k * 128 : (k + 1) * 128, :])[0:1] for k in range(4)]
    up_rows = jnp.concatenate(up_rows, axis=0)
    qkv_rows = jnp.concatenate([qkv_sum[0:1, k * 128 : (k + 1) * 128] for k in range(4)], axis=0)

    def place(value):
        return jnp.where(
            second, jnp.concatenate([blank, value], axis=0), jnp.concatenate([value, blank], axis=0)
        )

    up_rows, qkv_rows = place(up_rows), place(qkv_rows)
    for s in range(dp_n):
        small[s * tp_n, 1 + inner // 2] = up_rows
        small[s * tp_n + head_rel, 3] = qkv_rows
    back = []
    for k, (dp_xor, tp_xor, n) in enumerate(reversed(hops)):
        back.append(
            remote(
                small.at[pl.ds(n, n)], small_in.at[pl.ds(n, n)],
                back_send.at[k], back_recv.at[k], dp_xor, tp_xor,
            )
        )

    def back_step(k):
        n = hops[len(hops) - 1 - k][2]
        back[k].wait_recv()
        for a in range(n):
            small[a] = small[a] + small_in[n + a]
        if k + 1 < len(back):
            back[k + 1].start()

    back[0].start()
    for j in (7, 5, 6, 4):
        rs_add(1, 8, j)
        rs_start(1, 4, j - 4)
    back_step(0)
    for j in (3, 1, 2, 0):
        rs_add(1, 8, j)
    back_step(1)

    pl.semaphore_wait(credit.at[2], 1)
    pl.semaphore_wait(credit.at[3], 1)

    def rs_tail(a, between):
        rs_add(a, 4, 3)
        rs_start(a, 2, 1)
        between(0)
        rs_add(a, 4, 1)
        between(1)
        rs_add(a, 4, 2)
        rs_start(a, 2, 0)
        rs_add(a, 2, 1)
        rs_start(a, 1, 0)
        between(2)
        rs_add(a, 4, 0)
        rs_add(a, 2, 0)
        rs_add(a, 1, 0)

    outs = []

    def leave(src, dst):
        copy = pltpu.make_async_copy(src, dst, out_sem.at[len(outs)])
        copy.start()
        outs.append(copy)
        return copy

    rs_tail(0, lambda k: back_step(2 + k))
    x_again.wait()

    @pl.loop(0, rows // 16)
    def _(j):
        at = pl.ds(pl.multiple_of(j * 16, 16), 16)
        total = own_x[at, :].astype(F32) + cots[at, :].astype(F32) + vecs[4:5, :]
        cots[at, :] = total.astype(BF16)

    leave(slot(cots, 0), block_out)
    leave(small.at[0], tail_out)

    for a in (1, 0):
        for s in range(1, dp_n):
            g_send_copy(a, s).wait_recv()
    up_back = stay(ru_hbm, xs.at[0:hidden, :])
    down_back = stay(rd_hbm, xs.at[hidden : 2 * hidden, :])
    up_back.wait()
    down_back.wait()

    def total_of(base, k):
        total = xs[base : base + hidden, k * depth : (k + 1) * depth].astype(F32)
        for s in range(k + INNER, dp_n, INNER):
            total = total + xs[base : base + hidden, s * depth : (s + 1) * depth].astype(F32)
        return total

    waits = []
    for k in range(INNER):
        pre[0:depth, k * hidden : (k + 1) * hidden] = jnp.transpose(total_of(0, k))
        waits.append(
            leave(pre.at[0:depth, k * hidden : (k + 1) * hidden],
                  lane_cut(up_out, (inner ^ k) * hidden, hidden))
        )
    for copy in waits:
        copy.wait()
    waits = []
    for k in range(INNER):
        pre[0:hidden, k * depth : (k + 1) * depth] = total_of(hidden, k)
        waits.append(
            leave(pre.at[0:hidden, k * depth : (k + 1) * depth],
                  row_cut(down_out, (inner ^ k) * hidden, hidden))
        )
    for copy in waits:
        copy.wait()

    rs_tail(1, lambda k: None)
    cot_again.wait()

    @pl.loop(0, rows // 16)
    def _(j):
        at = pl.ds(pl.multiple_of(j * 16, 16), 16)
        scaled = n2[at, :].astype(F32)
        inv = stats[at, 64:65]
        normed = (own_x[at, :].astype(F32) - stats[at, 0:1]) * inv
        inner_mean = jnp.mean(scaled, axis=-1, keepdims=True)
        cross = jnp.mean(scaled * normed, axis=-1, keepdims=True)
        pre[at, :] = own_cot[at, :].astype(F32) + inv * (scaled - inner_mean - normed * cross)

    grad_out = leave(pre.at[0:rows, :], input_out)

    @pl.when(lead)
    def _():
        pltpu.make_async_copy(
            lane_cut(gx, d * depth, depth), ra_hbm.at[:, 0:depth], local_sem.at[22]
        ).wait()

    for s in range(1, dp_n):
        @pl.when(att_active(s))
        def _():
            ga_copy(s).wait_recv()

    base = 2 * hidden
    picks = []
    for hl in range(2):
        first = ((inner // 2) ^ core) * 2 + ((inner % 2) ^ hl)
        for o in range(dp_n // INNER):
            picks.append(
                stay(lane_cut(ra_hbm, (first + o * INNER) * depth, depth),
                     xs.at[base : base + 4 * HD, len(picks) * depth : (len(picks) + 1) * depth])
            )
    for copy in picks:
        copy.wait()
    grad_out.wait()
    groups = dp_n // INNER
    for hl in range(2):
        total = jnp.zeros((4 * HD, depth), F32)
        for o in range(groups):
            k = hl * groups + o
            total = total + xs[base : base + 4 * HD, k * depth : (k + 1) * depth].astype(F32)
        pre[0:depth, hl * 3 * HD : (hl + 1) * 3 * HD] = jnp.transpose(total[: 3 * HD])
        leave(pre.at[0:depth, hl * 3 * HD : (hl + 1) * 3 * HD], qkv_out.at[:, hl * 3 * HD : (hl + 1) * 3 * HD])
        pre[depth : depth + HD, hl * depth : (hl + 1) * depth] = total[3 * HD :]
        leave(pre.at[depth : depth + HD, hl * depth : (hl + 1) * depth], proj_out.at[hl * HD : (hl + 1) * HD, :])

    for s in range(1, dp_n):
        for a in range(2):
            g_send_copy(a, s).wait_send()

        @pl.when(att_active(s))
        def _():
            for a, (src, dst) in enumerate(att_pairs(s)):
                remote(src, dst, att_send.at[a, s], att_recv.at[a, s], s, 0).wait_send()

        @pl.when(lead)
        def _():
            ga_copy(s).wait_send()

    @pl.when(lead)
    def _():
        for s in range(dp_n):
            for copy in pass_att(s):
                copy.wait_send()

    @pl.when(follow)
    def _():
        for j in range(8):
            pair_copy(j).wait_send()

    for copy in started + mlp_started[1] + back:
        copy.wait_send()
    outs[0].wait()
    outs[1].wait()
    for copy in outs[3 + 2 * INNER :]:
        copy.wait()


def solution(mesh):
    dp_n, tp_n = mesh.shape["dp"], mesh.shape["tp"]
    outer = dp_n // INNER
    devices = dp_n * tp_n

    def send(value, dp_xor, tp_xor, keep=None):
        pairs = []
        for d in range(dp_n):
            for t in range(tp_n):
                if keep is None or keep(d, t):
                    pairs.append((d * tp_n + t, (d ^ dp_xor) * tp_n + (t ^ tp_xor)))
        return lax.ppermute(value, AXES, pairs)

    def scatter_small(value, flat):
        held = value
        step = devices // 2
        while step >= 1:
            dp_xor, tp_xor = step // tp_n, step % tp_n
            high = (flat // step) % 2 == 1
            first, second = held[:step], held[step:]
            other = send(jnp.where(high, first, second), dp_xor, tp_xor)
            held = jnp.where(high, second, first) + other
            step //= 2
        return held[0]

    def scatter_rows(value):
        for dp_xor, tp_xor in ((0, 1), (0, 2), (1, 0), (2, 0)):
            half = value.shape[0] // 2
            other = send(value[half:], dp_xor, tp_xor)
            value = value[:half].astype(F32) + other.astype(F32)
            if half > value.shape[0] or (dp_xor, tp_xor) != (2, 0):
                value = value.astype(BF16)
        return value

    def on_device(
        block_input, segment_ids, w_qkv, b_qkv, w_out, b_out, w_fc1, b_fc1, w_fc2, b_fc2,
        ln1_gain, ln1_bias, ln2_gain, ln2_bias, cotangent,
    ):
        d = lax.axis_index("dp")
        t = lax.axis_index("tp")
        flat = d * tp_n + t
        inner = d % INNER
        core = t % 2
        lead = (inner // 2) == core
        rows, width = block_input.shape
        depth = w_qkv.shape[0]
        hidden_here = w_fc1.shape[1] // INNER
        head_here = w_out.shape[0] // HD
        heads = head_here * tp_n
        quarter = SEQ // tp_n
        qkv_bits = b_qkv.shape[1]

        vec = jnp.stack([ln1_gain, ln1_bias, ln2_gain, ln2_bias, b_out + b_fc2]).reshape(-1)
        seg_part = lax.dynamic_slice(segment_ids.reshape(-1), (t * quarter,), (quarter,))
        sizes = [vec.size, b_qkv.size, b_fc1.size, quarter]
        payload = jnp.concatenate(
            [vec, b_qkv.reshape(-1), b_fc1.reshape(-1), seg_part.astype(F32)]
        )
        depth_wide = depth % 128 == 0
        flat_shape = lambda lead_n: (lead_n, width) if depth_wide else (dp_n, lead_n, depth)
        spread = lambda v: v if depth_wide else v.transpose(1, 0, 2).reshape(v.shape[1], width)
        payload = jnp.pad(payload, (0, PAY - payload.size)).reshape(8, PAY // 8)
        like = lambda *shape: jax.ShapeDtypeStruct(shape, BF16)
        dma = pltpu.SemaphoreType.DMA
        hop_count = (devices - 1).bit_length()
        any_spec = pl.BlockSpec(memory_space=pl.ANY)
        x_all, cot_all, up_w, down_w, qkv_w, out_w, small = pl.pallas_call(
            functools.partial(gather_kernel, dp_n, tp_n, depth_wide),
            out_shape=(
                like(16, rows, width),
                like(16, rows, width),
                like(width, hidden_here),
                like(*flat_shape(hidden_here)),
                like(width, 3 * HD),
                like(*flat_shape(HD)),
                jax.ShapeDtypeStruct((devices, 8, PAY // 8), F32),
            ),
            in_specs=[any_spec] * 7,
            out_specs=(any_spec,) * 7,
            scratch_shapes=[
                dma((2, 16)), dma((2, 16)), dma((2, dp_n)), dma((2, dp_n)),
                dma((2, dp_n)), dma((2, dp_n)), dma((2, dp_n)), dma((2, dp_n)),
                dma((hop_count,)), dma((hop_count,)), dma((6,)),
            ],
            compiler_params=pltpu.CompilerParams(collective_id=0, has_side_effects=True),
            name="gather_phase",
        )(block_input, cotangent, w_fc1, w_fc2, w_qkv, w_out, payload)
        down_w, out_w = spread(down_w), spread(out_w)
        small = jnp.take(small.reshape(devices, PAY), flat ^ jnp.arange(devices), axis=0)
        cuts = [0]
        for size in sizes:
            cuts.append(cuts[-1] + size)
        vecs = small[:, : cuts[1]].reshape(devices, 5, -1).transpose(1, 0, 2).reshape(5, width)
        gain_one, shift_one, gain_two, shift_two, out_bias = (vecs[k][None] for k in range(5))
        qkv_bias_all = (
            small[:, cuts[1] : cuts[2]]
            .reshape(dp_n, tp_n, head_here, qkv_bits)
            .transpose(1, 2, 0, 3)
            .reshape(heads, 2 * HD)
        )
        head = (t // 2) * INNER + inner
        qkv_bias = lax.dynamic_slice(qkv_bias_all, (head, 0), (1, 2 * HD))
        up_rows, up_cols = b_fc1.shape
        up_bias_all = (
            small[:, cuts[2] : cuts[3]]
            .reshape(dp_n, tp_n, up_rows, up_cols)
            .transpose(1, 2, 0, 3)
            .reshape(tp_n * INNER, hidden_here)
        )
        up_bias = lax.dynamic_slice(up_bias_all, (t * INNER + inner, 0), (1, hidden_here))
        seg_all = small[:, cuts[3] : cuts[4]].reshape(dp_n, tp_n, quarter)

        x_rows = x_all.reshape(16 * rows, width).astype(F32)
        cot_rows = cot_all.reshape(16 * rows, width)
        row_mean = jnp.mean(x_rows, axis=-1, keepdims=True)
        centered = x_rows - row_mean
        row_var = jnp.mean(centered * centered, axis=-1, keepdims=True)
        inv_std = lax.rsqrt(row_var + EPS)
        normed = centered * inv_std
        norm_two = (normed * gain_two + shift_two).astype(BF16)

        def mine(value):
            split = value.reshape((2, 2, 2, 2, rows) + value.shape[1:])
            cut = lax.dynamic_index_in_dim(split, core, 3, keepdims=False)
            return jnp.moveaxis(cut, 2, 0).reshape((2 * SEQ,) + value.shape[1:])

        def unmine(value):
            split = value.reshape((2, 2, 2, rows) + value.shape[1:])
            cut = jnp.moveaxis(split, 0, 2)[:, :, :, None]
            where = (jnp.arange(2) == core).reshape((1, 1, 1, 2) + (1,) * value.ndim)
            full = jnp.where(where, cut, jnp.zeros_like(cut))
            return full.reshape((16 * rows,) + value.shape[1:])

        norm_one = (mine(normed) * gain_one + shift_one).astype(BF16)
        cot_mine = mine(cot_rows)

        pre_act = mm(norm_two, up_w) + up_bias
        half_gelu = gelu_half(pre_act)
        hidden = (pre_act * half_gelu).astype(BF16)
        down_grad = mm_lead(hidden, cot_rows)
        act_cot = mm_tail(cot_rows, down_w) * gelu_slope(pre_act)
        up_bias_part = jnp.sum(act_cot, axis=0)
        act_low = act_cot.astype(BF16)
        up_grad = mm_lead(norm_two, act_low)
        up_grad, down_grad = up_grad.astype(BF16), down_grad.astype(BF16)

        def cut_block(value, s):
            return lax.dynamic_slice(value, ((d ^ s) * depth, 0), (depth, value.shape[1]))

        def cut_across(value, s):
            return lax.dynamic_slice(value, (0, (d ^ s) * depth), (value.shape[0], depth))

        with jax.named_scope("mlp_out"):
            up_back = [cut_block(up_grad, 0)] + [
                send(cut_block(up_grad, s), s, 0) for s in range(1, dp_n)
            ]
            down_back = [cut_across(down_grad, 0)] + [
                send(cut_across(down_grad, s), s, 0) for s in range(1, dp_n)
            ]

        order = jnp.stack([t ^ ((k % 2) * 2 + k // 2) for k in range(4)])
        position = (order[:, None] * quarter + jnp.arange(quarter)[None]).reshape(-1)
        inverse = jnp.exp(jnp.arange(ROT // 2, dtype=F32) * (-2.0 * math.log(10000.0) / ROT))
        angle = position.astype(F32)[:, None] * inverse[None]
        cosine, sine = jnp.cos(angle)[None], jnp.sin(angle)[None]
        segs = []
        for dy in range(2):
            seq = (d // INNER) * INNER + (inner ^ (core * 2 + dy))
            rows_of = lax.dynamic_index_in_dim(seg_all, seq, 0, keepdims=False)
            segs.append(jnp.take(rows_of, order, axis=0).reshape(-1))
        segs = jnp.stack(segs)
        allowed = (position[None, :] <= position[:, None])[None] & (
            segs[:, :, None] == segs[:, None, :]
        )
        qkv = mm(norm_one, qkv_w)
        query = rotate((qkv[:, :HD] + qkv_bias[:, :HD]).reshape(2, SEQ, HD), cosine, sine).astype(BF16)
        key = rotate(qkv[:, HD : 2 * HD].reshape(2, SEQ, HD), cosine, sine).astype(BF16)
        val = (qkv[:, 2 * HD :] + qkv_bias[:, HD:]).astype(BF16).reshape(2, SEQ, HD)
        scale = HD ** (-0.5)

        def ein(eq, left, right):
            return jnp.einsum(eq, left, right, preferred_element_type=F32)

        masked = jnp.where(allowed, ein("sqd,skd->sqk", query, key) * scale, NEG_FILL)
        peak = jnp.max(masked, axis=-1, keepdims=True)
        log_total = peak + jnp.log(
            jnp.sum(jnp.where(allowed, jnp.exp(masked - peak), 0.0), axis=-1, keepdims=True)
        )
        prob_full = jnp.where(allowed, jnp.exp(masked - log_total), 0.0)
        prob_low = prob_full.astype(BF16)
        context = ein("sqk,skd->sqd", prob_low, val).astype(BF16)
        context_cot = mm_tail(cot_mine, out_w).astype(BF16).reshape(2, SEQ, HD)
        prob_cot = ein("sqd,skd->sqk", context_cot, val)
        row_delta = jnp.sum(context_cot.astype(F32) * context.astype(F32), axis=-1, keepdims=True)
        score_cot = (prob_full * (prob_cot - row_delta)).astype(BF16)
        query_cot = rotate(ein("sqk,skd->sqd", score_cot, key) * scale, cosine, -sine)
        key_cot = rotate(ein("sqk,sqd->skd", score_cot, query) * scale, cosine, -sine)
        val_cot = ein("sqk,sqd->skd", prob_low, context_cot)
        qkv_cot = jnp.concatenate([query_cot, key_cot, val_cot], axis=-1).reshape(2 * SEQ, 3 * HD)
        qkv_bias_part = jnp.concatenate(
            [jnp.sum(query_cot, axis=(0, 1)), jnp.sum(val_cot, axis=(0, 1))]
        )
        qkv_low = qkv_cot.astype(BF16)
        context_flat = context.reshape(2 * SEQ, HD)
        att_grad = jnp.concatenate(
            [mm_lead(norm_one, qkv_low).astype(BF16), mm_lead(cot_mine, context_flat).astype(BF16)],
            axis=1,
        )
        att_pair = send(att_grad, 0, 1, lambda dd, tt: (dd % INNER) // 2 != tt % 2)
        att_grad = (att_grad.astype(F32) + att_pair.astype(F32)).astype(BF16)
        with jax.named_scope("att_out"):
            own_att = cut_block(att_grad, 0)
            att_back = [jnp.where(lead, own_att, jnp.zeros_like(own_att))] + [
                send(cut_block(att_grad, s), s, 0, lambda dd, tt: (dd % INNER) // 2 == tt % 2)
                for s in range(1, dp_n)
            ]

        left = jnp.concatenate([hidden, unmine(context_flat)], axis=1)
        right = jnp.concatenate([down_w, out_w], axis=0)
        with jax.named_scope("branch"):
            branch = scatter_rows(mm(left, right).astype(BF16))
        block_output = (block_input.astype(F32) + branch + out_bias).astype(BF16)

        one_part = mm_tail(qkv_low, qkv_w)
        two_part = mm_tail(act_low, up_w)
        vec_terms = jnp.stack(
            [
                jnp.sum(one_part * mine(normed), axis=0),
                jnp.sum(one_part, axis=0),
                jnp.sum(two_part * normed, axis=0),
                jnp.sum(two_part, axis=0),
                jnp.sum(cotangent.astype(F32), axis=0),
            ]
        )
        scaled_part = (two_part * gain_two + unmine(one_part * gain_one)).astype(BF16)
        with jax.named_scope("normback"):
            scaled = scatter_rows(scaled_part)
        normed_own = normed[:rows]
        input_grad = cotangent.astype(F32) + inv_std[:rows] * (
            scaled
            - jnp.mean(scaled, axis=-1, keepdims=True)
            - normed_own * jnp.mean(scaled * normed_own, axis=-1, keepdims=True)
        )

        head_hot = (jnp.arange(heads) == head).astype(F32)[:, None]
        qkv_small = (
            (head_hot * qkv_bias_part[None])
            .reshape(tp_n, head_here, dp_n, qkv_bits)
            .transpose(2, 0, 1, 3)
            .reshape(devices, -1)
        )
        up_hot = (jnp.arange(tp_n * INNER) == t * INNER + inner).astype(F32)[:, None]
        up_small = (
            (up_hot * up_bias_part[None])
            .reshape(tp_n, up_rows, dp_n, up_cols)
            .transpose(2, 0, 1, 3)
            .reshape(devices, -1)
        )
        vec_small = vec_terms.reshape(5, devices, -1).transpose(1, 0, 2).reshape(devices, -1)
        with jax.named_scope("small_out"):
            own = scatter_small(jnp.concatenate([vec_small, qkv_small, up_small], axis=1), flat)
        vec_own = own[: cuts[1]].reshape(5, -1)
        qkv_bias_grad = own[cuts[1] : cuts[2]].reshape(b_qkv.shape)
        up_bias_grad = own[cuts[2] : cuts[3]].reshape(b_fc1.shape)

        up_total = jnp.zeros(w_fc1.shape, F32)
        down_total = jnp.zeros(w_fc2.shape, F32)
        for k in range(INNER):
            at = (inner ^ k) * hidden_here
            up_sum = sum(up_back[s].astype(F32) for s in range(k, dp_n, INNER))
            down_sum = sum(down_back[s].astype(F32) for s in range(k, dp_n, INNER))
            up_total = lax.dynamic_update_slice(up_total, up_sum, (0, at))
            down_total = lax.dynamic_update_slice(down_total, down_sum, (at, 0))
        att_sum = [sum(att_back[s].astype(F32) for s in range(k, dp_n, 2)) for k in range(2)]
        odd = inner % 2 == 1
        att_first = jnp.where(odd, att_sum[1], att_sum[0])
        att_second = jnp.where(odd, att_sum[0], att_sum[1])
        qkv_total = jnp.concatenate([att_first[:, : 3 * HD], att_second[:, : 3 * HD]], axis=1)
        out_total = jnp.concatenate([att_first[:, 3 * HD :].T, att_second[:, 3 * HD :].T], axis=0)
        return (
            block_output, input_grad, qkv_total, qkv_bias_grad, out_total, vec_own[4],
            up_total, up_bias_grad, down_total, vec_own[4],
            vec_own[0], vec_own[1], vec_own[2], vec_own[3],
        )

    def on_device_fused(
        block_input, segment_ids, w_qkv, b_qkv, w_out, b_out, w_fc1, b_fc1, w_fc2, b_fc2,
        ln1_gain, ln1_bias, ln2_gain, ln2_bias, cotangent,
    ):
        d = lax.axis_index("dp")
        t = lax.axis_index("tp")
        flat = d * tp_n + t
        inner = d % INNER
        core = t % 2
        lead = (inner // 2) == core
        rows, width = block_input.shape
        depth = w_qkv.shape[0]
        hidden_here = w_fc1.shape[1] // INNER
        head_here = w_out.shape[0] // HD
        heads = head_here * tp_n
        quarter = SEQ // tp_n
        qkv_bits = b_qkv.shape[1]

        up_rows, up_cols = b_fc1.shape
        per = up_rows // INNER
        seg_part = lax.dynamic_slice(segment_ids.reshape(-1), (t * quarter,), (quarter,))
        two = lambda v: jnp.concatenate([v, v])
        vec_rows = [two(v) for v in (ln1_gain, ln1_bias, ln2_gain, ln2_bias, b_out + b_fc2)]
        spot = (jnp.arange(dp_n) == d).astype(F32)
        up_spread = (b_fc1.reshape(INNER, per, 1, up_cols) * spot[None, None, :, None]).reshape(2, 8, 128)
        qkv_spread = (b_qkv[:, None, :] * spot[None, :, None]).reshape(1, 8, 128)
        first = jnp.stack(vec_rows + [seg_part.astype(F32), jnp.zeros(128, F32), jnp.zeros(128, F32)])
        payload = jnp.concatenate([first[None], up_spread, qkv_spread])
        angle = np.arange(SEQ)[:, None] * np.exp(np.arange(ROT // 2) * (-2.0 * math.log(10000.0) / ROT))
        pad = np.zeros((SEQ, 128 - ROT))
        cosine = np.concatenate([np.cos(angle), np.cos(angle), pad + 1.0], axis=1)
        sine = np.concatenate([np.sin(angle), np.sin(angle), pad], axis=1)
        rope = jnp.asarray(np.stack([cosine, sine]), F32)
        like = lambda *shape: jax.ShapeDtypeStruct(shape, BF16)
        wide_f = lambda *shape: jax.ShapeDtypeStruct(shape, F32)
        dma = pltpu.SemaphoreType.DMA
        vb = lambda *shape: pltpu.VMEM(shape, BF16)
        vf = lambda *shape: pltpu.VMEM(shape, F32)
        hop_count = (devices - 1).bit_length()
        any_spec = pl.BlockSpec(memory_space=pl.ANY)
        group = 16 * rows
        per_peer = dma((2, dp_n))
        pair = 2 * SEQ
        results = pl.pallas_call(
            functools.partial(fused_kernel, dp_n, tp_n),
            out_shape=(
                like(rows, width), wide_f(rows, width), wide_f(*w_fc1.shape), wide_f(*w_fc2.shape),
                wide_f(*w_qkv.shape), wide_f(*w_out.shape), wide_f(4, 8, 128),
                like(hidden_here, width), like(hidden_here, width),
                like(hidden_here, width), like(hidden_here, width), like(4 * HD, width),
            ),
            in_specs=[any_spec] * 8,
            out_specs=(any_spec,) * 12,
            scratch_shapes=[
                vb(group, width), vb(group, width), vb(group, width),
                vb(hidden_here, width), vb(hidden_here, width), vf(hidden_here, group),
                vb(hidden_here, group), vb(hidden_here, group), vb(3, hidden_here, depth),
                vf(group, 128), vf(8, width), vf(8, width), vf(hidden_here, 128),
                vb(width, 3 * HD), vb(HD, width), vb(pair, width),
                vb(pair, HD), vb(pair, HD), vb(pair, HD), vb(pair, SEQ),
                vb(pair, HD), vb(HD, pair), vb(pair, HD), vb(pair, 3 * HD), vb(3 * HD, pair),
                vb(4 * HD, width), vf(2, SEQ, 128), vf(devices, 4, 8, 128), vf(devices, 4, 8, 128),
                vf(8, SEQ), vf(SEQ, 128), vf(8, 2 * HD), vf(8, 2 * HD),
                dma((2, 16)), dma((2, 16)), per_peer, per_peer, per_peer, per_peer, per_peer, per_peer,
                dma((hop_count,)), dma((hop_count,)), dma((hop_count,)), dma((hop_count,)),
                per_peer, per_peer, dma((3,)),
                dma((2, 16)), dma((2, 16)), dma((8,)), dma((8,)), dma((dp_n,)), dma((dp_n,)),
                dma((24,)), dma((24,)), pltpu.SemaphoreType.REGULAR((6,)),
            ],
            compiler_params=pltpu.CompilerParams(
                collective_id=0, has_side_effects=True, vmem_limit_bytes=67_000_000
            ),
            name="fused_block",
        )(block_input, cotangent, w_fc1, w_fc2, w_qkv, w_out, payload, rope)
        block_output, input_grad, up_total, down_total, qkv_total, out_total, tail = results[:7]
        vec_own = lax.dynamic_slice(tail[0, :5], (0, (flat % 2) * 64), (5, 64))
        up_bias_grad = lax.dynamic_slice(
            tail[1:3].reshape(up_rows, -1), (0, d * up_cols), (up_rows, up_cols)
        )
        qkv_bias_grad = lax.dynamic_slice(
            tail[3].reshape(head_here, -1), (0, d * qkv_bits), (head_here, qkv_bits)
        )
        return (
            block_output, input_grad, qkv_total, qkv_bias_grad, out_total, vec_own[4],
            up_total, up_bias_grad, down_total, vec_own[4],
            vec_own[0], vec_own[1], vec_own[2], vec_own[3],
        )

    row, vec = P(AXES, None), P(AXES)
    col, low = P("dp", "tp"), P("tp", "dp")
    def choose(*arrays):
        wide = arrays[2].shape[0] % 128 == 0
        return (on_device_fused if wide else on_device)(*arrays)

    return jax.shard_map(
        choose,
        mesh=mesh,
        in_specs=(row, P("dp", None), col, low, low, vec, col, low, low, vec, vec, vec, vec, vec, row),
        out_specs=(row, row, col, low, low, vec, col, low, low, vec, vec, vec, vec, vec),
        check_vma=False,
    )
```

```python
import functools
import math

import jax
import jax.numpy as jnp
import numpy as np
from jax import lax
from jax.experimental import pallas as pl
from jax.experimental.pallas import tpu as pltpu
from jax.sharding import PartitionSpec as P

HD = 256
ROT = 64
SEQ = 512
INNER = 4
EPS = 1e-05
NEG_FILL = -1e30
F32 = jnp.float32
BF16 = jnp.bfloat16
AXES = ("dp", "tp")
MESH = pl.DeviceIdType.MESH
PAY = 1024


def dot(left, right, contract):
    return lax.dot_general(left, right, (contract, ((), ())), preferred_element_type=F32)


def mm(left, right):
    return dot(left, right, ((1,), (0,)))


def mm_tail(left, right):
    return dot(left, right, ((1,), (1,)))


def mm_lead(left, right):
    return dot(left, right, ((0,), (0,)))


def gelu_half(pre_act):
    return 0.5 * (1.0 + jax.scipy.special.erf(pre_act * 2.0 ** (-0.5)))


def gelu_slope(pre_act):
    return gelu_half(pre_act) + pre_act * jnp.exp(-0.5 * pre_act * pre_act) * (2.0 * math.pi) ** (-0.5)


def rotate(block, cosine, sine):
    half = ROT // 2
    lower, upper = block[..., :half], block[..., half:ROT]
    return jnp.concatenate(
        [lower * cosine - upper * sine, upper * cosine + lower * sine, block[..., ROT:]], axis=-1
    )


def gather_kernel(
    dp_n, tp_n, wide,
    x_ref, cot_ref, fc1_ref, fc2_ref, qkv_ref, out_ref, pay_ref,
    xs_ref, cots_ref, up_ref, down_ref, att_ref, proj_ref, small_ref,
    row_send, row_recv, mlp_send, mlp_recv, att_send, att_recv, pass_send, pass_recv,
    small_send, small_recv, local_sem,
):
    d = lax.axis_index("dp")
    t = lax.axis_index("tp")
    inner = d % INNER
    core = t % 2
    depth = fc1_ref.shape[0]
    hidden = fc1_ref.shape[1] // INNER

    barrier = pltpu.get_barrier_semaphore()
    for s in range(1, dp_n):
        pl.semaphore_signal(barrier, inc=1, device_id=(d ^ s, t), device_id_type=MESH)
    for k in (1, 2):
        pl.semaphore_signal(barrier, inc=1, device_id=(d, t ^ k), device_id_type=MESH)

    def remote(src, dst, send_sem, recv_sem, dp_xor, tp_xor):
        return pltpu.make_async_remote_copy(
            src_ref=src, dst_ref=dst, send_sem=send_sem, recv_sem=recv_sem,
            device_id=(d ^ dp_xor, t ^ tp_xor), device_id_type=MESH,
        )

    hop = {1: (2, 0), 2: (1, 0), 4: (0, 2), 8: (0, 1)}
    pairs = ((x_ref, xs_ref), (cot_ref, cots_ref))

    def row_copy(a, k, bit):
        own, full = pairs[a]
        src = own if k == 0 else full.at[k]
        return remote(src, full.at[k + bit], row_send.at[a, k + bit], row_recv.at[a, k + bit], *hop[bit])

    def columns(ref, index, size):
        return ref.at[:, pl.ds(pl.multiple_of(index * size, 128), size)]

    def lines(ref, index, size):
        return ref.at[pl.ds(pl.multiple_of(index * size, 8), size), :]

    def across(ref, index, size):
        return columns(ref, index, size) if wide else ref.at[index]

    def mlp_copies(s):
        target = inner ^ (s % INNER)
        return (
            (columns(fc1_ref, target, hidden), lines(up_ref, d, depth)),
            (lines(fc2_ref, target, hidden), across(down_ref, d, depth)),
        )

    def att_copies(s):
        target = (inner ^ (s % INNER)) % 2
        return (
            (columns(qkv_ref, target, 3 * HD), lines(att_ref, d, depth)),
            (lines(out_ref, target, HD), across(proj_ref, d, depth)),
        )

    def att_land(s):
        return (lines(att_ref, d ^ s, depth), across(proj_ref, d ^ s, depth))

    def mlp_land(s):
        return (lines(up_ref, d ^ s, depth), across(down_ref, d ^ s, depth))

    local = []
    def stay(src, dst):
        copy = pltpu.make_async_copy(src, dst, local_sem.at[len(local)])
        copy.start()
        local.append(copy)

    lead = (inner // 2) == core
    pltpu.sync_copy(pay_ref, small_ref.at[0])
    pl.semaphore_wait(barrier, dp_n + 1)

    started = []
    def start(copy):
        copy.start()
        started.append(copy)

    def start_rows(k, bit):
        for a in range(2):
            start(row_copy(a, k, bit))

    def wait_rows(k):
        bit = 1
        while bit * 2 <= k:
            bit *= 2
        for a in range(2):
            row_copy(a, k - bit, bit).wait_recv()

    def start_mlp(s):
        for a, (src, dst) in enumerate(mlp_copies(s)):
            start(remote(src, dst, mlp_send.at[a, s], mlp_recv.at[a, s], s, 0))

    def att_active(s):
        return ((inner ^ (s % INNER)) // 2) == core

    def start_att(s):
        @pl.when(att_active(s))
        def _():
            for a, (src, dst) in enumerate(att_copies(s)):
                remote(src, dst, att_send.at[a, s], att_recv.at[a, s], s, 0).start()

    def pass_att(s):
        lands = att_land(s)
        return [
            remote(land, land, pass_send.at[a, s], pass_recv.at[a, s], 0, 1)
            for a, land in enumerate(lands)
        ]

    def small_copy(step, dp_xor, tp_xor, n):
        return remote(
            small_ref.at[pl.ds(0, n)], small_ref.at[pl.ds(n, n)],
            small_send.at[step], small_recv.at[step], dp_xor, tp_xor,
        )

    hops = []
    n = 1
    while n < dp_n * tp_n:
        hops.append((n // tp_n, n % tp_n, n))
        n *= 2
    even = [s for s in range(2, dp_n, 2)]
    even.sort(key=lambda s: -(s >= INNER))
    odd = [s for s in range(1, dp_n, 2)]
    odd.sort(key=lambda s: -(s >= INNER))

    small = [small_copy(k, *h) for k, h in enumerate(hops)]
    small[0].start()
    for bit in (1, 2, 4):
        start_rows(0, bit)
    start_rows(0, 8)
    for s in even:
        start_mlp(s)
    stay(x_ref, xs_ref.at[0])
    stay(cot_ref, cots_ref.at[0])
    for src, dst in mlp_copies(0):
        stay(src, dst)

    @pl.when(lead)
    def _():
        for a, (src, dst) in enumerate(att_copies(0)):
            copy = pltpu.make_async_copy(src, dst, local_sem.at[4 + a])
            copy.start()

    for k in range(len(small)):
        small[k].wait_recv()
        if k + 1 < len(small):
            small[k + 1].start()
    wait_rows(1)
    start_rows(1, 2)
    start_rows(1, 4)
    start_rows(1, 8)
    wait_rows(2)
    start_rows(2, 4)
    start_rows(2, 8)
    for s in odd:
        start_mlp(s)
    for s in even + odd:
        start_att(s)
    wait_rows(3)
    start_rows(3, 4)
    start_rows(3, 8)
    wait_rows(4)
    start_rows(4, 8)

    @pl.when(lead)
    def _():
        for a, (src, dst) in enumerate(att_copies(0)):
            pltpu.make_async_copy(src, dst, local_sem.at[4 + a]).wait()
        for copy in pass_att(0):
            copy.start()

    for k in (5, 6, 7):
        wait_rows(k)
        start_rows(k, 8)
    for k in range(8, 16):
        wait_rows(k)
    for s in even + odd:
        for a, dst in enumerate(mlp_land(s)):
            remote(dst, dst, mlp_send.at[a, s], mlp_recv.at[a, s], s, 0).wait_recv()
    for s in even + odd:
        @pl.when(lead)
        def _():
            for a, dst in enumerate(att_land(s)):
                remote(dst, dst, att_send.at[a, s], att_recv.at[a, s], s, 0).wait_recv()
            for copy in pass_att(s):
                copy.start()

    @pl.when(jnp.logical_not(lead))
    def _():
        for s in range(dp_n):
            for copy in pass_att(s):
                copy.wait_recv()

    @pl.when(lead)
    def _():
        for s in range(dp_n):
            for copy in pass_att(s):
                copy.wait_send()

    for s in range(1, dp_n):
        @pl.when(att_active(s))
        def _():
            for a, (src, dst) in enumerate(att_copies(s)):
                remote(src, dst, att_send.at[a, s], att_recv.at[a, s], s, 0).wait_send()
    for copy in started:
        copy.wait_send()
    for copy in small:
        copy.wait_send()
    for copy in local:
        copy.wait()


def span(start, size, unit):
    return pl.ds(start if isinstance(start, int) else pl.multiple_of(start, unit), size)


def lane_cut(ref, start, size):
    return ref.at[:, span(start, size, 128)]


def row_cut(ref, start, size):
    return ref.at[span(start, size, 16), :]


def columns_of(rows8):
    pad = jnp.zeros((120, 128), F32)
    return jnp.transpose(jnp.concatenate([rows8, pad], axis=0))


def fused_kernel(
    dp_n, tp_n,
    x_ref, cot_ref, fc1_ref, fc2_ref, qkv_ref, out_ref, pay_ref, rope_ref,
    block_out, input_out, up_out, down_out, qkv_out, proj_out, tail_out,
    gu_hbm, gd_hbm, ru_hbm, rd_hbm, ra_hbm,
    xs, cots, n2, up_t, down_w, pre, hid_t, act_t, ring, stats, vecs, sums, up_sum,
    att_w, proj_w, n1, q_s, k_s, v_s, prob, ctx, ctx_t, cctx, low, low_t, gx,
    rope, pay, vec_in, bias_in, head_in, vec_back, bias_back, head_back, up_place, head_place,
    keys, queries, qkv_bias, qkv_sum,
    row_send, row_recv, mlp_send, mlp_recv, att_send, att_recv, pass_send, pass_recv,
    small_send, small_recv, back_send, back_recv, headb_send, headb_recv, g_send, g_recv, g_local,
    rs_send, rs_recv, pair_send, pair_recv, ga_send, ga_recv,
    local_sem, out_sem, credit,
):
    d = lax.axis_index("dp")
    t = lax.axis_index("tp")
    flat = d * tp_n + t
    inner = d % INNER
    core = t % 2
    lead = (inner // 2) == core
    follow = jnp.logical_not(lead)
    rows, width = x_ref.shape
    depth = fc1_ref.shape[0]
    hidden = fc1_ref.shape[1] // INNER
    devices = dp_n * tp_n
    slots = 16
    tokens = slots * rows
    scale = HD ** (-0.5)
    chunk = 512

    barrier = pltpu.get_barrier_semaphore()
    for a in range(1, devices):
        peer = (d ^ (a // tp_n), t ^ (a % tp_n))
        pl.semaphore_signal(barrier, inc=1, device_id=peer, device_id_type=MESH)

    def remote(src, dst, send_sem, recv_sem, dp_xor, tp_xor):
        return pltpu.make_async_remote_copy(
            src_ref=src, dst_ref=dst, send_sem=send_sem, recv_sem=recv_sem,
            device_id=(d ^ dp_xor, t ^ tp_xor), device_id_type=MESH,
        )

    started = []

    def start(copy):
        copy.start()
        started.append(copy)

    hop = {1: (2, 0), 2: (1, 0), 4: (0, 2), 8: (0, 1)}

    def slot(ref, k):
        return row_cut(ref, k * rows, rows)

    def row_copy(a, k, bit):
        own, full = ((x_ref, xs), (cot_ref, cots))[a]
        src = own if k == 0 else slot(full, k)
        return remote(
            src, slot(full, k + bit), row_send.at[a, k + bit], row_recv.at[a, k + bit], *hop[bit]
        )

    row_started = ([], [])

    def start_row(a, k, *bits):
        for bit in bits:
            copy = row_copy(a, k, bit)
            copy.start()
            row_started[a].append(copy)

    def wait_row(a, k):
        bit = 1
        while bit * 2 <= k:
            bit *= 2
        row_copy(a, k - bit, bit).wait_recv()

    def w1_piece(i):
        return gx.at[depth : depth + hidden, pl.ds(pl.multiple_of(i * depth, 128), depth)]

    def mlp_copy(a, s):
        target = inner ^ (s % INNER)
        src = w1_piece(target) if a == 0 else row_cut(fc2_ref, target * hidden, hidden)
        dst = lane_cut((up_t, down_w)[a], d * depth, depth)
        if s == 0:
            return src, dst
        return remote(src, dst, mlp_send.at[a, s], mlp_recv.at[a, s], s, 0)

    mlp_started = tuple([mlp_copy(a, s) for s in range(1, dp_n)] for a in range(2))

    def start_mlp(a, s):
        mlp_started[a][s - 1].start()

    def mlp_wait(a, s):
        dst = lane_cut((up_t, down_w)[a], (d ^ s) * depth, depth)
        remote(dst, dst, mlp_send.at[a, s], mlp_recv.at[a, s], s, 0).wait_recv()

    def att_active(s):
        return ((inner ^ (s % INNER)) // 2) == core

    def att_pairs(s):
        target = (inner ^ (s % INNER)) % 2
        return (
            (lane_cut(qkv_ref, target * 3 * HD, 3 * HD), row_cut(att_w, d * depth, depth)),
            (row_cut(out_ref, target * HD, HD), lane_cut(proj_w, d * depth, depth)),
        )

    def att_land(s):
        return (row_cut(att_w, (d ^ s) * depth, depth), lane_cut(proj_w, (d ^ s) * depth, depth))

    def start_att(s):
        @pl.when(att_active(s))
        def _():
            for a, (src, dst) in enumerate(att_pairs(s)):
                remote(src, dst, att_send.at[a, s], att_recv.at[a, s], s, 0).start()

    def pass_att(s):
        return [
            remote(land, land, pass_send.at[a, s], pass_recv.at[a, s], 0, 1)
            for a, land in enumerate(att_land(s))
        ]

    local = []

    def stay(src, dst):
        copy = pltpu.make_async_copy(src, dst, local_sem.at[len(local)])
        copy.start()
        local.append(copy)
        return copy

    fc1_in = stay(fc1_ref, gx.at[0:depth, :])
    pay_in = stay(pay_ref, pay)
    x_in = stay(x_ref, slot(xs, 0))
    cot_in = stay(cot_ref, slot(cots, 0))
    down_in = stay(*mlp_copy(1, 0))
    rope_in = stay(rope_ref, rope)
    pay_in.wait()
    pl.semaphore_wait(barrier, devices - 1)

    even = sorted(range(2, dp_n, 2), key=lambda s: -(s >= INNER))
    odd = sorted(range(1, dp_n, 2), key=lambda s: -(s >= INNER))

    def small_copy(kind, src, dst, dp_xor, tp_xor):
        return remote(src, dst, small_send.at[kind], small_recv.at[kind], dp_xor, tp_xor)

    for a in range(1, devices):
        small_copy(0, pay.at[0], vec_in.at[a], a // tp_n, a % tp_n).start()
    for s in range(1, dp_n):
        group = 1 + (inner ^ (s % INNER)) // 2
        small_copy(1, pay.at[group], bias_in.at[s], s, 0).start()
    for k in range(1, 2 * dp_n):
        small_copy(2, pay.at[3], head_in.at[k], k // 2, k % 2).start()
    start_row(0, 0, 1, 2, 4, 8)
    start_row(1, 0, 1, 8)
    vec_in[0] = pay[0]
    bias_in[0] = pay[1 + inner // 2]
    head_in[0] = pay[3]
    fc1_in.wait()
    for i in range(INNER):
        piece = gx[0:depth, i * hidden : (i + 1) * hidden].astype(F32)
        gx[depth : depth + hidden, i * depth : (i + 1) * depth] = jnp.transpose(piece).astype(BF16)
    near = [2, 3]
    far = [s for s in (6, 4, 7, 5) if s < dp_n]
    plane = d // 2
    end = (plane == 0) | (plane == dp_n // 2 - 1)
    middle = jnp.logical_not(end)

    def start_all(s):
        start_mlp(0, s)
        start_mlp(1, s)
        start_att(s)

    start_all(2)
    for s in far:
        start_mlp(0, s)

    @pl.when(end)
    def _():
        start_all(3)

    for s in far:
        start_mlp(1, s)

    @pl.when(end)
    def _():
        for s in far:
            start_att(s)

    up_in = stay(*mlp_copy(0, 0))

    @pl.when(lead)
    def _():
        for a, (src, dst) in enumerate(att_pairs(0)):
            pltpu.make_async_copy(src, dst, local_sem.at[20 + a]).start()

    wait_row(0, 1)
    start_row(0, 1, 2, 4, 8)
    wait_row(0, 2)
    start_row(0, 2, 4, 8)
    start_row(1, 0, 2)

    def small_waits(kind):
        buf = (vec_in, bias_in, head_in)[kind]
        rest = buf.at[pl.ds(1, buf.shape[0] - 1)]
        return small_copy(kind, rest, rest, 0, 1)

    for kind in range(3):
        small_waits(kind).wait_recv()
    half = lax.broadcasted_iota(jnp.int32, (8, 128), 1) < 64
    for j in range(devices // 2):
        left = vec_in[flat ^ (2 * j)]
        right = vec_in[flat ^ (2 * j + 1)]
        vecs[:, j * 128 : (j + 1) * 128] = jnp.where(half, left, right)
    bias8 = jnp.zeros((8, 128), F32)
    head8 = jnp.zeros((8, 128), F32)
    head_rel = core ^ (inner // 2)
    for s in range(dp_n):
        bias8 = bias8 + bias_in[s]
        head8 = head8 + head_in[s * 2 + head_rel]
    second = inner % 2 == 1
    bias_t = columns_of(bias8)
    up_bias = jnp.concatenate(
        [jnp.where(second, bias_t[:, 4 + k : 5 + k], bias_t[:, k : k + 1]) for k in range(4)], axis=0
    )
    head4 = jnp.where(second, head8[4:], head8[:4])
    qkv_bias[0:1, :] = jnp.concatenate([head4[k : k + 1] for k in range(4)], axis=1)
    lane = lax.broadcasted_iota(jnp.int32, (1, 128), 1)
    keys[...] = jnp.zeros_like(keys)
    for q in range(4):
        at = slice(q * 128, (q + 1) * 128)
        keys[0:1, at] = ((t ^ ((q % 2) * 2 + q // 2)) * 128 + lane).astype(F32)
        for dy in range(2):
            peer = (core * 2 + dy) * tp_n + (q % 2) * 2 + q // 2
            keys[1 + dy : 2 + dy, at] = vec_in[peer][5:6, :]
        queries[at, :] = columns_of(keys[:, at])

    def norm_slot(k):
        @pl.loop(0, rows // 16)
        def _(j):
            at = pl.ds(pl.multiple_of(k * rows + j * 16, 16), 16)
            value = xs[at, :].astype(F32)
            mean = jnp.mean(value, axis=-1, keepdims=True)
            centered = value - mean
            inv = lax.rsqrt(jnp.mean(centered * centered, axis=-1, keepdims=True) + EPS)
            n2[at, :] = (centered * inv * vecs[2:3, :] + vecs[3:4, :]).astype(BF16)
            stats[at, 0:64] = jnp.broadcast_to(mean, (16, 64))
            stats[at, 64:128] = jnp.broadcast_to(inv, (16, 64))

    x_in.wait()
    norm_slot(0)
    wait_row(0, 3)
    start_row(0, 3, 4, 8)
    start_row(1, 0, 4)
    for k in (1, 2, 3):
        norm_slot(k)
    wait_row(1, 1)
    start_row(1, 1, 2, 4, 8)
    wait_row(1, 2)
    start_row(1, 2, 4, 8)

    @pl.when(middle)
    def _():
        start_all(3)

    start_all(1)
    for k in (4, 5, 6, 7):
        wait_row(0, k)
        start_row(0, k, 8)
        norm_slot(k)

    @pl.when(middle)
    def _():
        for s in far:
            start_att(s)

    for k in range(8, 16):
        wait_row(0, k)
        norm_slot(k)
    wait_row(1, 3)
    start_row(1, 3, 4, 8)

    def mine(dy, q):
        return ((q // 2) * 8 + (q % 2) * 4 + dy * 2 + core) * rows

    for dy in range(2):
        for q in range(4):
            @pl.loop(0, rows // 16)
            def _(j):
                at = pl.ds(pl.multiple_of(mine(dy, q) + j * 16, 16), 16)
                to = pl.ds(pl.multiple_of(dy * SEQ + q * rows + j * 16, 16), 16)
                normed = (xs[at, :].astype(F32) - stats[at, 0:1]) * stats[at, 64:65]
                n1[to, :] = (normed * vecs[0:1, :] + vecs[1:2, :]).astype(BF16)

    up_in.wait()
    for s in near + [1] + far:
        mlp_wait(0, s)

    @pl.loop(0, tokens // chunk)
    def _(j):
        at = pl.ds(pl.multiple_of(j * chunk, chunk), chunk)
        value = mm_tail(up_t[...], n2[at, :]) + up_bias
        pre[:, at] = value
        hid_t[:, at] = (value * gelu_half(value)).astype(BF16)

    for k in (4, 5, 6, 7):
        wait_row(1, k)
        start_row(1, k, 8)
    cot_in.wait()
    for k in range(8, 16):
        wait_row(1, k)
    sums[...] = jnp.zeros_like(sums)

    @pl.loop(0, rows // 16)
    def _(j):
        at = pl.ds(pl.multiple_of(j * 16, 16), 16)
        sums[4:5, :] += jnp.sum(cots[at, :].astype(F32), axis=0, keepdims=True)

    def g_send_copy(a, s):
        at = pl.ds(pl.multiple_of(s * depth, 128), depth)
        return remote(
            (gu_hbm, gd_hbm)[a].at[:, at], (ru_hbm, rd_hbm)[a].at[:, at],
            g_send.at[a, s], g_recv.at[a, s], s, 0,
        )

    def g_local_copy(a, s, b, dst):
        at = pl.ds(pl.multiple_of(s * depth, 128), depth)
        return pltpu.make_async_copy(ring.at[b], dst.at[:, at], g_local.at[b])

    def grads(a):
        left, right = ((act_t, n2), (hid_t, cots))[a]
        stage, own = ((gu_hbm, ru_hbm), (gd_hbm, rd_hbm))[a]

        def block(s, b):
            at = pl.ds(pl.multiple_of((d ^ s) * depth, 128), depth)
            ring[b] = mm(left[...], right[:, at]).astype(BF16)

        def at_step(k):
            return (k + 1) % (dp_n - 1) + 1

        @pl.loop(0, dp_n - 1)
        def _(k):
            s = at_step(k)
            b = k % 3

            @pl.when(k >= 2)
            def _():
                before = at_step(k - 2)
                g_local_copy(a, before, (k + 1) % 3, stage).wait()
                g_send_copy(a, before).start()

            block(s, b)
            g_local_copy(a, s, b, stage).start()

        last = dp_n - 2
        for k in (last - 1, last):
            s = at_step(k)
            g_local_copy(a, s, k % 3, stage).wait()
            g_send_copy(a, s).start()
        b = (last + 1) % 3
        block(0, b)
        copy = g_local_copy(a, 0, b, own)
        copy.start()
        copy.wait()

    grads(1)
    down_in.wait()
    for s in near + [1] + far:
        mlp_wait(1, s)
    up_sum[...] = jnp.zeros_like(up_sum)

    @pl.loop(0, tokens // chunk)
    def _(j):
        at = pl.ds(pl.multiple_of(j * chunk, chunk), chunk)
        value = mm_tail(down_w[...], cots[at, :]) * gelu_slope(pre[:, at])
        up_sum[:, 0:1] += jnp.sum(value, axis=1, keepdims=True)
        act_t[:, at] = value.astype(BF16)

    grads(0)

    @pl.loop(0, tokens // 256)
    def _(j):
        at = pl.ds(pl.multiple_of(j * 256, 256), 256)
        act = jnp.transpose(act_t[:, at].astype(F32)).astype(BF16)
        mean, inv = stats[at, 0:1], stats[at, 64:65]

        @pl.loop(0, width // chunk)
        def _(c):
            lanes = pl.ds(pl.multiple_of(c * chunk, chunk), chunk)
            part = mm(act, up_t[:, lanes])
            normed = (xs[at, lanes].astype(F32) - mean) * inv
            sums[2:3, lanes] += jnp.sum(part * normed, axis=0, keepdims=True)
            sums[3:4, lanes] += jnp.sum(part, axis=0, keepdims=True)
            n2[at, lanes] = (part * vecs[2:3, lanes]).astype(BF16)

    for copy in row_started[0] + mlp_started[0]:
        copy.wait_send()
    pl.semaphore_signal(credit.at[0], inc=1, device_id=(d, t ^ 1), device_id_type=MESH)
    pl.semaphore_signal(credit.at[1], inc=1, device_id=(d, t ^ 2), device_id_type=MESH)

    @pl.when(lead)
    def _():
        for a, (src, dst) in enumerate(att_pairs(0)):
            pltpu.make_async_copy(src, dst, local_sem.at[20 + a]).wait()
        for copy in pass_att(0):
            copy.start()
        for s in near + [1] + far:
            for a, dst in enumerate(att_land(s)):
                remote(dst, dst, att_send.at[a, s], att_recv.at[a, s], s, 0).wait_recv()
            for copy in pass_att(s):
                copy.start()

    @pl.when(follow)
    def _():
        for s in range(dp_n):
            for copy in pass_att(s):
                copy.wait_recv()

    rope_in.wait()
    lanes128 = lax.broadcasted_iota(jnp.int32, (SEQ, 128), 1)

    def rope_tables(sign):
        at = [pl.ds(pl.multiple_of((t ^ ((q % 2) * 2 + q // 2)) * 128, 128), 128) for q in range(4)]
        cosine = jnp.concatenate([rope[0, a, :] for a in at], axis=0)
        sine = jnp.concatenate([rope[1, a, :] for a in at], axis=0) * sign
        lower = jnp.where(lanes128 < ROT // 2, -sine, 0.0)
        upper = jnp.where((lanes128 >= ROT // 2) & (lanes128 < ROT), sine, 0.0)
        return cosine, lower, upper

    def turn(value, tables):
        cosine, lower, upper = tables
        head = value[:, :128]
        head = (
            head * cosine
            + pltpu.roll(head, 128 - ROT // 2, 1) * lower
            + pltpu.roll(head, ROT // 2, 1) * upper
        )
        return jnp.concatenate([head, value[:, 128:]], axis=1)

    @pl.loop(0, 2)
    def _(dy):
        at = pl.ds(pl.multiple_of(dy * SEQ, SEQ), SEQ)
        tables = rope_tables(1.0)
        rows_in = n1[at, :]
        value = mm(rows_in, att_w[:, :HD]) + qkv_bias[0:1, :HD]
        query = turn(value, tables).astype(BF16)
        key = turn(mm(rows_in, att_w[:, HD : 2 * HD]), tables).astype(BF16)
        val = (mm(rows_in, att_w[:, 2 * HD :]) + qkv_bias[0:1, HD:]).astype(BF16)
        q_s[at, :] = query
        k_s[at, :] = key
        v_s[at, :] = val
        seg_q = jnp.where(dy == 0, queries[:, 1:2], queries[:, 2:3])
        seg_k = jnp.where(dy == 0, keys[1:2, :], keys[2:3, :])
        allowed = (keys[0:1, :] <= queries[:, 0:1]) & (seg_q == seg_k)
        scores = jnp.where(allowed, mm_tail(query, key) * scale, NEG_FILL)
        peak = jnp.max(scores, axis=-1, keepdims=True)
        total = jnp.where(allowed, jnp.exp(scores - peak), 0.0)
        share = (total / jnp.sum(total, axis=-1, keepdims=True)).astype(BF16)
        prob[at, :] = share
        got = mm(share, val)
        ctx[at, :] = got.astype(BF16)
        ctx_t[:, at] = jnp.transpose(got).astype(BF16)

    def cot_mine(dy, lanes):
        parts = [cots[pl.ds(pl.multiple_of(mine(dy, q), 128), rows), lanes] for q in range(4)]
        return jnp.concatenate(parts, axis=0)

    for dy in range(2):
        cctx[dy * SEQ : (dy + 1) * SEQ, :] = mm_tail(cot_mine(dy, slice(None)), proj_w[...]).astype(BF16)

    @pl.loop(0, width // chunk)
    def _(c):
        lanes = pl.ds(pl.multiple_of(c * chunk, chunk), chunk)
        both = jnp.concatenate([cot_mine(0, lanes), cot_mine(1, lanes)], axis=0)
        gx[3 * HD : 4 * HD, lanes] = mm(ctx_t[...], both).astype(BF16)

    for copy in row_started[1]:
        copy.wait_send()
    for dc in range(2):
        for dx in range(2):
            for dy in range(2):
                pair = dc * 4 + dx * 2 + dy
                spot = dy * SEQ + (dc * 2 + dx) * rows
                at = slice(pair * 256, pair * 256 + 256)
                hid = jnp.transpose(hid_t[:, at].astype(F32)).astype(BF16)

                @pl.loop(0, width // chunk)
                def _(c):
                    lanes = pl.ds(pl.multiple_of(c * chunk, chunk), chunk)
                    base = mm(hid, down_w[:, lanes])
                    extra = mm(ctx[spot : spot + rows, :], proj_w[:, lanes])
                    here = core == 0
                    first = base[:rows] + jnp.where(here, extra, 0.0)
                    other = base[rows:] + jnp.where(here, 0.0, extra)
                    cots[at, lanes] = jnp.concatenate([first, other], axis=0).astype(BF16)
    for bit in (2, 1):
        dp_xor, tp_xor = hop[bit]
        pl.semaphore_signal(
            credit.at[1 + (3 - bit)], inc=1, device_id=(d ^ dp_xor, t ^ tp_xor), device_id_type=MESH
        )
    own_x = row_cut(hid_t, 3 * rows, rows)
    own_cot = row_cut(down_w, 3 * rows, rows)
    x_again = stay(x_ref, own_x)
    cot_again = stay(cot_ref, own_cot)

    bufs = (cots, n2)

    def landing(a, bit, j, there):
        if bit == 8:
            if a == 0:
                side = core if there else 1 - core
                return row_cut(xs, (2 * j + side) * rows, rows)
            return row_cut(n1, j * rows, rows)
        if bit == 4:
            return row_cut((act_t, up_t)[a], j * rows, rows)
        base = (down_w, hid_t)[a]
        return row_cut(base, (j if bit == 2 else 2) * rows, rows)

    def rs_copy(a, bit, j):
        return remote(
            slot(bufs[a], bit + j), landing(a, bit, j, True),
            rs_send.at[a, bit + j], rs_recv.at[a, bit + j], *hop[bit],
        )

    def rs_start(a, bit, j):
        start(rs_copy(a, bit, j))

    def rs_add(a, bit, j):
        land = landing(a, bit, j, False)
        remote(land, land, rs_send.at[a, bit + j], rs_recv.at[a, bit + j], *hop[bit]).wait_recv()
        here = slot(bufs[a], j)

        @pl.loop(0, rows // 16)
        def _(i):
            at = pl.ds(pl.multiple_of(i * 16, 16), 16)
            here[at, :] = (here[at, :].astype(F32) + land[at, :].astype(F32)).astype(BF16)

    pl.semaphore_wait(credit.at[0], 1)
    for j in (7, 5, 6, 4, 3, 1, 2, 0):
        rs_start(0, 8, j)

    qkv_sum[...] = jnp.zeros_like(qkv_sum)

    def backward(dy):
        at = slice(dy * SEQ, (dy + 1) * SEQ)
        tables = rope_tables(-1.0)
        share = prob[at, :].astype(F32)
        got = cctx[at, :]
        delta = jnp.sum(got.astype(F32) * ctx[at, :].astype(F32), axis=-1, keepdims=True)
        score_cot = share * (mm_tail(got, v_s[at, :]) - delta)
        value_cot = mm(jnp.transpose(share).astype(BF16), got)
        query_cot = turn(mm(score_cot.astype(BF16), k_s[at, :]) * scale, tables)
        key_cot = turn(mm(jnp.transpose(score_cot).astype(BF16), q_s[at, :]) * scale, tables)
        qkv_sum[0:1, :HD] += jnp.sum(query_cot, axis=0, keepdims=True)
        qkv_sum[0:1, HD:] += jnp.sum(value_cot, axis=0, keepdims=True)
        for k, part in enumerate((query_cot, key_cot, value_cot)):
            low[at, k * HD : (k + 1) * HD] = part.astype(BF16)
            low_t[k * HD : (k + 1) * HD, at] = jnp.transpose(part).astype(BF16)

    backward(0)
    pl.semaphore_wait(credit.at[1], 1)
    for j in (7, 5, 6, 4):
        rs_add(0, 8, j)
        rs_start(0, 4, j - 4)
    for j in (3, 1, 2, 0):
        rs_add(0, 8, j)

    @pl.when(lead)
    def _():
        pl.semaphore_signal(credit.at[4], inc=1, device_id=(d, t ^ 1), device_id_type=MESH)

    backward(1)

    @pl.loop(0, width // chunk)
    def _(c):
        lanes = pl.ds(pl.multiple_of(c * chunk, chunk), chunk)
        gx[0 : 3 * HD, lanes] = mm(low_t[...], n1[:, lanes]).astype(BF16)

    pl.semaphore_signal(credit.at[5], inc=1, device_id=(d, t ^ 1), device_id_type=MESH)

    def pair_copy(j):
        return remote(
            row_cut(gx, j * rows, rows), row_cut(xs, (2 * j + core) * rows, rows),
            pair_send.at[j], pair_recv.at[j], 0, 1,
        )

    @pl.when(follow)
    def _():
        pl.semaphore_wait(credit.at[4], 1)
        for j in range(8):
            pair_copy(j).start()

    for dy in range(2):
        for q in range(4):
            at = pl.ds(pl.multiple_of(mine(dy, q), 128), rows)
            piece = low[dy * SEQ + q * rows : dy * SEQ + (q + 1) * rows, :]

            @pl.loop(0, width // chunk)
            def _(c):
                lanes = pl.ds(pl.multiple_of(c * chunk, chunk), chunk)
                part = mm_tail(piece, att_w[lanes, :])
                normed = (xs[at, lanes].astype(F32) - stats[at, 0:1]) * stats[at, 64:65]
                sums[0:1, lanes] += jnp.sum(part * normed, axis=0, keepdims=True)
                sums[1:2, lanes] += jnp.sum(part, axis=0, keepdims=True)
                n2[at, lanes] = (n2[at, lanes].astype(F32) + part * vecs[0:1, lanes]).astype(BF16)

    blank = jnp.zeros((4, 128), F32)
    up_rows = [jnp.transpose(up_sum[k * 128 : (k + 1) * 128, :])[0:1] for k in range(4)]
    up_rows = jnp.concatenate(up_rows, axis=0)
    qkv_rows = jnp.concatenate([qkv_sum[0:1, k * 128 : (k + 1) * 128] for k in range(4)], axis=0)

    def place(value):
        return jnp.where(
            second, jnp.concatenate([blank, value], axis=0), jnp.concatenate([value, blank], axis=0)
        )

    up_place[...] = place(up_rows)
    head_place[...] = place(qkv_rows)

    def window(owner):
        return lane_cut(sums, (owner // 2) * 128, 128)

    def back_copy(kind, src, dst, dp_xor, tp_xor):
        return remote(src, dst, back_send.at[kind], back_recv.at[kind], dp_xor, tp_xor)

    def head_copy(s, dc):
        return remote(
            head_place, head_back.at[s * 2 + dc], headb_send.at[s * 2 + dc], headb_recv.at[s * 2 + dc], s, dc
        )

    for a in range(1, devices):
        back_copy(0, window(flat ^ a), vec_back.at[a], a // tp_n, a % tp_n).start()
    for s in range(1, dp_n):
        back_copy(1, up_place, bias_back.at[s], s, 0).start()

    @pl.when(lead)
    def _():
        for s in range(1, dp_n):
            head_copy(s, 0).start()

    @pl.when(follow)
    def _():
        for s in range(dp_n):
            head_copy(s, 1).start()

    pl.semaphore_wait(credit.at[5], 1)
    for j in (7, 5, 6, 4, 3, 1, 2, 0):
        rs_start(1, 8, j)

    def ga_copy(s):
        return remote(
            lane_cut(gx, (d ^ s) * depth, depth), ra_hbm.at[:, s * depth : (s + 1) * depth],
            ga_send.at[s], ga_recv.at[s], s, 0,
        )

    @pl.when(lead)
    def _():
        for j in range(8):
            land = row_cut(xs, (2 * j + 1 - core) * rows, rows)
            remote(land, land, pair_send.at[j], pair_recv.at[j], 0, 1).wait_recv()

            @pl.loop(0, rows // 16)
            def _(i):
                at = pl.ds(pl.multiple_of(j * rows + i * 16, 16), 16)
                there = pl.ds(pl.multiple_of(i * 16, 16), 16)
                gx[at, :] = (gx[at, :].astype(F32) + land[there, :].astype(F32)).astype(BF16)

        for s in near + [1] + far:
            ga_copy(s).start()
        pltpu.make_async_copy(
            lane_cut(gx, d * depth, depth), ra_hbm.at[:, 0:depth], local_sem.at[22]
        ).start()

    for j in (7, 5, 6, 4):
        rs_add(1, 8, j)
        rs_start(1, 4, j - 4)
    for j in (3, 1, 2, 0):
        rs_add(1, 8, j)

    pl.semaphore_wait(credit.at[2], 1)
    pl.semaphore_wait(credit.at[3], 1)

    def rs_tail(a):
        rs_add(a, 4, 3)
        rs_start(a, 2, 1)
        rs_add(a, 4, 1)
        rs_add(a, 4, 2)
        rs_start(a, 2, 0)
        rs_add(a, 2, 1)
        rs_start(a, 1, 0)
        rs_add(a, 4, 0)
        rs_add(a, 2, 0)
        rs_add(a, 1, 0)

    outs = []

    def leave(src, dst):
        copy = pltpu.make_async_copy(src, dst, out_sem.at[len(outs)])
        copy.start()
        outs.append(copy)
        return copy

    rs_tail(0)
    x_again.wait()

    @pl.loop(0, rows // 16)
    def _(j):
        at = pl.ds(pl.multiple_of(j * 16, 16), 16)
        total = own_x[at, :].astype(F32) + cots[at, :].astype(F32) + vecs[4:5, :]
        cots[at, :] = total.astype(BF16)

    leave(slot(cots, 0), block_out)

    def back_waits(kind):
        buf = (vec_back, bias_back)[kind]
        rest = buf.at[pl.ds(1, buf.shape[0] - 1)]
        return back_copy(kind, rest, rest, 0, 1)

    for kind in range(2):
        back_waits(kind).wait_recv()
    for kind in range(3):
        small_waits(kind).wait_send()
    total = window(flat)[...]
    for a in range(1, devices):
        total = total + vec_back[a]
    pay[0] = total
    pay[1] = jnp.zeros_like(total)
    pay[2] = jnp.zeros_like(total)
    pay[3] = jnp.zeros_like(total)
    pay[1 + inner // 2] += up_place[...]
    for s in range(1, dp_n):
        pay[1 + (inner ^ (s % INNER)) // 2] += bias_back[s]
    for s in range(dp_n):
        @pl.when(att_active(s))
        def _():
            if s == 0:
                pay[3] += head_place[...]
            else:
                head_copy(s, 0).wait_recv()
                pay[3] += head_back[2 * s]
            head_copy(s, 1).wait_recv()
            pay[3] += head_back[2 * s + 1]

    leave(pay, tail_out)

    for a in (1, 0):
        for s in range(1, dp_n):
            g_send_copy(a, s).wait_recv()
    up_back = stay(ru_hbm, xs.at[0:hidden, :])
    down_back = stay(rd_hbm, xs.at[hidden : 2 * hidden, :])
    up_back.wait()
    down_back.wait()

    def total_of(base, k):
        total = xs[base : base + hidden, k * depth : (k + 1) * depth].astype(F32)
        for s in range(k + INNER, dp_n, INNER):
            total = total + xs[base : base + hidden, s * depth : (s + 1) * depth].astype(F32)
        return total

    waits = []
    for k in range(INNER):
        pre[0:depth, k * hidden : (k + 1) * hidden] = jnp.transpose(total_of(0, k))
        waits.append(
            leave(pre.at[0:depth, k * hidden : (k + 1) * hidden],
                  lane_cut(up_out, (inner ^ k) * hidden, hidden))
        )
    for copy in waits:
        copy.wait()
    waits = []
    for k in range(INNER):
        pre[0:hidden, k * depth : (k + 1) * depth] = total_of(hidden, k)
        waits.append(
            leave(pre.at[0:hidden, k * depth : (k + 1) * depth],
                  row_cut(down_out, (inner ^ k) * hidden, hidden))
        )
    for copy in waits:
        copy.wait()

    rs_tail(1)
    cot_again.wait()

    @pl.loop(0, rows // 16)
    def _(j):
        at = pl.ds(pl.multiple_of(j * 16, 16), 16)
        scaled = n2[at, :].astype(F32)
        inv = stats[at, 64:65]
        normed = (own_x[at, :].astype(F32) - stats[at, 0:1]) * inv
        inner_mean = jnp.mean(scaled, axis=-1, keepdims=True)
        cross = jnp.mean(scaled * normed, axis=-1, keepdims=True)
        pre[at, :] = own_cot[at, :].astype(F32) + inv * (scaled - inner_mean - normed * cross)

    grad_out = leave(pre.at[0:rows, :], input_out)

    @pl.when(lead)
    def _():
        pltpu.make_async_copy(
            lane_cut(gx, d * depth, depth), ra_hbm.at[:, 0:depth], local_sem.at[22]
        ).wait()

    for s in range(1, dp_n):
        @pl.when(att_active(s))
        def _():
            ga_copy(s).wait_recv()

    base = 2 * hidden
    picks = []
    for hl in range(2):
        first = ((inner // 2) ^ core) * 2 + ((inner % 2) ^ hl)
        for o in range(dp_n // INNER):
            picks.append(
                stay(lane_cut(ra_hbm, (first + o * INNER) * depth, depth),
                     xs.at[base : base + 4 * HD, len(picks) * depth : (len(picks) + 1) * depth])
            )
    for copy in picks:
        copy.wait()
    grad_out.wait()
    groups = dp_n // INNER
    for hl in range(2):
        total = jnp.zeros((4 * HD, depth), F32)
        for o in range(groups):
            k = hl * groups + o
            total = total + xs[base : base + 4 * HD, k * depth : (k + 1) * depth].astype(F32)
        pre[0:depth, hl * 3 * HD : (hl + 1) * 3 * HD] = jnp.transpose(total[: 3 * HD])
        leave(pre.at[0:depth, hl * 3 * HD : (hl + 1) * 3 * HD], qkv_out.at[:, hl * 3 * HD : (hl + 1) * 3 * HD])
        pre[depth : depth + HD, hl * depth : (hl + 1) * depth] = total[3 * HD :]
        leave(pre.at[depth : depth + HD, hl * depth : (hl + 1) * depth], proj_out.at[hl * HD : (hl + 1) * HD, :])

    for s in range(1, dp_n):
        for a in range(2):
            g_send_copy(a, s).wait_send()

        @pl.when(att_active(s))
        def _():
            for a, (src, dst) in enumerate(att_pairs(s)):
                remote(src, dst, att_send.at[a, s], att_recv.at[a, s], s, 0).wait_send()

        @pl.when(lead)
        def _():
            ga_copy(s).wait_send()

    @pl.when(lead)
    def _():
        for s in range(dp_n):
            for copy in pass_att(s):
                copy.wait_send()

    @pl.when(follow)
    def _():
        for j in range(8):
            pair_copy(j).wait_send()

    @pl.when(lead)
    def _():
        for s in range(1, dp_n):
            head_copy(s, 0).wait_send()

    @pl.when(follow)
    def _():
        for s in range(dp_n):
            head_copy(s, 1).wait_send()

    for kind in range(2):
        back_waits(kind).wait_send()
    for copy in started + mlp_started[1]:
        copy.wait_send()
    outs[0].wait()
    outs[1].wait()
    for copy in outs[3 + 2 * INNER :]:
        copy.wait()


def solution(mesh):
    dp_n, tp_n = mesh.shape["dp"], mesh.shape["tp"]
    outer = dp_n // INNER
    devices = dp_n * tp_n

    def send(value, dp_xor, tp_xor, keep=None):
        pairs = []
        for d in range(dp_n):
            for t in range(tp_n):
                if keep is None or keep(d, t):
                    pairs.append((d * tp_n + t, (d ^ dp_xor) * tp_n + (t ^ tp_xor)))
        return lax.ppermute(value, AXES, pairs)

    def scatter_small(value, flat):
        held = value
        step = devices // 2
        while step >= 1:
            dp_xor, tp_xor = step // tp_n, step % tp_n
            high = (flat // step) % 2 == 1
            first, second = held[:step], held[step:]
            other = send(jnp.where(high, first, second), dp_xor, tp_xor)
            held = jnp.where(high, second, first) + other
            step //= 2
        return held[0]

    def scatter_rows(value):
        for dp_xor, tp_xor in ((0, 1), (0, 2), (1, 0), (2, 0)):
            half = value.shape[0] // 2
            other = send(value[half:], dp_xor, tp_xor)
            value = value[:half].astype(F32) + other.astype(F32)
            if half > value.shape[0] or (dp_xor, tp_xor) != (2, 0):
                value = value.astype(BF16)
        return value

    def on_device(
        block_input, segment_ids, w_qkv, b_qkv, w_out, b_out, w_fc1, b_fc1, w_fc2, b_fc2,
        ln1_gain, ln1_bias, ln2_gain, ln2_bias, cotangent,
    ):
        d = lax.axis_index("dp")
        t = lax.axis_index("tp")
        flat = d * tp_n + t
        inner = d % INNER
        core = t % 2
        lead = (inner // 2) == core
        rows, width = block_input.shape
        depth = w_qkv.shape[0]
        hidden_here = w_fc1.shape[1] // INNER
        head_here = w_out.shape[0] // HD
        heads = head_here * tp_n
        quarter = SEQ // tp_n
        qkv_bits = b_qkv.shape[1]

        vec = jnp.stack([ln1_gain, ln1_bias, ln2_gain, ln2_bias, b_out + b_fc2]).reshape(-1)
        seg_part = lax.dynamic_slice(segment_ids.reshape(-1), (t * quarter,), (quarter,))
        sizes = [vec.size, b_qkv.size, b_fc1.size, quarter]
        payload = jnp.concatenate(
            [vec, b_qkv.reshape(-1), b_fc1.reshape(-1), seg_part.astype(F32)]
        )
        depth_wide = depth % 128 == 0
        flat_shape = lambda lead_n: (lead_n, width) if depth_wide else (dp_n, lead_n, depth)
        spread = lambda v: v if depth_wide else v.transpose(1, 0, 2).reshape(v.shape[1], width)
        payload = jnp.pad(payload, (0, PAY - payload.size)).reshape(8, PAY // 8)
        like = lambda *shape: jax.ShapeDtypeStruct(shape, BF16)
        dma = pltpu.SemaphoreType.DMA
        hop_count = (devices - 1).bit_length()
        any_spec = pl.BlockSpec(memory_space=pl.ANY)
        x_all, cot_all, up_w, down_w, qkv_w, out_w, small = pl.pallas_call(
            functools.partial(gather_kernel, dp_n, tp_n, depth_wide),
            out_shape=(
                like(16, rows, width),
                like(16, rows, width),
                like(width, hidden_here),
                like(*flat_shape(hidden_here)),
                like(width, 3 * HD),
                like(*flat_shape(HD)),
                jax.ShapeDtypeStruct((devices, 8, PAY // 8), F32),
            ),
            in_specs=[any_spec] * 7,
            out_specs=(any_spec,) * 7,
            scratch_shapes=[
                dma((2, 16)), dma((2, 16)), dma((2, dp_n)), dma((2, dp_n)),
                dma((2, dp_n)), dma((2, dp_n)), dma((2, dp_n)), dma((2, dp_n)),
                dma((hop_count,)), dma((hop_count,)), dma((6,)),
            ],
            compiler_params=pltpu.CompilerParams(collective_id=0, has_side_effects=True),
            name="gather_phase",
        )(block_input, cotangent, w_fc1, w_fc2, w_qkv, w_out, payload)
        down_w, out_w = spread(down_w), spread(out_w)
        small = jnp.take(small.reshape(devices, PAY), flat ^ jnp.arange(devices), axis=0)
        cuts = [0]
        for size in sizes:
            cuts.append(cuts[-1] + size)
        vecs = small[:, : cuts[1]].reshape(devices, 5, -1).transpose(1, 0, 2).reshape(5, width)
        gain_one, shift_one, gain_two, shift_two, out_bias = (vecs[k][None] for k in range(5))
        qkv_bias_all = (
            small[:, cuts[1] : cuts[2]]
            .reshape(dp_n, tp_n, head_here, qkv_bits)
            .transpose(1, 2, 0, 3)
            .reshape(heads, 2 * HD)
        )
        head = (t // 2) * INNER + inner
        qkv_bias = lax.dynamic_slice(qkv_bias_all, (head, 0), (1, 2 * HD))
        up_rows, up_cols = b_fc1.shape
        up_bias_all = (
            small[:, cuts[2] : cuts[3]]
            .reshape(dp_n, tp_n, up_rows, up_cols)
            .transpose(1, 2, 0, 3)
            .reshape(tp_n * INNER, hidden_here)
        )
        up_bias = lax.dynamic_slice(up_bias_all, (t * INNER + inner, 0), (1, hidden_here))
        seg_all = small[:, cuts[3] : cuts[4]].reshape(dp_n, tp_n, quarter)

        x_rows = x_all.reshape(16 * rows, width).astype(F32)
        cot_rows = cot_all.reshape(16 * rows, width)
        row_mean = jnp.mean(x_rows, axis=-1, keepdims=True)
        centered = x_rows - row_mean
        row_var = jnp.mean(centered * centered, axis=-1, keepdims=True)
        inv_std = lax.rsqrt(row_var + EPS)
        normed = centered * inv_std
        norm_two = (normed * gain_two + shift_two).astype(BF16)

        def mine(value):
            split = value.reshape((2, 2, 2, 2, rows) + value.shape[1:])
            cut = lax.dynamic_index_in_dim(split, core, 3, keepdims=False)
            return jnp.moveaxis(cut, 2, 0).reshape((2 * SEQ,) + value.shape[1:])

        def unmine(value):
            split = value.reshape((2, 2, 2, rows) + value.shape[1:])
            cut = jnp.moveaxis(split, 0, 2)[:, :, :, None]
            where = (jnp.arange(2) == core).reshape((1, 1, 1, 2) + (1,) * value.ndim)
            full = jnp.where(where, cut, jnp.zeros_like(cut))
            return full.reshape((16 * rows,) + value.shape[1:])

        norm_one = (mine(normed) * gain_one + shift_one).astype(BF16)
        cot_mine = mine(cot_rows)

        pre_act = mm(norm_two, up_w) + up_bias
        half_gelu = gelu_half(pre_act)
        hidden = (pre_act * half_gelu).astype(BF16)
        down_grad = mm_lead(hidden, cot_rows)
        act_cot = mm_tail(cot_rows, down_w) * gelu_slope(pre_act)
        up_bias_part = jnp.sum(act_cot, axis=0)
        act_low = act_cot.astype(BF16)
        up_grad = mm_lead(norm_two, act_low)
        up_grad, down_grad = up_grad.astype(BF16), down_grad.astype(BF16)

        def cut_block(value, s):
            return lax.dynamic_slice(value, ((d ^ s) * depth, 0), (depth, value.shape[1]))

        def cut_across(value, s):
            return lax.dynamic_slice(value, (0, (d ^ s) * depth), (value.shape[0], depth))

        with jax.named_scope("mlp_out"):
            up_back = [cut_block(up_grad, 0)] + [
                send(cut_block(up_grad, s), s, 0) for s in range(1, dp_n)
            ]
            down_back = [cut_across(down_grad, 0)] + [
                send(cut_across(down_grad, s), s, 0) for s in range(1, dp_n)
            ]

        order = jnp.stack([t ^ ((k % 2) * 2 + k // 2) for k in range(4)])
        position = (order[:, None] * quarter + jnp.arange(quarter)[None]).reshape(-1)
        inverse = jnp.exp(jnp.arange(ROT // 2, dtype=F32) * (-2.0 * math.log(10000.0) / ROT))
        angle = position.astype(F32)[:, None] * inverse[None]
        cosine, sine = jnp.cos(angle)[None], jnp.sin(angle)[None]
        segs = []
        for dy in range(2):
            seq = (d // INNER) * INNER + (inner ^ (core * 2 + dy))
            rows_of = lax.dynamic_index_in_dim(seg_all, seq, 0, keepdims=False)
            segs.append(jnp.take(rows_of, order, axis=0).reshape(-1))
        segs = jnp.stack(segs)
        allowed = (position[None, :] <= position[:, None])[None] & (
            segs[:, :, None] == segs[:, None, :]
        )
        qkv = mm(norm_one, qkv_w)
        query = rotate((qkv[:, :HD] + qkv_bias[:, :HD]).reshape(2, SEQ, HD), cosine, sine).astype(BF16)
        key = rotate(qkv[:, HD : 2 * HD].reshape(2, SEQ, HD), cosine, sine).astype(BF16)
        val = (qkv[:, 2 * HD :] + qkv_bias[:, HD:]).astype(BF16).reshape(2, SEQ, HD)
        scale = HD ** (-0.5)

        def ein(eq, left, right):
            return jnp.einsum(eq, left, right, preferred_element_type=F32)

        masked = jnp.where(allowed, ein("sqd,skd->sqk", query, key) * scale, NEG_FILL)
        peak = jnp.max(masked, axis=-1, keepdims=True)
        log_total = peak + jnp.log(
            jnp.sum(jnp.where(allowed, jnp.exp(masked - peak), 0.0), axis=-1, keepdims=True)
        )
        prob_full = jnp.where(allowed, jnp.exp(masked - log_total), 0.0)
        prob_low = prob_full.astype(BF16)
        context = ein("sqk,skd->sqd", prob_low, val).astype(BF16)
        context_cot = mm_tail(cot_mine, out_w).astype(BF16).reshape(2, SEQ, HD)
        prob_cot = ein("sqd,skd->sqk", context_cot, val)
        row_delta = jnp.sum(context_cot.astype(F32) * context.astype(F32), axis=-1, keepdims=True)
        score_cot = (prob_full * (prob_cot - row_delta)).astype(BF16)
        query_cot = rotate(ein("sqk,skd->sqd", score_cot, key) * scale, cosine, -sine)
        key_cot = rotate(ein("sqk,sqd->skd", score_cot, query) * scale, cosine, -sine)
        val_cot = ein("sqk,sqd->skd", prob_low, context_cot)
        qkv_cot = jnp.concatenate([query_cot, key_cot, val_cot], axis=-1).reshape(2 * SEQ, 3 * HD)
        qkv_bias_part = jnp.concatenate(
            [jnp.sum(query_cot, axis=(0, 1)), jnp.sum(val_cot, axis=(0, 1))]
        )
        qkv_low = qkv_cot.astype(BF16)
        context_flat = context.reshape(2 * SEQ, HD)
        att_grad = jnp.concatenate(
            [mm_lead(norm_one, qkv_low).astype(BF16), mm_lead(cot_mine, context_flat).astype(BF16)],
            axis=1,
        )
        att_pair = send(att_grad, 0, 1, lambda dd, tt: (dd % INNER) // 2 != tt % 2)
        att_grad = (att_grad.astype(F32) + att_pair.astype(F32)).astype(BF16)
        with jax.named_scope("att_out"):
            own_att = cut_block(att_grad, 0)
            att_back = [jnp.where(lead, own_att, jnp.zeros_like(own_att))] + [
                send(cut_block(att_grad, s), s, 0, lambda dd, tt: (dd % INNER) // 2 == tt % 2)
                for s in range(1, dp_n)
            ]

        left = jnp.concatenate([hidden, unmine(context_flat)], axis=1)
        right = jnp.concatenate([down_w, out_w], axis=0)
        with jax.named_scope("branch"):
            branch = scatter_rows(mm(left, right).astype(BF16))
        block_output = (block_input.astype(F32) + branch + out_bias).astype(BF16)

        one_part = mm_tail(qkv_low, qkv_w)
        two_part = mm_tail(act_low, up_w)
        vec_terms = jnp.stack(
            [
                jnp.sum(one_part * mine(normed), axis=0),
                jnp.sum(one_part, axis=0),
                jnp.sum(two_part * normed, axis=0),
                jnp.sum(two_part, axis=0),
                jnp.sum(cotangent.astype(F32), axis=0),
            ]
        )
        scaled_part = (two_part * gain_two + unmine(one_part * gain_one)).astype(BF16)
        with jax.named_scope("normback"):
            scaled = scatter_rows(scaled_part)
        normed_own = normed[:rows]
        input_grad = cotangent.astype(F32) + inv_std[:rows] * (
            scaled
            - jnp.mean(scaled, axis=-1, keepdims=True)
            - normed_own * jnp.mean(scaled * normed_own, axis=-1, keepdims=True)
        )

        head_hot = (jnp.arange(heads) == head).astype(F32)[:, None]
        qkv_small = (
            (head_hot * qkv_bias_part[None])
            .reshape(tp_n, head_here, dp_n, qkv_bits)
            .transpose(2, 0, 1, 3)
            .reshape(devices, -1)
        )
        up_hot = (jnp.arange(tp_n * INNER) == t * INNER + inner).astype(F32)[:, None]
        up_small = (
            (up_hot * up_bias_part[None])
            .reshape(tp_n, up_rows, dp_n, up_cols)
            .transpose(2, 0, 1, 3)
            .reshape(devices, -1)
        )
        vec_small = vec_terms.reshape(5, devices, -1).transpose(1, 0, 2).reshape(devices, -1)
        with jax.named_scope("small_out"):
            own = scatter_small(jnp.concatenate([vec_small, qkv_small, up_small], axis=1), flat)
        vec_own = own[: cuts[1]].reshape(5, -1)
        qkv_bias_grad = own[cuts[1] : cuts[2]].reshape(b_qkv.shape)
        up_bias_grad = own[cuts[2] : cuts[3]].reshape(b_fc1.shape)

        up_total = jnp.zeros(w_fc1.shape, F32)
        down_total = jnp.zeros(w_fc2.shape, F32)
        for k in range(INNER):
            at = (inner ^ k) * hidden_here
            up_sum = sum(up_back[s].astype(F32) for s in range(k, dp_n, INNER))
            down_sum = sum(down_back[s].astype(F32) for s in range(k, dp_n, INNER))
            up_total = lax.dynamic_update_slice(up_total, up_sum, (0, at))
            down_total = lax.dynamic_update_slice(down_total, down_sum, (at, 0))
        att_sum = [sum(att_back[s].astype(F32) for s in range(k, dp_n, 2)) for k in range(2)]
        odd = inner % 2 == 1
        att_first = jnp.where(odd, att_sum[1], att_sum[0])
        att_second = jnp.where(odd, att_sum[0], att_sum[1])
        qkv_total = jnp.concatenate([att_first[:, : 3 * HD], att_second[:, : 3 * HD]], axis=1)
        out_total = jnp.concatenate([att_first[:, 3 * HD :].T, att_second[:, 3 * HD :].T], axis=0)
        return (
            block_output, input_grad, qkv_total, qkv_bias_grad, out_total, vec_own[4],
            up_total, up_bias_grad, down_total, vec_own[4],
            vec_own[0], vec_own[1], vec_own[2], vec_own[3],
        )

    def on_device_fused(
        block_input, segment_ids, w_qkv, b_qkv, w_out, b_out, w_fc1, b_fc1, w_fc2, b_fc2,
        ln1_gain, ln1_bias, ln2_gain, ln2_bias, cotangent,
    ):
        d = lax.axis_index("dp")
        t = lax.axis_index("tp")
        flat = d * tp_n + t
        inner = d % INNER
        core = t % 2
        lead = (inner // 2) == core
        rows, width = block_input.shape
        depth = w_qkv.shape[0]
        hidden_here = w_fc1.shape[1] // INNER
        head_here = w_out.shape[0] // HD
        heads = head_here * tp_n
        quarter = SEQ // tp_n
        qkv_bits = b_qkv.shape[1]

        up_rows, up_cols = b_fc1.shape
        per = up_rows // INNER
        seg_part = lax.dynamic_slice(segment_ids.reshape(-1), (t * quarter,), (quarter,))
        two = lambda v: jnp.concatenate([v, v])
        vec_rows = [two(v) for v in (ln1_gain, ln1_bias, ln2_gain, ln2_bias, b_out + b_fc2)]
        spot = (jnp.arange(dp_n) == d).astype(F32)
        up_spread = (b_fc1.reshape(INNER, per, 1, up_cols) * spot[None, None, :, None]).reshape(2, 8, 128)
        qkv_spread = (b_qkv[:, None, :] * spot[None, :, None]).reshape(1, 8, 128)
        first = jnp.stack(vec_rows + [seg_part.astype(F32), jnp.zeros(128, F32), jnp.zeros(128, F32)])
        payload = jnp.concatenate([first[None], up_spread, qkv_spread])
        angle = np.arange(SEQ)[:, None] * np.exp(np.arange(ROT // 2) * (-2.0 * math.log(10000.0) / ROT))
        pad = np.zeros((SEQ, 128 - ROT))
        cosine = np.concatenate([np.cos(angle), np.cos(angle), pad + 1.0], axis=1)
        sine = np.concatenate([np.sin(angle), np.sin(angle), pad], axis=1)
        rope = jnp.asarray(np.stack([cosine, sine]), F32)
        like = lambda *shape: jax.ShapeDtypeStruct(shape, BF16)
        wide_f = lambda *shape: jax.ShapeDtypeStruct(shape, F32)
        dma = pltpu.SemaphoreType.DMA
        vb = lambda *shape: pltpu.VMEM(shape, BF16)
        vf = lambda *shape: pltpu.VMEM(shape, F32)
        any_spec = pl.BlockSpec(memory_space=pl.ANY)
        group = 16 * rows
        per_peer = dma((2, dp_n))
        pair = 2 * SEQ
        results = pl.pallas_call(
            functools.partial(fused_kernel, dp_n, tp_n),
            out_shape=(
                like(rows, width), wide_f(rows, width), wide_f(*w_fc1.shape), wide_f(*w_fc2.shape),
                wide_f(*w_qkv.shape), wide_f(*w_out.shape), wide_f(4, 8, 128),
                like(hidden_here, width), like(hidden_here, width),
                like(hidden_here, width), like(hidden_here, width), like(4 * HD, width),
            ),
            in_specs=[any_spec] * 8,
            out_specs=(any_spec,) * 12,
            scratch_shapes=[
                vb(group, width), vb(group, width), vb(group, width),
                vb(hidden_here, width), vb(hidden_here, width), vf(hidden_here, group),
                vb(hidden_here, group), vb(hidden_here, group), vb(3, hidden_here, depth),
                vf(group, 128), vf(8, width), vf(8, width), vf(hidden_here, 128),
                vb(width, 3 * HD), vb(HD, width), vb(pair, width),
                vb(pair, HD), vb(pair, HD), vb(pair, HD), vb(pair, SEQ),
                vb(pair, HD), vb(HD, pair), vb(pair, HD), vb(pair, 3 * HD), vb(3 * HD, pair),
                vb(4 * HD, width), vf(2, SEQ, 128), vf(4, 8, 128), vf(devices, 8, 128), vf(dp_n, 8, 128), vf(2 * dp_n, 8, 128),
                vf(devices, 8, 128), vf(dp_n, 8, 128), vf(2 * dp_n, 8, 128), vf(8, 128), vf(8, 128),
                vf(8, SEQ), vf(SEQ, 128), vf(8, 2 * HD), vf(8, 2 * HD),
                dma((2, 16)), dma((2, 16)), per_peer, per_peer, per_peer, per_peer, per_peer, per_peer,
                dma((3,)), dma((3,)), dma((2,)), dma((2,)), dma((2 * dp_n,)), dma((2 * dp_n,)),
                per_peer, per_peer, dma((3,)),
                dma((2, 16)), dma((2, 16)), dma((8,)), dma((8,)), dma((dp_n,)), dma((dp_n,)),
                dma((24,)), dma((24,)), pltpu.SemaphoreType.REGULAR((6,)),
            ],
            compiler_params=pltpu.CompilerParams(
                collective_id=0, has_side_effects=True, vmem_limit_bytes=67_000_000
            ),
            name="fused_block",
        )(block_input, cotangent, w_fc1, w_fc2, w_qkv, w_out, payload, rope)
        block_output, input_grad, up_total, down_total, qkv_total, out_total, tail = results[:7]
        vec_own = lax.dynamic_slice(tail[0, :5], (0, (flat % 2) * 64), (5, 64))
        up_bias_grad = lax.dynamic_slice(
            tail[1:3].reshape(up_rows, -1), (0, d * up_cols), (up_rows, up_cols)
        )
        qkv_bias_grad = lax.dynamic_slice(
            tail[3].reshape(head_here, -1), (0, d * qkv_bits), (head_here, qkv_bits)
        )
        return (
            block_output, input_grad, qkv_total, qkv_bias_grad, out_total, vec_own[4],
            up_total, up_bias_grad, down_total, vec_own[4],
            vec_own[0], vec_own[1], vec_own[2], vec_own[3],
        )

    row, vec = P(AXES, None), P(AXES)
    col, low = P("dp", "tp"), P("tp", "dp")
    def choose(*arrays):
        wide = arrays[2].shape[0] % 128 == 0
        return (on_device_fused if wide else on_device)(*arrays)

    return jax.shard_map(
        choose,
        mesh=mesh,
        in_specs=(row, P("dp", None), col, low, low, vec, col, low, low, vec, vec, vec, vec, vec, row),
        out_specs=(row, row, col, low, low, vec, col, low, low, vec, vec, vec, vec, vec),
        check_vma=False,
    )
```

```python
import functools
import math

import jax
import jax.numpy as jnp
import numpy as np
from jax import lax
from jax.experimental import pallas as pl
from jax.experimental.pallas import tpu as pltpu
from jax.sharding import PartitionSpec as P

HD = 256
ROT = 64
SEQ = 512
INNER = 4
EPS = 1e-05
NEG_FILL = -1e30
F32 = jnp.float32
BF16 = jnp.bfloat16
AXES = ("dp", "tp")
MESH = pl.DeviceIdType.MESH
PAY = 1024


def dot(left, right, contract):
    return lax.dot_general(left, right, (contract, ((), ())), preferred_element_type=F32)


def mm(left, right):
    return dot(left, right, ((1,), (0,)))


def mm_tail(left, right):
    return dot(left, right, ((1,), (1,)))


def mm_lead(left, right):
    return dot(left, right, ((0,), (0,)))


def gelu_half(pre_act):
    return 0.5 * (1.0 + jax.scipy.special.erf(pre_act * 2.0 ** (-0.5)))


def gelu_slope(pre_act):
    return gelu_half(pre_act) + pre_act * jnp.exp(-0.5 * pre_act * pre_act) * (2.0 * math.pi) ** (-0.5)


def rotate(block, cosine, sine):
    half = ROT // 2
    lower, upper = block[..., :half], block[..., half:ROT]
    return jnp.concatenate(
        [lower * cosine - upper * sine, upper * cosine + lower * sine, block[..., ROT:]], axis=-1
    )


def gather_kernel(
    dp_n, tp_n, wide,
    x_ref, cot_ref, fc1_ref, fc2_ref, qkv_ref, out_ref, pay_ref,
    xs_ref, cots_ref, up_ref, down_ref, att_ref, proj_ref, small_ref,
    row_send, row_recv, mlp_send, mlp_recv, att_send, att_recv, pass_send, pass_recv,
    small_send, small_recv, local_sem,
):
    d = lax.axis_index("dp")
    t = lax.axis_index("tp")
    inner = d % INNER
    core = t % 2
    depth = fc1_ref.shape[0]
    hidden = fc1_ref.shape[1] // INNER

    barrier = pltpu.get_barrier_semaphore()
    for s in range(1, dp_n):
        pl.semaphore_signal(barrier, inc=1, device_id=(d ^ s, t), device_id_type=MESH)
    for k in (1, 2):
        pl.semaphore_signal(barrier, inc=1, device_id=(d, t ^ k), device_id_type=MESH)

    def remote(src, dst, send_sem, recv_sem, dp_xor, tp_xor):
        return pltpu.make_async_remote_copy(
            src_ref=src, dst_ref=dst, send_sem=send_sem, recv_sem=recv_sem,
            device_id=(d ^ dp_xor, t ^ tp_xor), device_id_type=MESH,
        )

    hop = {1: (2, 0), 2: (1, 0), 4: (0, 2), 8: (0, 1)}
    pairs = ((x_ref, xs_ref), (cot_ref, cots_ref))

    def row_copy(a, k, bit):
        own, full = pairs[a]
        src = own if k == 0 else full.at[k]
        return remote(src, full.at[k + bit], row_send.at[a, k + bit], row_recv.at[a, k + bit], *hop[bit])

    def columns(ref, index, size):
        return ref.at[:, pl.ds(pl.multiple_of(index * size, 128), size)]

    def lines(ref, index, size):
        return ref.at[pl.ds(pl.multiple_of(index * size, 8), size), :]

    def across(ref, index, size):
        return columns(ref, index, size) if wide else ref.at[index]

    def mlp_copies(s):
        target = inner ^ (s % INNER)
        return (
            (columns(fc1_ref, target, hidden), lines(up_ref, d, depth)),
            (lines(fc2_ref, target, hidden), across(down_ref, d, depth)),
        )

    def att_copies(s):
        target = (inner ^ (s % INNER)) % 2
        return (
            (columns(qkv_ref, target, 3 * HD), lines(att_ref, d, depth)),
            (lines(out_ref, target, HD), across(proj_ref, d, depth)),
        )

    def att_land(s):
        return (lines(att_ref, d ^ s, depth), across(proj_ref, d ^ s, depth))

    def mlp_land(s):
        return (lines(up_ref, d ^ s, depth), across(down_ref, d ^ s, depth))

    local = []
    def stay(src, dst):
        copy = pltpu.make_async_copy(src, dst, local_sem.at[len(local)])
        copy.start()
        local.append(copy)

    lead = (inner // 2) == core
    pltpu.sync_copy(pay_ref, small_ref.at[0])
    pl.semaphore_wait(barrier, dp_n + 1)

    started = []
    def start(copy):
        copy.start()
        started.append(copy)

    def start_rows(k, bit):
        for a in range(2):
            start(row_copy(a, k, bit))

    def wait_rows(k):
        bit = 1
        while bit * 2 <= k:
            bit *= 2
        for a in range(2):
            row_copy(a, k - bit, bit).wait_recv()

    def start_mlp(s):
        for a, (src, dst) in enumerate(mlp_copies(s)):
            start(remote(src, dst, mlp_send.at[a, s], mlp_recv.at[a, s], s, 0))

    def att_active(s):
        return ((inner ^ (s % INNER)) // 2) == core

    def start_att(s):
        @pl.when(att_active(s))
        def _():
            for a, (src, dst) in enumerate(att_copies(s)):
                remote(src, dst, att_send.at[a, s], att_recv.at[a, s], s, 0).start()

    def pass_att(s):
        lands = att_land(s)
        return [
            remote(land, land, pass_send.at[a, s], pass_recv.at[a, s], 0, 1)
            for a, land in enumerate(lands)
        ]

    def small_copy(step, dp_xor, tp_xor, n):
        return remote(
            small_ref.at[pl.ds(0, n)], small_ref.at[pl.ds(n, n)],
            small_send.at[step], small_recv.at[step], dp_xor, tp_xor,
        )

    hops = []
    n = 1
    while n < dp_n * tp_n:
        hops.append((n // tp_n, n % tp_n, n))
        n *= 2
    even = [s for s in range(2, dp_n, 2)]
    even.sort(key=lambda s: -(s >= INNER))
    odd = [s for s in range(1, dp_n, 2)]
    odd.sort(key=lambda s: -(s >= INNER))

    small = [small_copy(k, *h) for k, h in enumerate(hops)]
    small[0].start()
    for bit in (1, 2, 4):
        start_rows(0, bit)
    start_rows(0, 8)
    for s in even:
        start_mlp(s)
    stay(x_ref, xs_ref.at[0])
    stay(cot_ref, cots_ref.at[0])
    for src, dst in mlp_copies(0):
        stay(src, dst)

    @pl.when(lead)
    def _():
        for a, (src, dst) in enumerate(att_copies(0)):
            copy = pltpu.make_async_copy(src, dst, local_sem.at[4 + a])
            copy.start()

    for k in range(len(small)):
        small[k].wait_recv()
        if k + 1 < len(small):
            small[k + 1].start()
    wait_rows(1)
    start_rows(1, 2)
    start_rows(1, 4)
    start_rows(1, 8)
    wait_rows(2)
    start_rows(2, 4)
    start_rows(2, 8)
    for s in odd:
        start_mlp(s)
    for s in even + odd:
        start_att(s)
    wait_rows(3)
    start_rows(3, 4)
    start_rows(3, 8)
    wait_rows(4)
    start_rows(4, 8)

    @pl.when(lead)
    def _():
        for a, (src, dst) in enumerate(att_copies(0)):
            pltpu.make_async_copy(src, dst, local_sem.at[4 + a]).wait()
        for copy in pass_att(0):
            copy.start()

    for k in (5, 6, 7):
        wait_rows(k)
        start_rows(k, 8)
    for k in range(8, 16):
        wait_rows(k)
    for s in even + odd:
        for a, dst in enumerate(mlp_land(s)):
            remote(dst, dst, mlp_send.at[a, s], mlp_recv.at[a, s], s, 0).wait_recv()
    for s in even + odd:
        @pl.when(lead)
        def _():
            for a, dst in enumerate(att_land(s)):
                remote(dst, dst, att_send.at[a, s], att_recv.at[a, s], s, 0).wait_recv()
            for copy in pass_att(s):
                copy.start()

    @pl.when(jnp.logical_not(lead))
    def _():
        for s in range(dp_n):
            for copy in pass_att(s):
                copy.wait_recv()

    @pl.when(lead)
    def _():
        for s in range(dp_n):
            for copy in pass_att(s):
                copy.wait_send()

    for s in range(1, dp_n):
        @pl.when(att_active(s))
        def _():
            for a, (src, dst) in enumerate(att_copies(s)):
                remote(src, dst, att_send.at[a, s], att_recv.at[a, s], s, 0).wait_send()
    for copy in started:
        copy.wait_send()
    for copy in small:
        copy.wait_send()
    for copy in local:
        copy.wait()


def span(start, size, unit):
    return pl.ds(start if isinstance(start, int) else pl.multiple_of(start, unit), size)


def lane_cut(ref, start, size):
    return ref.at[:, span(start, size, 128)]


def row_cut(ref, start, size):
    return ref.at[span(start, size, 16), :]


def columns_of(rows8):
    pad = jnp.zeros((120, 128), F32)
    return jnp.transpose(jnp.concatenate([rows8, pad], axis=0))


def fused_kernel(
    dp_n, tp_n,
    x_ref, cot_ref, fc1_ref, fc2_ref, qkv_ref, out_ref, rope_ref,
    vec0_ref, vec1_ref, vec2_ref, vec3_ref, vec4_ref, vec5_ref, bq_ref, bf_ref, seg_ref,
    block_out, input_out, tail_out,
    gu_hbm, gd_hbm, ru_hbm, rd_hbm, ra_hbm, pair_hbm,
    xs, cots, n2, up_t, down_w, pre, hid_t, act_t, ring, stats, vecs, sums, up_sum,
    att_w, proj_w, n1, q_s, k_s, v_s, prob, ctx, ctx_t, cctx, low, low_t, gx,
    rope, raw, raw_q, raw_f, raw_seg, wide_f, pay, vec_in, bias_in, head_in, vec_back, bias_back, head_back, up_place, head_place,
    keys, queries, qkv_bias, qkv_sum,
    row_send, row_recv, mlp_send, mlp_recv, att_send, att_recv, pass_send, pass_recv,
    small_send, small_recv, back_send, back_recv, headb_send, headb_recv, g_send, g_recv, g_local,
    rs_send, rs_recv, pair_send, pair_recv, ga_send, ga_recv,
    local_sem, out_sem, credit,
):
    d = lax.axis_index("dp")
    t = lax.axis_index("tp")
    flat = d * tp_n + t
    inner = d % INNER
    core = t % 2
    lead = (inner // 2) == core
    follow = jnp.logical_not(lead)
    rows, width = x_ref.shape
    depth = fc1_ref.shape[0]
    hidden = fc1_ref.shape[1] // INNER
    devices = dp_n * tp_n
    slots = 16
    tokens = slots * rows
    scale = HD ** (-0.5)
    chunk = 512

    barrier = pltpu.get_barrier_semaphore()
    for a in range(1, devices):
        peer = (d ^ (a // tp_n), t ^ (a % tp_n))
        pl.semaphore_signal(barrier, inc=1, device_id=peer, device_id_type=MESH)

    def remote(src, dst, send_sem, recv_sem, dp_xor, tp_xor):
        return pltpu.make_async_remote_copy(
            src_ref=src, dst_ref=dst, send_sem=send_sem, recv_sem=recv_sem,
            device_id=(d ^ dp_xor, t ^ tp_xor), device_id_type=MESH,
        )

    started = []

    def start(copy):
        copy.start()
        started.append(copy)

    hop = {1: (2, 0), 2: (1, 0), 4: (0, 2), 8: (0, 1)}

    def slot(ref, k):
        return row_cut(ref, k * rows, rows)

    def row_copy(a, k, bit):
        own, full = ((x_ref, xs), (cot_ref, cots))[a]
        src = own if k == 0 else slot(full, k)
        return remote(
            src, slot(full, k + bit), row_send.at[a, k + bit], row_recv.at[a, k + bit], *hop[bit]
        )

    row_started = ([], [])

    def start_row(a, k, *bits):
        for bit in bits:
            copy = row_copy(a, k, bit)
            copy.start()
            row_started[a].append(copy)

    def wait_row(a, k):
        bit = 1
        while bit * 2 <= k:
            bit *= 2
        row_copy(a, k - bit, bit).wait_recv()

    def w1_piece(i):
        return gx.at[depth : depth + hidden, pl.ds(pl.multiple_of(i * depth, 128), depth)]

    def mlp_copy(a, s):
        target = inner ^ (s % INNER)
        src = w1_piece(target) if a == 0 else row_cut(fc2_ref, target * hidden, hidden)
        dst = lane_cut((up_t, down_w)[a], d * depth, depth)
        if s == 0:
            return src, dst
        return remote(src, dst, mlp_send.at[a, s], mlp_recv.at[a, s], s, 0)

    mlp_started = tuple([mlp_copy(a, s) for s in range(1, dp_n)] for a in range(2))

    def start_mlp(a, s):
        mlp_started[a][s - 1].start()

    def mlp_wait(a, s):
        dst = lane_cut((up_t, down_w)[a], (d ^ s) * depth, depth)
        remote(dst, dst, mlp_send.at[a, s], mlp_recv.at[a, s], s, 0).wait_recv()

    def att_active(s):
        return ((inner ^ (s % INNER)) // 2) == core

    def att_pairs(s):
        target = (inner ^ (s % INNER)) % 2
        return (
            (lane_cut(qkv_ref, target * 3 * HD, 3 * HD), row_cut(att_w, d * depth, depth)),
            (row_cut(out_ref, target * HD, HD), lane_cut(proj_w, d * depth, depth)),
        )

    def att_land(s):
        return (row_cut(att_w, (d ^ s) * depth, depth), lane_cut(proj_w, (d ^ s) * depth, depth))

    def start_att(s):
        @pl.when(att_active(s))
        def _():
            for a, (src, dst) in enumerate(att_pairs(s)):
                remote(src, dst, att_send.at[a, s], att_recv.at[a, s], s, 0).start()

    def pass_att(s):
        return [
            remote(land, land, pass_send.at[a, s], pass_recv.at[a, s], 0, 1)
            for a, land in enumerate(att_land(s))
        ]

    local = []

    def stay(src, dst):
        copy = pltpu.make_async_copy(src, dst, local_sem.at[len(local)])
        copy.start()
        local.append(copy)
        return copy

    fc1_in = stay(fc1_ref, gx.at[0:depth, :])
    raw_in = [
        stay(ref, raw.at[k])
        for k, ref in enumerate((vec0_ref, vec1_ref, vec2_ref, vec3_ref, vec4_ref, vec5_ref))
    ]
    raw_in += [stay(bq_ref, raw_q), stay(bf_ref, raw_f), stay(seg_ref, raw_seg)]
    x_in = stay(x_ref, slot(xs, 0))
    cot_in = stay(cot_ref, slot(cots, 0))
    down_in = stay(*mlp_copy(1, 0))
    rope_in = stay(rope_ref, rope)
    for copy in raw_in:
        copy.wait()
    zero64 = jnp.zeros((1, 64), F32)
    line = lax.broadcasted_iota(jnp.int32, (8, 128), 0)

    def wide(row):
        return jnp.broadcast_to(jnp.concatenate([row, zero64], axis=1), (8, 128))

    def onto(base, row, value):
        return jnp.where(line == row, value, base)

    odd_flat = flat % 2 == 1
    group = jnp.zeros((8, 128), F32)
    for k in range(5):
        row = raw[k] if k < 4 else raw[4] + raw[5]
        value = wide(row)
        group = onto(group, k, jnp.where(odd_flat, pltpu.roll(value, 64, 1), value))
    seg_row = raw_seg[:, pl.ds(pl.multiple_of(t * 128, 128), 128)].astype(F32)
    pay[0] = onto(group, 5, jnp.broadcast_to(seg_row, (8, 128)))
    group = jnp.zeros((8, 128), F32)
    for k in range(2):
        value = wide(raw_q[k : k + 1, :])
        value = jnp.where(d % 2 == 1, pltpu.roll(value, 64, 1), value)
        group = onto(group, k * 4 + d // 2, value)
    pay[3] = group
    up_lines, up_spots = raw_f.shape
    flat_f = jnp.concatenate([raw_f[...], jnp.zeros((up_lines, 128 - up_spots), F32)], axis=1)
    value = pltpu.roll(columns_of(flat_f)[:up_spots], d * up_lines, 1)
    odd_row = lax.broadcasted_iota(jnp.int32, value.shape, 0) % 2 == 1
    wide_f[...] = jnp.where(odd_row, pltpu.roll(value, 64, 1), value)
    merged = wide_f[pl.ds(0, 16, stride=2), :] + wide_f[pl.ds(1, 16, stride=2), :]
    pay[1] = merged[:8]
    pay[2] = merged[8:]
    pl.semaphore_wait(barrier, devices - 1)

    even = sorted(range(2, dp_n, 2), key=lambda s: -(s >= INNER))
    odd = sorted(range(1, dp_n, 2), key=lambda s: -(s >= INNER))

    def small_copy(kind, src, dst, dp_xor, tp_xor):
        return remote(src, dst, small_send.at[kind], small_recv.at[kind], dp_xor, tp_xor)

    for a in range(1, devices):
        small_copy(0, pay.at[0], vec_in.at[a], a // tp_n, a % tp_n).start()
    for s in range(1, dp_n):
        group = 1 + (inner ^ (s % INNER)) // 2
        small_copy(1, pay.at[group], bias_in.at[s], s, 0).start()
    for k in range(1, 2 * dp_n):
        small_copy(2, pay.at[3], head_in.at[k], k // 2, k % 2).start()
    start_row(0, 0, 1, 2, 4, 8)
    start_row(1, 0, 1, 8)
    vec_in[0] = pay[0]
    bias_in[0] = pay[1 + inner // 2]
    head_in[0] = pay[3]
    fc1_in.wait()
    for i in range(INNER):
        piece = gx[0:depth, i * hidden : (i + 1) * hidden].astype(F32)
        gx[depth : depth + hidden, i * depth : (i + 1) * depth] = jnp.transpose(piece).astype(BF16)
    near = [2, 3]
    far = [s for s in (6, 4, 7, 5) if s < dp_n]
    plane = d // 2
    end = (plane == 0) | (plane == dp_n // 2 - 1)
    middle = jnp.logical_not(end)

    def start_all(s):
        start_att(s)
        start_mlp(0, s)
        start_mlp(1, s)

    start_att(2)
    for s in far:
        start_att(s)
    start_mlp(0, 2)
    start_mlp(1, 2)

    @pl.when(end)
    def _():
        start_all(3)

    for s in far:
        start_mlp(0, s)

    @pl.when(end)
    def _():
        for s in far:
            start_mlp(1, s)

    up_in = stay(*mlp_copy(0, 0))

    @pl.when(lead)
    def _():
        for a, (src, dst) in enumerate(att_pairs(0)):
            pltpu.make_async_copy(src, dst, local_sem.at[20 + a]).start()

    wait_row(0, 1)
    start_row(0, 1, 2, 4, 8)
    wait_row(0, 2)
    start_row(0, 2, 4, 8)
    start_row(1, 0, 2)

    def small_waits(kind):
        buf = (vec_in, bias_in, head_in)[kind]
        rest = buf.at[pl.ds(1, buf.shape[0] - 1)]
        return small_copy(kind, rest, rest, 0, 1)

    for kind in range(3):
        small_waits(kind).wait_recv()
    half = lax.broadcasted_iota(jnp.int32, (8, 128), 1) < 64
    for j in range(devices // 2):
        left = vec_in[flat ^ (2 * j)]
        right = vec_in[flat ^ (2 * j + 1)]
        vecs[:, j * 128 : (j + 1) * 128] = jnp.where(half, left, right)
    bias8 = jnp.zeros((8, 128), F32)
    head8 = jnp.zeros((8, 128), F32)
    head_rel = core ^ (inner // 2)
    for s in range(dp_n):
        bias8 = bias8 + bias_in[s]
        head8 = head8 + head_in[s * 2 + head_rel]
    second = inner % 2 == 1
    bias_t = columns_of(bias8)
    up_bias = jnp.concatenate(
        [jnp.where(second, bias_t[:, 4 + k : 5 + k], bias_t[:, k : k + 1]) for k in range(4)], axis=0
    )
    head4 = jnp.where(second, head8[4:], head8[:4])
    qkv_bias[0:1, :] = jnp.concatenate([head4[k : k + 1] for k in range(4)], axis=1)
    lane = lax.broadcasted_iota(jnp.int32, (1, 128), 1)
    keys[...] = jnp.zeros_like(keys)
    for q in range(4):
        at = slice(q * 128, (q + 1) * 128)
        keys[0:1, at] = ((t ^ ((q % 2) * 2 + q // 2)) * 128 + lane).astype(F32)
        for dy in range(2):
            peer = (core * 2 + dy) * tp_n + (q % 2) * 2 + q // 2
            keys[1 + dy : 2 + dy, at] = vec_in[peer][5:6, :]
        queries[at, :] = columns_of(keys[:, at])

    def norm_slot(k):
        @pl.loop(0, rows // 16)
        def _(j):
            at = pl.ds(pl.multiple_of(k * rows + j * 16, 16), 16)
            value = xs[at, :].astype(F32)
            mean = jnp.mean(value, axis=-1, keepdims=True)
            centered = value - mean
            inv = lax.rsqrt(jnp.mean(centered * centered, axis=-1, keepdims=True) + EPS)
            n2[at, :] = (centered * inv * vecs[2:3, :] + vecs[3:4, :]).astype(BF16)
            stats[at, 0:64] = jnp.broadcast_to(mean, (16, 64))
            stats[at, 64:128] = jnp.broadcast_to(inv, (16, 64))

    x_in.wait()
    norm_slot(0)
    wait_row(0, 3)
    start_row(0, 3, 4, 8)
    start_row(1, 0, 4)
    for k in (1, 2, 3):
        norm_slot(k)
    wait_row(1, 1)
    start_row(1, 1, 2, 4, 8)
    wait_row(1, 2)
    start_row(1, 2, 4, 8)

    @pl.when(middle)
    def _():
        start_all(3)

    start_all(1)
    for k in (4, 5, 6, 7):
        wait_row(0, k)
        start_row(0, k, 8)
        norm_slot(k)

    @pl.when(middle)
    def _():
        for s in far:
            start_mlp(1, s)

    for k in range(8, 16):
        wait_row(0, k)
        norm_slot(k)
    wait_row(1, 3)
    start_row(1, 3, 4, 8)

    def mine(dy, q):
        return ((q // 2) * 8 + (q % 2) * 4 + dy * 2 + core) * rows

    for dy in range(2):
        for q in range(4):
            @pl.loop(0, rows // 16)
            def _(j):
                at = pl.ds(pl.multiple_of(mine(dy, q) + j * 16, 16), 16)
                to = pl.ds(pl.multiple_of(dy * SEQ + q * rows + j * 16, 16), 16)
                normed = (xs[at, :].astype(F32) - stats[at, 0:1]) * stats[at, 64:65]
                n1[to, :] = (normed * vecs[0:1, :] + vecs[1:2, :]).astype(BF16)

    @pl.when(lead)
    def _():
        for a, (src, dst) in enumerate(att_pairs(0)):
            pltpu.make_async_copy(src, dst, local_sem.at[20 + a]).wait()
        for copy in pass_att(0):
            copy.start()
        for s in near + [1] + far:
            for a, dst in enumerate(att_land(s)):
                remote(dst, dst, att_send.at[a, s], att_recv.at[a, s], s, 0).wait_recv()
            for copy in pass_att(s):
                copy.start()

    @pl.when(follow)
    def _():
        for s in range(dp_n):
            for copy in pass_att(s):
                copy.wait_recv()

    rope_in.wait()
    lanes128 = lax.broadcasted_iota(jnp.int32, (SEQ, 128), 1)

    def rope_tables(sign):
        at = [pl.ds(pl.multiple_of((t ^ ((q % 2) * 2 + q // 2)) * 128, 128), 128) for q in range(4)]
        cosine = jnp.concatenate([rope[0, a, :] for a in at], axis=0)
        sine = jnp.concatenate([rope[1, a, :] for a in at], axis=0) * sign
        lower = jnp.where(lanes128 < ROT // 2, -sine, 0.0)
        upper = jnp.where((lanes128 >= ROT // 2) & (lanes128 < ROT), sine, 0.0)
        return cosine, lower, upper

    def turn(value, tables):
        cosine, lower, upper = tables
        head = value[:, :128]
        head = (
            head * cosine
            + pltpu.roll(head, 128 - ROT // 2, 1) * lower
            + pltpu.roll(head, ROT // 2, 1) * upper
        )
        return jnp.concatenate([head, value[:, 128:]], axis=1)

    @pl.loop(0, 2)
    def _(dy):
        at = pl.ds(pl.multiple_of(dy * SEQ, SEQ), SEQ)
        tables = rope_tables(1.0)
        rows_in = n1[at, :]
        value = mm(rows_in, att_w[:, :HD]) + qkv_bias[0:1, :HD]
        query = turn(value, tables).astype(BF16)
        key = turn(mm(rows_in, att_w[:, HD : 2 * HD]), tables).astype(BF16)
        val = (mm(rows_in, att_w[:, 2 * HD :]) + qkv_bias[0:1, HD:]).astype(BF16)
        q_s[at, :] = query
        k_s[at, :] = key
        v_s[at, :] = val
        seg_q = jnp.where(dy == 0, queries[:, 1:2], queries[:, 2:3])
        seg_k = jnp.where(dy == 0, keys[1:2, :], keys[2:3, :])
        allowed = (keys[0:1, :] <= queries[:, 0:1]) & (seg_q == seg_k)
        scores = jnp.where(allowed, mm_tail(query, key) * scale, NEG_FILL)
        peak = jnp.max(scores, axis=-1, keepdims=True)
        total = jnp.where(allowed, jnp.exp(scores - peak), 0.0)
        share = (total / jnp.sum(total, axis=-1, keepdims=True)).astype(BF16)
        prob[at, :] = share
        got = mm(share, val)
        ctx[at, :] = got.astype(BF16)
        ctx_t[:, at] = jnp.transpose(got).astype(BF16)

    def cot_mine(dy, lanes):
        parts = [cots[pl.ds(pl.multiple_of(mine(dy, q), 128), rows), lanes] for q in range(4)]
        return jnp.concatenate(parts, axis=0)

    for k in (4, 5, 6, 7):
        wait_row(1, k)
        start_row(1, k, 8)
    cot_in.wait()
    for k in range(8, 16):
        wait_row(1, k)
    sums[...] = jnp.zeros_like(sums)

    @pl.loop(0, rows // 16)
    def _(j):
        at = pl.ds(pl.multiple_of(j * 16, 16), 16)
        sums[4:5, :] += jnp.sum(cots[at, :].astype(F32), axis=0, keepdims=True)

    for dy in range(2):
        cctx[dy * SEQ : (dy + 1) * SEQ, :] = mm_tail(cot_mine(dy, slice(None)), proj_w[...]).astype(BF16)

    @pl.loop(0, width // chunk)
    def _(c):
        lanes = pl.ds(pl.multiple_of(c * chunk, chunk), chunk)
        both = jnp.concatenate([cot_mine(0, lanes), cot_mine(1, lanes)], axis=0)
        gx[3 * HD : 4 * HD, lanes] = mm(ctx_t[...], both).astype(BF16)

    qkv_sum[...] = jnp.zeros_like(qkv_sum)

    def backward(dy):
        at = slice(dy * SEQ, (dy + 1) * SEQ)
        tables = rope_tables(-1.0)
        share = prob[at, :].astype(F32)
        got = cctx[at, :]
        delta = jnp.sum(got.astype(F32) * ctx[at, :].astype(F32), axis=-1, keepdims=True)
        score_cot = share * (mm_tail(got, v_s[at, :]) - delta)
        value_cot = mm(jnp.transpose(share).astype(BF16), got)
        query_cot = turn(mm(score_cot.astype(BF16), k_s[at, :]) * scale, tables)
        key_cot = turn(mm(jnp.transpose(score_cot).astype(BF16), q_s[at, :]) * scale, tables)
        qkv_sum[0:1, :HD] += jnp.sum(query_cot, axis=0, keepdims=True)
        qkv_sum[0:1, HD:] += jnp.sum(value_cot, axis=0, keepdims=True)
        for k, part in enumerate((query_cot, key_cot, value_cot)):
            low[at, k * HD : (k + 1) * HD] = part.astype(BF16)
            low_t[k * HD : (k + 1) * HD, at] = jnp.transpose(part).astype(BF16)

    backward(0)
    backward(1)

    up_in.wait()
    for copy in mlp_started[0]:
        copy.wait_send()

    @pl.loop(0, width // chunk)
    def _(c):
        lanes = pl.ds(pl.multiple_of(c * chunk, chunk), chunk)
        gx[0 : 3 * HD, lanes] = mm(low_t[...], n1[:, lanes]).astype(BF16)

    def pair_copy(s):
        return remote(
            lane_cut(gx, (d ^ s) * depth, depth), pair_hbm.at[:, s * depth : (s + 1) * depth],
            pair_send.at[s], pair_recv.at[s], 0, 1,
        )

    @pl.when(follow)
    def _():
        for s in near + [1] + far + [0]:
            pair_copy(s).start()

    for dy in range(2):
        @pl.loop(0, width // chunk)
        def _(c):
            lanes = pl.ds(pl.multiple_of(c * chunk, chunk), chunk)
            part = mm_tail(low[dy * SEQ : (dy + 1) * SEQ, :], att_w[lanes, :])
            gain = vecs[0:1, lanes]
            cross = jnp.zeros((1, chunk), F32)
            for q in range(4):
                at = pl.ds(pl.multiple_of(mine(dy, q), 128), rows)
                piece = part[q * rows : (q + 1) * rows]
                normed = (xs[at, lanes].astype(F32) - stats[at, 0:1]) * stats[at, 64:65]
                cross = cross + jnp.sum(piece * normed, axis=0, keepdims=True)
                n1[dy * SEQ + q * rows : dy * SEQ + (q + 1) * rows, lanes] = (piece * gain).astype(BF16)
            sums[0:1, lanes] += cross
            sums[1:2, lanes] += jnp.sum(part, axis=0, keepdims=True)

    def ga_copy(s):
        return remote(
            lane_cut(gx, (d ^ s) * depth, depth), ra_hbm.at[:, s * depth : (s + 1) * depth],
            ga_send.at[s], ga_recv.at[s], s, 0,
        )

    stages = (q_s, k_s, v_s)

    @pl.when(lead)
    def _():
        todo = near + [1] + far + [0]

        def fetch(k):
            s = todo[k]
            land = pair_hbm.at[:, s * depth : (s + 1) * depth]
            remote(land, land, pair_send.at[s], pair_recv.at[s], 0, 1).wait_recv()
            copy = pltpu.make_async_copy(land, stages[k % 3], g_local.at[k % 3])
            copy.start()
            return copy

        held = [fetch(0), fetch(1)]
        for k, s in enumerate(todo):
            if k + 2 < len(todo):
                held.append(fetch(k + 2))
            held[k].wait()
            stage = stages[k % 3]
            here = lane_cut(gx, (d ^ s) * depth, depth)

            @pl.loop(0, 4 * HD // 64)
            def _(i):
                at = pl.ds(pl.multiple_of(i * 64, 64), 64)
                here[at, :] = (here[at, :].astype(F32) + stage[at, :].astype(F32)).astype(BF16)

            if s:
                ga_copy(s).start()
            else:
                pltpu.make_async_copy(here, ra_hbm.at[:, 0:depth], local_sem.at[22]).start()

    for s in near + [1] + far:
        mlp_wait(0, s)

    @pl.loop(0, tokens // chunk)
    def _(j):
        at = pl.ds(pl.multiple_of(j * chunk, chunk), chunk)
        value = mm_tail(up_t[...], n2[at, :]) + up_bias
        pre[:, at] = value
        hid_t[:, at] = (value * gelu_half(value)).astype(BF16)

    def g_send_copy(a, s):
        at = pl.ds(pl.multiple_of(s * depth, 128), depth)
        return remote(
            (gu_hbm, gd_hbm)[a].at[:, at], (ru_hbm, rd_hbm)[a].at[:, at],
            g_send.at[a, s], g_recv.at[a, s], s, 0,
        )

    def g_local_copy(a, s, b, dst):
        at = pl.ds(pl.multiple_of(s * depth, 128), depth)
        return pltpu.make_async_copy(ring.at[b], dst.at[:, at], g_local.at[b])

    def grads(a, go):
        left, right = ((act_t, n2), (hid_t, cots))[a]
        stage, own = ((gu_hbm, ru_hbm), (gd_hbm, rd_hbm))[a]

        def block(s, b):
            at = pl.ds(pl.multiple_of((d ^ s) * depth, 128), depth)
            ring[b] = mm(left[...], right[:, at]).astype(BF16)

        def at_step(k):
            return (k + 1) % (dp_n - 1) + 1

        @pl.loop(0, dp_n - 1)
        def _(k):
            s = at_step(k)
            b = k % 3

            @pl.when(k >= 2)
            def _():
                before = at_step(k - 2)
                g_local_copy(a, before, (k + 1) % 3, stage).wait()
                if go:
                    g_send_copy(a, before).start()

            block(s, b)
            g_local_copy(a, s, b, stage).start()

        last = dp_n - 2
        for k in (last - 1, last):
            s = at_step(k)
            g_local_copy(a, s, k % 3, stage).wait()
            if go:
                g_send_copy(a, s).start()
        b = (last + 1) % 3
        block(0, b)
        copy = g_local_copy(a, 0, b, own)
        copy.start()
        copy.wait()

    grads(1, True)
    down_in.wait()
    for s in near + [1] + far:
        mlp_wait(1, s)
    up_sum[...] = jnp.zeros_like(up_sum)

    @pl.loop(0, tokens // chunk)
    def _(j):
        at = pl.ds(pl.multiple_of(j * chunk, chunk), chunk)
        value = mm_tail(down_w[...], cots[at, :]) * gelu_slope(pre[:, at])
        up_sum[:, 0:1] += jnp.sum(value, axis=1, keepdims=True)
        act_t[:, at] = value.astype(BF16)

    grads(0, False)

    @pl.loop(0, tokens // chunk)
    def _(j):
        at = pl.ds(pl.multiple_of(j * chunk, chunk), chunk)
        act = jnp.transpose(act_t[:, at].astype(F32)).astype(BF16)

        @pl.loop(0, width // chunk)
        def _(c):
            lanes = pl.ds(pl.multiple_of(c * chunk, chunk), chunk)
            part = mm(act, up_t[:, lanes])
            gain = vecs[2:3, lanes]
            cross = jnp.zeros((1, chunk), F32)
            for m in range(4):
                at = pl.ds(pl.multiple_of(j * chunk + m * rows, 128), rows)
                piece = part[m * rows : (m + 1) * rows]
                normed = (xs[at, lanes].astype(F32) - stats[at, 0:1]) * stats[at, 64:65]
                cross = cross + jnp.sum(piece * normed, axis=0, keepdims=True)
                spot = pl.ds(pl.multiple_of((m // 2) * SEQ + j * rows, 128), rows)
                extra = jnp.where(core == m % 2, n1[spot, lanes].astype(F32), 0.0)
                n2[at, lanes] = (piece * gain + extra).astype(BF16)
            sums[2:3, lanes] += cross
            sums[3:4, lanes] += jnp.sum(part, axis=0, keepdims=True)

    for copy in row_started[0]:
        copy.wait_send()
    pl.semaphore_signal(credit.at[0], inc=1, device_id=(d, t ^ 1), device_id_type=MESH)
    pl.semaphore_signal(credit.at[1], inc=1, device_id=(d, t ^ 2), device_id_type=MESH)

    blank = jnp.zeros((4, 128), F32)
    up_rows = [jnp.transpose(up_sum[k * 128 : (k + 1) * 128, :])[0:1] for k in range(4)]
    up_rows = jnp.concatenate(up_rows, axis=0)
    qkv_rows = jnp.concatenate([qkv_sum[0:1, k * 128 : (k + 1) * 128] for k in range(4)], axis=0)

    def place(value):
        return jnp.where(
            second, jnp.concatenate([blank, value], axis=0), jnp.concatenate([value, blank], axis=0)
        )

    up_place[...] = place(up_rows)
    head_place[...] = place(qkv_rows)

    def window(owner):
        return lane_cut(sums, (owner // 2) * 128, 128)

    def back_copy(kind, src, dst, dp_xor, tp_xor):
        return remote(src, dst, back_send.at[kind], back_recv.at[kind], dp_xor, tp_xor)

    def head_copy(s, dc):
        return remote(
            head_place, head_back.at[s * 2 + dc], headb_send.at[s * 2 + dc], headb_recv.at[s * 2 + dc], s, dc
        )

    for a in range(1, devices):
        back_copy(0, window(flat ^ a), vec_back.at[a], a // tp_n, a % tp_n).start()
    for s in range(1, dp_n):
        back_copy(1, up_place, bias_back.at[s], s, 0).start()

    @pl.when(lead)
    def _():
        for s in range(1, dp_n):
            head_copy(s, 0).start()

    @pl.when(follow)
    def _():
        for s in range(dp_n):
            head_copy(s, 1).start()

    bufs = (cots, n2)

    def landing(a, bit, j, there):
        if bit == 8:
            if a == 0:
                side = core if there else 1 - core
                return row_cut(xs, (2 * j + side) * rows, rows)
            return row_cut(n1, j * rows, rows)
        if bit == 4:
            return row_cut((act_t, up_t)[a], j * rows, rows)
        base = (down_w, hid_t)[a]
        return row_cut(base, (j if bit == 2 else 2) * rows, rows)

    def rs_copy(a, bit, j):
        return remote(
            slot(bufs[a], bit + j), landing(a, bit, j, True),
            rs_send.at[a, bit + j], rs_recv.at[a, bit + j], *hop[bit],
        )

    def rs_start(a, bit, j):
        start(rs_copy(a, bit, j))

    def rs_add(a, bit, j):
        land = landing(a, bit, j, False)
        remote(land, land, rs_send.at[a, bit + j], rs_recv.at[a, bit + j], *hop[bit]).wait_recv()
        here = slot(bufs[a], j)

        @pl.loop(0, rows // 16)
        def _(i):
            at = pl.ds(pl.multiple_of(i * 16, 16), 16)
            here[at, :] = (here[at, :].astype(F32) + land[at, :].astype(F32)).astype(BF16)

    for s in near + [1] + far[:2]:
        g_send_copy(0, s).start()

    pl.semaphore_wait(credit.at[0], 1)
    pl.semaphore_wait(credit.at[1], 1)
    for j in (7, 5, 6, 4, 3, 1, 2, 0):
        rs_start(1, 8, j)

    for copy in row_started[1]:
        copy.wait_send()
    for j in range(4):
        for k in {2: (7, 5), 3: (6, 4)}.get(j, ()):
            rs_add(1, 8, k)
            rs_start(1, 4, k - 4)
        hid = jnp.transpose(hid_t[:, j * chunk : (j + 1) * chunk].astype(F32)).astype(BF16)
        here = [ctx[h * SEQ + j * rows : h * SEQ + (j + 1) * rows, :] for h in range(2)]
        here = jnp.concatenate(here, axis=0)

        @pl.loop(0, width // chunk)
        def _(c):
            lanes = pl.ds(pl.multiple_of(c * chunk, chunk), chunk)
            base = mm(hid, down_w[:, lanes])
            extra = mm(here, proj_w[:, lanes])
            for m in range(4):
                more = jnp.where(core == m % 2, extra[(m // 2) * rows : (m // 2 + 1) * rows], 0.0)
                piece = base[m * rows : (m + 1) * rows] + more
                cots[j * chunk + m * rows : j * chunk + (m + 1) * rows, lanes] = piece.astype(BF16)

    for bit in (2, 1):
        dp_xor, tp_xor = hop[bit]
        pl.semaphore_signal(
            credit.at[1 + (3 - bit)], inc=1, device_id=(d ^ dp_xor, t ^ tp_xor), device_id_type=MESH
        )
    own_x = row_cut(hid_t, 3 * rows, rows)
    own_cot = row_cut(down_w, 3 * rows, rows)
    x_again = stay(x_ref, own_x)
    cot_again = stay(cot_ref, own_cot)

    for j in (7, 5, 6, 4, 3, 1, 2, 0):
        rs_start(0, 8, j)
    for j in (3, 1, 2, 0):
        rs_add(1, 8, j)
    for j in (7, 5, 6, 4):
        rs_add(0, 8, j)
        rs_start(0, 4, j - 4)
    for j in (3, 1, 2, 0):
        rs_add(0, 8, j)
    pl.semaphore_wait(credit.at[2], 1)
    pl.semaphore_wait(credit.at[3], 1)

    def rs_tail(a, after):
        rs_add(a, 4, 3)
        rs_start(a, 2, 1)
        rs_add(a, 4, 1)
        rs_add(a, 4, 2)
        rs_start(a, 2, 0)
        rs_add(a, 2, 1)
        rs_start(a, 1, 0)
        after()
        rs_add(a, 4, 0)
        rs_add(a, 2, 0)
        rs_add(a, 1, 0)

    outs = []

    def leave(src, dst):
        copy = pltpu.make_async_copy(src, dst, out_sem.at[len(outs)])
        copy.start()
        outs.append(copy)
        return copy

    def late():
        for s in far[2:]:
            g_send_copy(0, s).start()

    rs_tail(1, late)
    cot_again.wait()
    x_again.wait()

    @pl.loop(0, rows // 16)
    def _(j):
        at = pl.ds(pl.multiple_of(j * 16, 16), 16)
        scaled = n2[at, :].astype(F32)
        inv = stats[at, 64:65]
        normed = (own_x[at, :].astype(F32) - stats[at, 0:1]) * inv
        inner_mean = jnp.mean(scaled, axis=-1, keepdims=True)
        cross = jnp.mean(scaled * normed, axis=-1, keepdims=True)
        pre[at, :] = own_cot[at, :].astype(F32) + inv * (scaled - inner_mean - normed * cross)

    grad_out = leave(pre.at[0:rows, :], input_out)

    @pl.when(lead)
    def _():
        pltpu.make_async_copy(
            lane_cut(gx, d * depth, depth), ra_hbm.at[:, 0:depth], local_sem.at[22]
        ).wait()

    for s in range(1, dp_n):
        @pl.when(att_active(s))
        def _():
            ga_copy(s).wait_recv()

    for s in range(1, dp_n):
        g_send_copy(1, s).wait_recv()
    rs_tail(0, lambda: None)

    @pl.loop(0, rows // 16)
    def _(j):
        at = pl.ds(pl.multiple_of(j * 16, 16), 16)
        total = own_x[at, :].astype(F32) + cots[at, :].astype(F32) + vecs[4:5, :]
        cots[at, :] = total.astype(BF16)

    last = [leave(slot(cots, 0), block_out)]

    def back_waits(kind):
        buf = (vec_back, bias_back)[kind]
        rest = buf.at[pl.ds(1, buf.shape[0] - 1)]
        return back_copy(kind, rest, rest, 0, 1)

    for kind in range(2):
        back_waits(kind).wait_recv()
    for kind in range(3):
        small_waits(kind).wait_send()
    total = window(flat)[...]
    for a in range(1, devices):
        total = total + vec_back[a]
    pay[0] = total
    pay[1] = jnp.zeros_like(total)
    pay[2] = jnp.zeros_like(total)
    pay[3] = jnp.zeros_like(total)
    pay[1 + inner // 2] += up_place[...]
    for s in range(1, dp_n):
        pay[1 + (inner ^ (s % INNER)) // 2] += bias_back[s]
    for s in range(dp_n):
        @pl.when(att_active(s))
        def _():
            if s == 0:
                pay[3] += head_place[...]
            else:
                head_copy(s, 0).wait_recv()
                pay[3] += head_back[2 * s]
            head_copy(s, 1).wait_recv()
            pay[3] += head_back[2 * s + 1]

    last.append(leave(pay, tail_out))

    for s in range(1, dp_n):
        g_send_copy(0, s).wait_recv()
    for s in range(1, dp_n):
        for a in range(2):
            g_send_copy(a, s).wait_send()

        @pl.when(att_active(s))
        def _():
            for a, (src, dst) in enumerate(att_pairs(s)):
                remote(src, dst, att_send.at[a, s], att_recv.at[a, s], s, 0).wait_send()

        @pl.when(lead)
        def _():
            ga_copy(s).wait_send()

    @pl.when(lead)
    def _():
        for s in range(dp_n):
            for copy in pass_att(s):
                copy.wait_send()

    @pl.when(follow)
    def _():
        for s in range(dp_n):
            pair_copy(s).wait_send()

    @pl.when(lead)
    def _():
        for s in range(1, dp_n):
            head_copy(s, 0).wait_send()

    @pl.when(follow)
    def _():
        for s in range(dp_n):
            head_copy(s, 1).wait_send()

    for kind in range(2):
        back_waits(kind).wait_send()
    for copy in started + mlp_started[1]:
        copy.wait_send()
    for copy in [grad_out] + last:
        copy.wait()


def finish_kernel(
    dp_n, tp_n,
    block_ref, input_ref, tail_ref, ru_ref, rd_ref, ra_ref,
    block_out, input_out, up_out, down_out, qkv_out, proj_out,
    v0, v1, v2, v3, v4, v5, bq_out, bf_out,
    block, grad, ru, rd, ra, up, down, qkv, proj, tail, wide_f, in_sem, out_sem,
):
    d = lax.axis_index("dp")
    t = lax.axis_index("tp")
    inner = d % INNER
    core = t % 2
    hidden, width = ru.shape
    depth = width // dp_n
    groups = dp_n // INNER
    copies = []

    def fetch(src, dst):
        copy = pltpu.make_async_copy(src, dst, in_sem.at[len(copies)])
        copy.start()
        copies.append(copy)
        return copy

    rd_in = [fetch(row_cut(rd_ref, k * 128, 128), row_cut(rd, k * 128, 128)) for k in range(hidden // 128)]
    ru_in = [fetch(row_cut(ru_ref, k * 128, 128), row_cut(ru, k * 128, 128)) for k in range(hidden // 128)]
    ra_in = []
    for hl in range(2):
        first = ((inner // 2) ^ core) * 2 + ((inner % 2) ^ hl)
        for o in range(groups):
            k = hl * groups + o
            ra_in.append(fetch(lane_cut(ra_ref, (first + o * INNER) * depth, depth), lane_cut(ra, k * depth, depth)))
    tail_in = fetch(tail_ref, tail)
    block_in = fetch(block_ref, block)
    grad_in = fetch(input_ref, grad)
    outs = []

    def leave(src, dst):
        copy = pltpu.make_async_copy(src, dst, out_sem.at[len(outs)])
        copy.start()
        outs.append(copy)

    def total_of(ref, at, k):
        total = ref[at, k * depth : (k + 1) * depth].astype(F32)
        for s in range(k + INNER, dp_n, INNER):
            total = total + ref[at, s * depth : (s + 1) * depth].astype(F32)
        return total

    for c in range(hidden // 128):
        rd_in[c].wait()
        at = slice(c * 128, (c + 1) * 128)
        for k in range(INNER):
            down[k, at, :] = total_of(rd, at, k)
            leave(down.at[k, at, :], row_cut(down_out, (inner ^ k) * hidden + c * 128, 128))
    block_in.wait()
    leave(block, block_out)
    grad_in.wait()
    leave(grad, input_out)
    for c in range(hidden // 128):
        ru_in[c].wait()
        at = slice(c * 128, (c + 1) * 128)
        for k in range(INNER):
            up[k, :, at] = jnp.transpose(total_of(ru, at, k))
            leave(up.at[k, :, at], lane_cut(up_out, (inner ^ k) * hidden + c * 128, 128))
    for hl in range(2):
        total = jnp.zeros((4 * HD, depth), F32)
        for o in range(groups):
            k = hl * groups + o
            ra_in[k].wait()
            total = total + ra[:, k * depth : (k + 1) * depth].astype(F32)
        qkv[:, hl * 3 * HD : (hl + 1) * 3 * HD] = jnp.transpose(total[: 3 * HD])
        proj[hl * HD : (hl + 1) * HD, :] = total[3 * HD :]
    leave(qkv, qkv_out)
    leave(proj, proj_out)

    tail_in.wait()
    row = tail[0]
    row = jnp.where((t % 2) == 1, pltpu.roll(row, 64, 1), row)
    for k, ref in enumerate((v0, v1, v2, v3, v4, v5)):
        ref[...] = row[min(k, 4) : min(k, 4) + 1, :64]
    line = lax.broadcasted_iota(jnp.int32, (8, 128), 0)
    heads = tail[3]
    heads = jnp.where(d % 2 == 1, pltpu.roll(heads, 64, 1), heads)
    for k in range(2):
        picked = jnp.sum(jnp.where(line == k * 4 + d // 2, heads, 0.0), axis=0, keepdims=True)
        bq_out[k : k + 1, :] = picked[:, :64]
    cols = bf_out.shape[0]
    both = jnp.concatenate([tail[1], tail[2]], axis=0)
    both = pltpu.roll(both, (128 - d * cols) % 128, 1)
    wide_f[pl.ds(0, 16, stride=2), :] = both
    wide_f[pl.ds(1, 16, stride=2), :] = pltpu.roll(both, 64, 1)
    spots = wide_f.shape[0]
    full = jnp.concatenate([wide_f[...], jnp.zeros((128 - spots, 128), F32)], axis=0)
    bf_out[...] = jnp.transpose(full)[:cols, :spots]
    for copy in outs:
        copy.wait()


def solution(mesh):
    dp_n, tp_n = mesh.shape["dp"], mesh.shape["tp"]
    outer = dp_n // INNER
    devices = dp_n * tp_n

    def send(value, dp_xor, tp_xor, keep=None):
        pairs = []
        for d in range(dp_n):
            for t in range(tp_n):
                if keep is None or keep(d, t):
                    pairs.append((d * tp_n + t, (d ^ dp_xor) * tp_n + (t ^ tp_xor)))
        return lax.ppermute(value, AXES, pairs)

    def scatter_small(value, flat):
        held = value
        step = devices // 2
        while step >= 1:
            dp_xor, tp_xor = step // tp_n, step % tp_n
            high = (flat // step) % 2 == 1
            first, second = held[:step], held[step:]
            other = send(jnp.where(high, first, second), dp_xor, tp_xor)
            held = jnp.where(high, second, first) + other
            step //= 2
        return held[0]

    def scatter_rows(value):
        for dp_xor, tp_xor in ((0, 1), (0, 2), (1, 0), (2, 0)):
            half = value.shape[0] // 2
            other = send(value[half:], dp_xor, tp_xor)
            value = value[:half].astype(F32) + other.astype(F32)
            if half > value.shape[0] or (dp_xor, tp_xor) != (2, 0):
                value = value.astype(BF16)
        return value

    def on_device(
        block_input, segment_ids, w_qkv, b_qkv, w_out, b_out, w_fc1, b_fc1, w_fc2, b_fc2,
        ln1_gain, ln1_bias, ln2_gain, ln2_bias, cotangent,
    ):
        d = lax.axis_index("dp")
        t = lax.axis_index("tp")
        flat = d * tp_n + t
        inner = d % INNER
        core = t % 2
        lead = (inner // 2) == core
        rows, width = block_input.shape
        depth = w_qkv.shape[0]
        hidden_here = w_fc1.shape[1] // INNER
        head_here = w_out.shape[0] // HD
        heads = head_here * tp_n
        quarter = SEQ // tp_n
        qkv_bits = b_qkv.shape[1]

        vec = jnp.stack([ln1_gain, ln1_bias, ln2_gain, ln2_bias, b_out + b_fc2]).reshape(-1)
        seg_part = lax.dynamic_slice(segment_ids.reshape(-1), (t * quarter,), (quarter,))
        sizes = [vec.size, b_qkv.size, b_fc1.size, quarter]
        payload = jnp.concatenate(
            [vec, b_qkv.reshape(-1), b_fc1.reshape(-1), seg_part.astype(F32)]
        )
        depth_wide = depth % 128 == 0
        flat_shape = lambda lead_n: (lead_n, width) if depth_wide else (dp_n, lead_n, depth)
        spread = lambda v: v if depth_wide else v.transpose(1, 0, 2).reshape(v.shape[1], width)
        payload = jnp.pad(payload, (0, PAY - payload.size)).reshape(8, PAY // 8)
        like = lambda *shape: jax.ShapeDtypeStruct(shape, BF16)
        dma = pltpu.SemaphoreType.DMA
        hop_count = (devices - 1).bit_length()
        any_spec = pl.BlockSpec(memory_space=pl.ANY)
        x_all, cot_all, up_w, down_w, qkv_w, out_w, small = pl.pallas_call(
            functools.partial(gather_kernel, dp_n, tp_n, depth_wide),
            out_shape=(
                like(16, rows, width),
                like(16, rows, width),
                like(width, hidden_here),
                like(*flat_shape(hidden_here)),
                like(width, 3 * HD),
                like(*flat_shape(HD)),
                jax.ShapeDtypeStruct((devices, 8, PAY // 8), F32),
            ),
            in_specs=[any_spec] * 7,
            out_specs=(any_spec,) * 7,
            scratch_shapes=[
                dma((2, 16)), dma((2, 16)), dma((2, dp_n)), dma((2, dp_n)),
                dma((2, dp_n)), dma((2, dp_n)), dma((2, dp_n)), dma((2, dp_n)),
                dma((hop_count,)), dma((hop_count,)), dma((6,)),
            ],
            compiler_params=pltpu.CompilerParams(collective_id=0, has_side_effects=True),
            name="gather_phase",
        )(block_input, cotangent, w_fc1, w_fc2, w_qkv, w_out, payload)
        down_w, out_w = spread(down_w), spread(out_w)
        small = jnp.take(small.reshape(devices, PAY), flat ^ jnp.arange(devices), axis=0)
        cuts = [0]
        for size in sizes:
            cuts.append(cuts[-1] + size)
        vecs = small[:, : cuts[1]].reshape(devices, 5, -1).transpose(1, 0, 2).reshape(5, width)
        gain_one, shift_one, gain_two, shift_two, out_bias = (vecs[k][None] for k in range(5))
        qkv_bias_all = (
            small[:, cuts[1] : cuts[2]]
            .reshape(dp_n, tp_n, head_here, qkv_bits)
            .transpose(1, 2, 0, 3)
            .reshape(heads, 2 * HD)
        )
        head = (t // 2) * INNER + inner
        qkv_bias = lax.dynamic_slice(qkv_bias_all, (head, 0), (1, 2 * HD))
        up_rows, up_cols = b_fc1.shape
        up_bias_all = (
            small[:, cuts[2] : cuts[3]]
            .reshape(dp_n, tp_n, up_rows, up_cols)
            .transpose(1, 2, 0, 3)
            .reshape(tp_n * INNER, hidden_here)
        )
        up_bias = lax.dynamic_slice(up_bias_all, (t * INNER + inner, 0), (1, hidden_here))
        seg_all = small[:, cuts[3] : cuts[4]].reshape(dp_n, tp_n, quarter)

        x_rows = x_all.reshape(16 * rows, width).astype(F32)
        cot_rows = cot_all.reshape(16 * rows, width)
        row_mean = jnp.mean(x_rows, axis=-1, keepdims=True)
        centered = x_rows - row_mean
        row_var = jnp.mean(centered * centered, axis=-1, keepdims=True)
        inv_std = lax.rsqrt(row_var + EPS)
        normed = centered * inv_std
        norm_two = (normed * gain_two + shift_two).astype(BF16)

        def mine(value):
            split = value.reshape((2, 2, 2, 2, rows) + value.shape[1:])
            cut = lax.dynamic_index_in_dim(split, core, 3, keepdims=False)
            return jnp.moveaxis(cut, 2, 0).reshape((2 * SEQ,) + value.shape[1:])

        def unmine(value):
            split = value.reshape((2, 2, 2, rows) + value.shape[1:])
            cut = jnp.moveaxis(split, 0, 2)[:, :, :, None]
            where = (jnp.arange(2) == core).reshape((1, 1, 1, 2) + (1,) * value.ndim)
            full = jnp.where(where, cut, jnp.zeros_like(cut))
            return full.reshape((16 * rows,) + value.shape[1:])

        norm_one = (mine(normed) * gain_one + shift_one).astype(BF16)
        cot_mine = mine(cot_rows)

        pre_act = mm(norm_two, up_w) + up_bias
        half_gelu = gelu_half(pre_act)
        hidden = (pre_act * half_gelu).astype(BF16)
        down_grad = mm_lead(hidden, cot_rows)
        act_cot = mm_tail(cot_rows, down_w) * gelu_slope(pre_act)
        up_bias_part = jnp.sum(act_cot, axis=0)
        act_low = act_cot.astype(BF16)
        up_grad = mm_lead(norm_two, act_low)
        up_grad, down_grad = up_grad.astype(BF16), down_grad.astype(BF16)

        def cut_block(value, s):
            return lax.dynamic_slice(value, ((d ^ s) * depth, 0), (depth, value.shape[1]))

        def cut_across(value, s):
            return lax.dynamic_slice(value, (0, (d ^ s) * depth), (value.shape[0], depth))

        with jax.named_scope("mlp_out"):
            up_back = [cut_block(up_grad, 0)] + [
                send(cut_block(up_grad, s), s, 0) for s in range(1, dp_n)
            ]
            down_back = [cut_across(down_grad, 0)] + [
                send(cut_across(down_grad, s), s, 0) for s in range(1, dp_n)
            ]

        order = jnp.stack([t ^ ((k % 2) * 2 + k // 2) for k in range(4)])
        position = (order[:, None] * quarter + jnp.arange(quarter)[None]).reshape(-1)
        inverse = jnp.exp(jnp.arange(ROT // 2, dtype=F32) * (-2.0 * math.log(10000.0) / ROT))
        angle = position.astype(F32)[:, None] * inverse[None]
        cosine, sine = jnp.cos(angle)[None], jnp.sin(angle)[None]
        segs = []
        for dy in range(2):
            seq = (d // INNER) * INNER + (inner ^ (core * 2 + dy))
            rows_of = lax.dynamic_index_in_dim(seg_all, seq, 0, keepdims=False)
            segs.append(jnp.take(rows_of, order, axis=0).reshape(-1))
        segs = jnp.stack(segs)
        allowed = (position[None, :] <= position[:, None])[None] & (
            segs[:, :, None] == segs[:, None, :]
        )
        qkv = mm(norm_one, qkv_w)
        query = rotate((qkv[:, :HD] + qkv_bias[:, :HD]).reshape(2, SEQ, HD), cosine, sine).astype(BF16)
        key = rotate(qkv[:, HD : 2 * HD].reshape(2, SEQ, HD), cosine, sine).astype(BF16)
        val = (qkv[:, 2 * HD :] + qkv_bias[:, HD:]).astype(BF16).reshape(2, SEQ, HD)
        scale = HD ** (-0.5)

        def ein(eq, left, right):
            return jnp.einsum(eq, left, right, preferred_element_type=F32)

        masked = jnp.where(allowed, ein("sqd,skd->sqk", query, key) * scale, NEG_FILL)
        peak = jnp.max(masked, axis=-1, keepdims=True)
        log_total = peak + jnp.log(
            jnp.sum(jnp.where(allowed, jnp.exp(masked - peak), 0.0), axis=-1, keepdims=True)
        )
        prob_full = jnp.where(allowed, jnp.exp(masked - log_total), 0.0)
        prob_low = prob_full.astype(BF16)
        context = ein("sqk,skd->sqd", prob_low, val).astype(BF16)
        context_cot = mm_tail(cot_mine, out_w).astype(BF16).reshape(2, SEQ, HD)
        prob_cot = ein("sqd,skd->sqk", context_cot, val)
        row_delta = jnp.sum(context_cot.astype(F32) * context.astype(F32), axis=-1, keepdims=True)
        score_cot = (prob_full * (prob_cot - row_delta)).astype(BF16)
        query_cot = rotate(ein("sqk,skd->sqd", score_cot, key) * scale, cosine, -sine)
        key_cot = rotate(ein("sqk,sqd->skd", score_cot, query) * scale, cosine, -sine)
        val_cot = ein("sqk,sqd->skd", prob_low, context_cot)
        qkv_cot = jnp.concatenate([query_cot, key_cot, val_cot], axis=-1).reshape(2 * SEQ, 3 * HD)
        qkv_bias_part = jnp.concatenate(
            [jnp.sum(query_cot, axis=(0, 1)), jnp.sum(val_cot, axis=(0, 1))]
        )
        qkv_low = qkv_cot.astype(BF16)
        context_flat = context.reshape(2 * SEQ, HD)
        att_grad = jnp.concatenate(
            [mm_lead(norm_one, qkv_low).astype(BF16), mm_lead(cot_mine, context_flat).astype(BF16)],
            axis=1,
        )
        att_pair = send(att_grad, 0, 1, lambda dd, tt: (dd % INNER) // 2 != tt % 2)
        att_grad = (att_grad.astype(F32) + att_pair.astype(F32)).astype(BF16)
        with jax.named_scope("att_out"):
            own_att = cut_block(att_grad, 0)
            att_back = [jnp.where(lead, own_att, jnp.zeros_like(own_att))] + [
                send(cut_block(att_grad, s), s, 0, lambda dd, tt: (dd % INNER) // 2 == tt % 2)
                for s in range(1, dp_n)
            ]

        left = jnp.concatenate([hidden, unmine(context_flat)], axis=1)
        right = jnp.concatenate([down_w, out_w], axis=0)
        with jax.named_scope("branch"):
            branch = scatter_rows(mm(left, right).astype(BF16))
        block_output = (block_input.astype(F32) + branch + out_bias).astype(BF16)

        one_part = mm_tail(qkv_low, qkv_w)
        two_part = mm_tail(act_low, up_w)
        vec_terms = jnp.stack(
            [
                jnp.sum(one_part * mine(normed), axis=0),
                jnp.sum(one_part, axis=0),
                jnp.sum(two_part * normed, axis=0),
                jnp.sum(two_part, axis=0),
                jnp.sum(cotangent.astype(F32), axis=0),
            ]
        )
        scaled_part = (two_part * gain_two + unmine(one_part * gain_one)).astype(BF16)
        with jax.named_scope("normback"):
            scaled = scatter_rows(scaled_part)
        normed_own = normed[:rows]
        input_grad = cotangent.astype(F32) + inv_std[:rows] * (
            scaled
            - jnp.mean(scaled, axis=-1, keepdims=True)
            - normed_own * jnp.mean(scaled * normed_own, axis=-1, keepdims=True)
        )

        head_hot = (jnp.arange(heads) == head).astype(F32)[:, None]
        qkv_small = (
            (head_hot * qkv_bias_part[None])
            .reshape(tp_n, head_here, dp_n, qkv_bits)
            .transpose(2, 0, 1, 3)
            .reshape(devices, -1)
        )
        up_hot = (jnp.arange(tp_n * INNER) == t * INNER + inner).astype(F32)[:, None]
        up_small = (
            (up_hot * up_bias_part[None])
            .reshape(tp_n, up_rows, dp_n, up_cols)
            .transpose(2, 0, 1, 3)
            .reshape(devices, -1)
        )
        vec_small = vec_terms.reshape(5, devices, -1).transpose(1, 0, 2).reshape(devices, -1)
        with jax.named_scope("small_out"):
            own = scatter_small(jnp.concatenate([vec_small, qkv_small, up_small], axis=1), flat)
        vec_own = own[: cuts[1]].reshape(5, -1)
        qkv_bias_grad = own[cuts[1] : cuts[2]].reshape(b_qkv.shape)
        up_bias_grad = own[cuts[2] : cuts[3]].reshape(b_fc1.shape)

        up_total = jnp.zeros(w_fc1.shape, F32)
        down_total = jnp.zeros(w_fc2.shape, F32)
        for k in range(INNER):
            at = (inner ^ k) * hidden_here
            up_sum = sum(up_back[s].astype(F32) for s in range(k, dp_n, INNER))
            down_sum = sum(down_back[s].astype(F32) for s in range(k, dp_n, INNER))
            up_total = lax.dynamic_update_slice(up_total, up_sum, (0, at))
            down_total = lax.dynamic_update_slice(down_total, down_sum, (at, 0))
        att_sum = [sum(att_back[s].astype(F32) for s in range(k, dp_n, 2)) for k in range(2)]
        odd = inner % 2 == 1
        att_first = jnp.where(odd, att_sum[1], att_sum[0])
        att_second = jnp.where(odd, att_sum[0], att_sum[1])
        qkv_total = jnp.concatenate([att_first[:, : 3 * HD], att_second[:, : 3 * HD]], axis=1)
        out_total = jnp.concatenate([att_first[:, 3 * HD :].T, att_second[:, 3 * HD :].T], axis=0)
        return (
            block_output, input_grad, qkv_total, qkv_bias_grad, out_total, vec_own[4],
            up_total, up_bias_grad, down_total, vec_own[4],
            vec_own[0], vec_own[1], vec_own[2], vec_own[3],
        )

    def on_device_fused(
        block_input, segment_ids, w_qkv, b_qkv, w_out, b_out, w_fc1, b_fc1, w_fc2, b_fc2,
        ln1_gain, ln1_bias, ln2_gain, ln2_bias, cotangent,
    ):
        d = lax.axis_index("dp")
        t = lax.axis_index("tp")
        flat = d * tp_n + t
        inner = d % INNER
        core = t % 2
        lead = (inner // 2) == core
        rows, width = block_input.shape
        depth = w_qkv.shape[0]
        hidden_here = w_fc1.shape[1] // INNER
        head_here = w_out.shape[0] // HD
        heads = head_here * tp_n
        quarter = SEQ // tp_n
        qkv_bits = b_qkv.shape[1]

        up_rows = b_fc1.shape[0]
        per = ln1_gain.shape[0]
        seg_row = segment_ids.reshape(1, -1)
        small_in = [v.reshape(1, -1) for v in (ln1_gain, ln1_bias, ln2_gain, ln2_bias, b_out, b_fc2)]
        small_in += [b_qkv, b_fc1.T, seg_row]
        angle = np.arange(SEQ)[:, None] * np.exp(np.arange(ROT // 2) * (-2.0 * math.log(10000.0) / ROT))
        pad = np.zeros((SEQ, 128 - ROT))
        cosine = np.concatenate([np.cos(angle), np.cos(angle), pad + 1.0], axis=1)
        sine = np.concatenate([np.sin(angle), np.sin(angle), pad], axis=1)
        rope = jnp.asarray(np.stack([cosine, sine]), F32)
        like = lambda *shape: jax.ShapeDtypeStruct(shape, BF16)
        wide_f = lambda *shape: jax.ShapeDtypeStruct(shape, F32)
        dma = pltpu.SemaphoreType.DMA
        vb = lambda *shape: pltpu.VMEM(shape, BF16)
        vf = lambda *shape: pltpu.VMEM(shape, F32)
        any_spec = pl.BlockSpec(memory_space=pl.ANY)
        group = 16 * rows
        per_peer = dma((2, dp_n))
        pair = 2 * SEQ
        results = pl.pallas_call(
            functools.partial(fused_kernel, dp_n, tp_n),
            out_shape=(
                like(rows, width), wide_f(rows, width), wide_f(4, 8, 128),
                like(hidden_here, width), like(hidden_here, width),
                like(hidden_here, width), like(hidden_here, width), like(4 * HD, width),
                like(4 * HD, width),
            ),
            in_specs=[any_spec] * 16,
            out_specs=(any_spec,) * 9,
            scratch_shapes=[
                vb(group, width), vb(group, width), vb(group, width),
                vb(hidden_here, width), vb(hidden_here, width), vf(hidden_here, group),
                vb(hidden_here, group), vb(hidden_here, group), vb(3, hidden_here, depth),
                vf(group, 128), vf(8, width), vf(8, width), vf(hidden_here, 128),
                vb(width, 3 * HD), vb(HD, width), vb(pair, width),
                vb(pair, HD), vb(pair, HD), vb(pair, HD), vb(pair, SEQ),
                vb(pair, HD), vb(HD, pair), vb(pair, HD), vb(pair, 3 * HD), vb(3 * HD, pair),
                vb(4 * HD, width), vf(2, SEQ, 128),
                vf(6, 1, per), vf(*b_qkv.shape), vf(*b_fc1.T.shape), pltpu.VMEM(seg_row.shape, jnp.int32), vf(up_rows, 128),
                vf(4, 8, 128), vf(devices, 8, 128), vf(dp_n, 8, 128), vf(2 * dp_n, 8, 128),
                vf(devices, 8, 128), vf(dp_n, 8, 128), vf(2 * dp_n, 8, 128), vf(8, 128), vf(8, 128),
                vf(8, SEQ), vf(SEQ, 128), vf(8, 2 * HD), vf(8, 2 * HD),
                dma((2, 16)), dma((2, 16)), per_peer, per_peer, per_peer, per_peer, per_peer, per_peer,
                dma((3,)), dma((3,)), dma((2,)), dma((2,)), dma((2 * dp_n,)), dma((2 * dp_n,)),
                per_peer, per_peer, dma((3,)),
                dma((2, 16)), dma((2, 16)), dma((8,)), dma((8,)), dma((dp_n,)), dma((dp_n,)),
                dma((24,)), dma((24,)), pltpu.SemaphoreType.REGULAR((6,)),
            ],
            compiler_params=pltpu.CompilerParams(
                collective_id=0, has_side_effects=True, vmem_limit_bytes=67_043_328
            ),
            name="fused_block",
        )(block_input, cotangent, w_fc1, w_fc2, w_qkv, w_out, rope, *small_in)
        f32_out = lambda *shape: jax.ShapeDtypeStruct(shape, F32)
        ends = pl.pallas_call(
            functools.partial(finish_kernel, dp_n, tp_n),
            out_shape=(
                like(rows, width), f32_out(rows, width), f32_out(*w_fc1.shape), f32_out(*w_fc2.shape),
                f32_out(*w_qkv.shape), f32_out(*w_out.shape),
            ) + (f32_out(1, per),) * 6 + (f32_out(*b_qkv.shape), f32_out(*b_fc1.T.shape)),
            in_specs=[any_spec] * 6,
            out_specs=(any_spec,) * 6 + (pl.BlockSpec(memory_space=pltpu.VMEM),) * 8,
            scratch_shapes=[
                vb(rows, width), vf(rows, width), vb(hidden_here, width), vb(hidden_here, width),
                vb(4 * HD, width // 2), vf(INNER, depth, hidden_here), vf(INNER, hidden_here, depth),
                vf(*w_qkv.shape), vf(*w_out.shape), vf(4, 8, 128), vf(up_rows, 128),
                dma((24,)), dma((48,)),
            ],
            compiler_params=pltpu.CompilerParams(vmem_limit_bytes=60_000_000),
            name="finish",
        )(results[0], results[1], results[2], results[5], results[6], results[7])
        block_output, input_grad, up_total, down_total, qkv_total, out_total = ends[:6]
        small = [v.reshape(-1) for v in ends[6:12]]
        return (
            block_output, input_grad, qkv_total, ends[12], out_total, small[4],
            up_total, ends[13].T, down_total, small[5],
            small[0], small[1], small[2], small[3],
        )

    row, vec = P(AXES, None), P(AXES)
    col, low = P("dp", "tp"), P("tp", "dp")
    def choose(*arrays):
        wide = arrays[2].shape[0] % 128 == 0
        return (on_device_fused if wide else on_device)(*arrays)

    return jax.shard_map(
        choose,
        mesh=mesh,
        in_specs=(row, P("dp", None), col, low, low, vec, col, low, low, vec, vec, vec, vec, vec, row),
        out_specs=(row, row, col, low, low, vec, col, low, low, vec, vec, vec, vec, vec),
        check_vma=False,
    )
```

```python
import functools
import math

import jax
import jax.numpy as jnp
import numpy as np
from jax import lax
from jax.experimental import pallas as pl
from jax.experimental.pallas import tpu as pltpu
from jax.sharding import PartitionSpec as P

HD = 256
ROT = 64
SEQ = 512
INNER = 4
EPS = 1e-05
NEG_FILL = -1e30
F32 = jnp.float32
BF16 = jnp.bfloat16
AXES = ("dp", "tp")
MESH = pl.DeviceIdType.MESH
PAY = 1024


def dot(left, right, contract):
    return lax.dot_general(left, right, (contract, ((), ())), preferred_element_type=F32)


def mm(left, right):
    return dot(left, right, ((1,), (0,)))


def mm_tail(left, right):
    return dot(left, right, ((1,), (1,)))


def mm_lead(left, right):
    return dot(left, right, ((0,), (0,)))


def gelu_half(pre_act):
    return 0.5 * (1.0 + jax.scipy.special.erf(pre_act * 2.0 ** (-0.5)))


def gelu_slope(pre_act):
    return gelu_half(pre_act) + pre_act * jnp.exp(-0.5 * pre_act * pre_act) * (2.0 * math.pi) ** (-0.5)


def rotate(block, cosine, sine):
    half = ROT // 2
    lower, upper = block[..., :half], block[..., half:ROT]
    return jnp.concatenate(
        [lower * cosine - upper * sine, upper * cosine + lower * sine, block[..., ROT:]], axis=-1
    )


def gather_kernel(
    dp_n, tp_n, wide,
    x_ref, cot_ref, fc1_ref, fc2_ref, qkv_ref, out_ref, pay_ref,
    xs_ref, cots_ref, up_ref, down_ref, att_ref, proj_ref, small_ref,
    row_send, row_recv, mlp_send, mlp_recv, att_send, att_recv, pass_send, pass_recv,
    small_send, small_recv, local_sem,
):
    d = lax.axis_index("dp")
    t = lax.axis_index("tp")
    inner = d % INNER
    core = t % 2
    depth = fc1_ref.shape[0]
    hidden = fc1_ref.shape[1] // INNER

    barrier = pltpu.get_barrier_semaphore()
    for s in range(1, dp_n):
        pl.semaphore_signal(barrier, inc=1, device_id=(d ^ s, t), device_id_type=MESH)
    for k in (1, 2):
        pl.semaphore_signal(barrier, inc=1, device_id=(d, t ^ k), device_id_type=MESH)

    def remote(src, dst, send_sem, recv_sem, dp_xor, tp_xor):
        return pltpu.make_async_remote_copy(
            src_ref=src, dst_ref=dst, send_sem=send_sem, recv_sem=recv_sem,
            device_id=(d ^ dp_xor, t ^ tp_xor), device_id_type=MESH,
        )

    hop = {1: (2, 0), 2: (1, 0), 4: (0, 2), 8: (0, 1)}
    pairs = ((x_ref, xs_ref), (cot_ref, cots_ref))

    def row_copy(a, k, bit):
        own, full = pairs[a]
        src = own if k == 0 else full.at[k]
        return remote(src, full.at[k + bit], row_send.at[a, k + bit], row_recv.at[a, k + bit], *hop[bit])

    def columns(ref, index, size):
        return ref.at[:, pl.ds(pl.multiple_of(index * size, 128), size)]

    def lines(ref, index, size):
        return ref.at[pl.ds(pl.multiple_of(index * size, 8), size), :]

    def across(ref, index, size):
        return columns(ref, index, size) if wide else ref.at[index]

    def mlp_copies(s):
        target = inner ^ (s % INNER)
        return (
            (columns(fc1_ref, target, hidden), lines(up_ref, d, depth)),
            (lines(fc2_ref, target, hidden), across(down_ref, d, depth)),
        )

    def att_copies(s):
        target = (inner ^ (s % INNER)) % 2
        return (
            (columns(qkv_ref, target, 3 * HD), lines(att_ref, d, depth)),
            (lines(out_ref, target, HD), across(proj_ref, d, depth)),
        )

    def att_land(s):
        return (lines(att_ref, d ^ s, depth), across(proj_ref, d ^ s, depth))

    def mlp_land(s):
        return (lines(up_ref, d ^ s, depth), across(down_ref, d ^ s, depth))

    local = []
    def stay(src, dst):
        copy = pltpu.make_async_copy(src, dst, local_sem.at[len(local)])
        copy.start()
        local.append(copy)

    lead = (inner // 2) == core
    pltpu.sync_copy(pay_ref, small_ref.at[0])
    pl.semaphore_wait(barrier, dp_n + 1)

    started = []
    def start(copy):
        copy.start()
        started.append(copy)

    def start_rows(k, bit):
        for a in range(2):
            start(row_copy(a, k, bit))

    def wait_rows(k):
        bit = 1
        while bit * 2 <= k:
            bit *= 2
        for a in range(2):
            row_copy(a, k - bit, bit).wait_recv()

    def start_mlp(s):
        for a, (src, dst) in enumerate(mlp_copies(s)):
            start(remote(src, dst, mlp_send.at[a, s], mlp_recv.at[a, s], s, 0))

    def att_active(s):
        return ((inner ^ (s % INNER)) // 2) == core

    def start_att(s):
        @pl.when(att_active(s))
        def _():
            for a, (src, dst) in enumerate(att_copies(s)):
                remote(src, dst, att_send.at[a, s], att_recv.at[a, s], s, 0).start()

    def pass_att(s):
        lands = att_land(s)
        return [
            remote(land, land, pass_send.at[a, s], pass_recv.at[a, s], 0, 1)
            for a, land in enumerate(lands)
        ]

    def small_copy(step, dp_xor, tp_xor, n):
        return remote(
            small_ref.at[pl.ds(0, n)], small_ref.at[pl.ds(n, n)],
            small_send.at[step], small_recv.at[step], dp_xor, tp_xor,
        )

    hops = []
    n = 1
    while n < dp_n * tp_n:
        hops.append((n // tp_n, n % tp_n, n))
        n *= 2
    even = [s for s in range(2, dp_n, 2)]
    even.sort(key=lambda s: -(s >= INNER))
    odd = [s for s in range(1, dp_n, 2)]
    odd.sort(key=lambda s: -(s >= INNER))

    small = [small_copy(k, *h) for k, h in enumerate(hops)]
    small[0].start()
    for bit in (1, 2, 4):
        start_rows(0, bit)
    start_rows(0, 8)
    for s in even:
        start_mlp(s)
    stay(x_ref, xs_ref.at[0])
    stay(cot_ref, cots_ref.at[0])
    for src, dst in mlp_copies(0):
        stay(src, dst)

    @pl.when(lead)
    def _():
        for a, (src, dst) in enumerate(att_copies(0)):
            copy = pltpu.make_async_copy(src, dst, local_sem.at[4 + a])
            copy.start()

    for k in range(len(small)):
        small[k].wait_recv()
        if k + 1 < len(small):
            small[k + 1].start()
    wait_rows(1)
    start_rows(1, 2)
    start_rows(1, 4)
    start_rows(1, 8)
    wait_rows(2)
    start_rows(2, 4)
    start_rows(2, 8)
    for s in odd:
        start_mlp(s)
    for s in even + odd:
        start_att(s)
    wait_rows(3)
    start_rows(3, 4)
    start_rows(3, 8)
    wait_rows(4)
    start_rows(4, 8)

    @pl.when(lead)
    def _():
        for a, (src, dst) in enumerate(att_copies(0)):
            pltpu.make_async_copy(src, dst, local_sem.at[4 + a]).wait()
        for copy in pass_att(0):
            copy.start()

    for k in (5, 6, 7):
        wait_rows(k)
        start_rows(k, 8)
    for k in range(8, 16):
        wait_rows(k)
    for s in even + odd:
        for a, dst in enumerate(mlp_land(s)):
            remote(dst, dst, mlp_send.at[a, s], mlp_recv.at[a, s], s, 0).wait_recv()
    for s in even + odd:
        @pl.when(lead)
        def _():
            for a, dst in enumerate(att_land(s)):
                remote(dst, dst, att_send.at[a, s], att_recv.at[a, s], s, 0).wait_recv()
            for copy in pass_att(s):
                copy.start()

    @pl.when(jnp.logical_not(lead))
    def _():
        for s in range(dp_n):
            for copy in pass_att(s):
                copy.wait_recv()

    @pl.when(lead)
    def _():
        for s in range(dp_n):
            for copy in pass_att(s):
                copy.wait_send()

    for s in range(1, dp_n):
        @pl.when(att_active(s))
        def _():
            for a, (src, dst) in enumerate(att_copies(s)):
                remote(src, dst, att_send.at[a, s], att_recv.at[a, s], s, 0).wait_send()
    for copy in started:
        copy.wait_send()
    for copy in small:
        copy.wait_send()
    for copy in local:
        copy.wait()


def span(start, size, unit):
    return pl.ds(start if isinstance(start, int) else pl.multiple_of(start, unit), size)


def lane_cut(ref, start, size):
    return ref.at[:, span(start, size, 128)]


def row_cut(ref, start, size):
    return ref.at[span(start, size, 16), :]


def columns_of(rows8):
    pad = jnp.zeros((120, 128), F32)
    return jnp.transpose(jnp.concatenate([rows8, pad], axis=0))


def fused_kernel(
    dp_n, tp_n,
    x_ref, cot_ref, fc1_ref, fc2_ref, qkv_ref, out_ref, rope_ref,
    vec0_ref, vec1_ref, vec2_ref, vec3_ref, vec4_ref, vec5_ref, bq_ref, bf_ref, seg_ref,
    block_out, input_out, tail_out,
    gu_hbm, gd_hbm, ru_hbm, rd_hbm, ra_hbm, pair_hbm,
    xs, cots, n2, up_t, down_w, pre, hid_t, act_t, ring, stats, vecs, sums, up_sum,
    att_w, proj_w, n1, q_s, k_s, v_s, prob, ctx, ctx_t, cctx, low, low_t, gx,
    rope, raw, raw_q, raw_f, raw_seg, wide_f, pay, pair_in, pair_back, vec_in, bias_in, head_in, vec_back, bias_back, head_back, up_place, head_place,
    keys, queries, qkv_bias, qkv_sum,
    row_send, row_recv, mlp_send, mlp_recv, att_send, att_recv, pass_send, pass_recv,
    small_send, small_recv, head_send, head_recv, back_send, back_recv, headb_send, headb_recv, g_send, g_recv, g_local,
    rs_send, rs_recv, pair_send, pair_recv, ga_send, ga_recv,
    local_sem, out_sem, credit,
):
    d = lax.axis_index("dp")
    t = lax.axis_index("tp")
    flat = d * tp_n + t
    inner = d % INNER
    core = t % 2
    lead = (inner // 2) == core
    follow = jnp.logical_not(lead)
    rows, width = x_ref.shape
    depth = fc1_ref.shape[0]
    hidden = fc1_ref.shape[1] // INNER
    devices = dp_n * tp_n
    slots = 16
    tokens = slots * rows
    scale = HD ** (-0.5)
    chunk = 512

    barrier = pltpu.get_barrier_semaphore()
    for a in range(1, devices):
        peer = (d ^ (a // tp_n), t ^ (a % tp_n))
        pl.semaphore_signal(barrier, inc=1, device_id=peer, device_id_type=MESH)

    def remote(src, dst, send_sem, recv_sem, dp_xor, tp_xor):
        return pltpu.make_async_remote_copy(
            src_ref=src, dst_ref=dst, send_sem=send_sem, recv_sem=recv_sem,
            device_id=(d ^ dp_xor, t ^ tp_xor), device_id_type=MESH,
        )

    started = []

    def start(copy):
        copy.start()
        started.append(copy)

    hop = {1: (2, 0), 2: (1, 0), 4: (0, 2), 8: (0, 1)}

    def slot(ref, k):
        return row_cut(ref, k * rows, rows)

    def row_copy(a, k, bit):
        own, full = ((x_ref, xs), (cot_ref, cots))[a]
        src = own if k == 0 else slot(full, k)
        return remote(
            src, slot(full, k + bit), row_send.at[a, k + bit], row_recv.at[a, k + bit], *hop[bit]
        )

    row_started = ([], [])

    def start_row(a, k, *bits):
        for bit in bits:
            copy = row_copy(a, k, bit)
            copy.start()
            row_started[a].append(copy)

    def wait_row(a, k):
        bit = 1
        while bit * 2 <= k:
            bit *= 2
        row_copy(a, k - bit, bit).wait_recv()

    def w1_piece(i):
        return gx.at[depth : depth + hidden, pl.ds(pl.multiple_of(i * depth, 128), depth)]

    def mlp_copy(a, s):
        target = inner ^ (s % INNER)
        src = w1_piece(target) if a == 0 else row_cut(fc2_ref, target * hidden, hidden)
        dst = lane_cut((up_t, down_w)[a], d * depth, depth)
        if s == 0:
            return src, dst
        return remote(src, dst, mlp_send.at[a, s], mlp_recv.at[a, s], s, 0)

    mlp_started = tuple([mlp_copy(a, s) for s in range(1, dp_n)] for a in range(2))

    def start_mlp(a, s):
        mlp_started[a][s - 1].start()

    def mlp_wait(a, s):
        dst = lane_cut((up_t, down_w)[a], (d ^ s) * depth, depth)
        remote(dst, dst, mlp_send.at[a, s], mlp_recv.at[a, s], s, 0).wait_recv()

    def att_active(s):
        return ((inner ^ (s % INNER)) // 2) == core

    def att_pairs(s):
        target = (inner ^ (s % INNER)) % 2
        return (
            (lane_cut(qkv_ref, target * 3 * HD, 3 * HD), row_cut(att_w, d * depth, depth)),
            (row_cut(out_ref, target * HD, HD), lane_cut(proj_w, d * depth, depth)),
        )

    def att_land(s):
        return (row_cut(att_w, (d ^ s) * depth, depth), lane_cut(proj_w, (d ^ s) * depth, depth))

    def start_att(s):
        @pl.when(att_active(s))
        def _():
            for a, (src, dst) in enumerate(att_pairs(s)):
                remote(src, dst, att_send.at[a, s], att_recv.at[a, s], s, 0).start()

    def pass_att(s):
        return [
            remote(land, land, pass_send.at[a, s], pass_recv.at[a, s], 0, 1)
            for a, land in enumerate(att_land(s))
        ]

    local = []

    def stay(src, dst):
        copy = pltpu.make_async_copy(src, dst, local_sem.at[len(local)])
        copy.start()
        local.append(copy)
        return copy

    fc1_in = stay(fc1_ref, gx.at[0:depth, :])
    raw_in = [
        stay(ref, raw.at[k])
        for k, ref in enumerate((vec0_ref, vec1_ref, vec2_ref, vec3_ref, vec4_ref, vec5_ref))
    ]
    raw_in += [stay(bq_ref, raw_q), stay(bf_ref, raw_f), stay(seg_ref, raw_seg)]
    x_in = stay(x_ref, slot(xs, 0))
    cot_in = stay(cot_ref, slot(cots, 0))
    down_in = stay(*mlp_copy(1, 0))
    rope_in = stay(rope_ref, rope)
    for copy in raw_in:
        copy.wait()
    zero64 = jnp.zeros((1, 64), F32)
    line = lax.broadcasted_iota(jnp.int32, (8, 128), 0)

    def wide(row):
        return jnp.broadcast_to(jnp.concatenate([row, zero64], axis=1), (8, 128))

    def onto(base, row, value):
        return jnp.where(line == row, value, base)

    odd_flat = flat % 2 == 1
    group = jnp.zeros((8, 128), F32)
    for k in range(5):
        row = raw[k] if k < 4 else raw[4] + raw[5]
        value = wide(row)
        group = onto(group, k, jnp.where(odd_flat, pltpu.roll(value, 64, 1), value))
    seg_row = raw_seg[:, pl.ds(pl.multiple_of(t * 128, 128), 128)].astype(F32)
    pay[0] = onto(group, 5 + core, jnp.broadcast_to(seg_row, (8, 128)))
    group = jnp.zeros((8, 128), F32)
    for k in range(2):
        value = wide(raw_q[k : k + 1, :])
        value = jnp.where(d % 2 == 1, pltpu.roll(value, 64, 1), value)
        group = onto(group, k * 4 + d // 2, value)
    pay[3] = group
    up_lines, up_spots = raw_f.shape
    flat_f = jnp.concatenate([raw_f[...], jnp.zeros((up_lines, 128 - up_spots), F32)], axis=1)
    value = pltpu.roll(columns_of(flat_f)[:up_spots], d * up_lines, 1)
    odd_row = lax.broadcasted_iota(jnp.int32, value.shape, 0) % 2 == 1
    wide_f[...] = jnp.where(odd_row, pltpu.roll(value, 64, 1), value)
    merged = wide_f[pl.ds(0, 16, stride=2), :] + wide_f[pl.ds(1, 16, stride=2), :]
    pay[1] = merged[:8]
    pay[2] = merged[8:]
    pl.semaphore_wait(barrier, devices - 1)

    even = sorted(range(2, dp_n, 2), key=lambda s: -(s >= INNER))
    odd = sorted(range(1, dp_n, 2), key=lambda s: -(s >= INNER))

    def small_copy(kind, src, dst, dp_xor, tp_xor):
        return remote(src, dst, small_send.at[kind], small_recv.at[kind], dp_xor, tp_xor)

    chip = flat // 2
    chips = devices // 2
    meet = small_copy(2, pay.at[0], pair_in, 0, 1)
    meet.start()

    def head_in_copy(s, dc):
        return remote(
            pay.at[3], head_in.at[2 * s + dc], head_send.at[2 * s + dc], head_recv.at[2 * s + dc], s, dc
        )

    def head_in_each(act):
        @pl.when(lead)
        def _():
            act(head_in_copy(0, 1))

        for s in range(1, dp_n):
            @pl.when(att_active(s))
            def _():
                act(head_in_copy(s, 0))
                act(head_in_copy(s, 1))

    for s in range(1, dp_n):
        group = 1 + (inner ^ (s % INNER)) // 2
        small_copy(1, pay.at[group], bias_in.at[s], s, 0).start()
    head_in_each(lambda copy: copy.start())
    meet.wait_recv()
    vec_in[0] = pay[0] + pair_in[...]
    for r in range(1, chips):
        small_copy(0, vec_in.at[0], vec_in.at[r], r // 2, (r % 2) * 2).start()
    start_row(0, 0, 1, 2, 4, 8)
    start_row(1, 0, 1, 8)
    bias_in[0] = pay[1 + inner // 2]
    head_in[0] = pay[3]
    fc1_in.wait()
    for i in range(INNER):
        piece = gx[0:depth, i * hidden : (i + 1) * hidden].astype(F32)
        gx[depth : depth + hidden, i * depth : (i + 1) * depth] = jnp.transpose(piece).astype(BF16)
    near = [2, 3]
    far = [s for s in (6, 4, 7, 5) if s < dp_n]
    plane = d // 2
    end = (plane == 0) | (plane == dp_n // 2 - 1)
    middle = jnp.logical_not(end)

    def start_all(s):
        start_att(s)
        start_mlp(0, s)
        start_mlp(1, s)

    start_att(2)
    for s in far:
        start_att(s)
    start_mlp(0, 2)
    start_mlp(1, 2)

    @pl.when(end)
    def _():
        start_all(3)

    for s in far:
        start_mlp(0, s)

    @pl.when(end)
    def _():
        for s in far:
            start_mlp(1, s)

    up_in = stay(*mlp_copy(0, 0))

    @pl.when(lead)
    def _():
        for a, (src, dst) in enumerate(att_pairs(0)):
            pltpu.make_async_copy(src, dst, local_sem.at[20 + a]).start()

    wait_row(0, 1)
    start_row(0, 1, 2, 4, 8)
    wait_row(0, 2)
    start_row(0, 2, 4, 8)
    start_row(1, 0, 2)

    def small_waits(kind):
        buf = (vec_in, bias_in, head_in)[kind]
        rest = buf.at[pl.ds(1, buf.shape[0] - 1)]
        return small_copy(kind, rest, rest, 0, 1)

    for kind in range(2):
        small_waits(kind).wait_recv()

    @pl.when(lead)
    def _():
        for s in range(1, dp_n):
            head_in_copy(s, 0).wait_recv()

    @pl.when(follow)
    def _():
        for s in range(dp_n):
            head_in_copy(s, 1).wait_recv()

    for j in range(chips):
        vecs[:, j * 128 : (j + 1) * 128] = vec_in[chip ^ j]
    bias8 = jnp.zeros((8, 128), F32)
    head8 = jnp.zeros((8, 128), F32)
    head_rel = core ^ (inner // 2)
    for s in range(dp_n):
        bias8 = bias8 + bias_in[s]
        head8 = head8 + head_in[s * 2 + head_rel]
    second = inner % 2 == 1
    bias_t = columns_of(bias8)
    up_bias = jnp.concatenate(
        [jnp.where(second, bias_t[:, 4 + k : 5 + k], bias_t[:, k : k + 1]) for k in range(4)], axis=0
    )
    head4 = jnp.where(second, head8[4:], head8[:4])
    qkv_bias[0:1, :] = jnp.concatenate([head4[k : k + 1] for k in range(4)], axis=1)
    lane = lax.broadcasted_iota(jnp.int32, (1, 128), 1)
    keys[...] = jnp.zeros_like(keys)
    for q in range(4):
        at = slice(q * 128, (q + 1) * 128)
        keys[0:1, at] = ((t ^ ((q % 2) * 2 + q // 2)) * 128 + lane).astype(F32)
        for dy in range(2):
            peer = vec_in[(core * 2 + dy) * 2 + q % 2]
            keys[1 + dy : 2 + dy, at] = jnp.where((core ^ (q // 2)) == 1, peer[6:7, :], peer[5:6, :])
        queries[at, :] = columns_of(keys[:, at])

    def norm_slot(k):
        @pl.loop(0, rows // 16)
        def _(j):
            at = pl.ds(pl.multiple_of(k * rows + j * 16, 16), 16)
            value = xs[at, :].astype(F32)
            mean = jnp.mean(value, axis=-1, keepdims=True)
            centered = value - mean
            inv = lax.rsqrt(jnp.mean(centered * centered, axis=-1, keepdims=True) + EPS)
            n2[at, :] = (centered * inv * vecs[2:3, :] + vecs[3:4, :]).astype(BF16)
            stats[at, 0:64] = jnp.broadcast_to(mean, (16, 64))
            stats[at, 64:128] = jnp.broadcast_to(inv, (16, 64))

    x_in.wait()
    norm_slot(0)
    wait_row(0, 3)
    start_row(0, 3, 4, 8)
    start_row(1, 0, 4)
    for k in (1, 2, 3):
        norm_slot(k)
    wait_row(1, 1)
    start_row(1, 1, 2, 4, 8)
    wait_row(1, 2)
    start_row(1, 2, 4, 8)

    @pl.when(middle)
    def _():
        start_all(3)

    start_all(1)
    for k in (4, 5, 6, 7):
        wait_row(0, k)
        start_row(0, k, 8)
        norm_slot(k)

    @pl.when(middle)
    def _():
        for s in far:
            start_mlp(1, s)

    for k in range(8, 16):
        wait_row(0, k)
        norm_slot(k)
    wait_row(1, 3)
    start_row(1, 3, 4, 8)

    def mine(dy, q):
        return ((q // 2) * 8 + (q % 2) * 4 + dy * 2 + core) * rows

    for dy in range(2):
        for q in range(4):
            @pl.loop(0, rows // 16)
            def _(j):
                at = pl.ds(pl.multiple_of(mine(dy, q) + j * 16, 16), 16)
                to = pl.ds(pl.multiple_of(dy * SEQ + q * rows + j * 16, 16), 16)
                normed = (xs[at, :].astype(F32) - stats[at, 0:1]) * stats[at, 64:65]
                n1[to, :] = (normed * vecs[0:1, :] + vecs[1:2, :]).astype(BF16)

    @pl.when(lead)
    def _():
        for a, (src, dst) in enumerate(att_pairs(0)):
            pltpu.make_async_copy(src, dst, local_sem.at[20 + a]).wait()
        for copy in pass_att(0):
            copy.start()
        for s in near + [1] + far:
            for a, dst in enumerate(att_land(s)):
                remote(dst, dst, att_send.at[a, s], att_recv.at[a, s], s, 0).wait_recv()
            for copy in pass_att(s):
                copy.start()

    @pl.when(follow)
    def _():
        for s in range(dp_n):
            for copy in pass_att(s):
                copy.wait_recv()

    rope_in.wait()
    lanes128 = lax.broadcasted_iota(jnp.int32, (SEQ, 128), 1)

    def rope_tables(sign):
        at = [pl.ds(pl.multiple_of((t ^ ((q % 2) * 2 + q // 2)) * 128, 128), 128) for q in range(4)]
        cosine = jnp.concatenate([rope[0, a, :] for a in at], axis=0)
        sine = jnp.concatenate([rope[1, a, :] for a in at], axis=0) * sign
        lower = jnp.where(lanes128 < ROT // 2, -sine, 0.0)
        upper = jnp.where((lanes128 >= ROT // 2) & (lanes128 < ROT), sine, 0.0)
        return cosine, lower, upper

    def turn(value, tables):
        cosine, lower, upper = tables
        head = value[:, :128]
        head = (
            head * cosine
            + pltpu.roll(head, 128 - ROT // 2, 1) * lower
            + pltpu.roll(head, ROT // 2, 1) * upper
        )
        return jnp.concatenate([head, value[:, 128:]], axis=1)

    @pl.loop(0, 2)
    def _(dy):
        at = pl.ds(pl.multiple_of(dy * SEQ, SEQ), SEQ)
        tables = rope_tables(1.0)
        rows_in = n1[at, :]
        value = mm(rows_in, att_w[:, :HD]) + qkv_bias[0:1, :HD]
        query = turn(value, tables).astype(BF16)
        key = turn(mm(rows_in, att_w[:, HD : 2 * HD]), tables).astype(BF16)
        val = (mm(rows_in, att_w[:, 2 * HD :]) + qkv_bias[0:1, HD:]).astype(BF16)
        q_s[at, :] = query
        k_s[at, :] = key
        v_s[at, :] = val
        seg_q = jnp.where(dy == 0, queries[:, 1:2], queries[:, 2:3])
        seg_k = jnp.where(dy == 0, keys[1:2, :], keys[2:3, :])
        allowed = (keys[0:1, :] <= queries[:, 0:1]) & (seg_q == seg_k)
        scores = jnp.where(allowed, mm_tail(query, key) * scale, NEG_FILL)
        peak = jnp.max(scores, axis=-1, keepdims=True)
        total = jnp.where(allowed, jnp.exp(scores - peak), 0.0)
        share = (total / jnp.sum(total, axis=-1, keepdims=True)).astype(BF16)
        prob[at, :] = share
        got = mm(share, val)
        ctx[at, :] = got.astype(BF16)
        ctx_t[:, at] = jnp.transpose(got).astype(BF16)

    def cot_mine(dy, lanes):
        parts = [cots[pl.ds(pl.multiple_of(mine(dy, q), 128), rows), lanes] for q in range(4)]
        return jnp.concatenate(parts, axis=0)

    for k in (4, 5, 6, 7):
        wait_row(1, k)
        start_row(1, k, 8)
    cot_in.wait()
    for k in range(8, 16):
        wait_row(1, k)
    sums[...] = jnp.zeros_like(sums)

    @pl.loop(0, rows // 16)
    def _(j):
        at = pl.ds(pl.multiple_of(j * 16, 16), 16)
        sums[4:5, :] += jnp.sum(cots[at, :].astype(F32), axis=0, keepdims=True)

    for dy in range(2):
        cctx[dy * SEQ : (dy + 1) * SEQ, :] = mm_tail(cot_mine(dy, slice(None)), proj_w[...]).astype(BF16)

    @pl.loop(0, width // chunk)
    def _(c):
        lanes = pl.ds(pl.multiple_of(c * chunk, chunk), chunk)
        both = jnp.concatenate([cot_mine(0, lanes), cot_mine(1, lanes)], axis=0)
        gx[3 * HD : 4 * HD, lanes] = mm(ctx_t[...], both).astype(BF16)

    qkv_sum[...] = jnp.zeros_like(qkv_sum)

    def backward(dy):
        at = slice(dy * SEQ, (dy + 1) * SEQ)
        tables = rope_tables(-1.0)
        share = prob[at, :].astype(F32)
        got = cctx[at, :]
        delta = jnp.sum(got.astype(F32) * ctx[at, :].astype(F32), axis=-1, keepdims=True)
        score_cot = share * (mm_tail(got, v_s[at, :]) - delta)
        value_cot = mm(jnp.transpose(share).astype(BF16), got)
        query_cot = turn(mm(score_cot.astype(BF16), k_s[at, :]) * scale, tables)
        key_cot = turn(mm(jnp.transpose(score_cot).astype(BF16), q_s[at, :]) * scale, tables)
        qkv_sum[0:1, :HD] += jnp.sum(query_cot, axis=0, keepdims=True)
        qkv_sum[0:1, HD:] += jnp.sum(value_cot, axis=0, keepdims=True)
        for k, part in enumerate((query_cot, key_cot, value_cot)):
            low[at, k * HD : (k + 1) * HD] = part.astype(BF16)
            low_t[k * HD : (k + 1) * HD, at] = jnp.transpose(part).astype(BF16)

    backward(0)
    backward(1)

    up_in.wait()
    for copy in mlp_started[0]:
        copy.wait_send()

    @pl.loop(0, width // chunk)
    def _(c):
        lanes = pl.ds(pl.multiple_of(c * chunk, chunk), chunk)
        gx[0 : 3 * HD, lanes] = mm(low_t[...], n1[:, lanes]).astype(BF16)

    def pair_copy(s):
        return remote(
            lane_cut(gx, (d ^ s) * depth, depth), pair_hbm.at[:, s * depth : (s + 1) * depth],
            pair_send.at[s], pair_recv.at[s], 0, 1,
        )

    @pl.when(follow)
    def _():
        for s in near + [1] + far + [0]:
            pair_copy(s).start()

    for dy in range(2):
        @pl.loop(0, width // chunk)
        def _(c):
            lanes = pl.ds(pl.multiple_of(c * chunk, chunk), chunk)
            part = mm_tail(low[dy * SEQ : (dy + 1) * SEQ, :], att_w[lanes, :])
            gain = vecs[0:1, lanes]
            cross = jnp.zeros((1, chunk), F32)
            for q in range(4):
                at = pl.ds(pl.multiple_of(mine(dy, q), 128), rows)
                piece = part[q * rows : (q + 1) * rows]
                normed = (xs[at, lanes].astype(F32) - stats[at, 0:1]) * stats[at, 64:65]
                cross = cross + jnp.sum(piece * normed, axis=0, keepdims=True)
                n1[dy * SEQ + q * rows : dy * SEQ + (q + 1) * rows, lanes] = (piece * gain).astype(BF16)
            sums[0:1, lanes] += cross
            sums[1:2, lanes] += jnp.sum(part, axis=0, keepdims=True)

    def ga_copy(s):
        return remote(
            lane_cut(gx, (d ^ s) * depth, depth), ra_hbm.at[:, s * depth : (s + 1) * depth],
            ga_send.at[s], ga_recv.at[s], s, 0,
        )

    stages = (q_s, k_s, v_s)

    @pl.when(lead)
    def _():
        todo = near + [1] + far + [0]

        def fetch(k):
            s = todo[k]
            land = pair_hbm.at[:, s * depth : (s + 1) * depth]
            remote(land, land, pair_send.at[s], pair_recv.at[s], 0, 1).wait_recv()
            copy = pltpu.make_async_copy(land, stages[k % 3], g_local.at[k % 3])
            copy.start()
            return copy

        held = [fetch(0), fetch(1)]
        for k, s in enumerate(todo):
            if k + 2 < len(todo):
                held.append(fetch(k + 2))
            held[k].wait()
            stage = stages[k % 3]
            here = lane_cut(gx, (d ^ s) * depth, depth)

            @pl.loop(0, 4 * HD // 64)
            def _(i):
                at = pl.ds(pl.multiple_of(i * 64, 64), 64)
                here[at, :] = (here[at, :].astype(F32) + stage[at, :].astype(F32)).astype(BF16)

            if s:
                ga_copy(s).start()
            else:
                pltpu.make_async_copy(here, ra_hbm.at[:, 0:depth], local_sem.at[22]).start()

    for s in near + [1] + far:
        mlp_wait(0, s)

    @pl.loop(0, tokens // chunk)
    def _(j):
        at = pl.ds(pl.multiple_of(j * chunk, chunk), chunk)
        value = mm_tail(up_t[...], n2[at, :]) + up_bias
        pre[:, at] = value
        hid_t[:, at] = (value * gelu_half(value)).astype(BF16)

    def g_send_copy(a, s):
        at = pl.ds(pl.multiple_of(s * depth, 128), depth)
        return remote(
            (gu_hbm, gd_hbm)[a].at[:, at], (ru_hbm, rd_hbm)[a].at[:, at],
            g_send.at[a, s], g_recv.at[a, s], s, 0,
        )

    def g_local_copy(a, s, b, dst):
        at = pl.ds(pl.multiple_of(s * depth, 128), depth)
        return pltpu.make_async_copy(ring.at[b], dst.at[:, at], g_local.at[b])

    def grads(a, go):
        left, right = ((act_t, n2), (hid_t, cots))[a]
        stage, own = ((gu_hbm, ru_hbm), (gd_hbm, rd_hbm))[a]

        def block(s, b):
            at = pl.ds(pl.multiple_of((d ^ s) * depth, 128), depth)
            ring[b] = mm(left[...], right[:, at]).astype(BF16)

        def at_step(k):
            return (k + 1) % (dp_n - 1) + 1

        @pl.loop(0, dp_n - 1)
        def _(k):
            s = at_step(k)
            b = k % 3

            @pl.when(k >= 2)
            def _():
                before = at_step(k - 2)
                g_local_copy(a, before, (k + 1) % 3, stage).wait()
                if go:
                    g_send_copy(a, before).start()

            block(s, b)
            g_local_copy(a, s, b, stage).start()

        last = dp_n - 2
        for k in (last - 1, last):
            s = at_step(k)
            g_local_copy(a, s, k % 3, stage).wait()
            if go:
                g_send_copy(a, s).start()
        b = (last + 1) % 3
        block(0, b)
        copy = g_local_copy(a, 0, b, own)
        copy.start()
        copy.wait()

    grads(1, True)
    down_in.wait()
    for s in near + [1] + far:
        mlp_wait(1, s)
    up_sum[...] = jnp.zeros_like(up_sum)

    @pl.loop(0, tokens // chunk)
    def _(j):
        at = pl.ds(pl.multiple_of(j * chunk, chunk), chunk)
        value = mm_tail(down_w[...], cots[at, :]) * gelu_slope(pre[:, at])
        up_sum[:, 0:1] += jnp.sum(value, axis=1, keepdims=True)
        act_t[:, at] = value.astype(BF16)

    grads(0, False)

    @pl.loop(0, tokens // chunk)
    def _(j):
        at = pl.ds(pl.multiple_of(j * chunk, chunk), chunk)
        act = jnp.transpose(act_t[:, at].astype(F32)).astype(BF16)

        @pl.loop(0, width // chunk)
        def _(c):
            lanes = pl.ds(pl.multiple_of(c * chunk, chunk), chunk)
            part = mm(act, up_t[:, lanes])
            gain = vecs[2:3, lanes]
            cross = jnp.zeros((1, chunk), F32)
            for m in range(4):
                at = pl.ds(pl.multiple_of(j * chunk + m * rows, 128), rows)
                piece = part[m * rows : (m + 1) * rows]
                normed = (xs[at, lanes].astype(F32) - stats[at, 0:1]) * stats[at, 64:65]
                cross = cross + jnp.sum(piece * normed, axis=0, keepdims=True)
                spot = pl.ds(pl.multiple_of((m // 2) * SEQ + j * rows, 128), rows)
                extra = jnp.where(core == m % 2, n1[spot, lanes].astype(F32), 0.0)
                n2[at, lanes] = (piece * gain + extra).astype(BF16)
            sums[2:3, lanes] += cross
            sums[3:4, lanes] += jnp.sum(part, axis=0, keepdims=True)

    for copy in row_started[0]:
        copy.wait_send()
    pl.semaphore_signal(credit.at[0], inc=1, device_id=(d, t ^ 1), device_id_type=MESH)
    pl.semaphore_signal(credit.at[1], inc=1, device_id=(d, t ^ 2), device_id_type=MESH)

    blank = jnp.zeros((4, 128), F32)
    up_rows = [jnp.transpose(up_sum[k * 128 : (k + 1) * 128, :])[0:1] for k in range(4)]
    up_rows = jnp.concatenate(up_rows, axis=0)
    qkv_rows = jnp.concatenate([qkv_sum[0:1, k * 128 : (k + 1) * 128] for k in range(4)], axis=0)

    def place(value):
        return jnp.where(
            second, jnp.concatenate([blank, value], axis=0), jnp.concatenate([value, blank], axis=0)
        )

    up_place[...] = place(up_rows)
    head_place[...] = place(qkv_rows)

    def window(to):
        return lane_cut(sums, to * 128, 128)

    def back_copy(kind, src, dst, dp_xor, tp_xor):
        return remote(src, dst, back_send.at[kind], back_recv.at[kind], dp_xor, tp_xor)

    def head_copy(s, dc):
        return remote(
            head_place, head_back.at[s * 2 + dc], headb_send.at[s * 2 + dc], headb_recv.at[s * 2 + dc], s, dc
        )

    for r in range(1, chips):
        back_copy(0, window(chip ^ r), vec_back.at[r], r // 2, (r % 2) * 2).start()
    for s in range(1, dp_n):
        back_copy(1, up_place, bias_back.at[s], s, 0).start()

    @pl.when(lead)
    def _():
        for s in range(1, dp_n):
            head_copy(s, 0).start()

    @pl.when(follow)
    def _():
        for s in range(dp_n):
            head_copy(s, 1).start()

    bufs = (cots, n2)

    def landing(a, bit, j, there):
        if bit == 8:
            if a == 0:
                side = core if there else 1 - core
                return row_cut(xs, (2 * j + side) * rows, rows)
            return row_cut(n1, j * rows, rows)
        if bit == 4:
            return row_cut((act_t, up_t)[a], j * rows, rows)
        base = (down_w, hid_t)[a]
        return row_cut(base, (j if bit == 2 else 2) * rows, rows)

    def rs_copy(a, bit, j):
        return remote(
            slot(bufs[a], bit + j), landing(a, bit, j, True),
            rs_send.at[a, bit + j], rs_recv.at[a, bit + j], *hop[bit],
        )

    def rs_start(a, bit, j):
        start(rs_copy(a, bit, j))

    def rs_add(a, bit, j):
        land = landing(a, bit, j, False)
        remote(land, land, rs_send.at[a, bit + j], rs_recv.at[a, bit + j], *hop[bit]).wait_recv()
        here = slot(bufs[a], j)

        @pl.loop(0, rows // 16)
        def _(i):
            at = pl.ds(pl.multiple_of(i * 16, 16), 16)
            here[at, :] = (here[at, :].astype(F32) + land[at, :].astype(F32)).astype(BF16)

    for s in near + [1] + far[:2]:
        g_send_copy(0, s).start()

    pl.semaphore_wait(credit.at[0], 1)
    pl.semaphore_wait(credit.at[1], 1)
    for j in (7, 5, 6, 4, 3, 1, 2, 0):
        rs_start(1, 8, j)

    for copy in row_started[1]:
        copy.wait_send()
    for j in range(4):
        for k in {2: (7, 5), 3: (6, 4)}.get(j, ()):
            rs_add(1, 8, k)
            rs_start(1, 4, k - 4)
        hid = jnp.transpose(hid_t[:, j * chunk : (j + 1) * chunk].astype(F32)).astype(BF16)
        here = [ctx[h * SEQ + j * rows : h * SEQ + (j + 1) * rows, :] for h in range(2)]
        here = jnp.concatenate(here, axis=0)

        @pl.loop(0, width // chunk)
        def _(c):
            lanes = pl.ds(pl.multiple_of(c * chunk, chunk), chunk)
            base = mm(hid, down_w[:, lanes])
            extra = mm(here, proj_w[:, lanes])
            for m in range(4):
                more = jnp.where(core == m % 2, extra[(m // 2) * rows : (m // 2 + 1) * rows], 0.0)
                piece = base[m * rows : (m + 1) * rows] + more
                cots[j * chunk + m * rows : j * chunk + (m + 1) * rows, lanes] = piece.astype(BF16)

    for bit in (2, 1):
        dp_xor, tp_xor = hop[bit]
        pl.semaphore_signal(
            credit.at[1 + (3 - bit)], inc=1, device_id=(d ^ dp_xor, t ^ tp_xor), device_id_type=MESH
        )
    own_x = row_cut(hid_t, 3 * rows, rows)
    own_cot = row_cut(down_w, 3 * rows, rows)
    x_again = stay(x_ref, own_x)
    cot_again = stay(cot_ref, own_cot)

    for j in (7, 5, 6, 4, 3, 1, 2, 0):
        rs_start(0, 8, j)
    for j in (3, 1, 2, 0):
        rs_add(1, 8, j)
    for j in (7, 5, 6, 4):
        rs_add(0, 8, j)
        rs_start(0, 4, j - 4)
    for j in (3, 1, 2, 0):
        rs_add(0, 8, j)
    pl.semaphore_wait(credit.at[2], 1)
    pl.semaphore_wait(credit.at[3], 1)

    def rs_tail(a, after):
        rs_add(a, 4, 3)
        rs_start(a, 2, 1)
        rs_add(a, 4, 1)
        rs_add(a, 4, 2)
        rs_start(a, 2, 0)
        rs_add(a, 2, 1)
        rs_start(a, 1, 0)
        after()
        rs_add(a, 4, 0)
        rs_add(a, 2, 0)
        rs_add(a, 1, 0)

    outs = []

    def leave(src, dst):
        copy = pltpu.make_async_copy(src, dst, out_sem.at[len(outs)])
        copy.start()
        outs.append(copy)
        return copy

    def late():
        for s in far[2:]:
            g_send_copy(0, s).start()

    rs_tail(1, late)
    cot_again.wait()
    x_again.wait()

    @pl.loop(0, rows // 16)
    def _(j):
        at = pl.ds(pl.multiple_of(j * 16, 16), 16)
        scaled = n2[at, :].astype(F32)
        inv = stats[at, 64:65]
        normed = (own_x[at, :].astype(F32) - stats[at, 0:1]) * inv
        inner_mean = jnp.mean(scaled, axis=-1, keepdims=True)
        cross = jnp.mean(scaled * normed, axis=-1, keepdims=True)
        pre[at, :] = own_cot[at, :].astype(F32) + inv * (scaled - inner_mean - normed * cross)

    grad_out = leave(pre.at[0:rows, :], input_out)

    rs_tail(0, lambda: None)

    @pl.loop(0, rows // 16)
    def _(j):
        at = pl.ds(pl.multiple_of(j * 16, 16), 16)
        total = own_x[at, :].astype(F32) + cots[at, :].astype(F32) + vecs[4:5, :]
        cots[at, :] = total.astype(BF16)

    last = [leave(slot(cots, 0), block_out)]
    def back_waits(kind):
        buf = (vec_back, bias_back)[kind]
        rest = buf.at[pl.ds(1, buf.shape[0] - 1)]
        return back_copy(kind, rest, rest, 0, 1)

    for kind in range(2):
        back_waits(kind).wait_recv()
    for kind in range(2):
        small_waits(kind).wait_send()
    meet.wait_send()
    head_in_each(lambda copy: copy.wait_send())
    total = window(chip)[...]
    for r in range(1, chips):
        total = total + vec_back[r]
    pay[0] = total
    meet_back = back_copy(2, pay.at[0], pair_back, 0, 1)
    meet_back.start()
    for k in (1, 2, 3):
        pay[k] = jnp.zeros((8, 128), F32)
    pay[1 + inner // 2] += up_place[...]
    for s in range(1, dp_n):
        pay[1 + (inner ^ (s % INNER)) // 2] += bias_back[s]
    for s in range(dp_n):
        @pl.when(att_active(s))
        def _():
            if s == 0:
                pay[3] += head_place[...]
            else:
                head_copy(s, 0).wait_recv()
                pay[3] += head_back[2 * s]
            head_copy(s, 1).wait_recv()
            pay[3] += head_back[2 * s + 1]


    @pl.when(lead)
    def _():
        pltpu.make_async_copy(
            lane_cut(gx, d * depth, depth), ra_hbm.at[:, 0:depth], local_sem.at[22]
        ).wait()

    for s in range(1, dp_n):
        @pl.when(att_active(s))
        def _():
            ga_copy(s).wait_recv()

    for s in range(1, dp_n):
        g_send_copy(1, s).wait_recv()
    for s in range(1, dp_n):
        g_send_copy(0, s).wait_recv()
    meet_back.wait_recv()
    meet_back.wait_send()
    pay[0] += pair_back[...]
    last.append(leave(pay, tail_out))
    for s in range(1, dp_n):
        for a in range(2):
            g_send_copy(a, s).wait_send()

        @pl.when(att_active(s))
        def _():
            for a, (src, dst) in enumerate(att_pairs(s)):
                remote(src, dst, att_send.at[a, s], att_recv.at[a, s], s, 0).wait_send()

        @pl.when(lead)
        def _():
            ga_copy(s).wait_send()

    @pl.when(lead)
    def _():
        for s in range(dp_n):
            for copy in pass_att(s):
                copy.wait_send()

    @pl.when(follow)
    def _():
        for s in range(dp_n):
            pair_copy(s).wait_send()

    @pl.when(lead)
    def _():
        for s in range(1, dp_n):
            head_copy(s, 0).wait_send()

    @pl.when(follow)
    def _():
        for s in range(dp_n):
            head_copy(s, 1).wait_send()

    for kind in range(2):
        back_waits(kind).wait_send()
    for copy in started + mlp_started[1]:
        copy.wait_send()
    for copy in [grad_out] + last:
        copy.wait()


def finish_kernel(
    dp_n, tp_n,
    block_ref, input_ref, tail_ref, ru_ref, rd_ref, ra_ref,
    block_out, input_out, up_out, down_out, qkv_out, proj_out,
    v0, v1, v2, v3, v4, v5, bq_out, bf_out,
    block, grad, ru, rd, ra, up, down, qkv, proj, tail, wide_f, in_sem, out_sem,
):
    d = lax.axis_index("dp")
    t = lax.axis_index("tp")
    inner = d % INNER
    core = t % 2
    hidden, width = ru.shape
    depth = width // dp_n
    groups = dp_n // INNER
    copies = []

    def fetch(src, dst):
        copy = pltpu.make_async_copy(src, dst, in_sem.at[len(copies)])
        copy.start()
        copies.append(copy)
        return copy

    rd_in = [fetch(row_cut(rd_ref, k * 128, 128), row_cut(rd, k * 128, 128)) for k in range(hidden // 128)]
    ru_in = [fetch(row_cut(ru_ref, k * 128, 128), row_cut(ru, k * 128, 128)) for k in range(hidden // 128)]
    ra_in = []
    for hl in range(2):
        first = ((inner // 2) ^ core) * 2 + ((inner % 2) ^ hl)
        for o in range(groups):
            k = hl * groups + o
            ra_in.append(fetch(lane_cut(ra_ref, (first + o * INNER) * depth, depth), lane_cut(ra, k * depth, depth)))
    tail_in = fetch(tail_ref, tail)
    block_in = fetch(block_ref, block)
    grad_in = fetch(input_ref, grad)
    outs = []

    def leave(src, dst):
        copy = pltpu.make_async_copy(src, dst, out_sem.at[len(outs)])
        copy.start()
        outs.append(copy)

    def total_of(ref, at, k):
        total = ref[at, k * depth : (k + 1) * depth].astype(F32)
        for s in range(k + INNER, dp_n, INNER):
            total = total + ref[at, s * depth : (s + 1) * depth].astype(F32)
        return total

    for c in range(hidden // 128):
        rd_in[c].wait()
        at = slice(c * 128, (c + 1) * 128)
        for k in range(INNER):
            down[k, at, :] = total_of(rd, at, k)
            leave(down.at[k, at, :], row_cut(down_out, (inner ^ k) * hidden + c * 128, 128))
    block_in.wait()
    leave(block, block_out)
    grad_in.wait()
    leave(grad, input_out)
    for c in range(hidden // 128):
        ru_in[c].wait()
        at = slice(c * 128, (c + 1) * 128)
        for k in range(INNER):
            up[k, :, at] = jnp.transpose(total_of(ru, at, k))
            leave(up.at[k, :, at], lane_cut(up_out, (inner ^ k) * hidden + c * 128, 128))
    for hl in range(2):
        total = jnp.zeros((4 * HD, depth), F32)
        for o in range(groups):
            k = hl * groups + o
            ra_in[k].wait()
            total = total + ra[:, k * depth : (k + 1) * depth].astype(F32)
        qkv[:, hl * 3 * HD : (hl + 1) * 3 * HD] = jnp.transpose(total[: 3 * HD])
        proj[hl * HD : (hl + 1) * HD, :] = total[3 * HD :]
    leave(qkv, qkv_out)
    leave(proj, proj_out)

    tail_in.wait()
    row = tail[0]
    row = jnp.where((t % 2) == 1, pltpu.roll(row, 64, 1), row)
    for k, ref in enumerate((v0, v1, v2, v3, v4, v5)):
        ref[...] = row[min(k, 4) : min(k, 4) + 1, :64]
    line = lax.broadcasted_iota(jnp.int32, (8, 128), 0)
    heads = tail[3]
    heads = jnp.where(d % 2 == 1, pltpu.roll(heads, 64, 1), heads)
    for k in range(2):
        picked = jnp.sum(jnp.where(line == k * 4 + d // 2, heads, 0.0), axis=0, keepdims=True)
        bq_out[k : k + 1, :] = picked[:, :64]
    cols = bf_out.shape[0]
    both = jnp.concatenate([tail[1], tail[2]], axis=0)
    both = pltpu.roll(both, (128 - d * cols) % 128, 1)
    wide_f[pl.ds(0, 16, stride=2), :] = both
    wide_f[pl.ds(1, 16, stride=2), :] = pltpu.roll(both, 64, 1)
    spots = wide_f.shape[0]
    full = jnp.concatenate([wide_f[...], jnp.zeros((128 - spots, 128), F32)], axis=0)
    bf_out[...] = jnp.transpose(full)[:cols, :spots]
    for copy in outs:
        copy.wait()


def solution(mesh):
    dp_n, tp_n = mesh.shape["dp"], mesh.shape["tp"]
    outer = dp_n // INNER
    devices = dp_n * tp_n

    def send(value, dp_xor, tp_xor, keep=None):
        pairs = []
        for d in range(dp_n):
            for t in range(tp_n):
                if keep is None or keep(d, t):
                    pairs.append((d * tp_n + t, (d ^ dp_xor) * tp_n + (t ^ tp_xor)))
        return lax.ppermute(value, AXES, pairs)

    def scatter_small(value, flat):
        held = value
        step = devices // 2
        while step >= 1:
            dp_xor, tp_xor = step // tp_n, step % tp_n
            high = (flat // step) % 2 == 1
            first, second = held[:step], held[step:]
            other = send(jnp.where(high, first, second), dp_xor, tp_xor)
            held = jnp.where(high, second, first) + other
            step //= 2
        return held[0]

    def scatter_rows(value):
        for dp_xor, tp_xor in ((0, 1), (0, 2), (1, 0), (2, 0)):
            half = value.shape[0] // 2
            other = send(value[half:], dp_xor, tp_xor)
            value = value[:half].astype(F32) + other.astype(F32)
            if half > value.shape[0] or (dp_xor, tp_xor) != (2, 0):
                value = value.astype(BF16)
        return value

    def on_device(
        block_input, segment_ids, w_qkv, b_qkv, w_out, b_out, w_fc1, b_fc1, w_fc2, b_fc2,
        ln1_gain, ln1_bias, ln2_gain, ln2_bias, cotangent,
    ):
        d = lax.axis_index("dp")
        t = lax.axis_index("tp")
        flat = d * tp_n + t
        inner = d % INNER
        core = t % 2
        lead = (inner // 2) == core
        rows, width = block_input.shape
        depth = w_qkv.shape[0]
        hidden_here = w_fc1.shape[1] // INNER
        head_here = w_out.shape[0] // HD
        heads = head_here * tp_n
        quarter = SEQ // tp_n
        qkv_bits = b_qkv.shape[1]

        vec = jnp.stack([ln1_gain, ln1_bias, ln2_gain, ln2_bias, b_out + b_fc2]).reshape(-1)
        seg_part = lax.dynamic_slice(segment_ids.reshape(-1), (t * quarter,), (quarter,))
        sizes = [vec.size, b_qkv.size, b_fc1.size, quarter]
        payload = jnp.concatenate(
            [vec, b_qkv.reshape(-1), b_fc1.reshape(-1), seg_part.astype(F32)]
        )
        depth_wide = depth % 128 == 0
        flat_shape = lambda lead_n: (lead_n, width) if depth_wide else (dp_n, lead_n, depth)
        spread = lambda v: v if depth_wide else v.transpose(1, 0, 2).reshape(v.shape[1], width)
        payload = jnp.pad(payload, (0, PAY - payload.size)).reshape(8, PAY // 8)
        like = lambda *shape: jax.ShapeDtypeStruct(shape, BF16)
        dma = pltpu.SemaphoreType.DMA
        hop_count = (devices - 1).bit_length()
        any_spec = pl.BlockSpec(memory_space=pl.ANY)
        x_all, cot_all, up_w, down_w, qkv_w, out_w, small = pl.pallas_call(
            functools.partial(gather_kernel, dp_n, tp_n, depth_wide),
            out_shape=(
                like(16, rows, width),
                like(16, rows, width),
                like(width, hidden_here),
                like(*flat_shape(hidden_here)),
                like(width, 3 * HD),
                like(*flat_shape(HD)),
                jax.ShapeDtypeStruct((devices, 8, PAY // 8), F32),
            ),
            in_specs=[any_spec] * 7,
            out_specs=(any_spec,) * 7,
            scratch_shapes=[
                dma((2, 16)), dma((2, 16)), dma((2, dp_n)), dma((2, dp_n)),
                dma((2, dp_n)), dma((2, dp_n)), dma((2, dp_n)), dma((2, dp_n)),
                dma((hop_count,)), dma((hop_count,)), dma((6,)),
            ],
            compiler_params=pltpu.CompilerParams(collective_id=0, has_side_effects=True),
            name="gather_phase",
        )(block_input, cotangent, w_fc1, w_fc2, w_qkv, w_out, payload)
        down_w, out_w = spread(down_w), spread(out_w)
        small = jnp.take(small.reshape(devices, PAY), flat ^ jnp.arange(devices), axis=0)
        cuts = [0]
        for size in sizes:
            cuts.append(cuts[-1] + size)
        vecs = small[:, : cuts[1]].reshape(devices, 5, -1).transpose(1, 0, 2).reshape(5, width)
        gain_one, shift_one, gain_two, shift_two, out_bias = (vecs[k][None] for k in range(5))
        qkv_bias_all = (
            small[:, cuts[1] : cuts[2]]
            .reshape(dp_n, tp_n, head_here, qkv_bits)
            .transpose(1, 2, 0, 3)
            .reshape(heads, 2 * HD)
        )
        head = (t // 2) * INNER + inner
        qkv_bias = lax.dynamic_slice(qkv_bias_all, (head, 0), (1, 2 * HD))
        up_rows, up_cols = b_fc1.shape
        up_bias_all = (
            small[:, cuts[2] : cuts[3]]
            .reshape(dp_n, tp_n, up_rows, up_cols)
            .transpose(1, 2, 0, 3)
            .reshape(tp_n * INNER, hidden_here)
        )
        up_bias = lax.dynamic_slice(up_bias_all, (t * INNER + inner, 0), (1, hidden_here))
        seg_all = small[:, cuts[3] : cuts[4]].reshape(dp_n, tp_n, quarter)

        x_rows = x_all.reshape(16 * rows, width).astype(F32)
        cot_rows = cot_all.reshape(16 * rows, width)
        row_mean = jnp.mean(x_rows, axis=-1, keepdims=True)
        centered = x_rows - row_mean
        row_var = jnp.mean(centered * centered, axis=-1, keepdims=True)
        inv_std = lax.rsqrt(row_var + EPS)
        normed = centered * inv_std
        norm_two = (normed * gain_two + shift_two).astype(BF16)

        def mine(value):
            split = value.reshape((2, 2, 2, 2, rows) + value.shape[1:])
            cut = lax.dynamic_index_in_dim(split, core, 3, keepdims=False)
            return jnp.moveaxis(cut, 2, 0).reshape((2 * SEQ,) + value.shape[1:])

        def unmine(value):
            split = value.reshape((2, 2, 2, rows) + value.shape[1:])
            cut = jnp.moveaxis(split, 0, 2)[:, :, :, None]
            where = (jnp.arange(2) == core).reshape((1, 1, 1, 2) + (1,) * value.ndim)
            full = jnp.where(where, cut, jnp.zeros_like(cut))
            return full.reshape((16 * rows,) + value.shape[1:])

        norm_one = (mine(normed) * gain_one + shift_one).astype(BF16)
        cot_mine = mine(cot_rows)

        pre_act = mm(norm_two, up_w) + up_bias
        half_gelu = gelu_half(pre_act)
        hidden = (pre_act * half_gelu).astype(BF16)
        down_grad = mm_lead(hidden, cot_rows)
        act_cot = mm_tail(cot_rows, down_w) * gelu_slope(pre_act)
        up_bias_part = jnp.sum(act_cot, axis=0)
        act_low = act_cot.astype(BF16)
        up_grad = mm_lead(norm_two, act_low)
        up_grad, down_grad = up_grad.astype(BF16), down_grad.astype(BF16)

        def cut_block(value, s):
            return lax.dynamic_slice(value, ((d ^ s) * depth, 0), (depth, value.shape[1]))

        def cut_across(value, s):
            return lax.dynamic_slice(value, (0, (d ^ s) * depth), (value.shape[0], depth))

        with jax.named_scope("mlp_out"):
            up_back = [cut_block(up_grad, 0)] + [
                send(cut_block(up_grad, s), s, 0) for s in range(1, dp_n)
            ]
            down_back = [cut_across(down_grad, 0)] + [
                send(cut_across(down_grad, s), s, 0) for s in range(1, dp_n)
            ]

        order = jnp.stack([t ^ ((k % 2) * 2 + k // 2) for k in range(4)])
        position = (order[:, None] * quarter + jnp.arange(quarter)[None]).reshape(-1)
        inverse = jnp.exp(jnp.arange(ROT // 2, dtype=F32) * (-2.0 * math.log(10000.0) / ROT))
        angle = position.astype(F32)[:, None] * inverse[None]
        cosine, sine = jnp.cos(angle)[None], jnp.sin(angle)[None]
        segs = []
        for dy in range(2):
            seq = (d // INNER) * INNER + (inner ^ (core * 2 + dy))
            rows_of = lax.dynamic_index_in_dim(seg_all, seq, 0, keepdims=False)
            segs.append(jnp.take(rows_of, order, axis=0).reshape(-1))
        segs = jnp.stack(segs)
        allowed = (position[None, :] <= position[:, None])[None] & (
            segs[:, :, None] == segs[:, None, :]
        )
        qkv = mm(norm_one, qkv_w)
        query = rotate((qkv[:, :HD] + qkv_bias[:, :HD]).reshape(2, SEQ, HD), cosine, sine).astype(BF16)
        key = rotate(qkv[:, HD : 2 * HD].reshape(2, SEQ, HD), cosine, sine).astype(BF16)
        val = (qkv[:, 2 * HD :] + qkv_bias[:, HD:]).astype(BF16).reshape(2, SEQ, HD)
        scale = HD ** (-0.5)

        def ein(eq, left, right):
            return jnp.einsum(eq, left, right, preferred_element_type=F32)

        masked = jnp.where(allowed, ein("sqd,skd->sqk", query, key) * scale, NEG_FILL)
        peak = jnp.max(masked, axis=-1, keepdims=True)
        log_total = peak + jnp.log(
            jnp.sum(jnp.where(allowed, jnp.exp(masked - peak), 0.0), axis=-1, keepdims=True)
        )
        prob_full = jnp.where(allowed, jnp.exp(masked - log_total), 0.0)
        prob_low = prob_full.astype(BF16)
        context = ein("sqk,skd->sqd", prob_low, val).astype(BF16)
        context_cot = mm_tail(cot_mine, out_w).astype(BF16).reshape(2, SEQ, HD)
        prob_cot = ein("sqd,skd->sqk", context_cot, val)
        row_delta = jnp.sum(context_cot.astype(F32) * context.astype(F32), axis=-1, keepdims=True)
        score_cot = (prob_full * (prob_cot - row_delta)).astype(BF16)
        query_cot = rotate(ein("sqk,skd->sqd", score_cot, key) * scale, cosine, -sine)
        key_cot = rotate(ein("sqk,sqd->skd", score_cot, query) * scale, cosine, -sine)
        val_cot = ein("sqk,sqd->skd", prob_low, context_cot)
        qkv_cot = jnp.concatenate([query_cot, key_cot, val_cot], axis=-1).reshape(2 * SEQ, 3 * HD)
        qkv_bias_part = jnp.concatenate(
            [jnp.sum(query_cot, axis=(0, 1)), jnp.sum(val_cot, axis=(0, 1))]
        )
        qkv_low = qkv_cot.astype(BF16)
        context_flat = context.reshape(2 * SEQ, HD)
        att_grad = jnp.concatenate(
            [mm_lead(norm_one, qkv_low).astype(BF16), mm_lead(cot_mine, context_flat).astype(BF16)],
            axis=1,
        )
        att_pair = send(att_grad, 0, 1, lambda dd, tt: (dd % INNER) // 2 != tt % 2)
        att_grad = (att_grad.astype(F32) + att_pair.astype(F32)).astype(BF16)
        with jax.named_scope("att_out"):
            own_att = cut_block(att_grad, 0)
            att_back = [jnp.where(lead, own_att, jnp.zeros_like(own_att))] + [
                send(cut_block(att_grad, s), s, 0, lambda dd, tt: (dd % INNER) // 2 == tt % 2)
                for s in range(1, dp_n)
            ]

        left = jnp.concatenate([hidden, unmine(context_flat)], axis=1)
        right = jnp.concatenate([down_w, out_w], axis=0)
        with jax.named_scope("branch"):
            branch = scatter_rows(mm(left, right).astype(BF16))
        block_output = (block_input.astype(F32) + branch + out_bias).astype(BF16)

        one_part = mm_tail(qkv_low, qkv_w)
        two_part = mm_tail(act_low, up_w)
        vec_terms = jnp.stack(
            [
                jnp.sum(one_part * mine(normed), axis=0),
                jnp.sum(one_part, axis=0),
                jnp.sum(two_part * normed, axis=0),
                jnp.sum(two_part, axis=0),
                jnp.sum(cotangent.astype(F32), axis=0),
            ]
        )
        scaled_part = (two_part * gain_two + unmine(one_part * gain_one)).astype(BF16)
        with jax.named_scope("normback"):
            scaled = scatter_rows(scaled_part)
        normed_own = normed[:rows]
        input_grad = cotangent.astype(F32) + inv_std[:rows] * (
            scaled
            - jnp.mean(scaled, axis=-1, keepdims=True)
            - normed_own * jnp.mean(scaled * normed_own, axis=-1, keepdims=True)
        )

        head_hot = (jnp.arange(heads) == head).astype(F32)[:, None]
        qkv_small = (
            (head_hot * qkv_bias_part[None])
            .reshape(tp_n, head_here, dp_n, qkv_bits)
            .transpose(2, 0, 1, 3)
            .reshape(devices, -1)
        )
        up_hot = (jnp.arange(tp_n * INNER) == t * INNER + inner).astype(F32)[:, None]
        up_small = (
            (up_hot * up_bias_part[None])
            .reshape(tp_n, up_rows, dp_n, up_cols)
            .transpose(2, 0, 1, 3)
            .reshape(devices, -1)
        )
        vec_small = vec_terms.reshape(5, devices, -1).transpose(1, 0, 2).reshape(devices, -1)
        with jax.named_scope("small_out"):
            own = scatter_small(jnp.concatenate([vec_small, qkv_small, up_small], axis=1), flat)
        vec_own = own[: cuts[1]].reshape(5, -1)
        qkv_bias_grad = own[cuts[1] : cuts[2]].reshape(b_qkv.shape)
        up_bias_grad = own[cuts[2] : cuts[3]].reshape(b_fc1.shape)

        up_total = jnp.zeros(w_fc1.shape, F32)
        down_total = jnp.zeros(w_fc2.shape, F32)
        for k in range(INNER):
            at = (inner ^ k) * hidden_here
            up_sum = sum(up_back[s].astype(F32) for s in range(k, dp_n, INNER))
            down_sum = sum(down_back[s].astype(F32) for s in range(k, dp_n, INNER))
            up_total = lax.dynamic_update_slice(up_total, up_sum, (0, at))
            down_total = lax.dynamic_update_slice(down_total, down_sum, (at, 0))
        att_sum = [sum(att_back[s].astype(F32) for s in range(k, dp_n, 2)) for k in range(2)]
        odd = inner % 2 == 1
        att_first = jnp.where(odd, att_sum[1], att_sum[0])
        att_second = jnp.where(odd, att_sum[0], att_sum[1])
        qkv_total = jnp.concatenate([att_first[:, : 3 * HD], att_second[:, : 3 * HD]], axis=1)
        out_total = jnp.concatenate([att_first[:, 3 * HD :].T, att_second[:, 3 * HD :].T], axis=0)
        return (
            block_output, input_grad, qkv_total, qkv_bias_grad, out_total, vec_own[4],
            up_total, up_bias_grad, down_total, vec_own[4],
            vec_own[0], vec_own[1], vec_own[2], vec_own[3],
        )

    def on_device_fused(
        block_input, segment_ids, w_qkv, b_qkv, w_out, b_out, w_fc1, b_fc1, w_fc2, b_fc2,
        ln1_gain, ln1_bias, ln2_gain, ln2_bias, cotangent,
    ):
        d = lax.axis_index("dp")
        t = lax.axis_index("tp")
        flat = d * tp_n + t
        inner = d % INNER
        core = t % 2
        lead = (inner // 2) == core
        rows, width = block_input.shape
        depth = w_qkv.shape[0]
        hidden_here = w_fc1.shape[1] // INNER
        head_here = w_out.shape[0] // HD
        heads = head_here * tp_n
        quarter = SEQ // tp_n
        qkv_bits = b_qkv.shape[1]

        up_rows = b_fc1.shape[0]
        per = ln1_gain.shape[0]
        seg_row = segment_ids.reshape(1, -1)
        small_in = [v.reshape(1, -1) for v in (ln1_gain, ln1_bias, ln2_gain, ln2_bias, b_out, b_fc2)]
        small_in += [b_qkv, b_fc1.T, seg_row]
        angle = np.arange(SEQ)[:, None] * np.exp(np.arange(ROT // 2) * (-2.0 * math.log(10000.0) / ROT))
        pad = np.zeros((SEQ, 128 - ROT))
        cosine = np.concatenate([np.cos(angle), np.cos(angle), pad + 1.0], axis=1)
        sine = np.concatenate([np.sin(angle), np.sin(angle), pad], axis=1)
        rope = jnp.asarray(np.stack([cosine, sine]), F32)
        like = lambda *shape: jax.ShapeDtypeStruct(shape, BF16)
        wide_f = lambda *shape: jax.ShapeDtypeStruct(shape, F32)
        dma = pltpu.SemaphoreType.DMA
        vb = lambda *shape: pltpu.VMEM(shape, BF16)
        vf = lambda *shape: pltpu.VMEM(shape, F32)
        any_spec = pl.BlockSpec(memory_space=pl.ANY)
        group = 16 * rows
        per_peer = dma((2, dp_n))
        pair = 2 * SEQ
        results = pl.pallas_call(
            functools.partial(fused_kernel, dp_n, tp_n),
            out_shape=(
                like(rows, width), wide_f(rows, width), wide_f(4, 8, 128),
                like(hidden_here, width), like(hidden_here, width),
                like(hidden_here, width), like(hidden_here, width), like(4 * HD, width),
                like(4 * HD, width),
            ),
            in_specs=[any_spec] * 16,
            out_specs=(any_spec,) * 9,
            scratch_shapes=[
                vb(group, width), vb(group, width), vb(group, width),
                vb(hidden_here, width), vb(hidden_here, width), vf(hidden_here, group),
                vb(hidden_here, group), vb(hidden_here, group), vb(3, hidden_here, depth),
                vf(group, 128), vf(8, width), vf(8, width), vf(hidden_here, 128),
                vb(width, 3 * HD), vb(HD, width), vb(pair, width),
                vb(pair, HD), vb(pair, HD), vb(pair, HD), vb(pair, SEQ),
                vb(pair, HD), vb(HD, pair), vb(pair, HD), vb(pair, 3 * HD), vb(3 * HD, pair),
                vb(4 * HD, width), vf(2, SEQ, 128),
                vf(6, 1, per), vf(*b_qkv.shape), vf(*b_fc1.T.shape), pltpu.VMEM(seg_row.shape, jnp.int32), vf(up_rows, 128),
                vf(4, 8, 128), vf(8, 128), vf(8, 128), vf(devices // 2, 8, 128), vf(dp_n, 8, 128), vf(2 * dp_n, 8, 128),
                vf(devices // 2, 8, 128), vf(dp_n, 8, 128), vf(2 * dp_n, 8, 128), vf(8, 128), vf(8, 128),
                vf(8, SEQ), vf(SEQ, 128), vf(8, 2 * HD), vf(8, 2 * HD),
                dma((2, 16)), dma((2, 16)), per_peer, per_peer, per_peer, per_peer, per_peer, per_peer,
                dma((3,)), dma((3,)), dma((2 * dp_n,)), dma((2 * dp_n,)), dma((3,)), dma((3,)), dma((2 * dp_n,)), dma((2 * dp_n,)),
                per_peer, per_peer, dma((3,)),
                dma((2, 16)), dma((2, 16)), dma((8,)), dma((8,)), dma((dp_n,)), dma((dp_n,)),
                dma((24,)), dma((24,)), pltpu.SemaphoreType.REGULAR((6,)),
            ],
            compiler_params=pltpu.CompilerParams(
                collective_id=0, has_side_effects=True, vmem_limit_bytes=67_043_328
            ),
            name="fused_block",
        )(block_input, cotangent, w_fc1, w_fc2, w_qkv, w_out, rope, *small_in)
        f32_out = lambda *shape: jax.ShapeDtypeStruct(shape, F32)
        ends = pl.pallas_call(
            functools.partial(finish_kernel, dp_n, tp_n),
            out_shape=(
                like(rows, width), f32_out(rows, width), f32_out(*w_fc1.shape), f32_out(*w_fc2.shape),
                f32_out(*w_qkv.shape), f32_out(*w_out.shape),
            ) + (f32_out(1, per),) * 6 + (f32_out(*b_qkv.shape), f32_out(*b_fc1.T.shape)),
            in_specs=[any_spec] * 6,
            out_specs=(any_spec,) * 6 + (pl.BlockSpec(memory_space=pltpu.VMEM),) * 8,
            scratch_shapes=[
                vb(rows, width), vf(rows, width), vb(hidden_here, width), vb(hidden_here, width),
                vb(4 * HD, width // 2), vf(INNER, depth, hidden_here), vf(INNER, hidden_here, depth),
                vf(*w_qkv.shape), vf(*w_out.shape), vf(4, 8, 128), vf(up_rows, 128),
                dma((24,)), dma((48,)),
            ],
            compiler_params=pltpu.CompilerParams(vmem_limit_bytes=60_000_000),
            name="finish",
        )(results[0], results[1], results[2], results[5], results[6], results[7])
        block_output, input_grad, up_total, down_total, qkv_total, out_total = ends[:6]
        small = [v.reshape(-1) for v in ends[6:12]]
        return (
            block_output, input_grad, qkv_total, ends[12], out_total, small[4],
            up_total, ends[13].T, down_total, small[5],
            small[0], small[1], small[2], small[3],
        )

    row, vec = P(AXES, None), P(AXES)
    col, low = P("dp", "tp"), P("tp", "dp")
    def choose(*arrays):
        wide = arrays[2].shape[0] % 128 == 0
        return (on_device_fused if wide else on_device)(*arrays)

    return jax.shard_map(
        choose,
        mesh=mesh,
        in_specs=(row, P("dp", None), col, low, low, vec, col, low, low, vec, vec, vec, vec, vec, row),
        out_specs=(row, row, col, low, low, vec, col, low, low, vec, vec, vec, vec, vec),
        check_vma=False,
    )
```

```python
import functools
import math

import jax
import jax.numpy as jnp
import numpy as np
from jax import lax
from jax.experimental import pallas as pl
from jax.experimental.pallas import tpu as pltpu
from jax.sharding import PartitionSpec as P

HD = 256
ROT = 64
SEQ = 512
INNER = 4
EPS = 1e-05
NEG_FILL = -1e30
F32 = jnp.float32
BF16 = jnp.bfloat16
AXES = ("dp", "tp")
MESH = pl.DeviceIdType.MESH
PAY = 1024


def dot(left, right, contract):
    return lax.dot_general(left, right, (contract, ((), ())), preferred_element_type=F32)


def mm(left, right):
    return dot(left, right, ((1,), (0,)))


def mm_tail(left, right):
    return dot(left, right, ((1,), (1,)))


def mm_lead(left, right):
    return dot(left, right, ((0,), (0,)))


def gelu_half(pre_act):
    return 0.5 * (1.0 + jax.scipy.special.erf(pre_act * 2.0 ** (-0.5)))


def gelu_slope(pre_act):
    return gelu_half(pre_act) + pre_act * jnp.exp(-0.5 * pre_act * pre_act) * (2.0 * math.pi) ** (-0.5)


def rotate(block, cosine, sine):
    half = ROT // 2
    lower, upper = block[..., :half], block[..., half:ROT]
    return jnp.concatenate(
        [lower * cosine - upper * sine, upper * cosine + lower * sine, block[..., ROT:]], axis=-1
    )


def gather_kernel(
    dp_n, tp_n, wide,
    x_ref, cot_ref, fc1_ref, fc2_ref, qkv_ref, out_ref, pay_ref,
    xs_ref, cots_ref, up_ref, down_ref, att_ref, proj_ref, small_ref,
    row_send, row_recv, mlp_send, mlp_recv, att_send, att_recv, pass_send, pass_recv,
    small_send, small_recv, local_sem,
):
    d = lax.axis_index("dp")
    t = lax.axis_index("tp")
    inner = d % INNER
    core = t % 2
    depth = fc1_ref.shape[0]
    hidden = fc1_ref.shape[1] // INNER

    barrier = pltpu.get_barrier_semaphore()
    for s in range(1, dp_n):
        pl.semaphore_signal(barrier, inc=1, device_id=(d ^ s, t), device_id_type=MESH)
    for k in (1, 2):
        pl.semaphore_signal(barrier, inc=1, device_id=(d, t ^ k), device_id_type=MESH)

    def remote(src, dst, send_sem, recv_sem, dp_xor, tp_xor):
        return pltpu.make_async_remote_copy(
            src_ref=src, dst_ref=dst, send_sem=send_sem, recv_sem=recv_sem,
            device_id=(d ^ dp_xor, t ^ tp_xor), device_id_type=MESH,
        )

    hop = {1: (2, 0), 2: (1, 0), 4: (0, 2), 8: (0, 1)}
    pairs = ((x_ref, xs_ref), (cot_ref, cots_ref))

    def row_copy(a, k, bit):
        own, full = pairs[a]
        src = own if k == 0 else full.at[k]
        return remote(src, full.at[k + bit], row_send.at[a, k + bit], row_recv.at[a, k + bit], *hop[bit])

    def columns(ref, index, size):
        return ref.at[:, pl.ds(pl.multiple_of(index * size, 128), size)]

    def lines(ref, index, size):
        return ref.at[pl.ds(pl.multiple_of(index * size, 8), size), :]

    def across(ref, index, size):
        return columns(ref, index, size) if wide else ref.at[index]

    def mlp_copies(s):
        target = inner ^ (s % INNER)
        return (
            (columns(fc1_ref, target, hidden), lines(up_ref, d, depth)),
            (lines(fc2_ref, target, hidden), across(down_ref, d, depth)),
        )

    def att_copies(s):
        target = (inner ^ (s % INNER)) % 2
        return (
            (columns(qkv_ref, target, 3 * HD), lines(att_ref, d, depth)),
            (lines(out_ref, target, HD), across(proj_ref, d, depth)),
        )

    def att_land(s):
        return (lines(att_ref, d ^ s, depth), across(proj_ref, d ^ s, depth))

    def mlp_land(s):
        return (lines(up_ref, d ^ s, depth), across(down_ref, d ^ s, depth))

    local = []
    def stay(src, dst):
        copy = pltpu.make_async_copy(src, dst, local_sem.at[len(local)])
        copy.start()
        local.append(copy)

    lead = (inner // 2) == core
    pltpu.sync_copy(pay_ref, small_ref.at[0])
    pl.semaphore_wait(barrier, dp_n + 1)

    started = []
    def start(copy):
        copy.start()
        started.append(copy)

    def start_rows(k, bit):
        for a in range(2):
            start(row_copy(a, k, bit))

    def wait_rows(k):
        bit = 1
        while bit * 2 <= k:
            bit *= 2
        for a in range(2):
            row_copy(a, k - bit, bit).wait_recv()

    def start_mlp(s):
        for a, (src, dst) in enumerate(mlp_copies(s)):
            start(remote(src, dst, mlp_send.at[a, s], mlp_recv.at[a, s], s, 0))

    def att_active(s):
        return ((inner ^ (s % INNER)) // 2) == core

    def start_att(s):
        @pl.when(att_active(s))
        def _():
            for a, (src, dst) in enumerate(att_copies(s)):
                remote(src, dst, att_send.at[a, s], att_recv.at[a, s], s, 0).start()

    def pass_att(s):
        lands = att_land(s)
        return [
            remote(land, land, pass_send.at[a, s], pass_recv.at[a, s], 0, 1)
            for a, land in enumerate(lands)
        ]

    def small_copy(step, dp_xor, tp_xor, n):
        return remote(
            small_ref.at[pl.ds(0, n)], small_ref.at[pl.ds(n, n)],
            small_send.at[step], small_recv.at[step], dp_xor, tp_xor,
        )

    hops = []
    n = 1
    while n < dp_n * tp_n:
        hops.append((n // tp_n, n % tp_n, n))
        n *= 2
    even = [s for s in range(2, dp_n, 2)]
    even.sort(key=lambda s: -(s >= INNER))
    odd = [s for s in range(1, dp_n, 2)]
    odd.sort(key=lambda s: -(s >= INNER))

    small = [small_copy(k, *h) for k, h in enumerate(hops)]
    small[0].start()
    for bit in (1, 2, 4):
        start_rows(0, bit)
    start_rows(0, 8)
    for s in even:
        start_mlp(s)
    stay(x_ref, xs_ref.at[0])
    stay(cot_ref, cots_ref.at[0])
    for src, dst in mlp_copies(0):
        stay(src, dst)

    @pl.when(lead)
    def _():
        for a, (src, dst) in enumerate(att_copies(0)):
            copy = pltpu.make_async_copy(src, dst, local_sem.at[4 + a])
            copy.start()

    for k in range(len(small)):
        small[k].wait_recv()
        if k + 1 < len(small):
            small[k + 1].start()
    wait_rows(1)
    start_rows(1, 2)
    start_rows(1, 4)
    start_rows(1, 8)
    wait_rows(2)
    start_rows(2, 4)
    start_rows(2, 8)
    for s in odd:
        start_mlp(s)
    for s in even + odd:
        start_att(s)
    wait_rows(3)
    start_rows(3, 4)
    start_rows(3, 8)
    wait_rows(4)
    start_rows(4, 8)

    @pl.when(lead)
    def _():
        for a, (src, dst) in enumerate(att_copies(0)):
            pltpu.make_async_copy(src, dst, local_sem.at[4 + a]).wait()
        for copy in pass_att(0):
            copy.start()

    for k in (5, 6, 7):
        wait_rows(k)
        start_rows(k, 8)
    for k in range(8, 16):
        wait_rows(k)
    for s in even + odd:
        for a, dst in enumerate(mlp_land(s)):
            remote(dst, dst, mlp_send.at[a, s], mlp_recv.at[a, s], s, 0).wait_recv()
    for s in even + odd:
        @pl.when(lead)
        def _():
            for a, dst in enumerate(att_land(s)):
                remote(dst, dst, att_send.at[a, s], att_recv.at[a, s], s, 0).wait_recv()
            for copy in pass_att(s):
                copy.start()

    @pl.when(jnp.logical_not(lead))
    def _():
        for s in range(dp_n):
            for copy in pass_att(s):
                copy.wait_recv()

    @pl.when(lead)
    def _():
        for s in range(dp_n):
            for copy in pass_att(s):
                copy.wait_send()

    for s in range(1, dp_n):
        @pl.when(att_active(s))
        def _():
            for a, (src, dst) in enumerate(att_copies(s)):
                remote(src, dst, att_send.at[a, s], att_recv.at[a, s], s, 0).wait_send()
    for copy in started:
        copy.wait_send()
    for copy in small:
        copy.wait_send()
    for copy in local:
        copy.wait()


def span(start, size, unit):
    return pl.ds(start if isinstance(start, int) else pl.multiple_of(start, unit), size)


def lane_cut(ref, start, size):
    return ref.at[:, span(start, size, 128)]


def row_cut(ref, start, size):
    return ref.at[span(start, size, 16), :]


def columns_of(rows8):
    pad = jnp.zeros((120, 128), F32)
    return jnp.transpose(jnp.concatenate([rows8, pad], axis=0))


def fused_kernel(
    dp_n, tp_n,
    x_ref, cot_ref, fc1_ref, fc2_ref, qkv_ref, out_ref, rope_ref,
    vec0_ref, vec1_ref, vec2_ref, vec3_ref, vec4_ref, vec5_ref, bq_ref, bf_ref, seg_ref,
    block_out, input_out, tail_out,
    gu_hbm, gd_hbm, ru_hbm, rd_hbm, ra_hbm, pair_hbm,
    xs, cots, n2, up_t, down_w, pre, hid_t, act_t, ring, stats, vecs, sums, up_sum,
    att_w, proj_w, n1, q_s, k_s, v_s, prob, ctx, ctx_t, cctx, low, low_t, gx,
    rope, raw, raw_q, raw_f, raw_seg, wide_f, pay, pair_in, pair_back, vec_in, bias_in, head_in, vec_back, bias_back, head_back, up_place, head_place,
    keys, queries, qkv_bias, qkv_sum,
    row_send, row_recv, mlp_send, mlp_recv, att_send, att_recv, pass_send, pass_recv,
    small_send, small_recv, head_send, head_recv, back_send, back_recv, headb_send, headb_recv, g_send, g_recv, g_local,
    rs_send, rs_recv, pair_send, pair_recv, ga_send, ga_recv,
    local_sem, out_sem, credit,
):
    d = lax.axis_index("dp")
    t = lax.axis_index("tp")
    flat = d * tp_n + t
    inner = d % INNER
    core = t % 2
    lead = (inner // 2) == core
    follow = jnp.logical_not(lead)
    rows, width = x_ref.shape
    depth = fc1_ref.shape[0]
    hidden = fc1_ref.shape[1] // INNER
    devices = dp_n * tp_n
    slots = 16
    tokens = slots * rows
    scale = HD ** (-0.5)
    chunk = 512

    barrier = pltpu.get_barrier_semaphore()
    for a in range(1, devices):
        peer = (d ^ (a // tp_n), t ^ (a % tp_n))
        pl.semaphore_signal(barrier, inc=1, device_id=peer, device_id_type=MESH)

    def remote(src, dst, send_sem, recv_sem, dp_xor, tp_xor):
        return pltpu.make_async_remote_copy(
            src_ref=src, dst_ref=dst, send_sem=send_sem, recv_sem=recv_sem,
            device_id=(d ^ dp_xor, t ^ tp_xor), device_id_type=MESH,
        )

    started = []

    def start(copy):
        copy.start()
        started.append(copy)

    hop = {1: (2, 0), 2: (1, 0), 4: (0, 2), 8: (0, 1)}

    def slot(ref, k):
        return row_cut(ref, k * rows, rows)

    def row_copy(a, k, bit):
        own, full = ((x_ref, xs), (cot_ref, cots))[a]
        src = own if k == 0 else slot(full, k)
        return remote(
            src, slot(full, k + bit), row_send.at[a, k + bit], row_recv.at[a, k + bit], *hop[bit]
        )

    row_started = ([], [])

    def start_row(a, k, *bits):
        for bit in bits:
            copy = row_copy(a, k, bit)
            copy.start()
            row_started[a].append(copy)

    def wait_row(a, k):
        bit = 1
        while bit * 2 <= k:
            bit *= 2
        row_copy(a, k - bit, bit).wait_recv()

    def w1_piece(i):
        return gx.at[depth : depth + hidden, pl.ds(pl.multiple_of(i * depth, 128), depth)]

    def mlp_copy(a, s):
        target = inner ^ (s % INNER)
        src = w1_piece(target) if a == 0 else row_cut(fc2_ref, target * hidden, hidden)
        dst = lane_cut((up_t, down_w)[a], d * depth, depth)
        if s == 0:
            return src, dst
        return remote(src, dst, mlp_send.at[a, s], mlp_recv.at[a, s], s, 0)

    mlp_started = tuple([mlp_copy(a, s) for s in range(1, dp_n)] for a in range(2))

    def start_mlp(a, s):
        mlp_started[a][s - 1].start()

    def mlp_wait(a, s):
        dst = lane_cut((up_t, down_w)[a], (d ^ s) * depth, depth)
        remote(dst, dst, mlp_send.at[a, s], mlp_recv.at[a, s], s, 0).wait_recv()

    def att_active(s):
        return ((inner ^ (s % INNER)) // 2) == core

    def att_pairs(s):
        target = (inner ^ (s % INNER)) % 2
        return (
            (lane_cut(qkv_ref, target * 3 * HD, 3 * HD), row_cut(att_w, d * depth, depth)),
            (row_cut(out_ref, target * HD, HD), lane_cut(proj_w, d * depth, depth)),
        )

    def att_land(s):
        return (row_cut(att_w, (d ^ s) * depth, depth), lane_cut(proj_w, (d ^ s) * depth, depth))

    def start_att(s):
        @pl.when(att_active(s))
        def _():
            for a, (src, dst) in enumerate(att_pairs(s)):
                remote(src, dst, att_send.at[a, s], att_recv.at[a, s], s, 0).start()

    def pass_att(s):
        return [
            remote(land, land, pass_send.at[a, s], pass_recv.at[a, s], 0, 1)
            for a, land in enumerate(att_land(s))
        ]

    local = []

    def stay(src, dst):
        copy = pltpu.make_async_copy(src, dst, local_sem.at[len(local)])
        copy.start()
        local.append(copy)
        return copy

    fc1_in = stay(fc1_ref, gx.at[0:depth, :])
    raw_in = [
        stay(ref, raw.at[k])
        for k, ref in enumerate((vec0_ref, vec1_ref, vec2_ref, vec3_ref, vec4_ref, vec5_ref))
    ]
    raw_in += [stay(bq_ref, raw_q), stay(bf_ref, raw_f), stay(seg_ref, raw_seg)]
    x_in = stay(x_ref, slot(xs, 0))
    cot_in = stay(cot_ref, slot(cots, 0))
    down_in = stay(*mlp_copy(1, 0))
    rope_in = stay(rope_ref, rope)
    for copy in raw_in:
        copy.wait()
    zero64 = jnp.zeros((1, 64), F32)
    line = lax.broadcasted_iota(jnp.int32, (8, 128), 0)

    def wide(row):
        return jnp.broadcast_to(jnp.concatenate([row, zero64], axis=1), (8, 128))

    def onto(base, row, value):
        return jnp.where(line == row, value, base)

    odd_flat = flat % 2 == 1
    group = jnp.zeros((8, 128), F32)
    for k in range(5):
        row = raw[k] if k < 4 else raw[4] + raw[5]
        value = wide(row)
        group = onto(group, k, jnp.where(odd_flat, pltpu.roll(value, 64, 1), value))
    seg_row = raw_seg[:, pl.ds(pl.multiple_of(t * 128, 128), 128)].astype(F32)
    pay[0] = onto(group, 5 + core, jnp.broadcast_to(seg_row, (8, 128)))
    group = jnp.zeros((8, 128), F32)
    for k in range(2):
        value = wide(raw_q[k : k + 1, :])
        value = jnp.where(d % 2 == 1, pltpu.roll(value, 64, 1), value)
        group = onto(group, k * 4 + d // 2, value)
    pay[3] = group
    up_lines, up_spots = raw_f.shape
    flat_f = jnp.concatenate([raw_f[...], jnp.zeros((up_lines, 128 - up_spots), F32)], axis=1)
    value = pltpu.roll(columns_of(flat_f)[:up_spots], d * up_lines, 1)
    odd_row = lax.broadcasted_iota(jnp.int32, value.shape, 0) % 2 == 1
    wide_f[...] = jnp.where(odd_row, pltpu.roll(value, 64, 1), value)
    merged = wide_f[pl.ds(0, 16, stride=2), :] + wide_f[pl.ds(1, 16, stride=2), :]
    pay[1] = merged[:8]
    pay[2] = merged[8:]
    pl.semaphore_wait(barrier, devices - 1)

    even = sorted(range(2, dp_n, 2), key=lambda s: -(s >= INNER))
    odd = sorted(range(1, dp_n, 2), key=lambda s: -(s >= INNER))

    def small_copy(kind, src, dst, dp_xor, tp_xor):
        return remote(src, dst, small_send.at[kind], small_recv.at[kind], dp_xor, tp_xor)

    chip = flat // 2
    chips = devices // 2
    meet = small_copy(2, pay.at[0], pair_in, 0, 1)
    meet.start()

    def head_in_copy(s, dc):
        return remote(
            pay.at[3], head_in.at[2 * s + dc], head_send.at[2 * s + dc], head_recv.at[2 * s + dc], s, dc
        )

    def head_in_each(act):
        @pl.when(lead)
        def _():
            act(head_in_copy(0, 1))

        for s in range(1, dp_n):
            @pl.when(att_active(s))
            def _():
                act(head_in_copy(s, 0))
                act(head_in_copy(s, 1))

    for s in range(1, dp_n):
        group = 1 + (inner ^ (s % INNER)) // 2
        small_copy(1, pay.at[group], bias_in.at[s], s, 0).start()
    head_in_each(lambda copy: copy.start())
    meet.wait_recv()
    vec_in[0] = pay[0] + pair_in[...]
    for r in range(1, chips):
        small_copy(0, vec_in.at[0], vec_in.at[r], r // 2, (r % 2) * 2).start()
    start_row(0, 0, 1, 2, 4, 8)
    start_row(1, 0, 1, 8)
    bias_in[0] = pay[1 + inner // 2]
    head_in[0] = pay[3]
    fc1_in.wait()
    for i in range(INNER):
        piece = gx[0:depth, i * hidden : (i + 1) * hidden].astype(F32)
        gx[depth : depth + hidden, i * depth : (i + 1) * depth] = jnp.transpose(piece).astype(BF16)
    near = [2, 3]
    far = [s for s in (6, 4, 7, 5) if s < dp_n]
    plane = d // 2
    end = (plane == 0) | (plane == dp_n // 2 - 1)
    middle = jnp.logical_not(end)

    def start_all(s):
        start_att(s)
        start_mlp(0, s)
        start_mlp(1, s)

    start_att(2)
    for s in far:
        start_att(s)
    start_mlp(0, 2)
    start_mlp(1, 2)

    @pl.when(end)
    def _():
        start_all(3)

    for s in far:
        start_mlp(0, s)

    @pl.when(end)
    def _():
        for s in far:
            start_mlp(1, s)

    up_in = stay(*mlp_copy(0, 0))

    @pl.when(lead)
    def _():
        for a, (src, dst) in enumerate(att_pairs(0)):
            pltpu.make_async_copy(src, dst, local_sem.at[20 + a]).start()

    wait_row(0, 1)
    start_row(0, 1, 2, 4, 8)
    wait_row(0, 2)
    start_row(0, 2, 4, 8)
    start_row(1, 0, 2)

    def small_waits(kind):
        buf = (vec_in, bias_in, head_in)[kind]
        rest = buf.at[pl.ds(1, buf.shape[0] - 1)]
        return small_copy(kind, rest, rest, 0, 1)

    for kind in range(2):
        small_waits(kind).wait_recv()

    @pl.when(lead)
    def _():
        for s in range(1, dp_n):
            head_in_copy(s, 0).wait_recv()

    @pl.when(follow)
    def _():
        for s in range(dp_n):
            head_in_copy(s, 1).wait_recv()

    for j in range(chips):
        vecs[:, j * 128 : (j + 1) * 128] = vec_in[chip ^ j]
    bias8 = jnp.zeros((8, 128), F32)
    head8 = jnp.zeros((8, 128), F32)
    head_rel = core ^ (inner // 2)
    for s in range(dp_n):
        bias8 = bias8 + bias_in[s]
        head8 = head8 + head_in[s * 2 + head_rel]
    second = inner % 2 == 1
    bias_t = columns_of(bias8)
    up_bias = jnp.concatenate(
        [jnp.where(second, bias_t[:, 4 + k : 5 + k], bias_t[:, k : k + 1]) for k in range(4)], axis=0
    )
    head4 = jnp.where(second, head8[4:], head8[:4])
    qkv_bias[0:1, :] = jnp.concatenate([head4[k : k + 1] for k in range(4)], axis=1)
    lane = lax.broadcasted_iota(jnp.int32, (1, 128), 1)
    keys[...] = jnp.zeros_like(keys)
    for q in range(4):
        at = slice(q * 128, (q + 1) * 128)
        keys[0:1, at] = ((t ^ ((q % 2) * 2 + q // 2)) * 128 + lane).astype(F32)
        for dy in range(2):
            peer = vec_in[(core * 2 + dy) * 2 + q % 2]
            keys[1 + dy : 2 + dy, at] = jnp.where((core ^ (q // 2)) == 1, peer[6:7, :], peer[5:6, :])
        queries[at, :] = columns_of(keys[:, at])

    def norm_slot(k):
        @pl.loop(0, rows // 16)
        def _(j):
            at = pl.ds(pl.multiple_of(k * rows + j * 16, 16), 16)
            value = xs[at, :].astype(F32)
            mean = jnp.mean(value, axis=-1, keepdims=True)
            centered = value - mean
            inv = lax.rsqrt(jnp.mean(centered * centered, axis=-1, keepdims=True) + EPS)
            n2[at, :] = (centered * inv * vecs[2:3, :] + vecs[3:4, :]).astype(BF16)
            stats[at, 0:64] = jnp.broadcast_to(mean, (16, 64))
            stats[at, 64:128] = jnp.broadcast_to(inv, (16, 64))

    x_in.wait()
    norm_slot(0)
    wait_row(0, 3)
    start_row(0, 3, 4, 8)
    start_row(1, 0, 4)
    for k in (1, 2, 3):
        norm_slot(k)
    wait_row(1, 1)
    start_row(1, 1, 2, 4, 8)
    wait_row(1, 2)
    start_row(1, 2, 4, 8)

    @pl.when(middle)
    def _():
        start_all(3)

    start_all(1)
    for k in (4, 5, 6, 7):
        wait_row(0, k)
        start_row(0, k, 8)
        norm_slot(k)

    @pl.when(middle)
    def _():
        for s in far:
            start_mlp(1, s)

    for k in range(8, 16):
        wait_row(0, k)
        norm_slot(k)
    wait_row(1, 3)
    start_row(1, 3, 4, 8)

    def mine(dy, q):
        return ((q // 2) * 8 + (q % 2) * 4 + dy * 2 + core) * rows

    for dy in range(2):
        for q in range(4):
            @pl.loop(0, rows // 16)
            def _(j):
                at = pl.ds(pl.multiple_of(mine(dy, q) + j * 16, 16), 16)
                to = pl.ds(pl.multiple_of(dy * SEQ + q * rows + j * 16, 16), 16)
                normed = (xs[at, :].astype(F32) - stats[at, 0:1]) * stats[at, 64:65]
                n1[to, :] = (normed * vecs[0:1, :] + vecs[1:2, :]).astype(BF16)

    @pl.when(lead)
    def _():
        for a, (src, dst) in enumerate(att_pairs(0)):
            pltpu.make_async_copy(src, dst, local_sem.at[20 + a]).wait()
        for copy in pass_att(0):
            copy.start()
        for s in near + [1] + far:
            for a, dst in enumerate(att_land(s)):
                remote(dst, dst, att_send.at[a, s], att_recv.at[a, s], s, 0).wait_recv()
            for copy in pass_att(s):
                copy.start()

    @pl.when(follow)
    def _():
        for s in range(dp_n):
            for copy in pass_att(s):
                copy.wait_recv()

    rope_in.wait()
    lanes128 = lax.broadcasted_iota(jnp.int32, (SEQ, 128), 1)

    def rope_tables(sign):
        at = [pl.ds(pl.multiple_of((t ^ ((q % 2) * 2 + q // 2)) * 128, 128), 128) for q in range(4)]
        cosine = jnp.concatenate([rope[0, a, :] for a in at], axis=0)
        sine = jnp.concatenate([rope[1, a, :] for a in at], axis=0) * sign
        lower = jnp.where(lanes128 < ROT // 2, -sine, 0.0)
        upper = jnp.where((lanes128 >= ROT // 2) & (lanes128 < ROT), sine, 0.0)
        return cosine, lower, upper

    def turn(value, tables):
        cosine, lower, upper = tables
        head = value[:, :128]
        head = (
            head * cosine
            + pltpu.roll(head, 128 - ROT // 2, 1) * lower
            + pltpu.roll(head, ROT // 2, 1) * upper
        )
        return jnp.concatenate([head, value[:, 128:]], axis=1)

    @pl.loop(0, 2)
    def _(dy):
        at = pl.ds(pl.multiple_of(dy * SEQ, SEQ), SEQ)
        tables = rope_tables(1.0)
        rows_in = n1[at, :]
        value = mm(rows_in, att_w[:, :HD]) + qkv_bias[0:1, :HD]
        query = turn(value, tables).astype(BF16)
        key = turn(mm(rows_in, att_w[:, HD : 2 * HD]), tables).astype(BF16)
        val = (mm(rows_in, att_w[:, 2 * HD :]) + qkv_bias[0:1, HD:]).astype(BF16)
        q_s[at, :] = query
        k_s[at, :] = key
        v_s[at, :] = val
        seg_q = jnp.where(dy == 0, queries[:, 1:2], queries[:, 2:3])
        seg_k = jnp.where(dy == 0, keys[1:2, :], keys[2:3, :])
        allowed = (keys[0:1, :] <= queries[:, 0:1]) & (seg_q == seg_k)
        scores = jnp.where(allowed, mm_tail(query, key) * scale, NEG_FILL)
        peak = jnp.max(scores, axis=-1, keepdims=True)
        total = jnp.where(allowed, jnp.exp(scores - peak), 0.0)
        share = (total / jnp.sum(total, axis=-1, keepdims=True)).astype(BF16)
        prob[at, :] = share
        got = mm(share, val)
        ctx[at, :] = got.astype(BF16)
        ctx_t[:, at] = jnp.transpose(got).astype(BF16)

    def cot_mine(dy, lanes):
        parts = [cots[pl.ds(pl.multiple_of(mine(dy, q), 128), rows), lanes] for q in range(4)]
        return jnp.concatenate(parts, axis=0)

    for k in (4, 5, 6, 7):
        wait_row(1, k)
        start_row(1, k, 8)
    cot_in.wait()
    for k in range(8, 16):
        wait_row(1, k)
    sums[...] = jnp.zeros_like(sums)

    @pl.loop(0, rows // 16)
    def _(j):
        at = pl.ds(pl.multiple_of(j * 16, 16), 16)
        sums[4:5, :] += jnp.sum(cots[at, :].astype(F32), axis=0, keepdims=True)

    for dy in range(2):
        cctx[dy * SEQ : (dy + 1) * SEQ, :] = mm_tail(cot_mine(dy, slice(None)), proj_w[...]).astype(BF16)

    @pl.loop(0, width // chunk)
    def _(c):
        lanes = pl.ds(pl.multiple_of(c * chunk, chunk), chunk)
        both = jnp.concatenate([cot_mine(0, lanes), cot_mine(1, lanes)], axis=0)
        gx[3 * HD : 4 * HD, lanes] = mm(ctx_t[...], both).astype(BF16)

    qkv_sum[...] = jnp.zeros_like(qkv_sum)

    def backward(dy):
        at = slice(dy * SEQ, (dy + 1) * SEQ)
        tables = rope_tables(-1.0)
        share = prob[at, :].astype(F32)
        got = cctx[at, :]
        delta = jnp.sum(got.astype(F32) * ctx[at, :].astype(F32), axis=-1, keepdims=True)
        score_cot = share * (mm_tail(got, v_s[at, :]) - delta)
        value_cot = mm(jnp.transpose(share).astype(BF16), got)
        query_cot = turn(mm(score_cot.astype(BF16), k_s[at, :]) * scale, tables)
        key_cot = turn(mm(jnp.transpose(score_cot).astype(BF16), q_s[at, :]) * scale, tables)
        qkv_sum[0:1, :HD] += jnp.sum(query_cot, axis=0, keepdims=True)
        qkv_sum[0:1, HD:] += jnp.sum(value_cot, axis=0, keepdims=True)
        for k, part in enumerate((query_cot, key_cot, value_cot)):
            low[at, k * HD : (k + 1) * HD] = part.astype(BF16)
            low_t[k * HD : (k + 1) * HD, at] = jnp.transpose(part).astype(BF16)

    backward(0)
    backward(1)

    up_in.wait()
    for copy in mlp_started[0]:
        copy.wait_send()

    @pl.loop(0, width // chunk)
    def _(c):
        lanes = pl.ds(pl.multiple_of(c * chunk, chunk), chunk)
        gx[0 : 3 * HD, lanes] = mm(low_t[...], n1[:, lanes]).astype(BF16)

    def pair_copy(s):
        return remote(
            lane_cut(gx, (d ^ s) * depth, depth), pair_hbm.at[:, s * depth : (s + 1) * depth],
            pair_send.at[s], pair_recv.at[s], 0, 1,
        )

    @pl.when(follow)
    def _():
        for s in near + [1] + far + [0]:
            pair_copy(s).start()

    for dy in range(2):
        @pl.loop(0, width // chunk)
        def _(c):
            lanes = pl.ds(pl.multiple_of(c * chunk, chunk), chunk)
            part = mm_tail(low[dy * SEQ : (dy + 1) * SEQ, :], att_w[lanes, :])
            gain = vecs[0:1, lanes]
            cross = jnp.zeros((1, chunk), F32)
            for q in range(4):
                at = pl.ds(pl.multiple_of(mine(dy, q), 128), rows)
                piece = part[q * rows : (q + 1) * rows]
                normed = (xs[at, lanes].astype(F32) - stats[at, 0:1]) * stats[at, 64:65]
                cross = cross + jnp.sum(piece * normed, axis=0, keepdims=True)
                n1[dy * SEQ + q * rows : dy * SEQ + (q + 1) * rows, lanes] = (piece * gain).astype(BF16)
            sums[0:1, lanes] += cross
            sums[1:2, lanes] += jnp.sum(part, axis=0, keepdims=True)

    def ga_copy(s):
        return remote(
            lane_cut(gx, (d ^ s) * depth, depth), ra_hbm.at[:, s * depth : (s + 1) * depth],
            ga_send.at[s], ga_recv.at[s], s, 0,
        )

    stages = (q_s, k_s, v_s)

    @pl.when(lead)
    def _():
        todo = near + [1] + far + [0]

        def fetch(k):
            s = todo[k]
            land = pair_hbm.at[:, s * depth : (s + 1) * depth]
            remote(land, land, pair_send.at[s], pair_recv.at[s], 0, 1).wait_recv()
            copy = pltpu.make_async_copy(land, stages[k % 3], g_local.at[k % 3])
            copy.start()
            return copy

        held = [fetch(0), fetch(1)]
        for k, s in enumerate(todo):
            if k + 2 < len(todo):
                held.append(fetch(k + 2))
            held[k].wait()
            stage = stages[k % 3]
            here = lane_cut(gx, (d ^ s) * depth, depth)

            @pl.loop(0, 4 * HD // 64)
            def _(i):
                at = pl.ds(pl.multiple_of(i * 64, 64), 64)
                here[at, :] = (here[at, :].astype(F32) + stage[at, :].astype(F32)).astype(BF16)

            if s:
                ga_copy(s).start()
            else:
                pltpu.make_async_copy(here, ra_hbm.at[:, 0:depth], local_sem.at[22]).start()

    for s in near + [1] + far:
        mlp_wait(0, s)

    @pl.loop(0, tokens // chunk)
    def _(j):
        at = pl.ds(pl.multiple_of(j * chunk, chunk), chunk)
        value = mm_tail(up_t[...], n2[at, :]) + up_bias
        pre[:, at] = value
        hid_t[:, at] = (value * gelu_half(value)).astype(BF16)

    def g_send_copy(a, s):
        at = pl.ds(pl.multiple_of(s * depth, 128), depth)
        return remote(
            (gu_hbm, gd_hbm)[a].at[:, at], (ru_hbm, rd_hbm)[a].at[:, at],
            g_send.at[a, s], g_recv.at[a, s], s, 0,
        )

    def g_local_copy(a, s, b, dst):
        at = pl.ds(pl.multiple_of(s * depth, 128), depth)
        return pltpu.make_async_copy(ring.at[b], dst.at[:, at], g_local.at[b])

    def grads(a, go):
        left, right = ((act_t, n2), (hid_t, cots))[a]
        stage, own = ((gu_hbm, ru_hbm), (gd_hbm, rd_hbm))[a]

        def block(s, b):
            at = pl.ds(pl.multiple_of((d ^ s) * depth, 128), depth)
            ring[b] = mm(left[...], right[:, at]).astype(BF16)

        def at_step(k):
            return (k + 1) % (dp_n - 1) + 1

        @pl.loop(0, dp_n - 1)
        def _(k):
            s = at_step(k)
            b = k % 3

            @pl.when(k >= 2)
            def _():
                before = at_step(k - 2)
                g_local_copy(a, before, (k + 1) % 3, stage).wait()
                if go:
                    g_send_copy(a, before).start()

            block(s, b)
            g_local_copy(a, s, b, stage).start()

        last = dp_n - 2
        for k in (last - 1, last):
            s = at_step(k)
            g_local_copy(a, s, k % 3, stage).wait()
            if go:
                g_send_copy(a, s).start()
        b = (last + 1) % 3
        block(0, b)
        copy = g_local_copy(a, 0, b, own)
        copy.start()
        copy.wait()

    grads(1, True)
    down_in.wait()
    for s in near + [1] + far:
        mlp_wait(1, s)
    up_sum[...] = jnp.zeros_like(up_sum)

    @pl.loop(0, tokens // chunk)
    def _(j):
        at = pl.ds(pl.multiple_of(j * chunk, chunk), chunk)
        value = mm_tail(down_w[...], cots[at, :]) * gelu_slope(pre[:, at])
        up_sum[:, 0:1] += jnp.sum(value, axis=1, keepdims=True)
        act_t[:, at] = value.astype(BF16)

    grads(0, False)

    @pl.loop(0, tokens // chunk)
    def _(j):
        at = pl.ds(pl.multiple_of(j * chunk, chunk), chunk)
        act = jnp.transpose(act_t[:, at].astype(F32)).astype(BF16)

        @pl.loop(0, width // chunk)
        def _(c):
            lanes = pl.ds(pl.multiple_of(c * chunk, chunk), chunk)
            part = mm(act, up_t[:, lanes])
            gain = vecs[2:3, lanes]
            cross = jnp.zeros((1, chunk), F32)
            for m in range(4):
                at = pl.ds(pl.multiple_of(j * chunk + m * rows, 128), rows)
                piece = part[m * rows : (m + 1) * rows]
                normed = (xs[at, lanes].astype(F32) - stats[at, 0:1]) * stats[at, 64:65]
                cross = cross + jnp.sum(piece * normed, axis=0, keepdims=True)
                spot = pl.ds(pl.multiple_of((m // 2) * SEQ + j * rows, 128), rows)
                extra = jnp.where(core == m % 2, n1[spot, lanes].astype(F32), 0.0)
                n2[at, lanes] = (piece * gain + extra).astype(BF16)
            sums[2:3, lanes] += cross
            sums[3:4, lanes] += jnp.sum(part, axis=0, keepdims=True)

    for copy in row_started[0]:
        copy.wait_send()
    pl.semaphore_signal(credit.at[0], inc=1, device_id=(d, t ^ 1), device_id_type=MESH)
    pl.semaphore_signal(credit.at[1], inc=1, device_id=(d, t ^ 2), device_id_type=MESH)

    blank = jnp.zeros((4, 128), F32)
    up_rows = [jnp.transpose(up_sum[k * 128 : (k + 1) * 128, :])[0:1] for k in range(4)]
    up_rows = jnp.concatenate(up_rows, axis=0)
    qkv_rows = jnp.concatenate([qkv_sum[0:1, k * 128 : (k + 1) * 128] for k in range(4)], axis=0)

    def place(value):
        return jnp.where(
            second, jnp.concatenate([blank, value], axis=0), jnp.concatenate([value, blank], axis=0)
        )

    up_place[...] = place(up_rows)
    head_place[...] = place(qkv_rows)

    def window(to):
        return lane_cut(sums, to * 128, 128)

    def back_copy(kind, src, dst, dp_xor, tp_xor):
        return remote(src, dst, back_send.at[kind], back_recv.at[kind], dp_xor, tp_xor)

    def head_copy(s, dc):
        return remote(
            head_place, head_back.at[s * 2 + dc], headb_send.at[s * 2 + dc], headb_recv.at[s * 2 + dc], s, dc
        )

    for r in range(1, chips):
        back_copy(0, window(chip ^ r), vec_back.at[r], r // 2, (r % 2) * 2).start()
    for s in range(1, dp_n):
        back_copy(1, up_place, bias_back.at[s], s, 0).start()

    @pl.when(lead)
    def _():
        for s in range(1, dp_n):
            head_copy(s, 0).start()

    @pl.when(follow)
    def _():
        for s in range(dp_n):
            head_copy(s, 1).start()

    bufs = (cots, n2)

    def landing(a, bit, j, there):
        if bit == 8:
            if a == 0:
                side = core if there else 1 - core
                return row_cut(xs, (2 * j + side) * rows, rows)
            return row_cut(n1, j * rows, rows)
        if bit == 4:
            return row_cut((act_t, up_t)[a], j * rows, rows)
        base = (down_w, hid_t)[a]
        return row_cut(base, (j if bit == 2 else 2) * rows, rows)

    def rs_copy(a, bit, j):
        return remote(
            slot(bufs[a], bit + j), landing(a, bit, j, True),
            rs_send.at[a, bit + j], rs_recv.at[a, bit + j], *hop[bit],
        )

    def rs_start(a, bit, j):
        start(rs_copy(a, bit, j))

    def rs_add(a, bit, j):
        land = landing(a, bit, j, False)
        remote(land, land, rs_send.at[a, bit + j], rs_recv.at[a, bit + j], *hop[bit]).wait_recv()
        here = slot(bufs[a], j)

        @pl.loop(0, rows // 16)
        def _(i):
            at = pl.ds(pl.multiple_of(i * 16, 16), 16)
            here[at, :] = (here[at, :].astype(F32) + land[at, :].astype(F32)).astype(BF16)

    for s in near + far[:3]:
        g_send_copy(0, s).start()

    pl.semaphore_wait(credit.at[0], 1)
    pl.semaphore_wait(credit.at[1], 1)
    for j in (7, 5, 6, 4, 3, 1, 2, 0):
        rs_start(1, 8, j)

    for copy in row_started[1]:
        copy.wait_send()
    for j in range(4):
        for k in {2: (7, 5), 3: (6, 4)}.get(j, ()):
            rs_add(1, 8, k)
            rs_start(1, 4, k - 4)
        hid = jnp.transpose(hid_t[:, j * chunk : (j + 1) * chunk].astype(F32)).astype(BF16)
        here = [ctx[h * SEQ + j * rows : h * SEQ + (j + 1) * rows, :] for h in range(2)]
        here = jnp.concatenate(here, axis=0)

        @pl.loop(0, width // chunk)
        def _(c):
            lanes = pl.ds(pl.multiple_of(c * chunk, chunk), chunk)
            base = mm(hid, down_w[:, lanes])
            extra = mm(here, proj_w[:, lanes])
            for m in range(4):
                more = jnp.where(core == m % 2, extra[(m // 2) * rows : (m // 2 + 1) * rows], 0.0)
                piece = base[m * rows : (m + 1) * rows] + more
                cots[j * chunk + m * rows : j * chunk + (m + 1) * rows, lanes] = piece.astype(BF16)

    for bit in (2, 1):
        dp_xor, tp_xor = hop[bit]
        pl.semaphore_signal(
            credit.at[1 + (3 - bit)], inc=1, device_id=(d ^ dp_xor, t ^ tp_xor), device_id_type=MESH
        )
    own_x = row_cut(hid_t, 3 * rows, rows)
    own_cot = row_cut(down_w, 3 * rows, rows)
    x_again = stay(x_ref, own_x)
    cot_again = stay(cot_ref, own_cot)

    for j in (7, 5, 6, 4, 3, 1, 2, 0):
        rs_start(0, 8, j)
    for j in (3, 1, 2, 0):
        rs_add(1, 8, j)
    for j in (7, 5, 6, 4):
        rs_add(0, 8, j)
        rs_start(0, 4, j - 4)
    for j in (3, 1, 2, 0):
        rs_add(0, 8, j)
    pl.semaphore_wait(credit.at[2], 1)
    pl.semaphore_wait(credit.at[3], 1)

    def rs_tail(a, after):
        rs_add(a, 4, 3)
        rs_start(a, 2, 1)
        rs_add(a, 4, 1)
        rs_add(a, 4, 2)
        rs_start(a, 2, 0)
        rs_add(a, 2, 1)
        rs_start(a, 1, 0)
        after()
        rs_add(a, 4, 0)
        rs_add(a, 2, 0)
        rs_add(a, 1, 0)

    outs = []

    def leave(src, dst):
        copy = pltpu.make_async_copy(src, dst, out_sem.at[len(outs)])
        copy.start()
        outs.append(copy)
        return copy

    def late():
        for s in far[3:] + [1]:
            g_send_copy(0, s).start()

    rs_tail(1, late)
    cot_again.wait()
    x_again.wait()

    @pl.loop(0, rows // 16)
    def _(j):
        at = pl.ds(pl.multiple_of(j * 16, 16), 16)
        scaled = n2[at, :].astype(F32)
        inv = stats[at, 64:65]
        normed = (own_x[at, :].astype(F32) - stats[at, 0:1]) * inv
        inner_mean = jnp.mean(scaled, axis=-1, keepdims=True)
        cross = jnp.mean(scaled * normed, axis=-1, keepdims=True)
        pre[at, :] = own_cot[at, :].astype(F32) + inv * (scaled - inner_mean - normed * cross)

    grad_out = leave(pre.at[0:rows, :], input_out)

    rs_tail(0, lambda: None)

    @pl.loop(0, rows // 16)
    def _(j):
        at = pl.ds(pl.multiple_of(j * 16, 16), 16)
        total = own_x[at, :].astype(F32) + cots[at, :].astype(F32) + vecs[4:5, :]
        cots[at, :] = total.astype(BF16)

    last = [leave(slot(cots, 0), block_out)]
    def back_waits(kind):
        buf = (vec_back, bias_back)[kind]
        rest = buf.at[pl.ds(1, buf.shape[0] - 1)]
        return back_copy(kind, rest, rest, 0, 1)

    for kind in range(2):
        back_waits(kind).wait_recv()
    for kind in range(2):
        small_waits(kind).wait_send()
    meet.wait_send()
    head_in_each(lambda copy: copy.wait_send())
    total = window(chip)[...]
    for r in range(1, chips):
        total = total + vec_back[r]
    pay[0] = total
    meet_back = back_copy(2, pay.at[0], pair_back, 0, 1)
    meet_back.start()
    for k in (1, 2, 3):
        pay[k] = jnp.zeros((8, 128), F32)
    pay[1 + inner // 2] += up_place[...]
    for s in range(1, dp_n):
        pay[1 + (inner ^ (s % INNER)) // 2] += bias_back[s]
    for s in range(dp_n):
        @pl.when(att_active(s))
        def _():
            if s == 0:
                pay[3] += head_place[...]
            else:
                head_copy(s, 0).wait_recv()
                pay[3] += head_back[2 * s]
            head_copy(s, 1).wait_recv()
            pay[3] += head_back[2 * s + 1]


    @pl.when(lead)
    def _():
        pltpu.make_async_copy(
            lane_cut(gx, d * depth, depth), ra_hbm.at[:, 0:depth], local_sem.at[22]
        ).wait()

    for s in range(1, dp_n):
        @pl.when(att_active(s))
        def _():
            ga_copy(s).wait_recv()

    for s in range(1, dp_n):
        g_send_copy(1, s).wait_recv()
    for s in range(1, dp_n):
        g_send_copy(0, s).wait_recv()
    meet_back.wait_recv()
    meet_back.wait_send()
    pay[0] += pair_back[...]
    last.append(leave(pay, tail_out))
    for s in range(1, dp_n):
        for a in range(2):
            g_send_copy(a, s).wait_send()

        @pl.when(att_active(s))
        def _():
            for a, (src, dst) in enumerate(att_pairs(s)):
                remote(src, dst, att_send.at[a, s], att_recv.at[a, s], s, 0).wait_send()

        @pl.when(lead)
        def _():
            ga_copy(s).wait_send()

    @pl.when(lead)
    def _():
        for s in range(dp_n):
            for copy in pass_att(s):
                copy.wait_send()

    @pl.when(follow)
    def _():
        for s in range(dp_n):
            pair_copy(s).wait_send()

    @pl.when(lead)
    def _():
        for s in range(1, dp_n):
            head_copy(s, 0).wait_send()

    @pl.when(follow)
    def _():
        for s in range(dp_n):
            head_copy(s, 1).wait_send()

    for kind in range(2):
        back_waits(kind).wait_send()
    for copy in started + mlp_started[1]:
        copy.wait_send()
    for copy in [grad_out] + last:
        copy.wait()


def finish_kernel(
    dp_n, tp_n,
    block_ref, input_ref, tail_ref, ru_ref, rd_ref, ra_ref,
    block_out, input_out, up_out, down_out, qkv_out, proj_out,
    v0, v1, v2, v3, v4, v5, bq_out, bf_out,
    block, grad, ru, rd, ra, up, down, qkv, proj, tail, wide_f, in_sem, out_sem,
):
    d = lax.axis_index("dp")
    t = lax.axis_index("tp")
    inner = d % INNER
    core = t % 2
    hidden, width = ru.shape
    depth = width // dp_n
    groups = dp_n // INNER
    copies = []

    def fetch(src, dst):
        copy = pltpu.make_async_copy(src, dst, in_sem.at[len(copies)])
        copy.start()
        copies.append(copy)
        return copy

    rd_in = [fetch(row_cut(rd_ref, k * 128, 128), row_cut(rd, k * 128, 128)) for k in range(hidden // 128)]
    ru_in = [fetch(row_cut(ru_ref, k * 128, 128), row_cut(ru, k * 128, 128)) for k in range(hidden // 128)]
    ra_in = []
    for hl in range(2):
        first = ((inner // 2) ^ core) * 2 + ((inner % 2) ^ hl)
        for o in range(groups):
            k = hl * groups + o
            ra_in.append(fetch(lane_cut(ra_ref, (first + o * INNER) * depth, depth), lane_cut(ra, k * depth, depth)))
    tail_in = fetch(tail_ref, tail)
    block_in = fetch(block_ref, block)
    grad_in = fetch(input_ref, grad)
    outs = []

    def leave(src, dst):
        copy = pltpu.make_async_copy(src, dst, out_sem.at[len(outs)])
        copy.start()
        outs.append(copy)

    def total_of(ref, at, k):
        total = ref[at, k * depth : (k + 1) * depth].astype(F32)
        for s in range(k + INNER, dp_n, INNER):
            total = total + ref[at, s * depth : (s + 1) * depth].astype(F32)
        return total

    for c in range(hidden // 128):
        rd_in[c].wait()
        at = slice(c * 128, (c + 1) * 128)
        for k in range(INNER):
            down[k, at, :] = total_of(rd, at, k)
            leave(down.at[k, at, :], row_cut(down_out, (inner ^ k) * hidden + c * 128, 128))
    block_in.wait()
    leave(block, block_out)
    grad_in.wait()
    leave(grad, input_out)
    for c in range(hidden // 128):
        ru_in[c].wait()
        at = slice(c * 128, (c + 1) * 128)
        for k in range(INNER):
            up[k, :, at] = jnp.transpose(total_of(ru, at, k))
            leave(up.at[k, :, at], lane_cut(up_out, (inner ^ k) * hidden + c * 128, 128))
    for hl in range(2):
        total = jnp.zeros((4 * HD, depth), F32)
        for o in range(groups):
            k = hl * groups + o
            ra_in[k].wait()
            total = total + ra[:, k * depth : (k + 1) * depth].astype(F32)
        qkv[:, hl * 3 * HD : (hl + 1) * 3 * HD] = jnp.transpose(total[: 3 * HD])
        proj[hl * HD : (hl + 1) * HD, :] = total[3 * HD :]
    leave(qkv, qkv_out)
    leave(proj, proj_out)

    tail_in.wait()
    row = tail[0]
    row = jnp.where((t % 2) == 1, pltpu.roll(row, 64, 1), row)
    for k, ref in enumerate((v0, v1, v2, v3, v4, v5)):
        ref[...] = row[min(k, 4) : min(k, 4) + 1, :64]
    line = lax.broadcasted_iota(jnp.int32, (8, 128), 0)
    heads = tail[3]
    heads = jnp.where(d % 2 == 1, pltpu.roll(heads, 64, 1), heads)
    for k in range(2):
        picked = jnp.sum(jnp.where(line == k * 4 + d // 2, heads, 0.0), axis=0, keepdims=True)
        bq_out[k : k + 1, :] = picked[:, :64]
    cols = bf_out.shape[0]
    both = jnp.concatenate([tail[1], tail[2]], axis=0)
    both = pltpu.roll(both, (128 - d * cols) % 128, 1)
    wide_f[pl.ds(0, 16, stride=2), :] = both
    wide_f[pl.ds(1, 16, stride=2), :] = pltpu.roll(both, 64, 1)
    spots = wide_f.shape[0]
    full = jnp.concatenate([wide_f[...], jnp.zeros((128 - spots, 128), F32)], axis=0)
    bf_out[...] = jnp.transpose(full)[:cols, :spots]
    for copy in outs:
        copy.wait()


def solution(mesh):
    dp_n, tp_n = mesh.shape["dp"], mesh.shape["tp"]
    outer = dp_n // INNER
    devices = dp_n * tp_n

    def send(value, dp_xor, tp_xor, keep=None):
        pairs = []
        for d in range(dp_n):
            for t in range(tp_n):
                if keep is None or keep(d, t):
                    pairs.append((d * tp_n + t, (d ^ dp_xor) * tp_n + (t ^ tp_xor)))
        return lax.ppermute(value, AXES, pairs)

    def scatter_small(value, flat):
        held = value
        step = devices // 2
        while step >= 1:
            dp_xor, tp_xor = step // tp_n, step % tp_n
            high = (flat // step) % 2 == 1
            first, second = held[:step], held[step:]
            other = send(jnp.where(high, first, second), dp_xor, tp_xor)
            held = jnp.where(high, second, first) + other
            step //= 2
        return held[0]

    def scatter_rows(value):
        for dp_xor, tp_xor in ((0, 1), (0, 2), (1, 0), (2, 0)):
            half = value.shape[0] // 2
            other = send(value[half:], dp_xor, tp_xor)
            value = value[:half].astype(F32) + other.astype(F32)
            if half > value.shape[0] or (dp_xor, tp_xor) != (2, 0):
                value = value.astype(BF16)
        return value

    def on_device(
        block_input, segment_ids, w_qkv, b_qkv, w_out, b_out, w_fc1, b_fc1, w_fc2, b_fc2,
        ln1_gain, ln1_bias, ln2_gain, ln2_bias, cotangent,
    ):
        d = lax.axis_index("dp")
        t = lax.axis_index("tp")
        flat = d * tp_n + t
        inner = d % INNER
        core = t % 2
        lead = (inner // 2) == core
        rows, width = block_input.shape
        depth = w_qkv.shape[0]
        hidden_here = w_fc1.shape[1] // INNER
        head_here = w_out.shape[0] // HD
        heads = head_here * tp_n
        quarter = SEQ // tp_n
        qkv_bits = b_qkv.shape[1]

        vec = jnp.stack([ln1_gain, ln1_bias, ln2_gain, ln2_bias, b_out + b_fc2]).reshape(-1)
        seg_part = lax.dynamic_slice(segment_ids.reshape(-1), (t * quarter,), (quarter,))
        sizes = [vec.size, b_qkv.size, b_fc1.size, quarter]
        payload = jnp.concatenate(
            [vec, b_qkv.reshape(-1), b_fc1.reshape(-1), seg_part.astype(F32)]
        )
        depth_wide = depth % 128 == 0
        flat_shape = lambda lead_n: (lead_n, width) if depth_wide else (dp_n, lead_n, depth)
        spread = lambda v: v if depth_wide else v.transpose(1, 0, 2).reshape(v.shape[1], width)
        payload = jnp.pad(payload, (0, PAY - payload.size)).reshape(8, PAY // 8)
        like = lambda *shape: jax.ShapeDtypeStruct(shape, BF16)
        dma = pltpu.SemaphoreType.DMA
        hop_count = (devices - 1).bit_length()
        any_spec = pl.BlockSpec(memory_space=pl.ANY)
        x_all, cot_all, up_w, down_w, qkv_w, out_w, small = pl.pallas_call(
            functools.partial(gather_kernel, dp_n, tp_n, depth_wide),
            out_shape=(
                like(16, rows, width),
                like(16, rows, width),
                like(width, hidden_here),
                like(*flat_shape(hidden_here)),
                like(width, 3 * HD),
                like(*flat_shape(HD)),
                jax.ShapeDtypeStruct((devices, 8, PAY // 8), F32),
            ),
            in_specs=[any_spec] * 7,
            out_specs=(any_spec,) * 7,
            scratch_shapes=[
                dma((2, 16)), dma((2, 16)), dma((2, dp_n)), dma((2, dp_n)),
                dma((2, dp_n)), dma((2, dp_n)), dma((2, dp_n)), dma((2, dp_n)),
                dma((hop_count,)), dma((hop_count,)), dma((6,)),
            ],
            compiler_params=pltpu.CompilerParams(collective_id=0, has_side_effects=True),
            name="gather_phase",
        )(block_input, cotangent, w_fc1, w_fc2, w_qkv, w_out, payload)
        down_w, out_w = spread(down_w), spread(out_w)
        small = jnp.take(small.reshape(devices, PAY), flat ^ jnp.arange(devices), axis=0)
        cuts = [0]
        for size in sizes:
            cuts.append(cuts[-1] + size)
        vecs = small[:, : cuts[1]].reshape(devices, 5, -1).transpose(1, 0, 2).reshape(5, width)
        gain_one, shift_one, gain_two, shift_two, out_bias = (vecs[k][None] for k in range(5))
        qkv_bias_all = (
            small[:, cuts[1] : cuts[2]]
            .reshape(dp_n, tp_n, head_here, qkv_bits)
            .transpose(1, 2, 0, 3)
            .reshape(heads, 2 * HD)
        )
        head = (t // 2) * INNER + inner
        qkv_bias = lax.dynamic_slice(qkv_bias_all, (head, 0), (1, 2 * HD))
        up_rows, up_cols = b_fc1.shape
        up_bias_all = (
            small[:, cuts[2] : cuts[3]]
            .reshape(dp_n, tp_n, up_rows, up_cols)
            .transpose(1, 2, 0, 3)
            .reshape(tp_n * INNER, hidden_here)
        )
        up_bias = lax.dynamic_slice(up_bias_all, (t * INNER + inner, 0), (1, hidden_here))
        seg_all = small[:, cuts[3] : cuts[4]].reshape(dp_n, tp_n, quarter)

        x_rows = x_all.reshape(16 * rows, width).astype(F32)
        cot_rows = cot_all.reshape(16 * rows, width)
        row_mean = jnp.mean(x_rows, axis=-1, keepdims=True)
        centered = x_rows - row_mean
        row_var = jnp.mean(centered * centered, axis=-1, keepdims=True)
        inv_std = lax.rsqrt(row_var + EPS)
        normed = centered * inv_std
        norm_two = (normed * gain_two + shift_two).astype(BF16)

        def mine(value):
            split = value.reshape((2, 2, 2, 2, rows) + value.shape[1:])
            cut = lax.dynamic_index_in_dim(split, core, 3, keepdims=False)
            return jnp.moveaxis(cut, 2, 0).reshape((2 * SEQ,) + value.shape[1:])

        def unmine(value):
            split = value.reshape((2, 2, 2, rows) + value.shape[1:])
            cut = jnp.moveaxis(split, 0, 2)[:, :, :, None]
            where = (jnp.arange(2) == core).reshape((1, 1, 1, 2) + (1,) * value.ndim)
            full = jnp.where(where, cut, jnp.zeros_like(cut))
            return full.reshape((16 * rows,) + value.shape[1:])

        norm_one = (mine(normed) * gain_one + shift_one).astype(BF16)
        cot_mine = mine(cot_rows)

        pre_act = mm(norm_two, up_w) + up_bias
        half_gelu = gelu_half(pre_act)
        hidden = (pre_act * half_gelu).astype(BF16)
        down_grad = mm_lead(hidden, cot_rows)
        act_cot = mm_tail(cot_rows, down_w) * gelu_slope(pre_act)
        up_bias_part = jnp.sum(act_cot, axis=0)
        act_low = act_cot.astype(BF16)
        up_grad = mm_lead(norm_two, act_low)
        up_grad, down_grad = up_grad.astype(BF16), down_grad.astype(BF16)

        def cut_block(value, s):
            return lax.dynamic_slice(value, ((d ^ s) * depth, 0), (depth, value.shape[1]))

        def cut_across(value, s):
            return lax.dynamic_slice(value, (0, (d ^ s) * depth), (value.shape[0], depth))

        with jax.named_scope("mlp_out"):
            up_back = [cut_block(up_grad, 0)] + [
                send(cut_block(up_grad, s), s, 0) for s in range(1, dp_n)
            ]
            down_back = [cut_across(down_grad, 0)] + [
                send(cut_across(down_grad, s), s, 0) for s in range(1, dp_n)
            ]

        order = jnp.stack([t ^ ((k % 2) * 2 + k // 2) for k in range(4)])
        position = (order[:, None] * quarter + jnp.arange(quarter)[None]).reshape(-1)
        inverse = jnp.exp(jnp.arange(ROT // 2, dtype=F32) * (-2.0 * math.log(10000.0) / ROT))
        angle = position.astype(F32)[:, None] * inverse[None]
        cosine, sine = jnp.cos(angle)[None], jnp.sin(angle)[None]
        segs = []
        for dy in range(2):
            seq = (d // INNER) * INNER + (inner ^ (core * 2 + dy))
            rows_of = lax.dynamic_index_in_dim(seg_all, seq, 0, keepdims=False)
            segs.append(jnp.take(rows_of, order, axis=0).reshape(-1))
        segs = jnp.stack(segs)
        allowed = (position[None, :] <= position[:, None])[None] & (
            segs[:, :, None] == segs[:, None, :]
        )
        qkv = mm(norm_one, qkv_w)
        query = rotate((qkv[:, :HD] + qkv_bias[:, :HD]).reshape(2, SEQ, HD), cosine, sine).astype(BF16)
        key = rotate(qkv[:, HD : 2 * HD].reshape(2, SEQ, HD), cosine, sine).astype(BF16)
        val = (qkv[:, 2 * HD :] + qkv_bias[:, HD:]).astype(BF16).reshape(2, SEQ, HD)
        scale = HD ** (-0.5)

        def ein(eq, left, right):
            return jnp.einsum(eq, left, right, preferred_element_type=F32)

        masked = jnp.where(allowed, ein("sqd,skd->sqk", query, key) * scale, NEG_FILL)
        peak = jnp.max(masked, axis=-1, keepdims=True)
        log_total = peak + jnp.log(
            jnp.sum(jnp.where(allowed, jnp.exp(masked - peak), 0.0), axis=-1, keepdims=True)
        )
        prob_full = jnp.where(allowed, jnp.exp(masked - log_total), 0.0)
        prob_low = prob_full.astype(BF16)
        context = ein("sqk,skd->sqd", prob_low, val).astype(BF16)
        context_cot = mm_tail(cot_mine, out_w).astype(BF16).reshape(2, SEQ, HD)
        prob_cot = ein("sqd,skd->sqk", context_cot, val)
        row_delta = jnp.sum(context_cot.astype(F32) * context.astype(F32), axis=-1, keepdims=True)
        score_cot = (prob_full * (prob_cot - row_delta)).astype(BF16)
        query_cot = rotate(ein("sqk,skd->sqd", score_cot, key) * scale, cosine, -sine)
        key_cot = rotate(ein("sqk,sqd->skd", score_cot, query) * scale, cosine, -sine)
        val_cot = ein("sqk,sqd->skd", prob_low, context_cot)
        qkv_cot = jnp.concatenate([query_cot, key_cot, val_cot], axis=-1).reshape(2 * SEQ, 3 * HD)
        qkv_bias_part = jnp.concatenate(
            [jnp.sum(query_cot, axis=(0, 1)), jnp.sum(val_cot, axis=(0, 1))]
        )
        qkv_low = qkv_cot.astype(BF16)
        context_flat = context.reshape(2 * SEQ, HD)
        att_grad = jnp.concatenate(
            [mm_lead(norm_one, qkv_low).astype(BF16), mm_lead(cot_mine, context_flat).astype(BF16)],
            axis=1,
        )
        att_pair = send(att_grad, 0, 1, lambda dd, tt: (dd % INNER) // 2 != tt % 2)
        att_grad = (att_grad.astype(F32) + att_pair.astype(F32)).astype(BF16)
        with jax.named_scope("att_out"):
            own_att = cut_block(att_grad, 0)
            att_back = [jnp.where(lead, own_att, jnp.zeros_like(own_att))] + [
                send(cut_block(att_grad, s), s, 0, lambda dd, tt: (dd % INNER) // 2 == tt % 2)
                for s in range(1, dp_n)
            ]

        left = jnp.concatenate([hidden, unmine(context_flat)], axis=1)
        right = jnp.concatenate([down_w, out_w], axis=0)
        with jax.named_scope("branch"):
            branch = scatter_rows(mm(left, right).astype(BF16))
        block_output = (block_input.astype(F32) + branch + out_bias).astype(BF16)

        one_part = mm_tail(qkv_low, qkv_w)
        two_part = mm_tail(act_low, up_w)
        vec_terms = jnp.stack(
            [
                jnp.sum(one_part * mine(normed), axis=0),
                jnp.sum(one_part, axis=0),
                jnp.sum(two_part * normed, axis=0),
                jnp.sum(two_part, axis=0),
                jnp.sum(cotangent.astype(F32), axis=0),
            ]
        )
        scaled_part = (two_part * gain_two + unmine(one_part * gain_one)).astype(BF16)
        with jax.named_scope("normback"):
            scaled = scatter_rows(scaled_part)
        normed_own = normed[:rows]
        input_grad = cotangent.astype(F32) + inv_std[:rows] * (
            scaled
            - jnp.mean(scaled, axis=-1, keepdims=True)
            - normed_own * jnp.mean(scaled * normed_own, axis=-1, keepdims=True)
        )

        head_hot = (jnp.arange(heads) == head).astype(F32)[:, None]
        qkv_small = (
            (head_hot * qkv_bias_part[None])
            .reshape(tp_n, head_here, dp_n, qkv_bits)
            .transpose(2, 0, 1, 3)
            .reshape(devices, -1)
        )
        up_hot = (jnp.arange(tp_n * INNER) == t * INNER + inner).astype(F32)[:, None]
        up_small = (
            (up_hot * up_bias_part[None])
            .reshape(tp_n, up_rows, dp_n, up_cols)
            .transpose(2, 0, 1, 3)
            .reshape(devices, -1)
        )
        vec_small = vec_terms.reshape(5, devices, -1).transpose(1, 0, 2).reshape(devices, -1)
        with jax.named_scope("small_out"):
            own = scatter_small(jnp.concatenate([vec_small, qkv_small, up_small], axis=1), flat)
        vec_own = own[: cuts[1]].reshape(5, -1)
        qkv_bias_grad = own[cuts[1] : cuts[2]].reshape(b_qkv.shape)
        up_bias_grad = own[cuts[2] : cuts[3]].reshape(b_fc1.shape)

        up_total = jnp.zeros(w_fc1.shape, F32)
        down_total = jnp.zeros(w_fc2.shape, F32)
        for k in range(INNER):
            at = (inner ^ k) * hidden_here
            up_sum = sum(up_back[s].astype(F32) for s in range(k, dp_n, INNER))
            down_sum = sum(down_back[s].astype(F32) for s in range(k, dp_n, INNER))
            up_total = lax.dynamic_update_slice(up_total, up_sum, (0, at))
            down_total = lax.dynamic_update_slice(down_total, down_sum, (at, 0))
        att_sum = [sum(att_back[s].astype(F32) for s in range(k, dp_n, 2)) for k in range(2)]
        odd = inner % 2 == 1
        att_first = jnp.where(odd, att_sum[1], att_sum[0])
        att_second = jnp.where(odd, att_sum[0], att_sum[1])
        qkv_total = jnp.concatenate([att_first[:, : 3 * HD], att_second[:, : 3 * HD]], axis=1)
        out_total = jnp.concatenate([att_first[:, 3 * HD :].T, att_second[:, 3 * HD :].T], axis=0)
        return (
            block_output, input_grad, qkv_total, qkv_bias_grad, out_total, vec_own[4],
            up_total, up_bias_grad, down_total, vec_own[4],
            vec_own[0], vec_own[1], vec_own[2], vec_own[3],
        )

    def on_device_fused(
        block_input, segment_ids, w_qkv, b_qkv, w_out, b_out, w_fc1, b_fc1, w_fc2, b_fc2,
        ln1_gain, ln1_bias, ln2_gain, ln2_bias, cotangent,
    ):
        d = lax.axis_index("dp")
        t = lax.axis_index("tp")
        flat = d * tp_n + t
        inner = d % INNER
        core = t % 2
        lead = (inner // 2) == core
        rows, width = block_input.shape
        depth = w_qkv.shape[0]
        hidden_here = w_fc1.shape[1] // INNER
        head_here = w_out.shape[0] // HD
        heads = head_here * tp_n
        quarter = SEQ // tp_n
        qkv_bits = b_qkv.shape[1]

        up_rows = b_fc1.shape[0]
        per = ln1_gain.shape[0]
        seg_row = segment_ids.reshape(1, -1)
        small_in = [v.reshape(1, -1) for v in (ln1_gain, ln1_bias, ln2_gain, ln2_bias, b_out, b_fc2)]
        small_in += [b_qkv, b_fc1.T, seg_row]
        angle = np.arange(SEQ)[:, None] * np.exp(np.arange(ROT // 2) * (-2.0 * math.log(10000.0) / ROT))
        pad = np.zeros((SEQ, 128 - ROT))
        cosine = np.concatenate([np.cos(angle), np.cos(angle), pad + 1.0], axis=1)
        sine = np.concatenate([np.sin(angle), np.sin(angle), pad], axis=1)
        rope = jnp.asarray(np.stack([cosine, sine]), F32)
        like = lambda *shape: jax.ShapeDtypeStruct(shape, BF16)
        wide_f = lambda *shape: jax.ShapeDtypeStruct(shape, F32)
        dma = pltpu.SemaphoreType.DMA
        vb = lambda *shape: pltpu.VMEM(shape, BF16)
        vf = lambda *shape: pltpu.VMEM(shape, F32)
        any_spec = pl.BlockSpec(memory_space=pl.ANY)
        group = 16 * rows
        per_peer = dma((2, dp_n))
        pair = 2 * SEQ
        results = pl.pallas_call(
            functools.partial(fused_kernel, dp_n, tp_n),
            out_shape=(
                like(rows, width), wide_f(rows, width), wide_f(4, 8, 128),
                like(hidden_here, width), like(hidden_here, width),
                like(hidden_here, width), like(hidden_here, width), like(4 * HD, width),
                like(4 * HD, width),
            ),
            in_specs=[any_spec] * 16,
            out_specs=(any_spec,) * 9,
            scratch_shapes=[
                vb(group, width), vb(group, width), vb(group, width),
                vb(hidden_here, width), vb(hidden_here, width), vf(hidden_here, group),
                vb(hidden_here, group), vb(hidden_here, group), vb(3, hidden_here, depth),
                vf(group, 128), vf(8, width), vf(8, width), vf(hidden_here, 128),
                vb(width, 3 * HD), vb(HD, width), vb(pair, width),
                vb(pair, HD), vb(pair, HD), vb(pair, HD), vb(pair, SEQ),
                vb(pair, HD), vb(HD, pair), vb(pair, HD), vb(pair, 3 * HD), vb(3 * HD, pair),
                vb(4 * HD, width), vf(2, SEQ, 128),
                vf(6, 1, per), vf(*b_qkv.shape), vf(*b_fc1.T.shape), pltpu.VMEM(seg_row.shape, jnp.int32), vf(up_rows, 128),
                vf(4, 8, 128), vf(8, 128), vf(8, 128), vf(devices // 2, 8, 128), vf(dp_n, 8, 128), vf(2 * dp_n, 8, 128),
                vf(devices // 2, 8, 128), vf(dp_n, 8, 128), vf(2 * dp_n, 8, 128), vf(8, 128), vf(8, 128),
                vf(8, SEQ), vf(SEQ, 128), vf(8, 2 * HD), vf(8, 2 * HD),
                dma((2, 16)), dma((2, 16)), per_peer, per_peer, per_peer, per_peer, per_peer, per_peer,
                dma((3,)), dma((3,)), dma((2 * dp_n,)), dma((2 * dp_n,)), dma((3,)), dma((3,)), dma((2 * dp_n,)), dma((2 * dp_n,)),
                per_peer, per_peer, dma((3,)),
                dma((2, 16)), dma((2, 16)), dma((8,)), dma((8,)), dma((dp_n,)), dma((dp_n,)),
                dma((24,)), dma((24,)), pltpu.SemaphoreType.REGULAR((6,)),
            ],
            compiler_params=pltpu.CompilerParams(
                collective_id=0, has_side_effects=True, vmem_limit_bytes=67_043_328
            ),
            name="fused_block",
        )(block_input, cotangent, w_fc1, w_fc2, w_qkv, w_out, rope, *small_in)
        f32_out = lambda *shape: jax.ShapeDtypeStruct(shape, F32)
        ends = pl.pallas_call(
            functools.partial(finish_kernel, dp_n, tp_n),
            out_shape=(
                like(rows, width), f32_out(rows, width), f32_out(*w_fc1.shape), f32_out(*w_fc2.shape),
                f32_out(*w_qkv.shape), f32_out(*w_out.shape),
            ) + (f32_out(1, per),) * 6 + (f32_out(*b_qkv.shape), f32_out(*b_fc1.T.shape)),
            in_specs=[any_spec] * 6,
            out_specs=(any_spec,) * 6 + (pl.BlockSpec(memory_space=pltpu.VMEM),) * 8,
            scratch_shapes=[
                vb(rows, width), vf(rows, width), vb(hidden_here, width), vb(hidden_here, width),
                vb(4 * HD, width // 2), vf(INNER, depth, hidden_here), vf(INNER, hidden_here, depth),
                vf(*w_qkv.shape), vf(*w_out.shape), vf(4, 8, 128), vf(up_rows, 128),
                dma((24,)), dma((48,)),
            ],
            compiler_params=pltpu.CompilerParams(vmem_limit_bytes=60_000_000),
            name="finish",
        )(results[0], results[1], results[2], results[5], results[6], results[7])
        block_output, input_grad, up_total, down_total, qkv_total, out_total = ends[:6]
        small = [v.reshape(-1) for v in ends[6:12]]
        return (
            block_output, input_grad, qkv_total, ends[12], out_total, small[4],
            up_total, ends[13].T, down_total, small[5],
            small[0], small[1], small[2], small[3],
        )

    row, vec = P(AXES, None), P(AXES)
    col, low = P("dp", "tp"), P("tp", "dp")
    def choose(*arrays):
        wide = arrays[2].shape[0] % 128 == 0
        return (on_device_fused if wide else on_device)(*arrays)

    return jax.shard_map(
        choose,
        mesh=mesh,
        in_specs=(row, P("dp", None), col, low, low, vec, col, low, low, vec, vec, vec, vec, vec, row),
        out_specs=(row, row, col, low, low, vec, col, low, low, vec, vec, vec, vec, vec),
        check_vma=False,
    )
```

```python
import functools
import math

import jax
import jax.numpy as jnp
import numpy as np
from jax import lax
from jax.experimental import pallas as pl
from jax.experimental.pallas import tpu as pltpu
from jax.sharding import PartitionSpec as P

HD = 256
ROT = 64
SEQ = 512
INNER = 4
EPS = 1e-05
NEG_FILL = -1e30
F32 = jnp.float32
BF16 = jnp.bfloat16
AXES = ("dp", "tp")
MESH = pl.DeviceIdType.MESH
PAY = 1024


def dot(left, right, contract):
    return lax.dot_general(left, right, (contract, ((), ())), preferred_element_type=F32)


def mm(left, right):
    return dot(left, right, ((1,), (0,)))


def mm_tail(left, right):
    return dot(left, right, ((1,), (1,)))


def mm_lead(left, right):
    return dot(left, right, ((0,), (0,)))


def gelu_half(pre_act):
    return 0.5 * (1.0 + jax.scipy.special.erf(pre_act * 2.0 ** (-0.5)))


def gelu_slope(pre_act):
    return gelu_half(pre_act) + pre_act * jnp.exp(-0.5 * pre_act * pre_act) * (2.0 * math.pi) ** (-0.5)


def rotate(block, cosine, sine):
    half = ROT // 2
    lower, upper = block[..., :half], block[..., half:ROT]
    return jnp.concatenate(
        [lower * cosine - upper * sine, upper * cosine + lower * sine, block[..., ROT:]], axis=-1
    )


def gather_kernel(
    dp_n, tp_n, wide,
    x_ref, cot_ref, fc1_ref, fc2_ref, qkv_ref, out_ref, pay_ref,
    xs_ref, cots_ref, up_ref, down_ref, att_ref, proj_ref, small_ref,
    row_send, row_recv, mlp_send, mlp_recv, att_send, att_recv, pass_send, pass_recv,
    small_send, small_recv, local_sem,
):
    d = lax.axis_index("dp")
    t = lax.axis_index("tp")
    inner = d % INNER
    core = t % 2
    depth = fc1_ref.shape[0]
    hidden = fc1_ref.shape[1] // INNER

    barrier = pltpu.get_barrier_semaphore()
    for s in range(1, dp_n):
        pl.semaphore_signal(barrier, inc=1, device_id=(d ^ s, t), device_id_type=MESH)
    for k in (1, 2):
        pl.semaphore_signal(barrier, inc=1, device_id=(d, t ^ k), device_id_type=MESH)

    def remote(src, dst, send_sem, recv_sem, dp_xor, tp_xor):
        return pltpu.make_async_remote_copy(
            src_ref=src, dst_ref=dst, send_sem=send_sem, recv_sem=recv_sem,
            device_id=(d ^ dp_xor, t ^ tp_xor), device_id_type=MESH,
        )

    hop = {1: (2, 0), 2: (1, 0), 4: (0, 2), 8: (0, 1)}
    pairs = ((x_ref, xs_ref), (cot_ref, cots_ref))

    def row_copy(a, k, bit):
        own, full = pairs[a]
        src = own if k == 0 else full.at[k]
        return remote(src, full.at[k + bit], row_send.at[a, k + bit], row_recv.at[a, k + bit], *hop[bit])

    def columns(ref, index, size):
        return ref.at[:, pl.ds(pl.multiple_of(index * size, 128), size)]

    def lines(ref, index, size):
        return ref.at[pl.ds(pl.multiple_of(index * size, 8), size), :]

    def across(ref, index, size):
        return columns(ref, index, size) if wide else ref.at[index]

    def mlp_copies(s):
        target = inner ^ (s % INNER)
        return (
            (columns(fc1_ref, target, hidden), lines(up_ref, d, depth)),
            (lines(fc2_ref, target, hidden), across(down_ref, d, depth)),
        )

    def att_copies(s):
        target = (inner ^ (s % INNER)) % 2
        return (
            (columns(qkv_ref, target, 3 * HD), lines(att_ref, d, depth)),
            (lines(out_ref, target, HD), across(proj_ref, d, depth)),
        )

    def att_land(s):
        return (lines(att_ref, d ^ s, depth), across(proj_ref, d ^ s, depth))

    def mlp_land(s):
        return (lines(up_ref, d ^ s, depth), across(down_ref, d ^ s, depth))

    local = []
    def stay(src, dst):
        copy = pltpu.make_async_copy(src, dst, local_sem.at[len(local)])
        copy.start()
        local.append(copy)

    lead = (inner // 2) == core
    pltpu.sync_copy(pay_ref, small_ref.at[0])
    pl.semaphore_wait(barrier, dp_n + 1)

    started = []
    def start(copy):
        copy.start()
        started.append(copy)

    def start_rows(k, bit):
        for a in range(2):
            start(row_copy(a, k, bit))

    def wait_rows(k):
        bit = 1
        while bit * 2 <= k:
            bit *= 2
        for a in range(2):
            row_copy(a, k - bit, bit).wait_recv()

    def start_mlp(s):
        for a, (src, dst) in enumerate(mlp_copies(s)):
            start(remote(src, dst, mlp_send.at[a, s], mlp_recv.at[a, s], s, 0))

    def att_active(s):
        return ((inner ^ (s % INNER)) // 2) == core

    def start_att(s):
        @pl.when(att_active(s))
        def _():
            for a, (src, dst) in enumerate(att_copies(s)):
                remote(src, dst, att_send.at[a, s], att_recv.at[a, s], s, 0).start()

    def pass_att(s):
        lands = att_land(s)
        return [
            remote(land, land, pass_send.at[a, s], pass_recv.at[a, s], 0, 1)
            for a, land in enumerate(lands)
        ]

    def small_copy(step, dp_xor, tp_xor, n):
        return remote(
            small_ref.at[pl.ds(0, n)], small_ref.at[pl.ds(n, n)],
            small_send.at[step], small_recv.at[step], dp_xor, tp_xor,
        )

    hops = []
    n = 1
    while n < dp_n * tp_n:
        hops.append((n // tp_n, n % tp_n, n))
        n *= 2
    even = [s for s in range(2, dp_n, 2)]
    even.sort(key=lambda s: -(s >= INNER))
    odd = [s for s in range(1, dp_n, 2)]
    odd.sort(key=lambda s: -(s >= INNER))

    small = [small_copy(k, *h) for k, h in enumerate(hops)]
    small[0].start()
    for bit in (1, 2, 4):
        start_rows(0, bit)
    start_rows(0, 8)
    for s in even:
        start_mlp(s)
    stay(x_ref, xs_ref.at[0])
    stay(cot_ref, cots_ref.at[0])
    for src, dst in mlp_copies(0):
        stay(src, dst)

    @pl.when(lead)
    def _():
        for a, (src, dst) in enumerate(att_copies(0)):
            copy = pltpu.make_async_copy(src, dst, local_sem.at[4 + a])
            copy.start()

    for k in range(len(small)):
        small[k].wait_recv()
        if k + 1 < len(small):
            small[k + 1].start()
    wait_rows(1)
    start_rows(1, 2)
    start_rows(1, 4)
    start_rows(1, 8)
    wait_rows(2)
    start_rows(2, 4)
    start_rows(2, 8)
    for s in odd:
        start_mlp(s)
    for s in even + odd:
        start_att(s)
    wait_rows(3)
    start_rows(3, 4)
    start_rows(3, 8)
    wait_rows(4)
    start_rows(4, 8)

    @pl.when(lead)
    def _():
        for a, (src, dst) in enumerate(att_copies(0)):
            pltpu.make_async_copy(src, dst, local_sem.at[4 + a]).wait()
        for copy in pass_att(0):
            copy.start()

    for k in (5, 6, 7):
        wait_rows(k)
        start_rows(k, 8)
    for k in range(8, 16):
        wait_rows(k)
    for s in even + odd:
        for a, dst in enumerate(mlp_land(s)):
            remote(dst, dst, mlp_send.at[a, s], mlp_recv.at[a, s], s, 0).wait_recv()
    for s in even + odd:
        @pl.when(lead)
        def _():
            for a, dst in enumerate(att_land(s)):
                remote(dst, dst, att_send.at[a, s], att_recv.at[a, s], s, 0).wait_recv()
            for copy in pass_att(s):
                copy.start()

    @pl.when(jnp.logical_not(lead))
    def _():
        for s in range(dp_n):
            for copy in pass_att(s):
                copy.wait_recv()

    @pl.when(lead)
    def _():
        for s in range(dp_n):
            for copy in pass_att(s):
                copy.wait_send()

    for s in range(1, dp_n):
        @pl.when(att_active(s))
        def _():
            for a, (src, dst) in enumerate(att_copies(s)):
                remote(src, dst, att_send.at[a, s], att_recv.at[a, s], s, 0).wait_send()
    for copy in started:
        copy.wait_send()
    for copy in small:
        copy.wait_send()
    for copy in local:
        copy.wait()


def span(start, size, unit):
    return pl.ds(start if isinstance(start, int) else pl.multiple_of(start, unit), size)


def lane_cut(ref, start, size):
    return ref.at[:, span(start, size, 128)]


def row_cut(ref, start, size):
    return ref.at[span(start, size, 16), :]


def columns_of(rows8):
    pad = jnp.zeros((120, 128), F32)
    return jnp.transpose(jnp.concatenate([rows8, pad], axis=0))


def fused_kernel(
    dp_n, tp_n,
    x_ref, cot_ref, fc1_ref, fc2_ref, qkv_ref, out_ref, rope_ref,
    vec0_ref, vec1_ref, vec2_ref, vec3_ref, vec4_ref, vec5_ref, bq_ref, bf_ref, seg_ref,
    block_out, input_out, tail_out,
    gu_hbm, gd_hbm, ru_hbm, rd_hbm, ra_hbm, pair_hbm,
    xs, cots, n2, up_t, down_w, pre, hid_t, act_t, ring, stats, vecs, sums, up_sum,
    att_w, proj_w, n1, q_s, k_s, v_s, prob, ctx, ctx_t, cctx, low, low_t, gx,
    rope, raw, raw_q, raw_f, raw_seg, wide_f, pay, pair_in, pair_back, vec_in, bias_in, head_in, vec_back, bias_back, head_back, up_place, head_place,
    keys, queries, qkv_bias, qkv_sum,
    row_send, row_recv, mlp_send, mlp_recv, att_send, att_recv, pass_send, pass_recv,
    small_send, small_recv, head_send, head_recv, back_send, back_recv, headb_send, headb_recv, g_send, g_recv, g_local,
    rs_send, rs_recv, pair_send, pair_recv, ga_send, ga_recv,
    local_sem, out_sem, credit,
):
    d = lax.axis_index("dp")
    t = lax.axis_index("tp")
    flat = d * tp_n + t
    inner = d % INNER
    core = t % 2
    lead = (inner // 2) == core
    follow = jnp.logical_not(lead)
    rows, width = x_ref.shape
    depth = fc1_ref.shape[0]
    hidden = fc1_ref.shape[1] // INNER
    devices = dp_n * tp_n
    slots = 16
    tokens = slots * rows
    scale = HD ** (-0.5)
    chunk = 512

    barrier = pltpu.get_barrier_semaphore()
    for a in range(1, devices):
        peer = (d ^ (a // tp_n), t ^ (a % tp_n))
        pl.semaphore_signal(barrier, inc=1, device_id=peer, device_id_type=MESH)

    def remote(src, dst, send_sem, recv_sem, dp_xor, tp_xor):
        return pltpu.make_async_remote_copy(
            src_ref=src, dst_ref=dst, send_sem=send_sem, recv_sem=recv_sem,
            device_id=(d ^ dp_xor, t ^ tp_xor), device_id_type=MESH,
        )

    started = []

    def start(copy):
        copy.start()
        started.append(copy)

    hop = {1: (2, 0), 2: (1, 0), 4: (0, 2), 8: (0, 1)}

    def slot(ref, k):
        return row_cut(ref, k * rows, rows)

    def row_copy(a, k, bit):
        own, full = ((x_ref, xs), (cot_ref, cots))[a]
        src = own if k == 0 else slot(full, k)
        return remote(
            src, slot(full, k + bit), row_send.at[a, k + bit], row_recv.at[a, k + bit], *hop[bit]
        )

    row_started = ([], [])

    def start_row(a, k, *bits):
        for bit in bits:
            copy = row_copy(a, k, bit)
            copy.start()
            row_started[a].append(copy)

    def wait_row(a, k):
        bit = 1
        while bit * 2 <= k:
            bit *= 2
        row_copy(a, k - bit, bit).wait_recv()

    def w1_piece(i):
        return gx.at[depth : depth + hidden, pl.ds(pl.multiple_of(i * depth, 128), depth)]

    def mlp_copy(a, s):
        target = inner ^ (s % INNER)
        src = w1_piece(target) if a == 0 else row_cut(fc2_ref, target * hidden, hidden)
        dst = lane_cut((up_t, down_w)[a], d * depth, depth)
        if s == 0:
            return src, dst
        return remote(src, dst, mlp_send.at[a, s], mlp_recv.at[a, s], s, 0)

    mlp_started = tuple([mlp_copy(a, s) for s in range(1, dp_n)] for a in range(2))

    def start_mlp(a, s):
        mlp_started[a][s - 1].start()

    def mlp_wait(a, s):
        dst = lane_cut((up_t, down_w)[a], (d ^ s) * depth, depth)
        remote(dst, dst, mlp_send.at[a, s], mlp_recv.at[a, s], s, 0).wait_recv()

    def att_active(s):
        return ((inner ^ (s % INNER)) // 2) == core

    def att_pairs(s):
        target = (inner ^ (s % INNER)) % 2
        return (
            (lane_cut(qkv_ref, target * 3 * HD, 3 * HD), row_cut(att_w, d * depth, depth)),
            (row_cut(out_ref, target * HD, HD), lane_cut(proj_w, d * depth, depth)),
        )

    def att_land(s):
        return (row_cut(att_w, (d ^ s) * depth, depth), lane_cut(proj_w, (d ^ s) * depth, depth))

    def start_att(s):
        @pl.when(att_active(s))
        def _():
            for a, (src, dst) in enumerate(att_pairs(s)):
                remote(src, dst, att_send.at[a, s], att_recv.at[a, s], s, 0).start()

    def pass_att(s):
        return [
            remote(land, land, pass_send.at[a, s], pass_recv.at[a, s], 0, 1)
            for a, land in enumerate(att_land(s))
        ]

    local = []

    def stay(src, dst):
        copy = pltpu.make_async_copy(src, dst, local_sem.at[len(local)])
        copy.start()
        local.append(copy)
        return copy

    fc1_in = stay(fc1_ref, gx.at[0:depth, :])
    raw_in = [
        stay(ref, raw.at[k])
        for k, ref in enumerate((vec0_ref, vec1_ref, vec2_ref, vec3_ref, vec4_ref, vec5_ref))
    ]
    raw_in += [stay(bq_ref, raw_q), stay(bf_ref, raw_f), stay(seg_ref, raw_seg)]
    x_in = stay(x_ref, slot(xs, 0))
    cot_in = stay(cot_ref, slot(cots, 0))
    down_in = stay(*mlp_copy(1, 0))
    rope_in = stay(rope_ref, rope)
    for copy in raw_in:
        copy.wait()
    zero64 = jnp.zeros((1, 64), F32)
    line = lax.broadcasted_iota(jnp.int32, (8, 128), 0)

    def wide(row):
        return jnp.broadcast_to(jnp.concatenate([row, zero64], axis=1), (8, 128))

    def onto(base, row, value):
        return jnp.where(line == row, value, base)

    odd_flat = flat % 2 == 1
    group = jnp.zeros((8, 128), F32)
    for k in range(5):
        row = raw[k] if k < 4 else raw[4] + raw[5]
        value = wide(row)
        group = onto(group, k, jnp.where(odd_flat, pltpu.roll(value, 64, 1), value))
    seg_row = raw_seg[:, pl.ds(pl.multiple_of(t * 128, 128), 128)].astype(F32)
    pay[0] = onto(group, 5 + core, jnp.broadcast_to(seg_row, (8, 128)))
    group = jnp.zeros((8, 128), F32)
    for k in range(2):
        value = wide(raw_q[k : k + 1, :])
        value = jnp.where(d % 2 == 1, pltpu.roll(value, 64, 1), value)
        group = onto(group, k * 4 + d // 2, value)
    pay[3] = group
    up_lines, up_spots = raw_f.shape
    flat_f = jnp.concatenate([raw_f[...], jnp.zeros((up_lines, 128 - up_spots), F32)], axis=1)
    value = pltpu.roll(columns_of(flat_f)[:up_spots], d * up_lines, 1)
    odd_row = lax.broadcasted_iota(jnp.int32, value.shape, 0) % 2 == 1
    wide_f[...] = jnp.where(odd_row, pltpu.roll(value, 64, 1), value)
    merged = wide_f[pl.ds(0, 16, stride=2), :] + wide_f[pl.ds(1, 16, stride=2), :]
    pay[1] = merged[:8]
    pay[2] = merged[8:]
    pl.semaphore_wait(barrier, devices - 1)

    even = sorted(range(2, dp_n, 2), key=lambda s: -(s >= INNER))
    odd = sorted(range(1, dp_n, 2), key=lambda s: -(s >= INNER))

    def small_copy(kind, src, dst, dp_xor, tp_xor):
        return remote(src, dst, small_send.at[kind], small_recv.at[kind], dp_xor, tp_xor)

    chip = flat // 2
    chips = devices // 2
    meet = small_copy(2, pay.at[0], pair_in, 0, 1)
    meet.start()

    def head_in_copy(s, dc):
        return remote(
            pay.at[3], head_in.at[2 * s + dc], head_send.at[2 * s + dc], head_recv.at[2 * s + dc], s, dc
        )

    def head_in_each(act):
        @pl.when(lead)
        def _():
            act(head_in_copy(0, 1))

        for s in range(1, dp_n):
            @pl.when(att_active(s))
            def _():
                act(head_in_copy(s, 0))
                act(head_in_copy(s, 1))

    for s in range(1, dp_n):
        group = 1 + (inner ^ (s % INNER)) // 2
        small_copy(1, pay.at[group], bias_in.at[s], s, 0).start()
    head_in_each(lambda copy: copy.start())
    meet.wait_recv()
    vec_in[0] = pay[0] + pair_in[...]
    for r in range(1, chips):
        small_copy(0, vec_in.at[0], vec_in.at[r], r // 2, (r % 2) * 2).start()
    start_row(0, 0, 1, 2, 4, 8)
    start_row(1, 0, 1, 8)
    bias_in[0] = pay[1 + inner // 2]
    head_in[0] = pay[3]
    fc1_in.wait()
    for i in range(INNER):
        piece = gx[0:depth, i * hidden : (i + 1) * hidden].astype(F32)
        gx[depth : depth + hidden, i * depth : (i + 1) * depth] = jnp.transpose(piece).astype(BF16)
    near = [2, 3]
    far = [s for s in (6, 4, 7, 5) if s < dp_n]
    plane = d // 2
    end = (plane == 0) | (plane == dp_n // 2 - 1)
    middle = jnp.logical_not(end)

    def start_all(s):
        start_att(s)
        start_mlp(0, s)
        start_mlp(1, s)

    start_att(2)
    for s in far:
        start_att(s)
    start_mlp(0, 2)
    start_mlp(1, 2)

    @pl.when(end)
    def _():
        start_all(3)

    for s in far:
        start_mlp(0, s)

    @pl.when(end)
    def _():
        for s in far:
            start_mlp(1, s)

    up_in = stay(*mlp_copy(0, 0))

    @pl.when(lead)
    def _():
        for a, (src, dst) in enumerate(att_pairs(0)):
            pltpu.make_async_copy(src, dst, local_sem.at[20 + a]).start()

    wait_row(0, 1)
    start_row(0, 1, 2, 4, 8)
    wait_row(0, 2)
    start_row(0, 2, 4, 8)
    start_row(1, 0, 2)

    def small_waits(kind):
        buf = (vec_in, bias_in, head_in)[kind]
        rest = buf.at[pl.ds(1, buf.shape[0] - 1)]
        return small_copy(kind, rest, rest, 0, 1)

    for kind in range(2):
        small_waits(kind).wait_recv()

    @pl.when(lead)
    def _():
        for s in range(1, dp_n):
            head_in_copy(s, 0).wait_recv()

    @pl.when(follow)
    def _():
        for s in range(dp_n):
            head_in_copy(s, 1).wait_recv()

    for j in range(chips):
        vecs[:, j * 128 : (j + 1) * 128] = vec_in[chip ^ j]
    bias8 = jnp.zeros((8, 128), F32)
    head8 = jnp.zeros((8, 128), F32)
    head_rel = core ^ (inner // 2)
    for s in range(dp_n):
        bias8 = bias8 + bias_in[s]
        head8 = head8 + head_in[s * 2 + head_rel]
    second = inner % 2 == 1
    bias_t = columns_of(bias8)
    up_bias = jnp.concatenate(
        [jnp.where(second, bias_t[:, 4 + k : 5 + k], bias_t[:, k : k + 1]) for k in range(4)], axis=0
    )
    head4 = jnp.where(second, head8[4:], head8[:4])
    qkv_bias[0:1, :] = jnp.concatenate([head4[k : k + 1] for k in range(4)], axis=1)
    lane = lax.broadcasted_iota(jnp.int32, (1, 128), 1)
    keys[...] = jnp.zeros_like(keys)
    for q in range(4):
        at = slice(q * 128, (q + 1) * 128)
        keys[0:1, at] = ((t ^ ((q % 2) * 2 + q // 2)) * 128 + lane).astype(F32)
        for dy in range(2):
            peer = vec_in[(core * 2 + dy) * 2 + q % 2]
            keys[1 + dy : 2 + dy, at] = jnp.where((core ^ (q // 2)) == 1, peer[6:7, :], peer[5:6, :])
        queries[at, :] = columns_of(keys[:, at])

    def norm_slot(k):
        @pl.loop(0, rows // 16)
        def _(j):
            at = pl.ds(pl.multiple_of(k * rows + j * 16, 16), 16)
            value = xs[at, :].astype(F32)
            mean = jnp.mean(value, axis=-1, keepdims=True)
            centered = value - mean
            inv = lax.rsqrt(jnp.mean(centered * centered, axis=-1, keepdims=True) + EPS)
            n2[at, :] = (centered * inv * vecs[2:3, :] + vecs[3:4, :]).astype(BF16)
            stats[at, 0:64] = jnp.broadcast_to(mean, (16, 64))
            stats[at, 64:128] = jnp.broadcast_to(inv, (16, 64))

    x_in.wait()
    norm_slot(0)
    wait_row(0, 3)
    start_row(0, 3, 4, 8)
    start_row(1, 0, 4)
    for k in (1, 2, 3):
        norm_slot(k)
    wait_row(1, 1)
    start_row(1, 1, 2, 4, 8)
    wait_row(1, 2)
    start_row(1, 2, 4, 8)

    @pl.when(middle)
    def _():
        start_all(3)

    start_all(1)
    for k in (4, 5, 6, 7):
        wait_row(0, k)
        start_row(0, k, 8)
        norm_slot(k)

    @pl.when(middle)
    def _():
        for s in far:
            start_mlp(1, s)

    for k in range(8, 16):
        wait_row(0, k)
        norm_slot(k)
    wait_row(1, 3)
    start_row(1, 3, 4, 8)

    def mine(dy, q):
        return ((q // 2) * 8 + (q % 2) * 4 + dy * 2 + core) * rows

    for dy in range(2):
        for q in range(4):
            @pl.loop(0, rows // 16)
            def _(j):
                at = pl.ds(pl.multiple_of(mine(dy, q) + j * 16, 16), 16)
                to = pl.ds(pl.multiple_of(dy * SEQ + q * rows + j * 16, 16), 16)
                normed = (xs[at, :].astype(F32) - stats[at, 0:1]) * stats[at, 64:65]
                n1[to, :] = (normed * vecs[0:1, :] + vecs[1:2, :]).astype(BF16)

    @pl.when(lead)
    def _():
        for a, (src, dst) in enumerate(att_pairs(0)):
            pltpu.make_async_copy(src, dst, local_sem.at[20 + a]).wait()
        for copy in pass_att(0):
            copy.start()
        for s in near + [1] + far:
            for a, dst in enumerate(att_land(s)):
                remote(dst, dst, att_send.at[a, s], att_recv.at[a, s], s, 0).wait_recv()
            for copy in pass_att(s):
                copy.start()

    @pl.when(follow)
    def _():
        for s in range(dp_n):
            for copy in pass_att(s):
                copy.wait_recv()

    rope_in.wait()
    lanes128 = lax.broadcasted_iota(jnp.int32, (SEQ, 128), 1)

    def rope_tables(sign):
        at = [pl.ds(pl.multiple_of((t ^ ((q % 2) * 2 + q // 2)) * 128, 128), 128) for q in range(4)]
        cosine = jnp.concatenate([rope[0, a, :] for a in at], axis=0)
        sine = jnp.concatenate([rope[1, a, :] for a in at], axis=0) * sign
        lower = jnp.where(lanes128 < ROT // 2, -sine, 0.0)
        upper = jnp.where((lanes128 >= ROT // 2) & (lanes128 < ROT), sine, 0.0)
        return cosine, lower, upper

    def turn(value, tables):
        cosine, lower, upper = tables
        head = value[:, :128]
        head = (
            head * cosine
            + pltpu.roll(head, 128 - ROT // 2, 1) * lower
            + pltpu.roll(head, ROT // 2, 1) * upper
        )
        return jnp.concatenate([head, value[:, 128:]], axis=1)

    @pl.loop(0, 2)
    def _(dy):
        at = pl.ds(pl.multiple_of(dy * SEQ, SEQ), SEQ)
        tables = rope_tables(1.0)
        rows_in = n1[at, :]
        value = mm(rows_in, att_w[:, :HD]) + qkv_bias[0:1, :HD]
        query = turn(value, tables).astype(BF16)
        key = turn(mm(rows_in, att_w[:, HD : 2 * HD]), tables).astype(BF16)
        val = (mm(rows_in, att_w[:, 2 * HD :]) + qkv_bias[0:1, HD:]).astype(BF16)
        q_s[at, :] = query
        k_s[at, :] = key
        v_s[at, :] = val
        seg_q = jnp.where(dy == 0, queries[:, 1:2], queries[:, 2:3])
        seg_k = jnp.where(dy == 0, keys[1:2, :], keys[2:3, :])
        allowed = (keys[0:1, :] <= queries[:, 0:1]) & (seg_q == seg_k)
        scores = jnp.where(allowed, mm_tail(query, key) * scale, NEG_FILL)
        peak = jnp.max(scores, axis=-1, keepdims=True)
        total = jnp.where(allowed, jnp.exp(scores - peak), 0.0)
        share = (total / jnp.sum(total, axis=-1, keepdims=True)).astype(BF16)
        prob[at, :] = share
        got = mm(share, val)
        ctx[at, :] = got.astype(BF16)
        ctx_t[:, at] = jnp.transpose(got).astype(BF16)

    def cot_mine(dy, lanes):
        parts = [cots[pl.ds(pl.multiple_of(mine(dy, q), 128), rows), lanes] for q in range(4)]
        return jnp.concatenate(parts, axis=0)

    for k in (4, 5, 6, 7):
        wait_row(1, k)
        start_row(1, k, 8)
    cot_in.wait()
    for k in range(8, 16):
        wait_row(1, k)
    sums[...] = jnp.zeros_like(sums)

    @pl.loop(0, rows // 16)
    def _(j):
        at = pl.ds(pl.multiple_of(j * 16, 16), 16)
        sums[4:5, :] += jnp.sum(cots[at, :].astype(F32), axis=0, keepdims=True)

    for dy in range(2):
        cctx[dy * SEQ : (dy + 1) * SEQ, :] = mm_tail(cot_mine(dy, slice(None)), proj_w[...]).astype(BF16)

    @pl.loop(0, width // chunk)
    def _(c):
        lanes = pl.ds(pl.multiple_of(c * chunk, chunk), chunk)
        both = jnp.concatenate([cot_mine(0, lanes), cot_mine(1, lanes)], axis=0)
        gx[3 * HD : 4 * HD, lanes] = mm(ctx_t[...], both).astype(BF16)

    qkv_sum[...] = jnp.zeros_like(qkv_sum)

    def backward(dy):
        at = slice(dy * SEQ, (dy + 1) * SEQ)
        tables = rope_tables(-1.0)
        share = prob[at, :].astype(F32)
        got = cctx[at, :]
        delta = jnp.sum(got.astype(F32) * ctx[at, :].astype(F32), axis=-1, keepdims=True)
        score_cot = share * (mm_tail(got, v_s[at, :]) - delta)
        value_cot = mm(jnp.transpose(share).astype(BF16), got)
        query_cot = turn(mm(score_cot.astype(BF16), k_s[at, :]) * scale, tables)
        key_cot = turn(mm(jnp.transpose(score_cot).astype(BF16), q_s[at, :]) * scale, tables)
        qkv_sum[0:1, :HD] += jnp.sum(query_cot, axis=0, keepdims=True)
        qkv_sum[0:1, HD:] += jnp.sum(value_cot, axis=0, keepdims=True)
        for k, part in enumerate((query_cot, key_cot, value_cot)):
            low[at, k * HD : (k + 1) * HD] = part.astype(BF16)
            low_t[k * HD : (k + 1) * HD, at] = jnp.transpose(part).astype(BF16)

    backward(0)
    backward(1)

    up_in.wait()
    for copy in mlp_started[0]:
        copy.wait_send()

    @pl.loop(0, width // chunk)
    def _(c):
        lanes = pl.ds(pl.multiple_of(c * chunk, chunk), chunk)
        gx[0 : 3 * HD, lanes] = mm(low_t[...], n1[:, lanes]).astype(BF16)

    def pair_copy(s):
        return remote(
            lane_cut(gx, (d ^ s) * depth, depth), pair_hbm.at[:, s * depth : (s + 1) * depth],
            pair_send.at[s], pair_recv.at[s], 0, 1,
        )

    @pl.when(follow)
    def _():
        for s in near + [1] + far + [0]:
            pair_copy(s).start()

    for dy in range(2):
        @pl.loop(0, width // chunk)
        def _(c):
            lanes = pl.ds(pl.multiple_of(c * chunk, chunk), chunk)
            part = mm_tail(low[dy * SEQ : (dy + 1) * SEQ, :], att_w[lanes, :])
            gain = vecs[0:1, lanes]
            cross = jnp.zeros((1, chunk), F32)
            for q in range(4):
                at = pl.ds(pl.multiple_of(mine(dy, q), 128), rows)
                piece = part[q * rows : (q + 1) * rows]
                normed = (xs[at, lanes].astype(F32) - stats[at, 0:1]) * stats[at, 64:65]
                cross = cross + jnp.sum(piece * normed, axis=0, keepdims=True)
                n1[dy * SEQ + q * rows : dy * SEQ + (q + 1) * rows, lanes] = (piece * gain).astype(BF16)
            sums[0:1, lanes] += cross
            sums[1:2, lanes] += jnp.sum(part, axis=0, keepdims=True)

    def ga_copy(s):
        return remote(
            lane_cut(gx, (d ^ s) * depth, depth), ra_hbm.at[:, s * depth : (s + 1) * depth],
            ga_send.at[s], ga_recv.at[s], s, 0,
        )

    stages = (q_s, k_s, v_s)

    @pl.when(lead)
    def _():
        todo = near + [1] + far + [0]

        def fetch(k):
            s = todo[k]
            land = pair_hbm.at[:, s * depth : (s + 1) * depth]
            remote(land, land, pair_send.at[s], pair_recv.at[s], 0, 1).wait_recv()
            copy = pltpu.make_async_copy(land, stages[k % 3], g_local.at[k % 3])
            copy.start()
            return copy

        held = [fetch(0), fetch(1)]
        for k, s in enumerate(todo):
            if k + 2 < len(todo):
                held.append(fetch(k + 2))
            held[k].wait()
            stage = stages[k % 3]
            here = lane_cut(gx, (d ^ s) * depth, depth)

            @pl.loop(0, 4 * HD // 64)
            def _(i):
                at = pl.ds(pl.multiple_of(i * 64, 64), 64)
                here[at, :] = (here[at, :].astype(F32) + stage[at, :].astype(F32)).astype(BF16)

            if s:
                ga_copy(s).start()
            else:
                pltpu.make_async_copy(here, ra_hbm.at[:, 0:depth], local_sem.at[22]).start()

    for s in near + [1] + far:
        mlp_wait(0, s)

    @pl.loop(0, tokens // chunk)
    def _(j):
        at = pl.ds(pl.multiple_of(j * chunk, chunk), chunk)
        value = mm_tail(up_t[...], n2[at, :]) + up_bias
        pre[:, at] = value
        hid_t[:, at] = (value * gelu_half(value)).astype(BF16)

    def g_send_copy(a, s):
        at = pl.ds(pl.multiple_of(s * depth, 128), depth)
        return remote(
            (gu_hbm, gd_hbm)[a].at[:, at], (ru_hbm, rd_hbm)[a].at[:, at],
            g_send.at[a, s], g_recv.at[a, s], s, 0,
        )

    def g_local_copy(a, s, b, dst):
        at = pl.ds(pl.multiple_of(s * depth, 128), depth)
        return pltpu.make_async_copy(ring.at[b], dst.at[:, at], g_local.at[b])

    def grads(a, go):
        left, right = ((act_t, n2), (hid_t, cots))[a]
        stage, own = ((gu_hbm, ru_hbm), (gd_hbm, rd_hbm))[a]

        def block(s, b):
            at = pl.ds(pl.multiple_of((d ^ s) * depth, 128), depth)
            ring[b] = mm(left[...], right[:, at]).astype(BF16)

        def at_step(k):
            return (k + 1) % (dp_n - 1) + 1

        @pl.loop(0, dp_n - 1)
        def _(k):
            s = at_step(k)
            b = k % 3

            @pl.when(k >= 2)
            def _():
                before = at_step(k - 2)
                g_local_copy(a, before, (k + 1) % 3, stage).wait()
                if go:
                    g_send_copy(a, before).start()

            block(s, b)
            g_local_copy(a, s, b, stage).start()

        last = dp_n - 2
        for k in (last - 1, last):
            s = at_step(k)
            g_local_copy(a, s, k % 3, stage).wait()
            if go:
                g_send_copy(a, s).start()
        b = (last + 1) % 3
        block(0, b)
        copy = g_local_copy(a, 0, b, own)
        copy.start()
        copy.wait()

    grads(1, True)
    down_in.wait()
    for s in near + [1] + far:
        mlp_wait(1, s)
    up_sum[...] = jnp.zeros_like(up_sum)

    @pl.loop(0, tokens // chunk)
    def _(j):
        at = pl.ds(pl.multiple_of(j * chunk, chunk), chunk)
        value = mm_tail(down_w[...], cots[at, :]) * gelu_slope(pre[:, at])
        up_sum[:, 0:1] += jnp.sum(value, axis=1, keepdims=True)
        act_t[:, at] = value.astype(BF16)

    grads(0, False)

    @pl.loop(0, tokens // chunk)
    def _(j):
        at = pl.ds(pl.multiple_of(j * chunk, chunk), chunk)
        act = jnp.transpose(act_t[:, at].astype(F32)).astype(BF16)

        @pl.loop(0, width // chunk)
        def _(c):
            lanes = pl.ds(pl.multiple_of(c * chunk, chunk), chunk)
            part = mm(act, up_t[:, lanes])
            gain = vecs[2:3, lanes]
            cross = jnp.zeros((1, chunk), F32)
            for m in range(4):
                at = pl.ds(pl.multiple_of(j * chunk + m * rows, 128), rows)
                piece = part[m * rows : (m + 1) * rows]
                normed = (xs[at, lanes].astype(F32) - stats[at, 0:1]) * stats[at, 64:65]
                cross = cross + jnp.sum(piece * normed, axis=0, keepdims=True)
                spot = pl.ds(pl.multiple_of((m // 2) * SEQ + j * rows, 128), rows)
                extra = jnp.where(core == m % 2, n1[spot, lanes].astype(F32), 0.0)
                n2[at, lanes] = (piece * gain + extra).astype(BF16)
            sums[2:3, lanes] += cross
            sums[3:4, lanes] += jnp.sum(part, axis=0, keepdims=True)

    for copy in row_started[0]:
        copy.wait_send()
    pl.semaphore_signal(credit.at[0], inc=1, device_id=(d, t ^ 1), device_id_type=MESH)
    pl.semaphore_signal(credit.at[1], inc=1, device_id=(d, t ^ 2), device_id_type=MESH)

    blank = jnp.zeros((4, 128), F32)
    up_rows = [jnp.transpose(up_sum[k * 128 : (k + 1) * 128, :])[0:1] for k in range(4)]
    up_rows = jnp.concatenate(up_rows, axis=0)
    qkv_rows = jnp.concatenate([qkv_sum[0:1, k * 128 : (k + 1) * 128] for k in range(4)], axis=0)

    def place(value):
        return jnp.where(
            second, jnp.concatenate([blank, value], axis=0), jnp.concatenate([value, blank], axis=0)
        )

    up_place[...] = place(up_rows)
    head_place[...] = place(qkv_rows)

    def window(to):
        return lane_cut(sums, to * 128, 128)

    def back_copy(kind, src, dst, dp_xor, tp_xor):
        return remote(src, dst, back_send.at[kind], back_recv.at[kind], dp_xor, tp_xor)

    def head_copy(s, dc):
        return remote(
            head_place, head_back.at[s * 2 + dc], headb_send.at[s * 2 + dc], headb_recv.at[s * 2 + dc], s, dc
        )

    for r in range(1, chips):
        back_copy(0, window(chip ^ r), vec_back.at[r], r // 2, (r % 2) * 2).start()
    for s in range(1, dp_n):
        back_copy(1, up_place, bias_back.at[s], s, 0).start()

    @pl.when(lead)
    def _():
        for s in range(1, dp_n):
            head_copy(s, 0).start()

    @pl.when(follow)
    def _():
        for s in range(dp_n):
            head_copy(s, 1).start()

    bufs = (cots, n2)

    def landing(a, bit, j, there):
        if bit == 8:
            if a == 0:
                side = core if there else 1 - core
                return row_cut(xs, (2 * j + side) * rows, rows)
            return row_cut(n1, j * rows, rows)
        if bit == 4:
            return row_cut((act_t, up_t)[a], j * rows, rows)
        base = (down_w, hid_t)[a]
        return row_cut(base, (j if bit == 2 else 2) * rows, rows)

    def rs_copy(a, bit, j):
        return remote(
            slot(bufs[a], bit + j), landing(a, bit, j, True),
            rs_send.at[a, bit + j], rs_recv.at[a, bit + j], *hop[bit],
        )

    def rs_start(a, bit, j):
        start(rs_copy(a, bit, j))

    def rs_add(a, bit, j):
        land = landing(a, bit, j, False)
        remote(land, land, rs_send.at[a, bit + j], rs_recv.at[a, bit + j], *hop[bit]).wait_recv()
        here = slot(bufs[a], j)

        @pl.loop(0, rows // 16)
        def _(i):
            at = pl.ds(pl.multiple_of(i * 16, 16), 16)
            here[at, :] = (here[at, :].astype(F32) + land[at, :].astype(F32)).astype(BF16)

    for s in near + far[:3]:
        g_send_copy(0, s).start()

    pl.semaphore_wait(credit.at[0], 1)
    pl.semaphore_wait(credit.at[1], 1)
    for j in (7, 5, 6, 4, 3, 1, 2, 0):
        rs_start(1, 8, j)

    for copy in row_started[1]:
        copy.wait_send()
    for j in range(4):
        for k in {2: (7, 5), 3: (6, 4)}.get(j, ()):
            rs_add(1, 8, k)
            rs_start(1, 4, k - 4)
        hid = jnp.transpose(hid_t[:, j * chunk : (j + 1) * chunk].astype(F32)).astype(BF16)
        here = [ctx[h * SEQ + j * rows : h * SEQ + (j + 1) * rows, :] for h in range(2)]
        here = jnp.concatenate(here, axis=0)

        @pl.loop(0, width // chunk)
        def _(c):
            lanes = pl.ds(pl.multiple_of(c * chunk, chunk), chunk)
            base = mm(hid, down_w[:, lanes])
            extra = mm(here, proj_w[:, lanes])
            for m in range(4):
                more = jnp.where(core == m % 2, extra[(m // 2) * rows : (m // 2 + 1) * rows], 0.0)
                piece = base[m * rows : (m + 1) * rows] + more
                cots[j * chunk + m * rows : j * chunk + (m + 1) * rows, lanes] = piece.astype(BF16)

    for bit in (2, 1):
        dp_xor, tp_xor = hop[bit]
        pl.semaphore_signal(
            credit.at[1 + (3 - bit)], inc=1, device_id=(d ^ dp_xor, t ^ tp_xor), device_id_type=MESH
        )
    own_x = row_cut(hid_t, 3 * rows, rows)
    own_cot = row_cut(down_w, 3 * rows, rows)
    x_again = stay(x_ref, own_x)
    cot_again = stay(cot_ref, own_cot)

    for j in (7, 5, 6, 4, 3, 1, 2, 0):
        rs_start(0, 8, j)
    for j in (3, 1, 2, 0):
        rs_add(1, 8, j)
    for j in (7, 5, 6, 4):
        rs_add(0, 8, j)
        rs_start(0, 4, j - 4)
    for j in (3, 1, 2, 0):
        rs_add(0, 8, j)
    pl.semaphore_wait(credit.at[2], 1)
    pl.semaphore_wait(credit.at[3], 1)

    def rs_tail(a, after):
        rs_add(a, 4, 3)
        rs_start(a, 2, 1)
        rs_add(a, 4, 1)
        rs_add(a, 4, 2)
        rs_start(a, 2, 0)
        rs_add(a, 2, 1)
        rs_start(a, 1, 0)
        after()
        rs_add(a, 4, 0)
        rs_add(a, 2, 0)
        rs_add(a, 1, 0)

    outs = []

    def leave(src, dst):
        copy = pltpu.make_async_copy(src, dst, out_sem.at[len(outs)])
        copy.start()
        outs.append(copy)
        return copy

    def late():
        for s in far[3:] + [1]:
            g_send_copy(0, s).start()

    rs_tail(1, late)
    cot_again.wait()
    x_again.wait()

    @pl.loop(0, rows // 16)
    def _(j):
        at = pl.ds(pl.multiple_of(j * 16, 16), 16)
        scaled = n2[at, :].astype(F32)
        inv = stats[at, 64:65]
        normed = (own_x[at, :].astype(F32) - stats[at, 0:1]) * inv
        inner_mean = jnp.mean(scaled, axis=-1, keepdims=True)
        cross = jnp.mean(scaled * normed, axis=-1, keepdims=True)
        pre[at, :] = own_cot[at, :].astype(F32) + inv * (scaled - inner_mean - normed * cross)

    grad_out = leave(pre.at[0:rows, :], input_out)

    rs_tail(0, lambda: None)

    @pl.loop(0, rows // 16)
    def _(j):
        at = pl.ds(pl.multiple_of(j * 16, 16), 16)
        total = own_x[at, :].astype(F32) + cots[at, :].astype(F32) + vecs[4:5, :]
        cots[at, :] = total.astype(BF16)

    last = [leave(slot(cots, 0), block_out)]
    def back_waits(kind):
        buf = (vec_back, bias_back)[kind]
        rest = buf.at[pl.ds(1, buf.shape[0] - 1)]
        return back_copy(kind, rest, rest, 0, 1)

    for kind in range(2):
        back_waits(kind).wait_recv()
    for kind in range(2):
        small_waits(kind).wait_send()
    meet.wait_send()
    head_in_each(lambda copy: copy.wait_send())
    total = window(chip)[...]
    for r in range(1, chips):
        total = total + vec_back[r]
    pay[0] = total
    meet_back = back_copy(2, pay.at[0], pair_back, 0, 1)
    meet_back.start()
    for k in (1, 2, 3):
        pay[k] = jnp.zeros((8, 128), F32)
    pay[1 + inner // 2] += up_place[...]
    for s in range(1, dp_n):
        pay[1 + (inner ^ (s % INNER)) // 2] += bias_back[s]
    for s in range(dp_n):
        @pl.when(att_active(s))
        def _():
            if s == 0:
                pay[3] += head_place[...]
            else:
                head_copy(s, 0).wait_recv()
                pay[3] += head_back[2 * s]
            head_copy(s, 1).wait_recv()
            pay[3] += head_back[2 * s + 1]


    @pl.when(lead)
    def _():
        pltpu.make_async_copy(
            lane_cut(gx, d * depth, depth), ra_hbm.at[:, 0:depth], local_sem.at[22]
        ).wait()

    for s in range(1, dp_n):
        @pl.when(att_active(s))
        def _():
            ga_copy(s).wait_recv()

    for s in range(1, dp_n):
        g_send_copy(1, s).wait_recv()
    for s in range(1, dp_n):
        g_send_copy(0, s).wait_recv()
    meet_back.wait_recv()
    meet_back.wait_send()
    pay[0] += pair_back[...]
    last.append(leave(pay, tail_out))
    for s in range(1, dp_n):
        for a in range(2):
            g_send_copy(a, s).wait_send()

        @pl.when(att_active(s))
        def _():
            for a, (src, dst) in enumerate(att_pairs(s)):
                remote(src, dst, att_send.at[a, s], att_recv.at[a, s], s, 0).wait_send()

        @pl.when(lead)
        def _():
            ga_copy(s).wait_send()

    @pl.when(lead)
    def _():
        for s in range(dp_n):
            for copy in pass_att(s):
                copy.wait_send()

    @pl.when(follow)
    def _():
        for s in range(dp_n):
            pair_copy(s).wait_send()

    @pl.when(lead)
    def _():
        for s in range(1, dp_n):
            head_copy(s, 0).wait_send()

    @pl.when(follow)
    def _():
        for s in range(dp_n):
            head_copy(s, 1).wait_send()

    for kind in range(2):
        back_waits(kind).wait_send()
    for copy in started + mlp_started[1]:
        copy.wait_send()
    for copy in [grad_out] + last:
        copy.wait()


def finish_kernel(
    dp_n, tp_n,
    block_ref, input_ref, tail_ref, ru_ref, rd_ref, ra_ref,
    block_out, input_out, up_out, down_out, qkv_out, proj_out,
    v0, v1, v2, v3, v4, v5, bq_out, bf_out,
    block, grad, ru, rd, ra, up, down, qkv, proj, tail, wide_f, in_sem, out_sem,
):
    d = lax.axis_index("dp")
    t = lax.axis_index("tp")
    inner = d % INNER
    core = t % 2
    hidden, width = ru.shape
    depth = width // dp_n
    groups = dp_n // INNER
    copies = []

    def fetch(src, dst):
        copy = pltpu.make_async_copy(src, dst, in_sem.at[len(copies)])
        copy.start()
        copies.append(copy)
        return copy

    grad_in = fetch(input_ref, grad)
    block_in = fetch(block_ref, block)
    rd_in = [fetch(row_cut(rd_ref, k * 128, 128), row_cut(rd, k * 128, 128)) for k in range(hidden // 128)]
    ru_in = [fetch(row_cut(ru_ref, k * 128, 128), row_cut(ru, k * 128, 128)) for k in range(hidden // 128)]
    ra_in = []
    for hl in range(2):
        first = ((inner // 2) ^ core) * 2 + ((inner % 2) ^ hl)
        for o in range(groups):
            k = hl * groups + o
            ra_in.append(fetch(lane_cut(ra_ref, (first + o * INNER) * depth, depth), lane_cut(ra, k * depth, depth)))
    tail_in = fetch(tail_ref, tail)
    outs = []

    def leave(src, dst):
        copy = pltpu.make_async_copy(src, dst, out_sem.at[len(outs)])
        copy.start()
        outs.append(copy)

    def total_of(ref, at, k):
        total = ref[at, k * depth : (k + 1) * depth].astype(F32)
        for s in range(k + INNER, dp_n, INNER):
            total = total + ref[at, s * depth : (s + 1) * depth].astype(F32)
        return total

    grad_in.wait()
    leave(grad, input_out)
    block_in.wait()
    leave(block, block_out)
    for c in range(hidden // 128):
        rd_in[c].wait()
        at = slice(c * 128, (c + 1) * 128)
        for k in range(INNER):
            down[k, at, :] = total_of(rd, at, k)
            leave(down.at[k, at, :], row_cut(down_out, (inner ^ k) * hidden + c * 128, 128))
    for c in range(hidden // 128):
        ru_in[c].wait()
        at = slice(c * 128, (c + 1) * 128)
        for k in range(INNER):
            up[k, :, at] = jnp.transpose(total_of(ru, at, k))
            leave(up.at[k, :, at], lane_cut(up_out, (inner ^ k) * hidden + c * 128, 128))
    for hl in range(2):
        total = jnp.zeros((4 * HD, depth), F32)
        for o in range(groups):
            k = hl * groups + o
            ra_in[k].wait()
            total = total + ra[:, k * depth : (k + 1) * depth].astype(F32)
        qkv[:, hl * 3 * HD : (hl + 1) * 3 * HD] = jnp.transpose(total[: 3 * HD])
        proj[hl * HD : (hl + 1) * HD, :] = total[3 * HD :]
    leave(qkv, qkv_out)
    leave(proj, proj_out)

    tail_in.wait()
    row = tail[0]
    row = jnp.where((t % 2) == 1, pltpu.roll(row, 64, 1), row)
    for k, ref in enumerate((v0, v1, v2, v3, v4, v5)):
        ref[...] = row[min(k, 4) : min(k, 4) + 1, :64]
    line = lax.broadcasted_iota(jnp.int32, (8, 128), 0)
    heads = tail[3]
    heads = jnp.where(d % 2 == 1, pltpu.roll(heads, 64, 1), heads)
    for k in range(2):
        picked = jnp.sum(jnp.where(line == k * 4 + d // 2, heads, 0.0), axis=0, keepdims=True)
        bq_out[k : k + 1, :] = picked[:, :64]
    cols = bf_out.shape[0]
    both = jnp.concatenate([tail[1], tail[2]], axis=0)
    both = pltpu.roll(both, (128 - d * cols) % 128, 1)
    wide_f[pl.ds(0, 16, stride=2), :] = both
    wide_f[pl.ds(1, 16, stride=2), :] = pltpu.roll(both, 64, 1)
    spots = wide_f.shape[0]
    full = jnp.concatenate([wide_f[...], jnp.zeros((128 - spots, 128), F32)], axis=0)
    bf_out[...] = jnp.transpose(full)[:cols, :spots]
    for copy in outs:
        copy.wait()


def solution(mesh):
    dp_n, tp_n = mesh.shape["dp"], mesh.shape["tp"]
    outer = dp_n // INNER
    devices = dp_n * tp_n

    def send(value, dp_xor, tp_xor, keep=None):
        pairs = []
        for d in range(dp_n):
            for t in range(tp_n):
                if keep is None or keep(d, t):
                    pairs.append((d * tp_n + t, (d ^ dp_xor) * tp_n + (t ^ tp_xor)))
        return lax.ppermute(value, AXES, pairs)

    def scatter_small(value, flat):
        held = value
        step = devices // 2
        while step >= 1:
            dp_xor, tp_xor = step // tp_n, step % tp_n
            high = (flat // step) % 2 == 1
            first, second = held[:step], held[step:]
            other = send(jnp.where(high, first, second), dp_xor, tp_xor)
            held = jnp.where(high, second, first) + other
            step //= 2
        return held[0]

    def scatter_rows(value):
        for dp_xor, tp_xor in ((0, 1), (0, 2), (1, 0), (2, 0)):
            half = value.shape[0] // 2
            other = send(value[half:], dp_xor, tp_xor)
            value = value[:half].astype(F32) + other.astype(F32)
            if half > value.shape[0] or (dp_xor, tp_xor) != (2, 0):
                value = value.astype(BF16)
        return value

    def on_device(
        block_input, segment_ids, w_qkv, b_qkv, w_out, b_out, w_fc1, b_fc1, w_fc2, b_fc2,
        ln1_gain, ln1_bias, ln2_gain, ln2_bias, cotangent,
    ):
        d = lax.axis_index("dp")
        t = lax.axis_index("tp")
        flat = d * tp_n + t
        inner = d % INNER
        core = t % 2
        lead = (inner // 2) == core
        rows, width = block_input.shape
        depth = w_qkv.shape[0]
        hidden_here = w_fc1.shape[1] // INNER
        head_here = w_out.shape[0] // HD
        heads = head_here * tp_n
        quarter = SEQ // tp_n
        qkv_bits = b_qkv.shape[1]

        vec = jnp.stack([ln1_gain, ln1_bias, ln2_gain, ln2_bias, b_out + b_fc2]).reshape(-1)
        seg_part = lax.dynamic_slice(segment_ids.reshape(-1), (t * quarter,), (quarter,))
        sizes = [vec.size, b_qkv.size, b_fc1.size, quarter]
        payload = jnp.concatenate(
            [vec, b_qkv.reshape(-1), b_fc1.reshape(-1), seg_part.astype(F32)]
        )
        depth_wide = depth % 128 == 0
        flat_shape = lambda lead_n: (lead_n, width) if depth_wide else (dp_n, lead_n, depth)
        spread = lambda v: v if depth_wide else v.transpose(1, 0, 2).reshape(v.shape[1], width)
        payload = jnp.pad(payload, (0, PAY - payload.size)).reshape(8, PAY // 8)
        like = lambda *shape: jax.ShapeDtypeStruct(shape, BF16)
        dma = pltpu.SemaphoreType.DMA
        hop_count = (devices - 1).bit_length()
        any_spec = pl.BlockSpec(memory_space=pl.ANY)
        x_all, cot_all, up_w, down_w, qkv_w, out_w, small = pl.pallas_call(
            functools.partial(gather_kernel, dp_n, tp_n, depth_wide),
            out_shape=(
                like(16, rows, width),
                like(16, rows, width),
                like(width, hidden_here),
                like(*flat_shape(hidden_here)),
                like(width, 3 * HD),
                like(*flat_shape(HD)),
                jax.ShapeDtypeStruct((devices, 8, PAY // 8), F32),
            ),
            in_specs=[any_spec] * 7,
            out_specs=(any_spec,) * 7,
            scratch_shapes=[
                dma((2, 16)), dma((2, 16)), dma((2, dp_n)), dma((2, dp_n)),
                dma((2, dp_n)), dma((2, dp_n)), dma((2, dp_n)), dma((2, dp_n)),
                dma((hop_count,)), dma((hop_count,)), dma((6,)),
            ],
            compiler_params=pltpu.CompilerParams(collective_id=0, has_side_effects=True),
            name="gather_phase",
        )(block_input, cotangent, w_fc1, w_fc2, w_qkv, w_out, payload)
        down_w, out_w = spread(down_w), spread(out_w)
        small = jnp.take(small.reshape(devices, PAY), flat ^ jnp.arange(devices), axis=0)
        cuts = [0]
        for size in sizes:
            cuts.append(cuts[-1] + size)
        vecs = small[:, : cuts[1]].reshape(devices, 5, -1).transpose(1, 0, 2).reshape(5, width)
        gain_one, shift_one, gain_two, shift_two, out_bias = (vecs[k][None] for k in range(5))
        qkv_bias_all = (
            small[:, cuts[1] : cuts[2]]
            .reshape(dp_n, tp_n, head_here, qkv_bits)
            .transpose(1, 2, 0, 3)
            .reshape(heads, 2 * HD)
        )
        head = (t // 2) * INNER + inner
        qkv_bias = lax.dynamic_slice(qkv_bias_all, (head, 0), (1, 2 * HD))
        up_rows, up_cols = b_fc1.shape
        up_bias_all = (
            small[:, cuts[2] : cuts[3]]
            .reshape(dp_n, tp_n, up_rows, up_cols)
            .transpose(1, 2, 0, 3)
            .reshape(tp_n * INNER, hidden_here)
        )
        up_bias = lax.dynamic_slice(up_bias_all, (t * INNER + inner, 0), (1, hidden_here))
        seg_all = small[:, cuts[3] : cuts[4]].reshape(dp_n, tp_n, quarter)

        x_rows = x_all.reshape(16 * rows, width).astype(F32)
        cot_rows = cot_all.reshape(16 * rows, width)
        row_mean = jnp.mean(x_rows, axis=-1, keepdims=True)
        centered = x_rows - row_mean
        row_var = jnp.mean(centered * centered, axis=-1, keepdims=True)
        inv_std = lax.rsqrt(row_var + EPS)
        normed = centered * inv_std
        norm_two = (normed * gain_two + shift_two).astype(BF16)

        def mine(value):
            split = value.reshape((2, 2, 2, 2, rows) + value.shape[1:])
            cut = lax.dynamic_index_in_dim(split, core, 3, keepdims=False)
            return jnp.moveaxis(cut, 2, 0).reshape((2 * SEQ,) + value.shape[1:])

        def unmine(value):
            split = value.reshape((2, 2, 2, rows) + value.shape[1:])
            cut = jnp.moveaxis(split, 0, 2)[:, :, :, None]
            where = (jnp.arange(2) == core).reshape((1, 1, 1, 2) + (1,) * value.ndim)
            full = jnp.where(where, cut, jnp.zeros_like(cut))
            return full.reshape((16 * rows,) + value.shape[1:])

        norm_one = (mine(normed) * gain_one + shift_one).astype(BF16)
        cot_mine = mine(cot_rows)

        pre_act = mm(norm_two, up_w) + up_bias
        half_gelu = gelu_half(pre_act)
        hidden = (pre_act * half_gelu).astype(BF16)
        down_grad = mm_lead(hidden, cot_rows)
        act_cot = mm_tail(cot_rows, down_w) * gelu_slope(pre_act)
        up_bias_part = jnp.sum(act_cot, axis=0)
        act_low = act_cot.astype(BF16)
        up_grad = mm_lead(norm_two, act_low)
        up_grad, down_grad = up_grad.astype(BF16), down_grad.astype(BF16)

        def cut_block(value, s):
            return lax.dynamic_slice(value, ((d ^ s) * depth, 0), (depth, value.shape[1]))

        def cut_across(value, s):
            return lax.dynamic_slice(value, (0, (d ^ s) * depth), (value.shape[0], depth))

        with jax.named_scope("mlp_out"):
            up_back = [cut_block(up_grad, 0)] + [
                send(cut_block(up_grad, s), s, 0) for s in range(1, dp_n)
            ]
            down_back = [cut_across(down_grad, 0)] + [
                send(cut_across(down_grad, s), s, 0) for s in range(1, dp_n)
            ]

        order = jnp.stack([t ^ ((k % 2) * 2 + k // 2) for k in range(4)])
        position = (order[:, None] * quarter + jnp.arange(quarter)[None]).reshape(-1)
        inverse = jnp.exp(jnp.arange(ROT // 2, dtype=F32) * (-2.0 * math.log(10000.0) / ROT))
        angle = position.astype(F32)[:, None] * inverse[None]
        cosine, sine = jnp.cos(angle)[None], jnp.sin(angle)[None]
        segs = []
        for dy in range(2):
            seq = (d // INNER) * INNER + (inner ^ (core * 2 + dy))
            rows_of = lax.dynamic_index_in_dim(seg_all, seq, 0, keepdims=False)
            segs.append(jnp.take(rows_of, order, axis=0).reshape(-1))
        segs = jnp.stack(segs)
        allowed = (position[None, :] <= position[:, None])[None] & (
            segs[:, :, None] == segs[:, None, :]
        )
        qkv = mm(norm_one, qkv_w)
        query = rotate((qkv[:, :HD] + qkv_bias[:, :HD]).reshape(2, SEQ, HD), cosine, sine).astype(BF16)
        key = rotate(qkv[:, HD : 2 * HD].reshape(2, SEQ, HD), cosine, sine).astype(BF16)
        val = (qkv[:, 2 * HD :] + qkv_bias[:, HD:]).astype(BF16).reshape(2, SEQ, HD)
        scale = HD ** (-0.5)

        def ein(eq, left, right):
            return jnp.einsum(eq, left, right, preferred_element_type=F32)

        masked = jnp.where(allowed, ein("sqd,skd->sqk", query, key) * scale, NEG_FILL)
        peak = jnp.max(masked, axis=-1, keepdims=True)
        log_total = peak + jnp.log(
            jnp.sum(jnp.where(allowed, jnp.exp(masked - peak), 0.0), axis=-1, keepdims=True)
        )
        prob_full = jnp.where(allowed, jnp.exp(masked - log_total), 0.0)
        prob_low = prob_full.astype(BF16)
        context = ein("sqk,skd->sqd", prob_low, val).astype(BF16)
        context_cot = mm_tail(cot_mine, out_w).astype(BF16).reshape(2, SEQ, HD)
        prob_cot = ein("sqd,skd->sqk", context_cot, val)
        row_delta = jnp.sum(context_cot.astype(F32) * context.astype(F32), axis=-1, keepdims=True)
        score_cot = (prob_full * (prob_cot - row_delta)).astype(BF16)
        query_cot = rotate(ein("sqk,skd->sqd", score_cot, key) * scale, cosine, -sine)
        key_cot = rotate(ein("sqk,sqd->skd", score_cot, query) * scale, cosine, -sine)
        val_cot = ein("sqk,sqd->skd", prob_low, context_cot)
        qkv_cot = jnp.concatenate([query_cot, key_cot, val_cot], axis=-1).reshape(2 * SEQ, 3 * HD)
        qkv_bias_part = jnp.concatenate(
            [jnp.sum(query_cot, axis=(0, 1)), jnp.sum(val_cot, axis=(0, 1))]
        )
        qkv_low = qkv_cot.astype(BF16)
        context_flat = context.reshape(2 * SEQ, HD)
        att_grad = jnp.concatenate(
            [mm_lead(norm_one, qkv_low).astype(BF16), mm_lead(cot_mine, context_flat).astype(BF16)],
            axis=1,
        )
        att_pair = send(att_grad, 0, 1, lambda dd, tt: (dd % INNER) // 2 != tt % 2)
        att_grad = (att_grad.astype(F32) + att_pair.astype(F32)).astype(BF16)
        with jax.named_scope("att_out"):
            own_att = cut_block(att_grad, 0)
            att_back = [jnp.where(lead, own_att, jnp.zeros_like(own_att))] + [
                send(cut_block(att_grad, s), s, 0, lambda dd, tt: (dd % INNER) // 2 == tt % 2)
                for s in range(1, dp_n)
            ]

        left = jnp.concatenate([hidden, unmine(context_flat)], axis=1)
        right = jnp.concatenate([down_w, out_w], axis=0)
        with jax.named_scope("branch"):
            branch = scatter_rows(mm(left, right).astype(BF16))
        block_output = (block_input.astype(F32) + branch + out_bias).astype(BF16)

        one_part = mm_tail(qkv_low, qkv_w)
        two_part = mm_tail(act_low, up_w)
        vec_terms = jnp.stack(
            [
                jnp.sum(one_part * mine(normed), axis=0),
                jnp.sum(one_part, axis=0),
                jnp.sum(two_part * normed, axis=0),
                jnp.sum(two_part, axis=0),
                jnp.sum(cotangent.astype(F32), axis=0),
            ]
        )
        scaled_part = (two_part * gain_two + unmine(one_part * gain_one)).astype(BF16)
        with jax.named_scope("normback"):
            scaled = scatter_rows(scaled_part)
        normed_own = normed[:rows]
        input_grad = cotangent.astype(F32) + inv_std[:rows] * (
            scaled
            - jnp.mean(scaled, axis=-1, keepdims=True)
            - normed_own * jnp.mean(scaled * normed_own, axis=-1, keepdims=True)
        )

        head_hot = (jnp.arange(heads) == head).astype(F32)[:, None]
        qkv_small = (
            (head_hot * qkv_bias_part[None])
            .reshape(tp_n, head_here, dp_n, qkv_bits)
            .transpose(2, 0, 1, 3)
            .reshape(devices, -1)
        )
        up_hot = (jnp.arange(tp_n * INNER) == t * INNER + inner).astype(F32)[:, None]
        up_small = (
            (up_hot * up_bias_part[None])
            .reshape(tp_n, up_rows, dp_n, up_cols)
            .transpose(2, 0, 1, 3)
            .reshape(devices, -1)
        )
        vec_small = vec_terms.reshape(5, devices, -1).transpose(1, 0, 2).reshape(devices, -1)
        with jax.named_scope("small_out"):
            own = scatter_small(jnp.concatenate([vec_small, qkv_small, up_small], axis=1), flat)
        vec_own = own[: cuts[1]].reshape(5, -1)
        qkv_bias_grad = own[cuts[1] : cuts[2]].reshape(b_qkv.shape)
        up_bias_grad = own[cuts[2] : cuts[3]].reshape(b_fc1.shape)

        up_total = jnp.zeros(w_fc1.shape, F32)
        down_total = jnp.zeros(w_fc2.shape, F32)
        for k in range(INNER):
            at = (inner ^ k) * hidden_here
            up_sum = sum(up_back[s].astype(F32) for s in range(k, dp_n, INNER))
            down_sum = sum(down_back[s].astype(F32) for s in range(k, dp_n, INNER))
            up_total = lax.dynamic_update_slice(up_total, up_sum, (0, at))
            down_total = lax.dynamic_update_slice(down_total, down_sum, (at, 0))
        att_sum = [sum(att_back[s].astype(F32) for s in range(k, dp_n, 2)) for k in range(2)]
        odd = inner % 2 == 1
        att_first = jnp.where(odd, att_sum[1], att_sum[0])
        att_second = jnp.where(odd, att_sum[0], att_sum[1])
        qkv_total = jnp.concatenate([att_first[:, : 3 * HD], att_second[:, : 3 * HD]], axis=1)
        out_total = jnp.concatenate([att_first[:, 3 * HD :].T, att_second[:, 3 * HD :].T], axis=0)
        return (
            block_output, input_grad, qkv_total, qkv_bias_grad, out_total, vec_own[4],
            up_total, up_bias_grad, down_total, vec_own[4],
            vec_own[0], vec_own[1], vec_own[2], vec_own[3],
        )

    def on_device_fused(
        block_input, segment_ids, w_qkv, b_qkv, w_out, b_out, w_fc1, b_fc1, w_fc2, b_fc2,
        ln1_gain, ln1_bias, ln2_gain, ln2_bias, cotangent,
    ):
        d = lax.axis_index("dp")
        t = lax.axis_index("tp")
        flat = d * tp_n + t
        inner = d % INNER
        core = t % 2
        lead = (inner // 2) == core
        rows, width = block_input.shape
        depth = w_qkv.shape[0]
        hidden_here = w_fc1.shape[1] // INNER
        head_here = w_out.shape[0] // HD
        heads = head_here * tp_n
        quarter = SEQ // tp_n
        qkv_bits = b_qkv.shape[1]

        up_rows = b_fc1.shape[0]
        per = ln1_gain.shape[0]
        seg_row = segment_ids.reshape(1, -1)
        small_in = [v.reshape(1, -1) for v in (ln1_gain, ln1_bias, ln2_gain, ln2_bias, b_out, b_fc2)]
        small_in += [b_qkv, b_fc1.T, seg_row]
        angle = np.arange(SEQ)[:, None] * np.exp(np.arange(ROT // 2) * (-2.0 * math.log(10000.0) / ROT))
        pad = np.zeros((SEQ, 128 - ROT))
        cosine = np.concatenate([np.cos(angle), np.cos(angle), pad + 1.0], axis=1)
        sine = np.concatenate([np.sin(angle), np.sin(angle), pad], axis=1)
        rope = jnp.asarray(np.stack([cosine, sine]), F32)
        like = lambda *shape: jax.ShapeDtypeStruct(shape, BF16)
        wide_f = lambda *shape: jax.ShapeDtypeStruct(shape, F32)
        dma = pltpu.SemaphoreType.DMA
        vb = lambda *shape: pltpu.VMEM(shape, BF16)
        vf = lambda *shape: pltpu.VMEM(shape, F32)
        any_spec = pl.BlockSpec(memory_space=pl.ANY)
        group = 16 * rows
        per_peer = dma((2, dp_n))
        pair = 2 * SEQ
        results = pl.pallas_call(
            functools.partial(fused_kernel, dp_n, tp_n),
            out_shape=(
                like(rows, width), wide_f(rows, width), wide_f(4, 8, 128),
                like(hidden_here, width), like(hidden_here, width),
                like(hidden_here, width), like(hidden_here, width), like(4 * HD, width),
                like(4 * HD, width),
            ),
            in_specs=[any_spec] * 16,
            out_specs=(any_spec,) * 9,
            scratch_shapes=[
                vb(group, width), vb(group, width), vb(group, width),
                vb(hidden_here, width), vb(hidden_here, width), vf(hidden_here, group),
                vb(hidden_here, group), vb(hidden_here, group), vb(3, hidden_here, depth),
                vf(group, 128), vf(8, width), vf(8, width), vf(hidden_here, 128),
                vb(width, 3 * HD), vb(HD, width), vb(pair, width),
                vb(pair, HD), vb(pair, HD), vb(pair, HD), vb(pair, SEQ),
                vb(pair, HD), vb(HD, pair), vb(pair, HD), vb(pair, 3 * HD), vb(3 * HD, pair),
                vb(4 * HD, width), vf(2, SEQ, 128),
                vf(6, 1, per), vf(*b_qkv.shape), vf(*b_fc1.T.shape), pltpu.VMEM(seg_row.shape, jnp.int32), vf(up_rows, 128),
                vf(4, 8, 128), vf(8, 128), vf(8, 128), vf(devices // 2, 8, 128), vf(dp_n, 8, 128), vf(2 * dp_n, 8, 128),
                vf(devices // 2, 8, 128), vf(dp_n, 8, 128), vf(2 * dp_n, 8, 128), vf(8, 128), vf(8, 128),
                vf(8, SEQ), vf(SEQ, 128), vf(8, 2 * HD), vf(8, 2 * HD),
                dma((2, 16)), dma((2, 16)), per_peer, per_peer, per_peer, per_peer, per_peer, per_peer,
                dma((3,)), dma((3,)), dma((2 * dp_n,)), dma((2 * dp_n,)), dma((3,)), dma((3,)), dma((2 * dp_n,)), dma((2 * dp_n,)),
                per_peer, per_peer, dma((3,)),
                dma((2, 16)), dma((2, 16)), dma((8,)), dma((8,)), dma((dp_n,)), dma((dp_n,)),
                dma((24,)), dma((24,)), pltpu.SemaphoreType.REGULAR((6,)),
            ],
            compiler_params=pltpu.CompilerParams(
                collective_id=0, has_side_effects=True, vmem_limit_bytes=67_043_328
            ),
            name="fused_block",
        )(block_input, cotangent, w_fc1, w_fc2, w_qkv, w_out, rope, *small_in)
        f32_out = lambda *shape: jax.ShapeDtypeStruct(shape, F32)
        ends = pl.pallas_call(
            functools.partial(finish_kernel, dp_n, tp_n),
            out_shape=(
                like(rows, width), f32_out(rows, width), f32_out(*w_fc1.shape), f32_out(*w_fc2.shape),
                f32_out(*w_qkv.shape), f32_out(*w_out.shape),
            ) + (f32_out(1, per),) * 6 + (f32_out(*b_qkv.shape), f32_out(*b_fc1.T.shape)),
            in_specs=[any_spec] * 6,
            out_specs=(any_spec,) * 6 + (pl.BlockSpec(memory_space=pltpu.VMEM),) * 8,
            scratch_shapes=[
                vb(rows, width), vf(rows, width), vb(hidden_here, width), vb(hidden_here, width),
                vb(4 * HD, width // 2), vf(INNER, depth, hidden_here), vf(INNER, hidden_here, depth),
                vf(*w_qkv.shape), vf(*w_out.shape), vf(4, 8, 128), vf(up_rows, 128),
                dma((24,)), dma((48,)),
            ],
            compiler_params=pltpu.CompilerParams(vmem_limit_bytes=60_000_000),
            name="finish",
        )(results[0], results[1], results[2], results[5], results[6], results[7])
        block_output, input_grad, up_total, down_total, qkv_total, out_total = ends[:6]
        small = [v.reshape(-1) for v in ends[6:12]]
        return (
            block_output, input_grad, qkv_total, ends[12], out_total, small[4],
            up_total, ends[13].T, down_total, small[5],
            small[0], small[1], small[2], small[3],
        )

    row, vec = P(AXES, None), P(AXES)
    col, low = P("dp", "tp"), P("tp", "dp")
    def choose(*arrays):
        wide = arrays[2].shape[0] % 128 == 0
        return (on_device_fused if wide else on_device)(*arrays)

    return jax.shard_map(
        choose,
        mesh=mesh,
        in_specs=(row, P("dp", None), col, low, low, vec, col, low, low, vec, vec, vec, vec, vec, row),
        out_specs=(row, row, col, low, low, vec, col, low, low, vec, vec, vec, vec, vec),
        check_vma=False,
    )
```
